128 devices in a mesh: batch: 1, cols: 2 (over core), rows: 64 (over z, y, x).
Axes of the slice: x: 4, y: 4, z: 4, core: 2. Of those that a mesh axis runs over, the one named last changes fastest.
Arguments:
- frames: bfloat16 [16, 2, 2048, 64, 64], P(None, 'batch', 'rows', 'cols')
- w_x: bfloat16 [3, 3, 64, 256], replicated
- w_h: bfloat16 [3, 3, 64, 256], replicated
- gate_bias: float32 [256], replicated
- h_init: bfloat16 [2, 2048, 64, 64], P('batch', 'rows', 'cols')
- c_init: float32 [2, 2048, 64, 64], P('batch', 'rows', 'cols')
Outputs:
- output 1: bfloat16 [16, 2, 2048, 64, 64], P(None, 'batch', 'rows', 'cols')
- output 2: float32 [2, 2048, 64, 64], P('batch', 'rows', 'cols')
All inputs are finite; a program needn't handle non-finite values.
Results may differ from the reference program's by a relative error of at most 0.00242049.
Values are sent between devices in bfloat16 or wider.
A program may use at most 1 GiB of HBM per device.

```python
import jax
import jax.numpy as jnp
from jax import lax

STEPS = 16
SAMPLES = 2
GRID_HEIGHT = 2048
GRID_WIDTH = 64
IN_CHANNELS = 64
HIDDEN = 64
BAND_ROWS = 8


def setup_inputs(seed: int = 0, part: int = 0) -> dict:
    root_key = jax.random.key(seed)
    shared_key, local_root = jax.random.split(root_key)
    local_key = jax.random.fold_in(local_root, part)
    key_wx, key_wh, key_bias = jax.random.split(shared_key, 3)
    key_frames, key_hidden, key_cell = jax.random.split(local_key, 3)
    gate_width = 4 * HIDDEN
    frames = jax.random.normal(key_frames, (STEPS, SAMPLES, GRID_HEIGHT, GRID_WIDTH, IN_CHANNELS), jnp.float32)
    w_x = jax.random.normal(key_wx, (3, 3, IN_CHANNELS, gate_width), jnp.float32) * (0.8 * (9 * IN_CHANNELS) ** -0.5)
    w_h = jax.random.normal(key_wh, (3, 3, HIDDEN, gate_width), jnp.float32) * (1.5 * (9 * HIDDEN) ** -0.5)
    forget_shift = jnp.concatenate([jnp.zeros((HIDDEN,), jnp.float32), jnp.ones((HIDDEN,), jnp.float32), jnp.zeros((2 * HIDDEN,), jnp.float32)])
    gate_bias = 0.5 * jax.random.normal(key_bias, (gate_width,), jnp.float32) + forget_shift
    h_init = 0.5 * jax.random.normal(key_hidden, (SAMPLES, GRID_HEIGHT, GRID_WIDTH, HIDDEN), jnp.float32)
    c_init = jax.random.normal(key_cell, (SAMPLES, GRID_HEIGHT, GRID_WIDTH, HIDDEN), jnp.float32)
    return {"frames": frames.astype(jnp.bfloat16), "w_x": w_x.astype(jnp.bfloat16), "w_h": w_h.astype(jnp.bfloat16), "gate_bias": gate_bias, "h_init": h_init.astype(jnp.bfloat16), "c_init": c_init}


def conv_taps(padded, weights, out_rows, out_cols):
    tap_list = [padded[:, row_off:row_off + out_rows, col_off:col_off + out_cols, :] for row_off in range(3) for col_off in range(3)]
    patches = jnp.concatenate(tap_list, axis=-1)
    flat_patches = patches.reshape(-1, patches.shape[-1])
    flat_weights = weights.reshape(-1, weights.shape[-1])
    product = jnp.dot(flat_patches, flat_weights, preferred_element_type=jnp.float32)
    return product.reshape(padded.shape[0], out_rows, out_cols, -1)


def lstm_cell(gate_sum, cell_prev):
    hidden_width = cell_prev.shape[-1]
    in_gate = jax.nn.sigmoid(gate_sum[..., :hidden_width])
    forget_gate = jax.nn.sigmoid(gate_sum[..., hidden_width:2 * hidden_width])
    out_gate = jax.nn.sigmoid(gate_sum[..., 2 * hidden_width:3 * hidden_width])
    cand_gate = jnp.tanh(gate_sum[..., 3 * hidden_width:])
    cell_next = forget_gate * cell_prev + in_gate * cand_gate
    hidden_next = (out_gate * jnp.tanh(cell_next)).astype(jnp.bfloat16)
    return hidden_next, cell_next


def reference(frames, w_x, w_h, gate_bias, h_init, c_init):
    num_bands = GRID_HEIGHT // BAND_ROWS
    pad_cfg = ((0, 0), (1, 1), (1, 1), (0, 0))

    def step_fn(state_pair, frame_t):
        hidden, cell_state = state_pair
        frame_pad = jnp.pad(frame_t, pad_cfg)
        hidden_pad = jnp.pad(hidden, pad_cfg)

        def band_update(band_index):
            row_start = band_index * BAND_ROWS
            frame_band = lax.dynamic_slice_in_dim(frame_pad, row_start, BAND_ROWS + 2, axis=1)
            hidden_band = lax.dynamic_slice_in_dim(hidden_pad, row_start, BAND_ROWS + 2, axis=1)
            cell_band = lax.dynamic_slice_in_dim(cell_state, row_start, BAND_ROWS, axis=1)
            gate_sum = conv_taps(frame_band, w_x, BAND_ROWS, GRID_WIDTH) + conv_taps(hidden_band, w_h, BAND_ROWS, GRID_WIDTH) + gate_bias
            return lstm_cell(gate_sum, cell_band)

        band_hidden, band_cell = lax.map(band_update, jnp.arange(num_bands))
        hidden_next = jnp.moveaxis(band_hidden, 0, 1).reshape(SAMPLES, GRID_HEIGHT, GRID_WIDTH, HIDDEN)
        cell_next = jnp.moveaxis(band_cell, 0, 1).reshape(SAMPLES, GRID_HEIGHT, GRID_WIDTH, HIDDEN)
        return (hidden_next, cell_next), hidden_next

    final_pair, all_hidden = lax.scan(step_fn, (h_init, c_init), frames)
    return all_hidden, final_pair[1]
```

```python
import functools

import jax
import jax.numpy as jnp
from jax import lax
from jax.experimental import pallas as pl
from jax.experimental.pallas import tpu as pltpu
from jax.sharding import PartitionSpec as P

MESH = pl.DeviceIdType.MESH
CH = 64
LANES = 128
PIECE = 4
RING = 8


def cuts(lo, hi):
    n = max(1, (hi - lo) // PIECE)
    edges = [lo + i * PIECE for i in range(n)] + [hi]
    return list(zip(edges[:-1], edges[1:]))


def kernel(T, K, R, W, n_rows, frames, w_x, w_h, bias, h_init, c_init, h_out, c_out,
           xin, hout, cst, hst, xh_even, xh_odd, cbuf, shift, wbuf,
           xs_ref, xr_ref, hs_ref, hr_ref, cs_ref, cr_ref,
           s_w, s_x, s_xr, s_xs, s_i, s_ir, s_is, s_hx, s_hxs, s_hh, s_hhs, s_hc, s_hcs,
           s_o, s_os, s_or):
    s = lax.axis_index("cols")
    n = lax.axis_index("rows")
    p = 1 - s
    HW = W // 2
    NB = T // K
    per_block = K * (K + 1) // 2
    off = [sum(K - i for i in range(o)) for o in range(K)]
    mine = pl.ds(pl.multiple_of(s * HW, HW), HW)
    theirs = pl.ds(pl.multiple_of(p * HW, HW), HW)
    has_up, has_dn = n > 0, n < n_rows - 1

    def local(src, dst, sem):
        return pltpu.make_async_copy(src, dst, sem)

    def remote(src, dst, ssem, rsem, dev):
        return pltpu.make_async_remote_copy(
            src_ref=src, dst_ref=dst, send_sem=ssem, recv_sem=rsem, device_id=dev, device_id_type=MESH)

    peer = {"cols": p}
    side_dev = [{"rows": n - 1}, {"rows": n + 1}]
    side_ok = [has_up, has_dn]

    local(w_h, wbuf.at[:, :, 0], s_w.at[0]).start()
    local(w_x, wbuf.at[:, :, 1], s_w.at[1]).start()
    local(h_init.at[s], hst.at[:, mine], s_i.at[0]).start()
    local(c_init.at[s], cst.at[:, mine], s_i.at[1]).start()

    def own_x(t, _):
        local(frames.at[t, s], xin.at[t, :, mine], s_x.at[t]).start()
        return 0

    lax.fori_loop(0, T, own_x, 0)

    barrier = pltpu.get_barrier_semaphore()
    pl.semaphore_signal(barrier, inc=1, device_id=peer, device_id_type=MESH)
    for ok, dev in zip(side_ok, side_dev):
        @pl.when(ok)
        def _():
            pl.semaphore_signal(barrier, inc=1, device_id=dev, device_id_type=MESH)
    pl.semaphore_wait(barrier, 1 + has_up.astype(jnp.int32) + has_dn.astype(jnp.int32))

    h_push = remote(h_init.at[p], hst.at[:, mine], s_is.at[0], s_ir.at[0], peer)
    c_push = remote(c_init.at[p], cst.at[:, mine], s_is.at[1], s_ir.at[1], peer)
    h_push.start()

    def push_x(t, _):
        remote(frames.at[t, p], xin.at[t, :, mine], s_xs, s_xr.at[t], peer).start()
        return 0

    push_x(0, 0)
    c_push.start()
    lax.fori_loop(1, T, push_x, 0)

    shift[...] = jnp.zeros_like(shift)
    lane = lax.broadcasted_iota(jnp.int32, (W, LANES), 1)
    low = lane < CH
    low_half = lane[: HW] < CH
    low_row = lax.broadcasted_iota(jnp.int32, (1, LANES), 1) < CH
    scale = jnp.where(low_row, 0.5, 1.0)
    shiftup = jnp.where(low_row, 0.5, 0.0)

    local(w_h, wbuf.at[:, :, 0], s_w.at[0]).wait()
    local(w_x, wbuf.at[:, :, 1], s_w.at[1]).wait()
    for dr in range(3):
        for dc in range(3):
            for half in range(2):
                tile = wbuf[dr, dc, half, :, 0:LANES]
                wbuf[dr, dc, half, :, 0:LANES] = jnp.concatenate([tile[:, CH:], tile[:, :CH]], axis=1)
    b_first = bias[:, 0:LANES]
    b_fi = jnp.concatenate([b_first[:, CH:], b_first[:, :CH]], axis=1) * 0.5
    b_og = bias[:, LANES:] * scale

    def wait_x(t):
        local(frames.at[t, s], xin.at[t, :, mine], s_x.at[t]).wait()
        local(frames.at[t, s], xin.at[t, :, theirs], s_xr.at[t]).wait()

    def emit(nxt, r, hx):
        slot = (r + K) % RING
        row = r + K
        shift[slot, 8:8 + W, :] = hx
        nxt[1, row] = hx.astype(jnp.bfloat16)
        nxt[0, row] = shift[slot, 7:7 + W, :].astype(jnp.bfloat16)
        nxt[2, row] = shift[slot, 9:9 + W, :].astype(jnp.bfloat16)

    def x_row(t, b, o, r):
        if 0 <= r < R:
            return xin[t, r].astype(jnp.float32)
        side, i = (0, r + (K - o)) if r < 0 else (1, r - R)
        packed = xr_ref[side, b * per_block + off[o] + i].astype(jnp.float32)
        return jnp.concatenate([packed[:, :CH], packed[:, CH:]], axis=0)

    def masked(r, v):
        if r < 0:
            return jnp.where(has_up, v, 0.0)
        if r >= R:
            return jnp.where(has_dn, v, 0.0)
        return v

    def pack(v):
        return jnp.concatenate([v[:HW], v[HW:]], axis=1)

    def send_x(t, b, o):
        for side in range(2):
            lo = b * per_block + off[o]
            for i in range(K - o):
                r = i if side == 0 else R - (K - o) + i
                xs_ref[side, lo + i] = pack(xin[t, r])

    def copy_x(b, o, side):
        rows = pl.ds(b * per_block + off[o], K - o)
        return remote(xs_ref.at[side, rows], xr_ref.at[1 - side, rows], s_hxs.at[side],
                      s_hx.at[1 - side, b * K + o], side_dev[side])

    def start_x(b, o):
        for side in range(2):
            @pl.when(side_ok[side])
            def _():
                copy_x(b, o, side).start()

    def send_state(b, h_rows):
        for side in range(2):
            for i in range(K):
                r = i if side == 0 else R - K + i
                hs_ref[side, b * K + i] = pack(h_rows[r])
            for i in range(K - 1):
                r = i if side == 0 else R - (K - 1) + i
                c = cbuf[r + K]
                cs_ref[side, b * (K - 1) + i] = jnp.where(low_half, c[:HW], c[HW:])

    def copy_h(b, side):
        rows = pl.ds(b * K, K)
        return remote(hs_ref.at[side, rows], hr_ref.at[1 - side, rows], s_hhs.at[side, b],
                      s_hh.at[1 - side, b], side_dev[side])

    def copy_c(b, side):
        rows = pl.ds(b * (K - 1), K - 1)
        return remote(cs_ref.at[side, rows], cr_ref.at[1 - side, rows], s_hcs.at[side, b],
                      s_hc.at[1 - side, b], side_dev[side])

    def start_state(b):
        for side in range(2):
            @pl.when(side_ok[side])
            def _():
                copy_h(b, side).start()
                copy_c(b, side).start()

    wait_x(0)
    local(h_init.at[s], hst.at[:, mine], s_i.at[0]).wait()
    h_push.wait_recv()
    local(c_init.at[s], cst.at[:, mine], s_i.at[1]).wait()
    c_push.wait_recv()
    for r in range(R):
        c = cst[r]
        cbuf[r + K] = jnp.concatenate([c, c], axis=1)
    send_state(0, hst)
    send_x(0, 0, 0)
    start_state(0)
    start_x(0, 0)
    for r in range(R):
        emit(xh_even, r, jnp.concatenate([hst[r].astype(jnp.float32), x_row(0, 0, 0, r)], axis=1))

    weights = wbuf[...].reshape(9 * LANES, 4 * CH)

    def piece(b, o, lo, hi):
        cur, nxt = (xh_even, xh_odd) if o % 2 == 0 else (xh_odd, xh_even)
        t = b * K + o
        t_next = jnp.minimum(t + 1, T - 1)
        b_next, o_next = (b, o + 1) if o + 1 < K else (b + 1, 0)
        m = hi - lo
        taps = [cur[dc, lo + K + dr - 1:hi + K + dr - 1].reshape(m * W, LANES) for dr in range(3) for dc in range(3)]
        gates = jnp.dot(jnp.concatenate(taps, axis=1), weights, preferred_element_type=jnp.float32)
        for q in range(m):
            r = lo + q
            g = gates[q * W:(q + 1) * W]
            fi = jnp.tanh(g[:, :LANES] * 0.5 + b_fi) * 0.5 + 0.5
            og = jnp.tanh(g[:, LANES:] * scale + b_og) * scale + shiftup
            prod = fi * jnp.where(low, cbuf[r + K], og)
            c = prod + pltpu.roll(prod, CH, 1)
            cbuf[r + K] = c
            h = masked(r, og * jnp.tanh(c))
            if 0 <= r < R:
                hout[t, r] = h[:, :CH].astype(jnp.bfloat16)
            x = masked(r, x_row(t_next, b_next, o_next, r))
            emit(nxt, r, jnp.concatenate([h[:, :CH], x], axis=1))

    def out_own(t):
        return local(hout.at[t, :, mine], h_out.at[t, s], s_o)

    def out_peer(t):
        return remote(hout.at[t, :, theirs], h_out.at[t, s], s_os, s_or, peer)

    def block(b, _):
        more = b + 1 < NB
        for o in range(K):
            t = b * K + o
            if o + 1 < K:
                wait_x(t + 1)
                send_x(t + 1, b, o + 1)
                start_x(b, o + 1)
            else:
                @pl.when(more)
                def _():
                    wait_x(t + 1)
                    send_x(t + 1, b + 1, 0)
                    start_x(b + 1, 0)
            for lo, hi in cuts(o + 1, R - 1 - o):
                piece(b, o, lo, hi)
        for side in range(2):
            @pl.when(side_ok[side])
            def _():
                copy_h(b, 1 - side).wait_recv()
                copy_c(b, 1 - side).wait_recv()
                copy_x(b, 0, 1 - side).wait_recv()
        for side in range(2):
            for i in range(K):
                r = i - K if side == 0 else R + i
                packed = hr_ref[side, b * K + i].astype(jnp.float32)
                h = jnp.concatenate([packed[:, :CH], packed[:, CH:]], axis=0)
                hx = jnp.concatenate([h, x_row(b * K, b, 0, r)], axis=1)
                emit(xh_even, r, masked(r, hx))
            for i in range(K - 1):
                r = i - (K - 1) if side == 0 else R + i
                packed = cr_ref[side, b * (K - 1) + i]
                cbuf[r + K, 0:HW] = packed
                cbuf[r + K, HW:W] = pltpu.roll(packed, CH, 1)
        for o in range(K):
            if o + 1 < K:
                for side in range(2):
                    @pl.when(side_ok[side])
                    def _():
                        copy_x(b, o + 1, 1 - side).wait_recv()
            m = K - 1 - o
            for (a, e), (a2, e2) in zip(cuts(-m, o + 1), cuts(R - 1 - o, R + m)):
                piece(b, o, a, e)
                piece(b, o, a2, e2)
            out_own(b * K + o).start()
            out_peer(b * K + o).start()

        @pl.when(more)
        def _():
            send_state(b + 1, hout.at[b * K + K - 1])
            start_state(b + 1)
        return 0

    lax.fori_loop(0, NB, block, 0)

    for r in range(R):
        cst[r] = cbuf[r + K, :, 0:CH]
    c_own = local(cst.at[:, mine], c_out.at[s], s_i.at[0])
    c_peer = remote(cst.at[:, theirs], c_out.at[s], s_is.at[2], s_ir.at[2], peer)
    c_own.start()
    c_peer.start()

    h_push.wait_send()
    c_push.wait_send()
    local(xin.at[:, :, mine], xin.at[:, :, mine], s_xs).wait()
    for side in range(2):
        @pl.when(side_ok[side])
        def _():
            local(xs_ref.at[side], xs_ref.at[side], s_hxs.at[side]).wait()
            for b in range(NB):
                copy_h(b, side).wait_send()
                copy_c(b, side).wait_send()
    local(hout.at[:, :, mine], hout.at[:, :, mine], s_o).wait()
    local(hout.at[:, :, mine], hout.at[:, :, mine], s_os).wait()
    local(hout.at[:, :, mine], hout.at[:, :, mine], s_or).wait()
    c_own.wait()
    c_peer.wait()


def run(K, n_rows, frames, w_x, w_h, gate_bias, h_init, c_init):
    T, S, R, HW = frames.shape[:4]
    W = 2 * HW
    NB = T // K
    per_block = K * (K + 1) // 2
    bf, f32 = jnp.bfloat16, jnp.float32
    vm, dma = pltpu.VMEM, pltpu.SemaphoreType.DMA
    hbm = pl.BlockSpec(memory_space=pltpu.HBM)
    return pl.pallas_call(
        functools.partial(kernel, T, K, R, W, n_rows),
        out_shape=(jax.ShapeDtypeStruct(frames.shape, bf), jax.ShapeDtypeStruct(c_init.shape, f32)),
        in_specs=[hbm, hbm, hbm, pl.BlockSpec(memory_space=pltpu.VMEM), hbm, hbm],
        out_specs=(hbm, hbm),
        scratch_shapes=[
            vm((T, R, W, CH), bf), vm((T, R, W, CH), bf), vm((R, W, CH), f32), vm((R, W, CH), bf),
            vm((3, R + 2 * K, W, LANES), bf), vm((3, R + 2 * K, W, LANES), bf),
            vm((R + 2 * K, W, LANES), f32), vm((RING, W + 16, LANES), f32), vm((3, 3, 2, CH, 4 * CH), bf),
            vm((2, NB * per_block, HW, LANES), bf), vm((2, NB * per_block, HW, LANES), bf),
            vm((2, NB * K, HW, LANES), bf), vm((2, NB * K, HW, LANES), bf),
            vm((2, NB * (K - 1), HW, LANES), f32), vm((2, NB * (K - 1), HW, LANES), f32),
            dma((2,)), dma((T,)), dma((T,)), dma, dma((2,)), dma((3,)), dma((3,)),
            dma((2, T)), dma((2,)), dma((2, NB)), dma((2, NB)), dma((2, NB)), dma((2, NB)),
            dma, dma, dma],
        compiler_params=pltpu.CompilerParams(collective_id=0, has_side_effects=True, vmem_limit_bytes=62 * 2**20),
    )(frames, w_x, w_h, gate_bias.reshape(1, -1), h_init, c_init)


def solution(mesh, K=4):
    n_rows = mesh.shape["rows"]
    frame_spec = P(None, "batch", "rows", "cols", None)
    state_spec = P("batch", "rows", "cols", None)
    return jax.shard_map(functools.partial(run, K, n_rows), mesh=mesh,
                         in_specs=(frame_spec, P(), P(), P(), state_spec, state_spec),
                         out_specs=(frame_spec, state_spec), check_vma=False)
```

```python
import functools

import jax
import jax.numpy as jnp
from jax import lax
from jax.experimental import pallas as pl
from jax.experimental.pallas import tpu as pltpu
from jax.sharding import PartitionSpec as P

MESH = pl.DeviceIdType.MESH
CH = 64
LANES = 128
PIECE = 4
RING = 8
BLOCKS = (4, 4, 4, 4)


def cuts(lo, hi, size=PIECE):
    n = max(1, (hi - lo) // size)
    edges = [lo + i * size for i in range(n)] + [hi]
    return list(zip(edges[:-1], edges[1:]))


class Plan:
    def __init__(self, blocks, T, R, W):
        assert sum(blocks) == T
        self.blocks, self.T, self.R, self.W, self.HW = blocks, T, R, W, W // 2
        self.K = max(blocks)
        self.first = [sum(blocks[:b]) for b in range(len(blocks))]
        self.of = [(b, o) for b, k in enumerate(blocks) for o in range(k)]
        self.xrows = [blocks[b] - o for b, o in self.of]
        self.xat = [sum(self.xrows[:t]) for t in range(T + 1)]
        self.hat = [sum(blocks[:b]) for b in range(len(blocks) + 1)]
        self.cat = [sum(k - 1 for k in blocks[:b]) for b in range(len(blocks) + 1)]
        ends = [0, 1] + [min(f + k + 1, T) for f, k in zip(self.first, blocks)]
        self.groups = [(a, e) for a, e in zip(ends[:-1], ends[1:]) if e > a]


def kernel(plan, n_rows, frames, w_x, w_h, bias, h_init, c_init, hout, hpeer, cout, cpeer,
           xin, hst, cst, xh_even, xh_odd, cbuf, shift, wbuf,
           xs_ref, xr_ref, hs_ref, hr_ref, cs_ref, cr_ref,
           s_w, s_i, s_ir, s_is, s_x, s_xr, s_xs, s_b, s_bs, s_or, s_os, s_c):
    T, R, W, HW = plan.T, plan.R, plan.W, plan.HW
    PAD = plan.K
    NB = len(plan.blocks)
    s = lax.axis_index("cols")
    n = lax.axis_index("rows")
    p = 1 - s
    mine = pl.ds(pl.multiple_of(s * HW, HW), HW)
    theirs = pl.ds(pl.multiple_of(p * HW, HW), HW)
    has_up, has_dn = n > 0, n < n_rows - 1
    bf, f32 = jnp.bfloat16, jnp.float32

    def local(src, dst, sem):
        return pltpu.make_async_copy(src, dst, sem)

    def remote(src, dst, ssem, rsem, dev):
        return pltpu.make_async_remote_copy(
            src_ref=src, dst_ref=dst, send_sem=ssem, recv_sem=rsem, device_id=dev, device_id_type=MESH)

    peer = {"cols": p}
    side_dev = [{"rows": lax.rem(n + n_rows - 1, n_rows)}, {"rows": lax.rem(n + 1, n_rows)}]

    w_copies = [local(w_h, wbuf.at[:, :, 0], s_w.at[0]), local(w_x, wbuf.at[:, :, 1], s_w.at[1])]
    h_own = local(h_init.at[s], hst.at[:, mine], s_i.at[0])
    c_own = local(c_init.at[s], cst.at[:, mine], s_i.at[1])
    x_own = [local(frames.at[a:e, s], xin.at[a:e, :, mine], s_x.at[g]) for g, (a, e) in enumerate(plan.groups)]
    for c in [h_own, c_own, x_own[0], *w_copies, *x_own[1:]]:
        c.start()

    barrier = pltpu.get_barrier_semaphore()
    for dev in [peer, *side_dev]:
        pl.semaphore_signal(barrier, inc=1, device_id=dev, device_id_type=MESH)
    pl.semaphore_wait(barrier, 3)

    h_push = remote(h_init.at[p], hst.at[:, mine], s_is.at[0], s_ir.at[0], peer)
    c_push = remote(c_init.at[p], cst.at[:, mine], s_is.at[1], s_ir.at[1], peer)
    x_push = [remote(frames.at[a:e, p], xin.at[a:e, :, mine], s_xs.at[g], s_xr.at[g], peer)
              for g, (a, e) in enumerate(plan.groups)]
    for c in [h_push, c_push, *x_push]:
        c.start()

    shift[...] = jnp.zeros_like(shift)
    low = lax.broadcasted_iota(jnp.int32, (1, LANES), 1) < CH
    low_half = low_row = low
    turn = [0]
    scale = jnp.where(low_row, 0.5, 1.0)
    lift = jnp.where(low_row, 0.5, 0.0)

    for c in w_copies:
        c.wait()
    for dr in range(3):
        for dc in range(3):
            for half in range(2):
                tile = wbuf[dr, dc, half, :, 0:LANES]
                wbuf[dr, dc, half, :, 0:LANES] = jnp.concatenate([tile[:, CH:], tile[:, :CH]], axis=1)
    b_first = bias[:, 0:LANES]
    b_fi = jnp.concatenate([b_first[:, CH:], b_first[:, :CH]], axis=1) * 0.5
    b_og = bias[:, LANES:] * scale

    def pack(v):
        return jnp.concatenate([v[:, :HW], v[:, HW:]], axis=2)

    def unpack(v):
        return jnp.concatenate([v[:, :, :CH], v[:, :, CH:]], axis=1)

    def masked(r, v):
        if r < 0:
            return jnp.where(has_up, v, 0.0)
        if r >= R:
            return jnp.where(has_dn, v, 0.0)
        return v

    def emit(t, lo, hi, hx):
        nxt = xh_even if t % 2 == 0 else xh_odd
        at, to = slot(lo, hi), slice(lo + PAD, hi + PAD)
        shift[at, 8:8 + W, :] = hx
        nxt[1, to] = hx.astype(bf)
        nxt[0, to] = shift[at, 7:7 + W, :].astype(bf)
        nxt[2, to] = shift[at, 9:9 + W, :].astype(bf)

    def slot(lo, hi):
        if turn[0] + hi - lo > RING:
            turn[0] = 0
        turn[0] += hi - lo
        return slice(turn[0] - (hi - lo), turn[0])

    def x_rows(t, lo, hi):
        if lo >= 0 and hi <= R:
            return xin[t, lo:hi].astype(f32)
        side, i = (0, lo + plan.xrows[t]) if lo < 0 else (1, lo - R)
        return unpack(xr_ref[side, plan.xat[t] + i:plan.xat[t] + i + hi - lo].astype(f32))

    def wait_x(g):
        if g < len(plan.groups):
            x_own[g].wait()
            x_push[g].wait_recv()

    def border(b, kind, side):
        k, f = plan.blocks[b], plan.first[b]
        src, dst, at, count = [
            (xs_ref, xr_ref, plan.xat[f], plan.xat[f + k] - plan.xat[f]),
            (hs_ref, hr_ref, plan.hat[b], k),
            (cs_ref, cr_ref, plan.cat[b], k - 1)][kind]
        return remote(src.at[side, at:at + count], dst.at[1 - side, at:at + count],
                      s_bs.at[kind, side, b], s_b.at[kind, 1 - side, b], side_dev[side])

    def send_x(b):
        k, f = plan.blocks[b], plan.first[b]
        for side in range(2):
            for t in range(f, f + k):
                m = plan.xrows[t]
                lo = 0 if side == 0 else R - m
                xs_ref[side, plan.xat[t]:plan.xat[t] + m] = pack(xin[t, lo:lo + m])
            border(b, 0, side).start()

    def send_state(b, h_rows):
        k = plan.blocks[b]
        for side in range(2):
            lo = 0 if side == 0 else R - k
            hs_ref[side, plan.hat[b]:plan.hat[b] + k] = pack(h_rows[lo:lo + k])
            lo = PAD if side == 0 else PAD + R - (k - 1)
            c = cbuf[lo:lo + k - 1]
            cs_ref[side, plan.cat[b]:plan.cat[b] + k - 1] = jnp.where(low_half, c[:, :HW], c[:, HW:])
        for side in range(2):
            border(b, 1, side).start()
            border(b, 2, side).start()

    weights = wbuf[...].reshape(9 * LANES, 4 * CH)

    def dot(t, lo, hi):
        cur = xh_even if t % 2 == 0 else xh_odd
        taps = [cur[dc, lo + PAD + dr - 1:hi + PAD + dr - 1].reshape((hi - lo) * W, LANES)
                for dr in range(3) for dc in range(3)]
        return jnp.dot(jnp.concatenate(taps, axis=1), weights, preferred_element_type=f32)

    def cells(t, lo, hi, gates):
        m, g = hi - lo, gates
        fi = jnp.tanh(g[:, :LANES] * 0.5 + b_fi) * 0.5 + 0.5
        og = jnp.tanh(g[:, LANES:] * scale + b_og) * scale + lift
        prod = fi * jnp.where(low, cbuf[lo + PAD:hi + PAD].reshape(m * W, LANES), og)
        c = prod + pltpu.roll(prod, CH, 1)
        h = (og * jnp.tanh(c)).reshape(m, W, LANES)
        c = c.reshape(m, W, LANES)
        if t == T - 1:
            cout[lo:hi] = c[:, :, :CH]
        else:
            cbuf[lo + PAD:hi + PAD] = c
        for a, e in ((lo, min(hi, 0)), (max(lo, 0), min(hi, R)), (max(lo, R), hi)):
            if a >= e:
                continue
            part = h[a - lo:e - lo, :, :CH]
            if a >= 0 and e <= R:
                hout[t, a:e] = part.astype(bf)
            if t < T - 1:
                emit(t + 1, a, e, masked(a, jnp.concatenate([part, x_rows(t + 1, a, e)], axis=2)))

    pending = []

    def piece(t, lo, hi):
        gates = dot(t, lo, hi)
        flush()
        pending.append((t, lo, hi, gates))

    def flush():
        while pending:
            cells(*pending.pop())

    def out_peer(t0, t1, g):
        return remote(hout.at[t0:t1, :, theirs], hpeer.at[t0:t1], s_os.at[g], s_or.at[g], peer)

    h_own.wait()
    h_push.wait_recv()
    c_own.wait()
    c_push.wait_recv()
    c0 = cst[...]
    cbuf[PAD:PAD + R] = jnp.concatenate([c0, c0], axis=2)
    send_state(0, hst)
    wait_x(0)
    wait_x(1)
    send_x(0)
    for lo, hi in cuts(0, R):
        emit(0, lo, hi, jnp.concatenate([hst[lo:hi].astype(f32), x_rows(0, lo, hi)], axis=2))

    outs = []
    for b, k in enumerate(plan.blocks):
        f = plan.first[b]
        for o in range(k):
            t = f + o
            if o == 0:
                inner = [(1, k + 1), *cuts(k + 1, R - 1 - k), (R - 1 - k, R - 1)]
            else:
                inner = cuts(o + 1, R - 1 - o)
            for i, (lo, hi) in enumerate(inner[1:-1] + [inner[0], inner[-1]]):
                piece(t, lo, hi)
                if b and o == 0 and i == 0:
                    send_state(b, hout.at[f - 1])
                    outs.append(out_peer(plan.first[b - 1], f, b - 1))
                    outs[-1].start()
        for kind in (1, 2, 0):
            for side in range(2):
                border(b, kind, side).wait_recv()
        wait_x(b + 2)
        for side in range(2):
            lo = -k if side == 0 else R
            h = unpack(hr_ref[side, plan.hat[b]:plan.hat[b] + k].astype(f32))
            emit(f, lo, lo + k, masked(lo, jnp.concatenate([h, x_rows(f, lo, lo + k)], axis=2)))
            lo = PAD - (k - 1) if side == 0 else PAD + R
            packed = cr_ref[side, plan.cat[b]:plan.cat[b] + k - 1]
            cbuf[lo:lo + k - 1, 0:HW] = packed
            cbuf[lo:lo + k - 1, HW:W] = pltpu.roll(packed, CH, 2)
        if b + 1 < NB:
            send_x(b + 1)
        for o in range(k):
            m = k - 1 - o
            for (a, e), (a2, e2) in zip(cuts(-m, o + 1, max(PIECE, k)), cuts(R - 1 - o, R + m, max(PIECE, k))):
                piece(f + o, a, e)
                piece(f + o, a2, e2)
    flush()
    outs.append(out_peer(plan.first[-1], T, NB - 1))
    outs[-1].start()
    c_out = remote(cout.at[:, theirs], cpeer, s_c.at[0], s_c.at[1], peer)
    c_out.start()

    for c in [h_push, c_push, *x_push]:
        c.wait_send()
    for b in range(NB):
        for kind in range(3):
            for side in range(2):
                border(b, kind, side).wait_send()
    for c in [*outs, c_out]:
        c.wait()


def store(hout, hpeer, cout, cpeer, h_all, c_final, sems):
    s = lax.axis_index("cols")
    HW = hpeer.shape[2]
    mine = pl.ds(pl.multiple_of(s * HW, HW), HW)
    copies = [pltpu.make_async_copy(hout.at[:, :, mine], h_all.at[:, s], sems.at[0]),
              pltpu.make_async_copy(hpeer, h_all.at[:, 1 - s], sems.at[1]),
              pltpu.make_async_copy(cout.at[:, mine], c_final.at[s], sems.at[2]),
              pltpu.make_async_copy(cpeer, c_final.at[1 - s], sems.at[3])]
    for c in copies:
        c.start()
    for c in copies:
        c.wait()


def run(blocks, n_rows, frames, w_x, w_h, gate_bias, h_init, c_init):
    T, S, R, HW = frames.shape[:4]
    W = 2 * HW
    plan = Plan(blocks, T, R, W)
    NB, PAD, G = len(blocks), plan.K, len(plan.groups)
    bf, f32 = jnp.bfloat16, jnp.float32
    vm, dma = pltpu.VMEM, pltpu.SemaphoreType.DMA
    hbm = pl.BlockSpec(memory_space=pltpu.HBM)
    vmem = pl.BlockSpec(memory_space=pltpu.VMEM)
    parts = pl.pallas_call(
        functools.partial(kernel, plan, n_rows),
        out_shape=(vm((T, R, W, CH), bf), vm((T, R, HW, CH), bf), vm((R, W, CH), f32), vm((R, HW, CH), f32)),
        in_specs=[hbm, hbm, hbm, vmem, hbm, hbm],
        out_specs=(vmem,) * 4,
        scratch_shapes=[
            vm((T, R, W, CH), bf), vm((R, W, CH), bf), vm((R, W, CH), f32),
            vm((3, R + 2 * PAD, W, LANES), bf), vm((3, R + 2 * PAD, W, LANES), bf),
            vm((R + 2 * PAD, W, LANES), f32), vm((RING, W + 16, LANES), f32), vm((3, 3, 2, CH, 4 * CH), bf),
            vm((2, plan.xat[-1], HW, LANES), bf), vm((2, plan.xat[-1], HW, LANES), bf),
            vm((2, plan.hat[-1], HW, LANES), bf), vm((2, plan.hat[-1], HW, LANES), bf),
            vm((2, plan.cat[-1], HW, LANES), f32), vm((2, plan.cat[-1], HW, LANES), f32),
            dma((2,)), dma((2,)), dma((2,)), dma((2,)), dma((G,)), dma((G,)), dma((G,)),
            dma((3, 2, NB)), dma((3, 2, NB)), dma((NB,)), dma((NB,)), dma((2,))],
        compiler_params=pltpu.CompilerParams(collective_id=0, has_side_effects=True, vmem_limit_bytes=46 * 2**20),
    )(frames, w_x, w_h, gate_bias.reshape(1, -1), h_init, c_init)
    return pl.pallas_call(
        store,
        out_shape=(jax.ShapeDtypeStruct(frames.shape, bf), jax.ShapeDtypeStruct(c_init.shape, f32)),
        in_specs=[vmem] * 4,
        out_specs=(hbm, hbm),
        scratch_shapes=[dma((4,))],
        compiler_params=pltpu.CompilerParams(vmem_limit_bytes=2**20),
    )(*[pltpu.with_memory_space_constraint(a, pltpu.VMEM) for a in parts])


def solution(mesh, K=None):
    n_rows = mesh.shape["rows"]
    frame_spec = P(None, "batch", "rows", "cols", None)
    state_spec = P("batch", "rows", "cols", None)
    blocks = BLOCKS if K is None else K
    return jax.shard_map(functools.partial(run, blocks, n_rows), mesh=mesh,
                         in_specs=(frame_spec, P(), P(), P(), state_spec, state_spec),
                         out_specs=(frame_spec, state_spec), check_vma=False)
```

```python
import functools

import jax
import jax.numpy as jnp
from jax import lax
from jax.experimental import pallas as pl
from jax.experimental.pallas import tpu as pltpu
from jax.sharding import PartitionSpec as P

MESH = pl.DeviceIdType.MESH
CH = 64
LANES = 128
PIECE = 4
RING = 8
BLOCKS = (4, 4, 4, 4)
FILL = (1, 1, 1, 1)


def cuts(lo, hi, size=PIECE):
    n = max(1, (hi - lo) // size)
    edges = [lo + i * size for i in range(n)] + [hi]
    return list(zip(edges[:-1], edges[1:]))


class Plan:
    def __init__(self, blocks, T, R, W):
        assert sum(blocks) == T
        self.blocks, self.T, self.R, self.W, self.HW = blocks, T, R, W, W // 2
        self.K = max(blocks)
        self.first = [sum(blocks[:b]) for b in range(len(blocks))]
        self.of = [(b, o) for b, k in enumerate(blocks) for o in range(k)]
        self.xrows = [blocks[b] - o for b, o in self.of]
        self.xat = [sum(self.xrows[:t]) for t in range(T + 1)]
        self.hat = [sum(blocks[:b]) for b in range(len(blocks) + 1)]
        self.cat = [sum(k - 1 for k in blocks[:b]) for b in range(len(blocks) + 1)]
        ends = [0, 1] + [min(f + k + 1, T) for f, k in zip(self.first, blocks)]
        self.groups = [(a, e) for a, e in zip(ends[:-1], ends[1:]) if e > a]


def kernel(plan, n_rows, frames, w_x, w_h, bias, h_init, c_init, hout, hpeer, cout, cpeer,
           hgo, cgo, xgo, xin, hst, cst, xh_even, xh_odd, cbuf, shift, wbuf,
           xs_ref, xr_ref, hs_ref, hr_ref, cs_ref, cr_ref,
           s_w, s_i, s_ir, s_is, s_x, s_xr, s_xs, s_b, s_bs, s_or, s_os):
    T, R, W, HW = plan.T, plan.R, plan.W, plan.HW
    PAD = plan.K
    NB = len(plan.blocks)
    s = lax.axis_index("cols")
    n = lax.axis_index("rows")
    p = 1 - s
    mine = pl.ds(pl.multiple_of(s * HW, HW), HW)
    theirs = pl.ds(pl.multiple_of(p * HW, HW), HW)
    has_up, has_dn = n > 0, n < n_rows - 1
    bf, f32 = jnp.bfloat16, jnp.float32

    def local(src, dst, sem):
        return pltpu.make_async_copy(src, dst, sem)

    def remote(src, dst, ssem, rsem, dev):
        return pltpu.make_async_remote_copy(
            src_ref=src, dst_ref=dst, send_sem=ssem, recv_sem=rsem, device_id=dev, device_id_type=MESH)

    peer = {"cols": p}
    side_dev = [{"rows": n - 1}, {"rows": n + 1}]
    side_ok = [has_up, has_dn]

    def each_side(do):
        for side in range(2):
            @pl.when(side_ok[side])
            def _():
                do(side)

    barrier = pltpu.get_barrier_semaphore()

    def signal(dev):
        pl.semaphore_signal(barrier, inc=1, device_id=dev, device_id_type=MESH)

    signal(peer)
    each_side(lambda side: signal(side_dev[side]))

    h_own = local(h_init.at[s], hst.at[:, mine], s_i.at[0])
    c_own = local(c_init.at[s], cst.at[:, mine], s_i.at[1])
    x_own = [local(frames.at[a:e, s], xin.at[a:e, :, mine], s_x.at[g]) for g, (a, e) in enumerate(plan.groups)]
    h_got = local(h_init.at[p], hgo, s_i.at[2])
    c_got = local(c_init.at[p], cgo, s_i.at[3])
    x_got = [local(frames.at[a:e, p], xgo.at[a:e], s_i.at[4 + g]) for g, (a, e) in enumerate(plan.groups[:2])]
    w_copies = [local(w_h, wbuf.at[:, :, 0], s_w.at[0]), local(w_x, wbuf.at[:, :, 1], s_w.at[1])]
    for c in [h_got, x_got[0], h_own, x_own[0], c_got, c_own, x_got[1], x_own[1], *w_copies, *x_own[2:]]:
        c.start()
    pl.semaphore_wait(barrier, 1 + has_up.astype(jnp.int32) + has_dn.astype(jnp.int32))

    h_push = remote(hgo, hst.at[:, mine], s_is.at[0], s_ir.at[0], peer)
    c_push = remote(cgo, cst.at[:, mine], s_is.at[1], s_ir.at[1], peer)
    x_push = [remote((xgo if g < 2 else frames.at[:, p]).at[a:e], xin.at[a:e, :, mine], s_xs.at[g], s_xr.at[g], peer)
              for g, (a, e) in enumerate(plan.groups)]
    for got, push in [(h_got, h_push), (x_got[0], x_push[0]), (c_got, c_push), (x_got[1], x_push[1])]:
        got.wait()
        push.start()
    for push in x_push[2:]:
        push.start()

    shift[...] = jnp.zeros_like(shift)
    low = lax.broadcasted_iota(jnp.int32, (1, LANES), 1) < CH
    low_half = low_row = low
    turn = [0]
    scale = jnp.where(low_row, 0.5, 1.0)
    lift = jnp.where(low_row, 0.5, 0.0)

    for c in w_copies:
        c.wait()
    for dr in range(3):
        for dc in range(3):
            for half in range(2):
                tile = wbuf[dr, dc, half, :, 0:LANES]
                wbuf[dr, dc, half, :, 0:LANES] = jnp.concatenate([tile[:, CH:], tile[:, :CH]], axis=1)
    b_first = bias[:, 0:LANES]
    b_fi = jnp.concatenate([b_first[:, CH:], b_first[:, :CH]], axis=1) * 0.5
    b_og = bias[:, LANES:] * scale

    def pack(v):
        return jnp.concatenate([v[:, :HW], v[:, HW:]], axis=2)

    def unpack(v):
        return jnp.concatenate([v[:, :, :CH], v[:, :, CH:]], axis=1)

    def masked(r, v):
        if r < 0:
            return jnp.where(has_up, v, 0.0)
        if r >= R:
            return jnp.where(has_dn, v, 0.0)
        return v

    def emit(t, lo, hi, hx):
        nxt = xh_even if t % 2 == 0 else xh_odd
        at, to = slot(lo, hi), slice(lo + PAD, hi + PAD)
        shift[at, 8:8 + W, :] = hx
        nxt[1, to] = hx.astype(bf)
        nxt[0, to] = shift[at, 7:7 + W, :].astype(bf)
        nxt[2, to] = shift[at, 9:9 + W, :].astype(bf)

    def slot(lo, hi):
        if turn[0] + hi - lo > RING:
            turn[0] = 0
        turn[0] += hi - lo
        return slice(turn[0] - (hi - lo), turn[0])

    def x_rows(t, lo, hi):
        if lo >= 0 and hi <= R:
            return xin[t, lo:hi].astype(f32)
        side, i = (0, lo + plan.xrows[t]) if lo < 0 else (1, lo - R)
        return unpack(xr_ref[side, plan.xat[t] + i:plan.xat[t] + i + hi - lo].astype(f32))

    def wait_x(g):
        if g < len(plan.groups):
            x_own[g].wait()
            x_push[g].wait_recv()

    def border(b, kind, side):
        k, f = plan.blocks[b], plan.first[b]
        src, dst, at, count = [
            (xs_ref, xr_ref, plan.xat[f], plan.xat[f + k] - plan.xat[f]),
            (hs_ref, hr_ref, plan.hat[b], k),
            (cs_ref, cr_ref, plan.cat[b], k - 1)][kind]
        return remote(src.at[side, at:at + count], dst.at[1 - side, at:at + count],
                      s_bs.at[kind, side, b], s_b.at[kind, 1 - side, b], side_dev[side])

    def send_x(b):
        k, f = plan.blocks[b], plan.first[b]
        for side in range(2):
            for t in range(f, f + k):
                m = plan.xrows[t]
                lo = 0 if side == 0 else R - m
                xs_ref[side, plan.xat[t]:plan.xat[t] + m] = pack(xin[t, lo:lo + m])
        each_side(lambda side: border(b, 0, side).start())

    def send_state(b, h_rows):
        k = plan.blocks[b]
        for side in range(2):
            lo = 0 if side == 0 else R - k
            hs_ref[side, plan.hat[b]:plan.hat[b] + k] = pack(h_rows[lo:lo + k])
            lo = PAD if side == 0 else PAD + R - (k - 1)
            c = cbuf[lo:lo + k - 1]
            cs_ref[side, plan.cat[b]:plan.cat[b] + k - 1] = jnp.where(low_half, c[:, :HW], c[:, HW:])
        def start(side):
            border(b, 1, side).start()
            border(b, 2, side).start()

        each_side(start)

    weights = wbuf[...].reshape(9 * LANES, 4 * CH)

    def dot(t, lo, hi):
        cur = xh_even if t % 2 == 0 else xh_odd
        taps = [cur[dc, lo + PAD + dr - 1:hi + PAD + dr - 1].reshape((hi - lo) * W, LANES)
                for dr in range(3) for dc in range(3)]
        return jnp.dot(jnp.concatenate(taps, axis=1), weights, preferred_element_type=f32)

    def cells(t, lo, hi, gates):
        m, g = hi - lo, gates
        fi = jnp.tanh(g[:, :LANES] * 0.5 + b_fi) * 0.5 + 0.5
        og = jnp.tanh(g[:, LANES:] * scale + b_og) * scale + lift
        prod = fi * jnp.where(low, cbuf[lo + PAD:hi + PAD].reshape(m * W, LANES), og)
        c = prod + pltpu.roll(prod, CH, 1)
        h = (og * jnp.tanh(c)).reshape(m, W, LANES)
        c = c.reshape(m, W, LANES)
        if t == T - 1:
            cout[lo:hi] = c[:, :, :CH]
        else:
            cbuf[lo + PAD:hi + PAD] = c
        for a, e in ((lo, min(hi, 0)), (max(lo, 0), min(hi, R)), (max(lo, R), hi)):
            if a >= e:
                continue
            part = h[a - lo:e - lo, :, :CH]
            if a >= 0 and e <= R:
                hout[t, a:e] = part.astype(bf)
            if t < T - 1:
                emit(t + 1, a, e, masked(a, jnp.concatenate([part, x_rows(t + 1, a, e)], axis=2)))

    pending = []

    def piece(t, lo, hi):
        gates = dot(t, lo, hi)
        flush()
        pending.append((t, lo, hi, gates))

    def flush():
        while pending:
            cells(*pending.pop())

    outs = []

    def push_h(t0, t1, lo=0, hi=R):
        g = len(outs)
        rows = slice(lo, hi)
        outs.append(remote(hout.at[t0:t1, rows, theirs], hpeer.at[t0:t1, rows], s_os.at[g], s_or.at[g], peer))
        outs[-1].start()

    def push_c(lo, hi):
        g = len(outs)
        outs.append(remote(cout.at[lo:hi, theirs], cpeer.at[lo:hi], s_os.at[g], s_or.at[g], peer))
        outs[-1].start()

    for c in [h_own, c_own]:
        c.wait()
    for c in [h_push, c_push]:
        c.wait_recv()
    c0 = cst[...]
    cbuf[PAD:PAD + R] = jnp.concatenate([c0, c0], axis=2)
    send_state(0, hst)
    wait_x(0)
    for lo, hi in cuts(0, R):
        emit(0, lo, hi, jnp.concatenate([hst[lo:hi].astype(f32), x_rows(0, lo, hi)], axis=2))

    for b, k in enumerate(plan.blocks):
        f = plan.first[b]
        last = b + 1 == NB

        def inner(o):
            if o == 0:
                got = [(1, k + 1), *cuts(k + 1, R - 1 - k), (R - 1 - k, R - 1)]
            else:
                got = cuts(o + 1, R - 1 - o)
            return [(f + o, lo, hi) for lo, hi in got[1:-1] + [got[0], got[-1]]]

        fill = FILL[b]
        for o in range(k - fill):
            for i, at in enumerate(inner(o)):
                piece(*at)
                if o == 0 and i == 0:
                    if b == 0:
                        wait_x(1)
                        send_x(0)
                    else:
                        send_state(b, hout.at[f - 1])
                        push_h(plan.first[b - 1], f)
        each_side(lambda side: [border(b, kind, 1 - side).wait_recv() for kind in (1, 2, 0)])
        wait_x(b + 2)
        for side in range(2):
            lo = -k if side == 0 else R
            h = unpack(hr_ref[side, plan.hat[b]:plan.hat[b] + k].astype(f32))
            emit(f, lo, lo + k, masked(lo, jnp.concatenate([h, x_rows(f, lo, lo + k)], axis=2)))
            lo = PAD - (k - 1) if side == 0 else PAD + R
            packed = cr_ref[side, plan.cat[b]:plan.cat[b] + k - 1]
            cbuf[lo:lo + k - 1, 0:HW] = packed
            cbuf[lo:lo + k - 1, HW:W] = pltpu.roll(packed, CH, 2)
        if not last:
            send_x(b + 1)
        rest = inner(k - 1) if fill else []
        for o in range(k):
            m = k - 1 - o
            edges = zip(cuts(-m, o + 1, max(PIECE, k)), cuts(R - 1 - o, R + m, max(PIECE, k)))
            for (a, e), (a2, e2) in edges:
                piece(f + o, a, e)
                piece(f + o, a2, e2)
            if o < k - 1:
                part = rest[len(rest) * o // (k - 1):len(rest) * (o + 1) // (k - 1)]
                for at in part:
                    piece(*at)
        if last:
            push_h(f, T - 1)
            push_h(T - 1, T, k, R - k)
            push_c(k, R - k)
    flush()
    k = plan.blocks[-1]
    for lo, hi in ((0, k), (R - k, R)):
        push_h(T - 1, T, lo, hi)
        push_c(lo, hi)

    for c in [h_push, c_push, *x_push]:
        c.wait_send()
    each_side(lambda side: [border(b, kind, side).wait_send() for b in range(NB) for kind in range(3)])
    for c in outs:
        c.wait()


def store(hout, hpeer, cout, cpeer, h_all, c_final, sems):
    s = lax.axis_index("cols")
    HW = hpeer.shape[2]
    mine = pl.ds(pl.multiple_of(s * HW, HW), HW)
    copies = [pltpu.make_async_copy(hout.at[:, :, mine], h_all.at[:, s], sems.at[0]),
              pltpu.make_async_copy(hpeer, h_all.at[:, 1 - s], sems.at[1]),
              pltpu.make_async_copy(cout.at[:, mine], c_final.at[s], sems.at[2]),
              pltpu.make_async_copy(cpeer, c_final.at[1 - s], sems.at[3])]
    for c in copies:
        c.start()
    for c in copies:
        c.wait()


def run(blocks, n_rows, frames, w_x, w_h, gate_bias, h_init, c_init):
    T, S, R, HW = frames.shape[:4]
    W = 2 * HW
    plan = Plan(blocks, T, R, W)
    NB, PAD, G = len(blocks), plan.K, len(plan.groups)
    bf, f32 = jnp.bfloat16, jnp.float32
    vm, dma = pltpu.VMEM, pltpu.SemaphoreType.DMA
    hbm = pl.BlockSpec(memory_space=pltpu.HBM)
    vmem = pl.BlockSpec(memory_space=pltpu.VMEM)
    parts = pl.pallas_call(
        functools.partial(kernel, plan, n_rows),
        out_shape=(vm((T, R, W, CH), bf), vm((T, R, HW, CH), bf), vm((R, W, CH), f32), vm((R, HW, CH), f32)),
        in_specs=[hbm, hbm, hbm, vmem, hbm, hbm],
        out_specs=(vmem,) * 4,
        scratch_shapes=[
            vm((R, HW, CH), bf), vm((R, HW, CH), f32), vm((plan.groups[1][1], R, HW, CH), bf),
            vm((T, R, W, CH), bf), vm((R, W, CH), bf), vm((R, W, CH), f32),
            vm((3, R + 2 * PAD, W, LANES), bf), vm((3, R + 2 * PAD, W, LANES), bf),
            vm((R + 2 * PAD, W, LANES), f32), vm((RING, W + 16, LANES), f32), vm((3, 3, 2, CH, 4 * CH), bf),
            vm((2, plan.xat[-1], HW, LANES), bf), vm((2, plan.xat[-1], HW, LANES), bf),
            vm((2, plan.hat[-1], HW, LANES), bf), vm((2, plan.hat[-1], HW, LANES), bf),
            vm((2, plan.cat[-1], HW, LANES), f32), vm((2, plan.cat[-1], HW, LANES), f32),
            dma((2,)), dma((6,)), dma((2,)), dma((2,)), dma((G,)), dma((G,)), dma((G,)),
            dma((3, 2, NB)), dma((3, 2, NB)), dma((NB + 6,)), dma((NB + 6,))],
        compiler_params=pltpu.CompilerParams(collective_id=0, has_side_effects=True, vmem_limit_bytes=46 * 2**20),
    )(frames, w_x, w_h, gate_bias.reshape(1, -1), h_init, c_init)
    return pl.pallas_call(
        store,
        out_shape=(jax.ShapeDtypeStruct(frames.shape, bf), jax.ShapeDtypeStruct(c_init.shape, f32)),
        in_specs=[vmem] * 4,
        out_specs=(hbm, hbm),
        scratch_shapes=[dma((4,))],
        compiler_params=pltpu.CompilerParams(vmem_limit_bytes=2**20),
    )(*[pltpu.with_memory_space_constraint(a, pltpu.VMEM) for a in parts])


def solution(mesh, K=None):
    n_rows = mesh.shape["rows"]
    frame_spec = P(None, "batch", "rows", "cols", None)
    state_spec = P("batch", "rows", "cols", None)
    blocks = BLOCKS if K is None else K
    return jax.shard_map(functools.partial(run, blocks, n_rows), mesh=mesh,
                         in_specs=(frame_spec, P(), P(), P(), state_spec, state_spec),
                         out_specs=(frame_spec, state_spec), check_vma=False)
```

```python
import functools

import jax
import jax.numpy as jnp
from jax import lax
from jax.experimental import pallas as pl
from jax.experimental.pallas import tpu as pltpu
from jax.sharding import PartitionSpec as P

MESH = pl.DeviceIdType.MESH
CH = 64
LANES = 128
PIECE = 4
RING = 8
BLOCKS = (8, 8)
FILL = (0, 0)


def cuts(lo, hi, size=PIECE):
    n = max(1, (hi - lo) // size)
    edges = [lo + i * size for i in range(n)] + [hi]
    return list(zip(edges[:-1], edges[1:]))


class Plan:
    def __init__(self, blocks, T, R, W):
        assert sum(blocks) == T
        self.blocks, self.T, self.R, self.W, self.HW = blocks, T, R, W, W // 2
        self.K = max(blocks)
        self.first = [sum(blocks[:b]) for b in range(len(blocks))]
        self.of = [(b, o) for b, k in enumerate(blocks) for o in range(k)]
        self.xrows = [blocks[b] - o for b, o in self.of]
        self.xat = [sum(self.xrows[:t]) for t in range(T + 1)]
        self.hat = [sum(blocks[:b]) for b in range(len(blocks) + 1)]
        self.cat = [sum(k - 1 for k in blocks[:b]) for b in range(len(blocks) + 1)]
        ends = [0, 1, 3] + [min(f + k + 1, T) for f, k in zip(self.first, blocks)]
        self.groups = [(a, e) for a, e in zip(ends[:-1], ends[1:]) if e > a]


def kernel(plan, n_rows, frames, w_x, w_h, bias_in, h_init, c_init, hout, hpeer, cout, cpeer,
           bias, hgo, cgo, xgo, xin, hst, cst, xh_even, xh_odd, cbuf, shift, wbuf,
           xs_ref, xr_ref, hs_ref, hr_ref, cs_ref, cr_ref,
           s_w, s_i, s_ir, s_is, s_x, s_xr, s_xs, s_b, s_bs, s_or, s_os):
    T, R, W, HW = plan.T, plan.R, plan.W, plan.HW
    PAD = plan.K
    NB = len(plan.blocks)
    s = lax.axis_index("cols")
    n = lax.axis_index("rows")
    p = 1 - s
    mine = pl.ds(pl.multiple_of(s * HW, HW), HW)
    theirs = pl.ds(pl.multiple_of(p * HW, HW), HW)
    has_up, has_dn = n > 0, n < n_rows - 1
    bf, f32 = jnp.bfloat16, jnp.float32

    def local(src, dst, sem):
        return pltpu.make_async_copy(src, dst, sem)

    def remote(src, dst, ssem, rsem, dev):
        return pltpu.make_async_remote_copy(
            src_ref=src, dst_ref=dst, send_sem=ssem, recv_sem=rsem, device_id=dev, device_id_type=MESH)

    peer = {"cols": p}
    side_dev = [{"rows": n - 1}, {"rows": n + 1}]
    side_ok = [has_up, has_dn]

    def each_side(do):
        for side in range(2):
            @pl.when(side_ok[side])
            def _():
                do(side)

    barrier = pltpu.get_barrier_semaphore()

    def signal(dev):
        pl.semaphore_signal(barrier, inc=1, device_id=dev, device_id_type=MESH)

    signal(peer)
    each_side(lambda side: signal(side_dev[side]))

    h_own = local(h_init.at[s], hst.at[:, mine], s_i.at[0])
    c_own = local(c_init.at[s], cst.at[:, mine], s_i.at[1])
    x_own = [local(frames.at[a:e, s], xin.at[a:e, :, mine], s_x.at[g]) for g, (a, e) in enumerate(plan.groups)]
    h_got = local(h_init.at[p], hgo, s_i.at[2])
    c_got = local(c_init.at[p], cgo, s_i.at[3])
    x_got = [local(frames.at[a:e, p], xgo.at[a:e], s_i.at[4 + g]) for g, (a, e) in enumerate(plan.groups[:2])]
    w_copies = [local(w_h, wbuf.at[:, :, 0], s_w.at[0]), local(w_x, wbuf.at[:, :, 1], s_w.at[1]),
                local(bias_in, bias, s_w.at[2])]
    for c in [h_got, x_got[0], c_got, h_own, x_own[0], c_own, *w_copies, x_got[1], *x_own[1:]]:
        c.start()
    with jax.named_scope('barrier'):
        pl.semaphore_wait(barrier, 1 + has_up.astype(jnp.int32) + has_dn.astype(jnp.int32))

    h_push = remote(hgo, hst.at[:, mine], s_is.at[0], s_ir.at[0], peer)
    c_push = remote(cgo, cst.at[:, mine], s_is.at[1], s_ir.at[1], peer)
    x_push = [remote((xgo if g < 2 else frames.at[:, p]).at[a:e], xin.at[a:e, :, mine], s_xs.at[g], s_xr.at[g], peer)
              for g, (a, e) in enumerate(plan.groups)]
    with jax.named_scope('got_wait'):
        for got, push in [(h_got, h_push), (x_got[0], x_push[0]), (c_got, c_push), (x_got[1], x_push[1])]:
            got.wait()
            push.start()
    for push in x_push[2:]:
        push.start()

    shift[...] = jnp.zeros_like(shift)
    low = lax.broadcasted_iota(jnp.int32, (1, LANES), 1) < CH
    low_half = low_row = low
    turn = [0]
    scale = jnp.where(low_row, 0.5, 1.0)
    lift = jnp.where(low_row, 0.5, 0.0)

    with jax.named_scope('w_wait'):
        for c in w_copies:
            c.wait()
    for dr in range(3):
        for dc in range(3):
            for half in range(2):
                tile = wbuf[dr, dc, half, :, 0:LANES]
                wbuf[dr, dc, half, :, 0:LANES] = jnp.concatenate([tile[:, CH:], tile[:, :CH]], axis=1)
    b_first = bias[:, 0:LANES]
    b_fi = jnp.concatenate([b_first[:, CH:], b_first[:, :CH]], axis=1) * 0.5
    b_og = bias[:, LANES:] * scale

    def pack(v):
        return jnp.concatenate([v[:, :HW], v[:, HW:]], axis=2)

    def unpack(v):
        return jnp.concatenate([v[:, :, :CH], v[:, :, CH:]], axis=1)

    def masked(r, v):
        if 0 <= r < R:
            return v
        return lax.select(jnp.broadcast_to(has_up if r < 0 else has_dn, v.shape), v, jnp.zeros_like(v))

    def emit(t, lo, hi, hx):
        nxt = xh_even if t % 2 == 0 else xh_odd
        at, to = slot(lo, hi), cells_of(lo, hi)
        shift[at, 8:8 + W, :] = hx.reshape(hi - lo, W, LANES)
        nxt[1, to] = hx.astype(bf)
        nxt[0, to] = shift[at, 7:7 + W, :].reshape(hx.shape).astype(bf)
        nxt[2, to] = shift[at, 9:9 + W, :].reshape(hx.shape).astype(bf)

    def cells_of(lo, hi):
        return slice((lo + PAD) * W, (hi + PAD) * W)

    def slot(lo, hi):
        if turn[0] + hi - lo > RING:
            turn[0] = 0
        turn[0] += hi - lo
        return slice(turn[0] - (hi - lo), turn[0])

    def flat(v):
        return v.reshape(-1, v.shape[-1])

    def x_rows(t, lo, hi):
        if lo >= 0 and hi <= R:
            return flat(xin[t, lo:hi]).astype(f32)
        side, i = (0, lo + plan.xrows[t]) if lo < 0 else (1, lo - R)
        return flat(unpack(xr_ref[side, plan.xat[t] + i:plan.xat[t] + i + hi - lo])).astype(f32)

    def wait_x(g):
        if g < len(plan.groups):
            x_own[g].wait()
            x_push[g].wait_recv()

    def border(b, kind, side):
        k, f = plan.blocks[b], plan.first[b]
        src, dst, at, end = [
            (hs_ref, hr_ref, plan.hat[b], plan.hat[b + 1]),
            (cs_ref, cr_ref, plan.cat[b], plan.cat[b + 1]),
            (xs_ref, xr_ref, plan.xat[f], plan.xat[f + 1]),
            (xs_ref, xr_ref, plan.xat[f + 1], plan.xat[f + k])][kind]
        return remote(src.at[side, at:end], dst.at[1 - side, at:end],
                      s_bs.at[kind, side, b], s_b.at[kind, 1 - side, b], side_dev[side])

    def pack_x(t0, t1):
        for side in range(2):
            for t in range(t0, t1):
                m = plan.xrows[t]
                lo = 0 if side == 0 else R - m
                xs_ref[side, plan.xat[t]:plan.xat[t] + m] = pack(xin[t, lo:lo + m])

    def start_border(b, *kinds):
        each_side(lambda side: [border(b, kind, side).start() for kind in kinds])

    def wait_border(b, *kinds):
        each_side(lambda side: [border(b, kind, 1 - side).wait_recv() for kind in kinds])

    def pack_state(b, h_rows):
        k = plan.blocks[b]
        for side in range(2):
            lo = 0 if side == 0 else R - k
            hs_ref[side, plan.hat[b]:plan.hat[b] + k] = pack(h_rows[lo:lo + k])
            lo = 0 if side == 0 else R - (k - 1)
            c = cbuf[cells_of(lo, lo + k - 1)].reshape(k - 1, W, LANES)
            cs_ref[side, plan.cat[b]:plan.cat[b] + k - 1] = jnp.where(low_half, c[:, :HW], c[:, HW:])

    weights = wbuf[...].reshape(9 * LANES, 4 * CH)

    def dot(t, lo, hi):
        cur = xh_even if t % 2 == 0 else xh_odd
        taps = [cur[dc, cells_of(lo + dr - 1, hi + dr - 1)] for dr in range(3) for dc in range(3)]
        return jnp.dot(jnp.concatenate(taps, axis=1), weights, preferred_element_type=f32)

    def cells(t, lo, hi, gates):
        fi = jnp.tanh(gates[:, :LANES] * 0.5 + b_fi) * 0.5 + 0.5
        og = jnp.tanh(gates[:, LANES:] * scale + b_og) * scale + lift
        at = cells_of(lo, hi)
        prod = fi * lax.select(jnp.broadcast_to(low, og.shape), cbuf[at], og)
        c = prod + pltpu.roll(prod, CH, 1)
        h = (og * jnp.tanh(c))[:, :CH]
        if t == T - 1:
            cout[lo:hi] = c[:, :CH].reshape(hi - lo, W, CH)
        else:
            cbuf[at] = c
        for a, e in ((lo, min(hi, 0)), (max(lo, 0), min(hi, R)), (max(lo, R), hi)):
            if a >= e:
                continue
            part = h[(a - lo) * W:(e - lo) * W]
            if a >= 0 and e <= R:
                hout[t, a:e] = part.reshape(e - a, W, CH).astype(bf)
            if t < T - 1:
                emit(t + 1, a, e, masked(a, jnp.concatenate([part, x_rows(t + 1, a, e)], axis=1)))

    pending = []

    def piece(t, lo, hi):
        gates = dot(t, lo, hi)
        flush()
        pending.append((t, lo, hi, gates))

    def flush():
        while pending:
            cells(*pending.pop())

    outs = []

    def push_h(t0, t1, lo=0, hi=R):
        g = len(outs)
        rows = slice(lo, hi)
        outs.append(remote(hout.at[t0:t1, rows, theirs], hpeer.at[t0:t1, rows], s_os.at[g], s_or.at[g], peer))
        outs[-1].start()

    def push_c(lo, hi):
        g = len(outs)
        outs.append(remote(cout.at[lo:hi, theirs], cpeer.at[lo:hi], s_os.at[g], s_or.at[g], peer))
        outs[-1].start()

    with jax.named_scope('state_wait'):
        for c in [h_own, x_own[0], c_own]:
            c.wait()
        for c in [h_push, x_push[0], c_push]:
            c.wait_recv()
    c0 = flat(cst[...])
    cbuf[cells_of(0, R)] = jnp.concatenate([c0, c0], axis=1)
    pack_state(0, hst)
    pack_x(0, 1)
    start_border(0, 0, 1, 2)
    for lo, hi in cuts(0, R):
        emit(0, lo, hi, jnp.concatenate([flat(hst[lo:hi]).astype(f32), x_rows(0, lo, hi)], axis=1))

    for b, k in enumerate(plan.blocks):
        f = plan.first[b]
        last = b + 1 == NB

        def inner(o):
            if o == 0:
                got = [*cuts(k + 1, R - 1 - k), *cuts(1, k + 1), *cuts(R - 1 - k, R - 1)]
            else:
                got = cuts(o + 1, R - 1 - o)
                got = got[1:-1] + [got[0], got[-1]]
            return [(f + o, lo, hi) for lo, hi in got]

        fill = FILL[b]
        for o in range(k - fill):
            for i, at in enumerate(inner(o)):
                piece(*at)
                if i == 0 and b == 0 and o == 0:
                    with jax.named_scope('x1_wait'):
                        wait_x(1)
                if i == 0 and b == 0 and o == 2:
                    with jax.named_scope('x2_wait'):
                        wait_x(2)
                    pack_x(1, k)
                    start_border(0, 3)
                if i == 0 and b and o == 0:
                    pack_state(b, hout.at[f - 1])
                    start_border(b, 0, 1)
        with jax.named_scope(f'mid{b}'):
            wait_border(b, *(range(3) if b == 0 else range(4)))
            wait_x(b + 3)
        for side in range(2):
            lo = -k if side == 0 else R
            h = flat(unpack(hr_ref[side, plan.hat[b]:plan.hat[b] + k])).astype(f32)
            emit(f, lo, lo + k, masked(lo, jnp.concatenate([h, x_rows(f, lo, lo + k)], axis=1)))
            lo = -(k - 1) if side == 0 else R
            packed = cr_ref[side, plan.cat[b]:plan.cat[b] + k - 1]
            both = jnp.concatenate([packed, pltpu.roll(packed, CH, 2)], axis=1)
            cbuf[cells_of(lo, lo + k - 1)] = flat(both)
        if not last:
            pack_x(f + k, f + k + plan.blocks[b + 1])
            start_border(b + 1, 2, 3)
        if b:
            push_h(plan.first[b - 1], f)
        rest = inner(k - 1) if fill else []
        for o in range(k):
            m = k - 1 - o
            edges = zip(cuts(-m, o + 1), cuts(R - 1 - o, R + m))
            for i, ((a, e), (a2, e2)) in enumerate(edges):
                piece(f + o, a, e)
                if i == 0 and b == 0 and o == 0:
                    with jax.named_scope('x3b_wait'):
                        wait_border(0, 3)
                piece(f + o, a2, e2)
                if last and i == 0 and o == k // 2:
                    push_h(f, f + o)
                if last and i == 0 and o == k - 1:
                    push_h(f + k // 2, T - 1)
                    push_h(T - 1, T, k, R - k)
                    push_c(k, R - k)
            if o < k - 1:
                part = rest[len(rest) * o // (k - 1):len(rest) * (o + 1) // (k - 1)]
                for at in part:
                    piece(*at)
    flush()
    k = plan.blocks[-1]
    for lo, hi in ((0, k), (R - k, R)):
        push_h(T - 1, T, lo, hi)
        push_c(lo, hi)

    with jax.named_scope('end_wait'):
        for c in [h_push, c_push, *x_push]:
            c.wait_send()
        each_side(lambda side: [border(b, kind, side).wait_send() for b in range(NB) for kind in range(4)])
        for c in outs:
            c.wait()


def store(hout, hpeer, cout, cpeer, h_all, c_final, sems):
    s = lax.axis_index("cols")
    HW = hpeer.shape[2]
    mine = pl.ds(pl.multiple_of(s * HW, HW), HW)
    copies = [pltpu.make_async_copy(hout.at[:, :, mine], h_all.at[:, s], sems.at[0]),
              pltpu.make_async_copy(hpeer, h_all.at[:, 1 - s], sems.at[1]),
              pltpu.make_async_copy(cout.at[:, mine], c_final.at[s], sems.at[2]),
              pltpu.make_async_copy(cpeer, c_final.at[1 - s], sems.at[3])]
    for c in copies:
        c.start()
    for c in copies:
        c.wait()


def run(blocks, n_rows, frames, w_x, w_h, gate_bias, h_init, c_init):
    T, S, R, HW = frames.shape[:4]
    W = 2 * HW
    plan = Plan(blocks, T, R, W)
    NB, PAD, G = len(blocks), plan.K, len(plan.groups)
    bf, f32 = jnp.bfloat16, jnp.float32
    vm, dma = pltpu.VMEM, pltpu.SemaphoreType.DMA
    hbm = pl.BlockSpec(memory_space=pltpu.HBM)
    vmem = pl.BlockSpec(memory_space=pltpu.VMEM)
    parts = pl.pallas_call(
        functools.partial(kernel, plan, n_rows),
        out_shape=(vm((T, R, W, CH), bf), vm((T, R, HW, CH), bf), vm((R, W, CH), f32), vm((R, HW, CH), f32)),
        in_specs=[hbm] * 6,
        out_specs=(vmem,) * 4,
        scratch_shapes=[
            vm((1, 4 * CH), f32), vm((R, HW, CH), bf), vm((R, HW, CH), f32), vm((plan.groups[1][1], R, HW, CH), bf),
            vm((T, R, W, CH), bf), vm((R, W, CH), bf), vm((R, W, CH), f32),
            vm((3, (R + 2 * PAD) * W, LANES), bf), vm((3, (R + 2 * PAD) * W, LANES), bf),
            vm(((R + 2 * PAD) * W, LANES), f32), vm((RING, W + 16, LANES), f32), vm((3, 3, 2, CH, 4 * CH), bf),
            vm((2, plan.xat[-1], HW, LANES), bf), vm((2, plan.xat[-1], HW, LANES), bf),
            vm((2, plan.hat[-1], HW, LANES), bf), vm((2, plan.hat[-1], HW, LANES), bf),
            vm((2, plan.cat[-1], HW, LANES), f32), vm((2, plan.cat[-1], HW, LANES), f32),
            dma((3,)), dma((6,)), dma((2,)), dma((2,)), dma((G,)), dma((G,)), dma((G,)),
            dma((4, 2, NB)), dma((4, 2, NB)), dma((NB + 8,)), dma((NB + 8,))],
        compiler_params=pltpu.CompilerParams(collective_id=0, has_side_effects=True, vmem_limit_bytes=46 * 2**20),
    )(frames, w_x, w_h, gate_bias.reshape(1, -1), h_init, c_init)
    return pl.pallas_call(
        store,
        out_shape=(jax.ShapeDtypeStruct(frames.shape, bf), jax.ShapeDtypeStruct(c_init.shape, f32)),
        in_specs=[vmem] * 4,
        out_specs=(hbm, hbm),
        scratch_shapes=[dma((4,))],
        compiler_params=pltpu.CompilerParams(vmem_limit_bytes=2**20),
    )(*[pltpu.with_memory_space_constraint(a, pltpu.VMEM) for a in parts])


def solution(mesh, K=None):
    n_rows = mesh.shape["rows"]
    frame_spec = P(None, "batch", "rows", "cols", None)
    state_spec = P("batch", "rows", "cols", None)
    blocks = BLOCKS if K is None else K
    return jax.shard_map(functools.partial(run, blocks, n_rows), mesh=mesh,
                         in_specs=(frame_spec, P(), P(), P(), state_spec, state_spec),
                         out_specs=(frame_spec, state_spec), check_vma=False)
```

```python
import functools

import jax
import jax.numpy as jnp
from jax import lax
from jax.experimental import pallas as pl
from jax.experimental.pallas import tpu as pltpu
from jax.sharding import PartitionSpec as P

MESH = pl.DeviceIdType.MESH
CH = 64
LANES = 128
PIECE = 4
RING = 8
BLOCKS = (8, 8)
LATE = (2, 2)


def cuts(lo, hi, size=PIECE):
    n = max(1, (hi - lo) // size)
    edges = [lo + i * size for i in range(n)] + [hi]
    return list(zip(edges[:-1], edges[1:]))


class Plan:
    def __init__(self, blocks, T, R, W):
        assert sum(blocks) == T
        self.blocks, self.T, self.R, self.W, self.HW = blocks, T, R, W, W // 2
        self.K = max(blocks)
        self.first = [sum(blocks[:b]) for b in range(len(blocks))]
        self.of = [(b, o) for b, k in enumerate(blocks) for o in range(k)]
        self.xrows = [blocks[b] - o for b, o in self.of]
        self.xat = [sum(self.xrows[:t]) for t in range(T + 1)]
        self.hat = [sum(blocks[:b]) for b in range(len(blocks) + 1)]
        self.cat = [sum(k - 1 for k in blocks[:b]) for b in range(len(blocks) + 1)]
        ends = [0, 1, 3] + [min(f + k + 1, T) for f, k in zip(self.first, blocks)]
        self.groups = [(a, e) for a, e in zip(ends[:-1], ends[1:]) if e > a]


def kernel(plan, n_rows, frames, w_x, w_h, bias_in, h_init, c_init, hout, hpeer, cout, cpeer,
           bias, hgo, cgo, xgo, xin, hst, cst, xh_even, xh_odd, cbuf, shift, wbuf,
           xs_ref, xr_ref, hs_ref, hr_ref, cs_ref, cr_ref,
           s_w, s_i, s_ir, s_is, s_x, s_xr, s_xs, s_b, s_bs, s_or, s_os):
    T, R, W, HW = plan.T, plan.R, plan.W, plan.HW
    PAD = plan.K
    NB = len(plan.blocks)
    s = lax.axis_index("cols")
    n = lax.axis_index("rows")
    p = 1 - s
    mine = pl.ds(pl.multiple_of(s * HW, HW), HW)
    theirs = pl.ds(pl.multiple_of(p * HW, HW), HW)
    has_up, has_dn = n > 0, n < n_rows - 1
    bf, f32 = jnp.bfloat16, jnp.float32

    def local(src, dst, sem):
        return pltpu.make_async_copy(src, dst, sem)

    def remote(src, dst, ssem, rsem, dev):
        return pltpu.make_async_remote_copy(
            src_ref=src, dst_ref=dst, send_sem=ssem, recv_sem=rsem, device_id=dev, device_id_type=MESH)

    peer = {"cols": p}
    side_dev = [{"rows": n - 1}, {"rows": n + 1}]
    side_ok = [has_up, has_dn]

    def each_side(do):
        for side in range(2):
            @pl.when(side_ok[side])
            def _():
                do(side)

    barrier = pltpu.get_barrier_semaphore()

    def signal(dev):
        pl.semaphore_signal(barrier, inc=1, device_id=dev, device_id_type=MESH)

    signal(peer)
    each_side(lambda side: signal(side_dev[side]))

    h_own = local(h_init.at[s], hst.at[:, mine], s_i.at[0])
    c_own = local(c_init.at[s], cst.at[:, mine], s_i.at[1])
    x_own = [local(frames.at[a:e, s], xin.at[a:e, :, mine], s_x.at[g]) for g, (a, e) in enumerate(plan.groups)]
    h_got = local(h_init.at[p], hgo, s_i.at[2])
    c_got = local(c_init.at[p], cgo, s_i.at[3])
    x_got = [local(frames.at[a:e, p], xgo.at[a:e], s_i.at[4 + g]) for g, (a, e) in enumerate(plan.groups[:2])]
    w_copies = [local(w_h, wbuf.at[:, :, 0], s_w.at[0]), local(w_x, wbuf.at[:, :, 1], s_w.at[1]),
                local(bias_in, bias, s_w.at[2])]
    for c in [h_got, x_got[0], c_got, h_own, x_own[0], c_own, *w_copies, x_got[1], *x_own[1:]]:
        c.start()
    with jax.named_scope('barrier'):
        pl.semaphore_wait(barrier, 1 + has_up.astype(jnp.int32) + has_dn.astype(jnp.int32))

    h_push = remote(hgo, hst.at[:, mine], s_is.at[0], s_ir.at[0], peer)
    c_push = remote(cgo, cst.at[:, mine], s_is.at[1], s_ir.at[1], peer)
    x_push = [remote((xgo if g < 2 else frames.at[:, p]).at[a:e], xin.at[a:e, :, mine], s_xs.at[g], s_xr.at[g], peer)
              for g, (a, e) in enumerate(plan.groups)]
    with jax.named_scope('got_wait'):
        for got, push in [(h_got, h_push), (x_got[0], x_push[0]), (c_got, c_push), (x_got[1], x_push[1])]:
            got.wait()
            push.start()
    for push in x_push[2:]:
        push.start()

    shift[...] = jnp.zeros_like(shift)
    low = lax.broadcasted_iota(jnp.int32, (1, LANES), 1) < CH
    low_half = low_row = low
    turn = [0]
    scale = jnp.where(low_row, 0.5, 1.0)
    lift = jnp.where(low_row, 0.5, 0.0)

    with jax.named_scope('w_wait'):
        for c in w_copies:
            c.wait()
    for dr in range(3):
        for dc in range(3):
            for half in range(2):
                tile = wbuf[dr, dc, half, :, 0:LANES]
                wbuf[dr, dc, half, :, 0:LANES] = jnp.concatenate([tile[:, CH:], tile[:, :CH]], axis=1)
    b_first = bias[:, 0:LANES]
    b_fi = jnp.concatenate([b_first[:, CH:], b_first[:, :CH]], axis=1) * 0.5
    b_og = bias[:, LANES:] * scale

    def pack(v):
        return jnp.concatenate([v[:, :HW], v[:, HW:]], axis=2)

    def unpack(v):
        return jnp.concatenate([v[:, :, :CH], v[:, :, CH:]], axis=1)

    def masked(r, v):
        if 0 <= r < R:
            return v
        return lax.select(jnp.broadcast_to(has_up if r < 0 else has_dn, v.shape), v, jnp.zeros_like(v))

    def emit(t, lo, hi, hx):
        nxt = xh_even if t % 2 == 0 else xh_odd
        at, to = slot(lo, hi), cells_of(lo, hi)
        shift[at, 8:8 + W, :] = hx.reshape(hi - lo, W, LANES)
        nxt[1, to] = hx.astype(bf)
        nxt[0, to] = shift[at, 7:7 + W, :].reshape(hx.shape).astype(bf)
        nxt[2, to] = shift[at, 9:9 + W, :].reshape(hx.shape).astype(bf)

    def cells_of(lo, hi):
        return slice((lo + PAD) * W, (hi + PAD) * W)

    def slot(lo, hi):
        if turn[0] + hi - lo > RING:
            turn[0] = 0
        turn[0] += hi - lo
        return slice(turn[0] - (hi - lo), turn[0])

    def flat(v):
        return v.reshape(-1, v.shape[-1])

    def x_rows(t, lo, hi):
        if lo >= 0 and hi <= R:
            return flat(xin[t, lo:hi]).astype(f32)
        side, i = (0, lo + plan.xrows[t]) if lo < 0 else (1, lo - R)
        return flat(unpack(xr_ref[side, plan.xat[t] + i:plan.xat[t] + i + hi - lo])).astype(f32)

    def wait_x(g):
        if g < len(plan.groups):
            x_own[g].wait()
            x_push[g].wait_recv()

    def border(b, kind, side):
        k, f = plan.blocks[b], plan.first[b]
        src, dst, at, end = [
            (hs_ref, hr_ref, plan.hat[b], plan.hat[b + 1]),
            (cs_ref, cr_ref, plan.cat[b], plan.cat[b + 1]),
            (xs_ref, xr_ref, plan.xat[f], plan.xat[f + 1]),
            (xs_ref, xr_ref, plan.xat[f + 1], plan.xat[f + k])][kind]
        return remote(src.at[side, at:end], dst.at[1 - side, at:end],
                      s_bs.at[min(kind, 2), side], s_b.at[kind, 1 - side, b], side_dev[side])

    def pack_x(t0, t1):
        for side in range(2):
            for t in range(t0, t1):
                m = plan.xrows[t]
                lo = 0 if side == 0 else R - m
                xs_ref[side, plan.xat[t]:plan.xat[t] + m] = pack(xin[t, lo:lo + m])

    def start_border(b, *kinds):
        each_side(lambda side: [border(b, kind, side).start() for kind in kinds])

    def wait_border(b, *kinds):
        each_side(lambda side: [border(b, kind, 1 - side).wait_recv() for kind in kinds])

    def pack_state(b, h_rows):
        k = plan.blocks[b]
        for side in range(2):
            lo = 0 if side == 0 else R - k
            hs_ref[side, plan.hat[b]:plan.hat[b] + k] = pack(h_rows[lo:lo + k])
            lo = 0 if side == 0 else R - (k - 1)
            c = cbuf[cells_of(lo, lo + k - 1)].reshape(k - 1, W, LANES)
            cs_ref[side, plan.cat[b]:plan.cat[b] + k - 1] = jnp.where(low_half, c[:, :HW], c[:, HW:])

    weights = wbuf[...].reshape(9 * LANES, 4 * CH)

    def dot(t, lo, hi):
        cur = xh_even if t % 2 == 0 else xh_odd
        taps = [cur[dc, cells_of(lo + dr - 1, hi + dr - 1)] for dr in range(3) for dc in range(3)]
        return jnp.dot(jnp.concatenate(taps, axis=1), weights, preferred_element_type=f32)

    def cells(t, lo, hi, gates):
        fi = jnp.tanh(gates[:, :LANES] * 0.5 + b_fi) * 0.5 + 0.5
        og = jnp.tanh(gates[:, LANES:] * scale + b_og) * scale + lift
        at = cells_of(lo, hi)
        prod = fi * lax.select(jnp.broadcast_to(low, og.shape), cbuf[at], og)
        c = prod + pltpu.roll(prod, CH, 1)
        h = (og * jnp.tanh(c))[:, :CH]
        if t == T - 1:
            cout[lo:hi] = c[:, :CH].reshape(hi - lo, W, CH)
        else:
            cbuf[at] = c
        for a, e in ((lo, min(hi, 0)), (max(lo, 0), min(hi, R)), (max(lo, R), hi)):
            if a >= e:
                continue
            part = h[(a - lo) * W:(e - lo) * W]
            if a >= 0 and e <= R:
                hout[t, a:e] = part.reshape(e - a, W, CH).astype(bf)
            if t < T - 1:
                emit(t + 1, a, e, masked(a, jnp.concatenate([part, x_rows(t + 1, a, e)], axis=1)))

    pending = []

    def piece(at, ahead=1):
        t, lo, hi = at
        while any(u == t - 1 and a <= hi and lo <= e for u, a, e, _ in pending):
            cells(*pending.pop(0))
        pending.append((*at, dot(*at)))
        flush(ahead)

    def flush(left=0):
        while len(pending) > left:
            cells(*pending.pop(0))

    def push_h(t0, t1, lo=0, hi=R):
        rows = slice(lo, hi)
        remote(hout.at[t0:t1, rows, theirs], hpeer.at[t0:t1, rows], s_os.at[0], s_or.at[0], peer).start()

    def push_c(lo, hi):
        remote(cout.at[lo:hi, theirs], cpeer.at[lo:hi], s_os.at[1], s_or.at[1], peer).start()

    with jax.named_scope('state_wait'):
        for c in [h_own, x_own[0], c_own]:
            c.wait()
        for c in [h_push, x_push[0], c_push]:
            c.wait_recv()
    c0 = flat(cst[...])
    cbuf[cells_of(0, R)] = jnp.concatenate([c0, c0], axis=1)
    pack_state(0, hst)
    pack_x(0, 1)
    start_border(0, 0, 1, 2)
    for lo, hi in cuts(0, R):
        emit(0, lo, hi, jnp.concatenate([flat(hst[lo:hi]).astype(f32), x_rows(0, lo, hi)], axis=1))

    for b, k in enumerate(plan.blocks):
        f = plan.first[b]
        last = b + 1 == NB

        def inner(o):
            if o == 0:
                got = [*cuts(k + 1, R - 1 - k), *cuts(1, k + 1), *cuts(R - 1 - k, R - 1)]
            else:
                got = cuts(o + 1, R - 1 - o)
                got = got[1:-1] + [got[0], got[-1]]
            return [(f + o, lo, hi) for lo, hi in got]

        steps = [inner(o) for o in range(k)]
        late = steps[-1][-LATE[b]:]
        steps[-1] = steps[-1][:-LATE[b]]
        for o, pieces in enumerate(steps):
            first = 0
            if o == 0 and b:
                for at in pieces[:3]:
                    piece(at, 9)
                flush(3)
                pack_state(b, hout.at[f - 1])
                start_border(b, 0, 1)
                first = 3
            if b == 0 and o in (0, 2):
                for at in pieces[:2]:
                    piece(at, 2)
                with jax.named_scope(f'x_wait{o}'):
                    wait_x(1 if o == 0 else 2)
                if o == 2:
                    pack_x(1, k)
                    start_border(0, 3)
                first = 2
            for at in pieces[first:]:
                piece(at)
        with jax.named_scope(f'mid{b}'):
            wait_border(b, *(range(3) if b == 0 else range(4)))
            wait_x(b + 3)
        if b:
            push_h(plan.first[b - 1], f)
        for at in late:
            piece(at, 2)
        for side in range(2):
            lo = -k if side == 0 else R
            h = flat(unpack(hr_ref[side, plan.hat[b]:plan.hat[b] + k])).astype(f32)
            emit(f, lo, lo + k, masked(lo, jnp.concatenate([h, x_rows(f, lo, lo + k)], axis=1)))
            lo = -(k - 1) if side == 0 else R
            packed = cr_ref[side, plan.cat[b]:plan.cat[b] + k - 1]
            both = jnp.concatenate([packed, pltpu.roll(packed, CH, 2)], axis=1)
            cbuf[cells_of(lo, lo + k - 1)] = flat(both)
        for o in range(k):
            m = k - 1 - o
            top, bottom = cuts(-m, o + 1), cuts(R - 1 - o, R + m)
            for i, (lo, hi) in enumerate(top + bottom):
                piece((f + o, lo, hi))
                if o == 0 and i == 0 and b == 0:
                    with jax.named_scope('x3b_wait'):
                        wait_border(0, 3)
            if o == 0 and not last:
                pack_x(f + k, f + k + plan.blocks[b + 1])
                start_border(b + 1, 2, 3)
            if o == 0 and last:
                push_h(T - 1, T, k, R - k)
                push_c(k, R - k)
            if last and o == k // 2:
                push_h(f, f + o)
            if last and o == k - 2:
                push_h(f + k // 2, f + o)
    flush()
    k = plan.blocks[-1]
    push_h(T - 2, T - 1)
    for lo, hi in ((0, k), (R - k, R)):
        push_h(T - 1, T, lo, hi)
        push_c(lo, hi)

    with jax.named_scope('end_wait'):
        for c in [h_push, c_push, *x_push]:
            c.wait_send()

        def wait_sends(side):
            for kind, ref in enumerate((hs_ref, cs_ref, xs_ref)):
                local(ref.at[side], ref.at[side], s_bs.at[kind, side]).wait()

        each_side(wait_sends)
        for sem in (s_os, s_or):
            local(hpeer, hpeer, sem.at[0]).wait()
            local(cpeer, cpeer, sem.at[1]).wait()


def store(hout, hpeer, cout, cpeer, h_all, c_final, sems):
    s = lax.axis_index("cols")
    HW = hpeer.shape[2]
    mine = pl.ds(pl.multiple_of(s * HW, HW), HW)
    copies = [pltpu.make_async_copy(hout.at[:, :, mine], h_all.at[:, s], sems.at[0]),
              pltpu.make_async_copy(hpeer, h_all.at[:, 1 - s], sems.at[1]),
              pltpu.make_async_copy(cout.at[:, mine], c_final.at[s], sems.at[2]),
              pltpu.make_async_copy(cpeer, c_final.at[1 - s], sems.at[3])]
    for c in copies:
        c.start()
    for c in copies:
        c.wait()


def run(blocks, n_rows, frames, w_x, w_h, gate_bias, h_init, c_init):
    T, S, R, HW = frames.shape[:4]
    W = 2 * HW
    plan = Plan(blocks, T, R, W)
    NB, PAD, G = len(blocks), plan.K, len(plan.groups)
    bf, f32 = jnp.bfloat16, jnp.float32
    vm, dma = pltpu.VMEM, pltpu.SemaphoreType.DMA
    hbm = pl.BlockSpec(memory_space=pltpu.HBM)
    vmem = pl.BlockSpec(memory_space=pltpu.VMEM)
    parts = pl.pallas_call(
        functools.partial(kernel, plan, n_rows),
        out_shape=(vm((T, R, W, CH), bf), vm((T, R, HW, CH), bf), vm((R, W, CH), f32), vm((R, HW, CH), f32)),
        in_specs=[hbm] * 6,
        out_specs=(vmem,) * 4,
        scratch_shapes=[
            vm((1, 4 * CH), f32), vm((R, HW, CH), bf), vm((R, HW, CH), f32), vm((plan.groups[1][1], R, HW, CH), bf),
            vm((T, R, W, CH), bf), vm((R, W, CH), bf), vm((R, W, CH), f32),
            vm((3, (R + 2 * PAD) * W, LANES), bf), vm((3, (R + 2 * PAD) * W, LANES), bf),
            vm(((R + 2 * PAD) * W, LANES), f32), vm((RING, W + 16, LANES), f32), vm((3, 3, 2, CH, 4 * CH), bf),
            vm((2, plan.xat[-1], HW, LANES), bf), vm((2, plan.xat[-1], HW, LANES), bf),
            vm((2, plan.hat[-1], HW, LANES), bf), vm((2, plan.hat[-1], HW, LANES), bf),
            vm((2, plan.cat[-1], HW, LANES), f32), vm((2, plan.cat[-1], HW, LANES), f32),
            dma((3,)), dma((6,)), dma((2,)), dma((2,)), dma((G,)), dma((G,)), dma((G,)),
            dma((4, 2, NB)), dma((3, 2)), dma((2,)), dma((2,))],
        compiler_params=pltpu.CompilerParams(collective_id=0, has_side_effects=True, vmem_limit_bytes=46 * 2**20),
    )(frames, w_x, w_h, gate_bias.reshape(1, -1), h_init, c_init)
    return pl.pallas_call(
        store,
        out_shape=(jax.ShapeDtypeStruct(frames.shape, bf), jax.ShapeDtypeStruct(c_init.shape, f32)),
        in_specs=[vmem] * 4,
        out_specs=(hbm, hbm),
        scratch_shapes=[dma((4,))],
        compiler_params=pltpu.CompilerParams(vmem_limit_bytes=2**20),
    )(*[pltpu.with_memory_space_constraint(a, pltpu.VMEM) for a in parts])


def solution(mesh, K=None):
    n_rows = mesh.shape["rows"]
    frame_spec = P(None, "batch", "rows", "cols", None)
    state_spec = P("batch", "rows", "cols", None)
    blocks = BLOCKS if K is None else K
    return jax.shard_map(functools.partial(run, blocks, n_rows), mesh=mesh,
                         in_specs=(frame_spec, P(), P(), P(), state_spec, state_spec),
                         out_specs=(frame_spec, state_spec), check_vma=False)
```

```python
import functools

import jax
import jax.numpy as jnp
from jax import lax
from jax.experimental import pallas as pl
from jax.experimental.pallas import tpu as pltpu
from jax.sharding import PartitionSpec as P

MESH = pl.DeviceIdType.MESH
CH = 64
LANES = 128
PIECE = 4
RING = 8
BLOCKS = (5, 5, 6)
LATE = (5, 5, 5)
BORDER = 6
FAR = 16


def cuts(lo, hi, size=PIECE):
    n = max(1, (hi - lo) // size)
    edges = [lo + i * size for i in range(n)] + [hi]
    return list(zip(edges[:-1], edges[1:]))


class Plan:
    def __init__(self, blocks, T, R, W):
        assert sum(blocks) == T
        self.blocks, self.T, self.R, self.W, self.HW = blocks, T, R, W, W // 2
        self.K = max(blocks)
        self.first = [sum(blocks[:b]) for b in range(len(blocks))]
        self.of = [(b, o) for b, k in enumerate(blocks) for o in range(k)]
        self.xrows = [blocks[b] - o for b, o in self.of]
        self.xat = [sum(self.xrows[:t]) for t in range(T + 1)]
        self.hat = [sum(blocks[:b]) for b in range(len(blocks) + 1)]
        self.cat = [sum(k - 1 for k in blocks[:b]) for b in range(len(blocks) + 1)]
        ends = [0, 1, 3] + [min(f + k + 1, T) for f, k in zip(self.first, blocks)]
        self.groups = [(a, e) for a, e in zip(ends[:-1], ends[1:]) if e > a]


def kernel(plan, n_rows, frames, w_x, w_h, bias_in, h_init, c_init, hout, hpeer, cout, cpeer,
           bias, hgo, cgo, xgo, xin, hst, cst, xh_even, xh_odd, cbuf, shift, wbuf,
           xs_ref, xr_ref, hs_ref, hr_ref, cs_ref, cr_ref,
           s_w, s_i, s_ir, s_is, s_x, s_xr, s_xs, s_b, s_bs, s_or, s_os, here_sem):
    T, R, W, HW = plan.T, plan.R, plan.W, plan.HW
    PAD = plan.K
    NB = len(plan.blocks)
    s = lax.axis_index("cols")
    n = lax.axis_index("rows")
    p = 1 - s
    mine = pl.ds(pl.multiple_of(s * HW, HW), HW)
    theirs = pl.ds(pl.multiple_of(p * HW, HW), HW)
    has_up, has_dn = n > 0, n < n_rows - 1
    bf, f32 = jnp.bfloat16, jnp.float32

    def local(src, dst, sem):
        return pltpu.make_async_copy(src, dst, sem)

    def remote(src, dst, ssem, rsem, dev):
        return pltpu.make_async_remote_copy(
            src_ref=src, dst_ref=dst, send_sem=ssem, recv_sem=rsem, device_id=dev, device_id_type=MESH)

    peer = {"cols": p}
    side_dev = [{"rows": n - 1}, {"rows": n + 1}]
    side_ok = [has_up, has_dn]

    def each_side(do):
        for side in range(2):
            @pl.when(side_ok[side])
            def _():
                do(side)

    barrier = pltpu.get_barrier_semaphore()

    def signal(dev):
        pl.semaphore_signal(barrier, inc=1, device_id=dev, device_id_type=MESH)

    signal(peer)

    @pl.when(has_up)
    def _():
        signal(side_dev[0])


    h_own = local(h_init.at[s], hst.at[:, mine], s_i.at[0])
    c_own = local(c_init.at[s], cst.at[:, mine], s_i.at[1])
    x_own = [local(frames.at[a:e, s], xin.at[a:e, :, mine], s_x.at[g]) for g, (a, e) in enumerate(plan.groups)]
    h_got = local(h_init.at[p], hgo, s_i.at[2])
    c_got = local(c_init.at[p], cgo, s_i.at[3])
    x_got = [local(frames.at[a:e, p], xgo.at[a:e], s_i.at[4 + g]) for g, (a, e) in enumerate(plan.groups[:2])]
    w_copies = [local(w_h, wbuf.at[:, :, 0], s_w.at[0]), local(w_x, wbuf.at[:, :, 1], s_w.at[1]),
                local(bias_in, bias, s_w.at[2])]
    for c in [h_got, x_got[0], c_got, h_own, x_own[0], c_own, *w_copies, x_got[1], *x_own[1:]]:
        c.start()
    with jax.named_scope('barrier'):
        pl.semaphore_wait(barrier, 1 + has_dn.astype(jnp.int32))

    @pl.when(has_dn)
    def _():
        pl.semaphore_signal(here_sem, inc=1, device_id=side_dev[1], device_id_type=MESH)


    h_push = remote(hgo, hst.at[:, mine], s_is.at[0], s_ir.at[0], peer)
    c_push = remote(cgo, cst.at[:, mine], s_is.at[1], s_ir.at[1], peer)
    x_push = [remote((xgo if g < 2 else frames.at[:, p]).at[a:e], xin.at[a:e, :, mine], s_xs.at[g], s_xr.at[g], peer)
              for g, (a, e) in enumerate(plan.groups)]
    with jax.named_scope('got_wait'):
        for got, push in [(h_got, h_push), (x_got[0], x_push[0]), (c_got, c_push), (x_got[1], x_push[1])]:
            got.wait()
            push.start()
    for push in x_push[2:]:
        push.start()

    shift[...] = jnp.zeros_like(shift)
    low = lax.broadcasted_iota(jnp.int32, (1, LANES), 1) < CH
    low_half = low_row = low
    turn = [0]
    scale = jnp.where(low_row, 0.5, 1.0)
    lift = jnp.where(low_row, 0.5, 0.0)

    with jax.named_scope('w_wait'):
        for c in w_copies:
            c.wait()
    for dr in range(3):
        for dc in range(3):
            for half in range(2):
                tile = wbuf[dr, dc, half, :, 0:LANES]
                wbuf[dr, dc, half, :, 0:LANES] = jnp.concatenate([tile[:, CH:], tile[:, :CH]], axis=1)
    b_first = bias[:, 0:LANES]
    b_fi = jnp.concatenate([b_first[:, CH:], b_first[:, :CH]], axis=1) * 0.5
    b_og = bias[:, LANES:] * scale

    def pack(v):
        return jnp.concatenate([v[:, :HW], v[:, HW:]], axis=2)

    def unpack(v):
        return jnp.concatenate([v[:, :, :CH], v[:, :, CH:]], axis=1)

    def masked(r, v):
        if 0 <= r < R:
            return v
        return lax.select(jnp.broadcast_to(has_up if r < 0 else has_dn, v.shape), v, jnp.zeros_like(v))

    def emit(t, lo, hi, hx):
        nxt = xh_even if t % 2 == 0 else xh_odd
        at, to = slot(lo, hi), cells_of(lo, hi)
        shift[at, 8:8 + W, :] = hx.reshape(hi - lo, W, LANES)
        nxt[1, to] = hx.astype(bf)
        nxt[0, to] = shift[at, 7:7 + W, :].reshape(hx.shape).astype(bf)
        nxt[2, to] = shift[at, 9:9 + W, :].reshape(hx.shape).astype(bf)

    def cells_of(lo, hi):
        return slice((lo + PAD) * W, (hi + PAD) * W)

    def slot(lo, hi):
        if turn[0] + hi - lo > RING:
            turn[0] = 0
        turn[0] += hi - lo
        return slice(turn[0] - (hi - lo), turn[0])

    def flat(v):
        return v.reshape(-1, v.shape[-1])

    def x_rows(t, lo, hi):
        if lo >= 0 and hi <= R:
            return flat(xin[t, lo:hi]).astype(f32)
        side, i = (0, lo + plan.xrows[t]) if lo < 0 else (1, lo - R)
        return flat(unpack(xr_ref[side, plan.xat[t] + i:plan.xat[t] + i + hi - lo])).astype(f32)

    def wait_x(g):
        if g < len(plan.groups):
            x_own[g].wait()
            x_push[g].wait_recv()

    def border(b, kind, side):
        k, f = plan.blocks[b], plan.first[b]
        src, dst, at, end = [
            (hs_ref, hr_ref, plan.hat[b], plan.hat[b + 1]),
            (cs_ref, cr_ref, plan.cat[b], plan.cat[b + 1]),
            (xs_ref, xr_ref, plan.xat[f], plan.xat[f + 1]),
            (xs_ref, xr_ref, plan.xat[f + 1], plan.xat[f + 3]),
            (xs_ref, xr_ref, plan.xat[f + 3], plan.xat[f + k])][kind]
        return remote(src.at[side, at:end], dst.at[1 - side, at:end],
                      s_bs.at[min(kind, 2), side], s_b.at[kind, 1 - side, b], side_dev[side])

    def pack_x(t0, t1):
        for side in range(2):
            for t in range(t0, t1):
                m = plan.xrows[t]
                lo = 0 if side == 0 else R - m
                xs_ref[side, plan.xat[t]:plan.xat[t] + m] = pack(xin[t, lo:lo + m])

    def start_border(b, *kinds):
        each_side(lambda side: [border(b, kind, side).start() for kind in kinds])

    far = lax.rem(n, FAR) == 0

    def start_first(side, late, *kinds):
        ok = has_dn if side else jnp.logical_and(has_up, far if late else jnp.logical_not(far))

        @pl.when(ok)
        def _():
            if not side and 0 in kinds:
                pl.semaphore_wait(here_sem, 1)
            for kind in kinds:
                border(0, kind, side).start()

    def wait_border(b, *kinds):
        each_side(lambda side: [border(b, kind, 1 - side).wait_recv() for kind in kinds])

    def pack_state(b, h_rows):
        k = plan.blocks[b]
        for side in range(2):
            lo = 0 if side == 0 else R - k
            hs_ref[side, plan.hat[b]:plan.hat[b] + k] = pack(h_rows[lo:lo + k])
            lo = 0 if side == 0 else R - (k - 1)
            c = cbuf[cells_of(lo, lo + k - 1)].reshape(k - 1, W, LANES)
            cs_ref[side, plan.cat[b]:plan.cat[b] + k - 1] = jnp.where(low_half, c[:, :HW], c[:, HW:])

    weights = wbuf[...].reshape(9 * LANES, 4 * CH)

    def dot(t, lo, hi):
        cur = xh_even if t % 2 == 0 else xh_odd
        taps = [cur[dc, cells_of(lo + dr - 1, hi + dr - 1)] for dr in range(3) for dc in range(3)]
        return jnp.dot(jnp.concatenate(taps, axis=1), weights, preferred_element_type=f32)

    def cells(t, lo, hi, gates):
        fi = jnp.tanh(gates[:, :LANES] * 0.5 + b_fi) * 0.5 + 0.5
        og = jnp.tanh(gates[:, LANES:] * scale + b_og) * scale + lift
        at = cells_of(lo, hi)
        prod = fi * lax.select(jnp.broadcast_to(low, og.shape), cbuf[at], og)
        c = prod + pltpu.roll(prod, CH, 1)
        h = (og * jnp.tanh(c))[:, :CH]
        if t == T - 1:
            cout[lo:hi] = c[:, :CH].reshape(hi - lo, W, CH)
        else:
            cbuf[at] = c
        for a, e in ((lo, min(hi, 0)), (max(lo, 0), min(hi, R)), (max(lo, R), hi)):
            if a >= e:
                continue
            part = h[(a - lo) * W:(e - lo) * W]
            if a >= 0 and e <= R:
                hout[t, a:e] = part.reshape(e - a, W, CH).astype(bf)
            if t < T - 1:
                emit(t + 1, a, e, masked(a, jnp.concatenate([part, x_rows(t + 1, a, e)], axis=1)))

    pending = []

    def piece(at, ahead=1):
        t, lo, hi = at
        while any(u == t - 1 and a <= hi and lo <= e for u, a, e, _ in pending):
            cells(*pending.pop(0))
        pending.append((*at, dot(*at)))
        flush(ahead)

    def flush(left=0):
        while len(pending) > left:
            cells(*pending.pop(0))

    def push_h(t0, t1, lo=0, hi=R):
        rows = slice(lo, hi)
        remote(hout.at[t0:t1, rows, theirs], hpeer.at[t0:t1, rows], s_os.at[0], s_or.at[0], peer).start()

    def push_c(lo, hi):
        remote(cout.at[lo:hi, theirs], cpeer.at[lo:hi], s_os.at[1], s_or.at[1], peer).start()

    with jax.named_scope('state_wait'):
        for c in [h_own, x_own[0], c_own]:
            c.wait()
        for c in [h_push, x_push[0], c_push]:
            c.wait_recv()
    c0 = flat(cst[...])
    cbuf[cells_of(0, R)] = jnp.concatenate([c0, c0], axis=1)
    pack_state(0, hst)
    pack_x(0, 1)
    start_first(1, False, 0, 1, 2)
    start_first(0, False, 0, 1, 2)
    for lo, hi in cuts(0, R):
        emit(0, lo, hi, jnp.concatenate([flat(hst[lo:hi]).astype(f32), x_rows(0, lo, hi)], axis=1))

    for b, k in enumerate(plan.blocks):
        f = plan.first[b]
        last = b + 1 == NB

        def inner(o):
            if o == 0:
                got = [*cuts(k + 1, R - 1 - k), *cuts(1, k + 1), *cuts(R - 1 - k, R - 1)]
            else:
                got = cuts(o + 1, R - 1 - o)
                got = got[1:-1] + [got[0], got[-1]]
            return [(f + o, lo, hi) for lo, hi in got]

        steps = [inner(o) for o in range(k)]
        late = steps[-1][-LATE[b]:]
        steps[-1] = steps[-1][:-LATE[b]]
        for o, pieces in enumerate(steps):
            first = 0
            if o == 0 and b:
                for at in pieces[:3]:
                    piece(at, 9)
                flush(3)
                pack_state(b, hout.at[f - 1])
                start_border(b, 0, 1)
                first = 3
            if b == 0 and o in (0, 2):
                for at in pieces[:2]:
                    piece(at, 2)
                with jax.named_scope(f'x_wait{o}'):
                    wait_x(1 if o == 0 else 2)
                pack_x(*((1, 3) if o == 0 else (3, k)))
                kind = 3 if o == 0 else 4
                start_first(1, False, kind)
                start_first(0, False, kind)
                if o == 2:
                    start_first(0, True, kind)
                first = 2
            for at in pieces[first:]:
                piece(at)
            if b == 0 and o == 0:
                start_first(0, True, 0, 1, 2, 3)
        with jax.named_scope(f'mid{b}'):
            wait_border(b, *(range(3) if b == 0 else range(5)))
            wait_x(b + 3)
        if b:
            push_h(plan.first[b - 1], f)
        piece(late.pop(0), 2)
        for side in range(2):
            lo = -k if side == 0 else R
            h = flat(unpack(hr_ref[side, plan.hat[b]:plan.hat[b] + k])).astype(f32)
            emit(f, lo, lo + k, masked(lo, jnp.concatenate([h, x_rows(f, lo, lo + k)], axis=1)))
            lo = -(k - 1) if side == 0 else R
            packed = cr_ref[side, plan.cat[b]:plan.cat[b] + k - 1]
            both = jnp.concatenate([packed, pltpu.roll(packed, CH, 2)], axis=1)
            cbuf[cells_of(lo, lo + k - 1)] = flat(both)
        for o in range(k):
            m = k - 1 - o
            top, bottom = cuts(-m, o + 1, BORDER), cuts(R - 1 - o, R + m, BORDER)
            for i, (lo, hi) in enumerate(top):
                piece((f + o, lo, hi))
                if i == 0 and b == 0 and o in (0, 2):
                    wait_border(0, 3 if o == 0 else 4)
            if late:
                piece(late.pop(0))
            for lo, hi in bottom:
                piece((f + o, lo, hi))
            if o == 0 and not last:
                pack_x(f + k, f + k + plan.blocks[b + 1])
                start_border(b + 1, 2, 3, 4)
            if last and o == k // 2:
                push_h(f, f + o)
            if last and o == k - 2:
                push_h(f + k // 2, f + o)
            if last and o == k - 1:
                push_h(T - 1, T, k, R - k)
                push_c(k, R - k)
    flush()
    k = plan.blocks[-1]
    push_h(T - 2, T - 1)
    for lo, hi in ((0, k), (R - k, R)):
        push_h(T - 1, T, lo, hi)
        push_c(lo, hi)

    with jax.named_scope('end_wait'):
        for c in [h_push, c_push, *x_push]:
            c.wait_send()

        def wait_sends(side):
            for kind, ref in enumerate((hs_ref, cs_ref, xs_ref)):
                local(ref.at[side], ref.at[side], s_bs.at[kind, side]).wait()

        each_side(wait_sends)
        for sem in (s_os, s_or):
            local(hpeer, hpeer, sem.at[0]).wait()
            local(cpeer, cpeer, sem.at[1]).wait()


def store(hout, hpeer, cout, cpeer, h_all, c_final, sems):
    s = lax.axis_index("cols")
    HW = hpeer.shape[2]
    mine = pl.ds(pl.multiple_of(s * HW, HW), HW)
    copies = [pltpu.make_async_copy(hout.at[:, :, mine], h_all.at[:, s], sems.at[0]),
              pltpu.make_async_copy(hpeer, h_all.at[:, 1 - s], sems.at[1]),
              pltpu.make_async_copy(cout.at[:, mine], c_final.at[s], sems.at[2]),
              pltpu.make_async_copy(cpeer, c_final.at[1 - s], sems.at[3])]
    for c in copies:
        c.start()
    for c in copies:
        c.wait()


def run(blocks, n_rows, frames, w_x, w_h, gate_bias, h_init, c_init):
    T, S, R, HW = frames.shape[:4]
    W = 2 * HW
    plan = Plan(blocks, T, R, W)
    NB, PAD, G = len(blocks), plan.K, len(plan.groups)
    bf, f32 = jnp.bfloat16, jnp.float32
    vm, dma = pltpu.VMEM, pltpu.SemaphoreType.DMA
    hbm = pl.BlockSpec(memory_space=pltpu.HBM)
    vmem = pl.BlockSpec(memory_space=pltpu.VMEM)
    parts = pl.pallas_call(
        functools.partial(kernel, plan, n_rows),
        out_shape=(vm((T, R, W, CH), bf), vm((T, R, HW, CH), bf), vm((R, W, CH), f32), vm((R, HW, CH), f32)),
        in_specs=[hbm] * 6,
        out_specs=(vmem,) * 4,
        scratch_shapes=[
            vm((1, 4 * CH), f32), vm((R, HW, CH), bf), vm((R, HW, CH), f32), vm((plan.groups[1][1], R, HW, CH), bf),
            vm((T, R, W, CH), bf), vm((R, W, CH), bf), vm((R, W, CH), f32),
            vm((3, (R + 2 * PAD) * W, LANES), bf), vm((3, (R + 2 * PAD) * W, LANES), bf),
            vm(((R + 2 * PAD) * W, LANES), f32), vm((RING, W + 16, LANES), f32), vm((3, 3, 2, CH, 4 * CH), bf),
            vm((2, plan.xat[-1], HW, LANES), bf), vm((2, plan.xat[-1], HW, LANES), bf),
            vm((2, plan.hat[-1], HW, LANES), bf), vm((2, plan.hat[-1], HW, LANES), bf),
            vm((2, plan.cat[-1], HW, LANES), f32), vm((2, plan.cat[-1], HW, LANES), f32),
            dma((3,)), dma((6,)), dma((2,)), dma((2,)), dma((G,)), dma((G,)), dma((G,)),
            dma((5, 2, NB)), dma((3, 2)), dma((2,)), dma((2,)), pltpu.SemaphoreType.REGULAR],
        compiler_params=pltpu.CompilerParams(collective_id=0, has_side_effects=True, vmem_limit_bytes=46 * 2**20),
    )(frames, w_x, w_h, gate_bias.reshape(1, -1), h_init, c_init)
    return pl.pallas_call(
        store,
        out_shape=(jax.ShapeDtypeStruct(frames.shape, bf), jax.ShapeDtypeStruct(c_init.shape, f32)),
        in_specs=[vmem] * 4,
        out_specs=(hbm, hbm),
        scratch_shapes=[dma((4,))],
        compiler_params=pltpu.CompilerParams(vmem_limit_bytes=2**20),
    )(*[pltpu.with_memory_space_constraint(a, pltpu.VMEM) for a in parts])


def solution(mesh, K=None):
    n_rows = mesh.shape["rows"]
    frame_spec = P(None, "batch", "rows", "cols", None)
    state_spec = P("batch", "rows", "cols", None)
    blocks = BLOCKS if K is None else K
    return jax.shard_map(functools.partial(run, blocks, n_rows), mesh=mesh,
                         in_specs=(frame_spec, P(), P(), P(), state_spec, state_spec),
                         out_specs=(frame_spec, state_spec), check_vma=False)
```

```python
import functools

import jax
import jax.numpy as jnp
from jax import lax
from jax.experimental import pallas as pl
from jax.experimental.pallas import tpu as pltpu
from jax.sharding import PartitionSpec as P

MESH = pl.DeviceIdType.MESH
CH = 64
LANES = 128
COLS = 8
PIECE = 4
RING = 8
BLOCKS = (5, 5, 6)
LATE = (5, 5, 5)
BORDER = 6
FAR = 16


def cuts(lo, hi, size=PIECE):
    n = max(1, (hi - lo) // size)
    edges = [lo + i * size for i in range(n)] + [hi]
    return list(zip(edges[:-1], edges[1:]))


class Plan:
    def __init__(self, blocks, T, R, W):
        assert sum(blocks) == T
        self.blocks, self.T, self.R, self.W, self.HW, self.HG = blocks, T, R, W, W // 2, W // 2 // COLS
        self.K = max(blocks)
        self.first = [sum(blocks[:b]) for b in range(len(blocks))]
        self.of = [(b, o) for b, k in enumerate(blocks) for o in range(k)]
        self.xrows = [blocks[b] - o for b, o in self.of]
        self.xat = [sum(self.xrows[:t]) for t in range(T + 1)]
        self.hat = [sum(blocks[:b]) for b in range(len(blocks) + 1)]
        self.cat = [sum(k - 1 for k in blocks[:b]) for b in range(len(blocks) + 1)]
        ends = [0, 1, 3, blocks[0] + 1, T]
        self.groups = [(a, e) for a, e in zip(ends[:-1], ends[1:]) if e > a]


def kernel(plan, n_rows, frames, w_x, w_h, bias_in, h_init, c_init, hout, hpeer, cout, cpeer,
           bias, hgo, cgo, xgo, xin, hst, cst, xh_even, xh_odd, cbuf, shift, wbuf,
           xs_ref, xr_ref, hs_ref, hr_ref, cs_ref, cr_ref,
           s_w, s_i, s_ir, s_is, s_x, s_xr, s_xs, s_b, s_bs, s_or, s_os, here_sem):
    T, R, W, HW, HG = plan.T, plan.R, plan.W, plan.HW, plan.HG
    PAD = plan.K
    NB = len(plan.blocks)
    s = lax.axis_index("cols")
    n = lax.axis_index("rows")
    p = 1 - s
    mine, theirs = pl.ds(s * HG, HG), pl.ds(p * HG, HG)
    mine_c, theirs_c = [pl.ds(pl.multiple_of(i * HW, HW), HW) for i in (s, p)]
    has_up, has_dn = n > 0, n < n_rows - 1
    bf, f32 = jnp.bfloat16, jnp.float32

    def local(src, dst, sem):
        return pltpu.make_async_copy(src, dst, sem)

    def remote(src, dst, ssem, rsem, dev):
        return pltpu.make_async_remote_copy(
            src_ref=src, dst_ref=dst, send_sem=ssem, recv_sem=rsem, device_id=dev, device_id_type=MESH)

    peer = {"cols": p}
    side_dev = [{"rows": n - 1}, {"rows": n + 1}]
    side_ok = [has_up, has_dn]

    def each_side(do):
        for side in range(2):
            @pl.when(side_ok[side])
            def _():
                do(side)

    barrier = pltpu.get_barrier_semaphore()

    def signal(dev):
        pl.semaphore_signal(barrier, inc=1, device_id=dev, device_id_type=MESH)

    signal(peer)

    @pl.when(has_up)
    def _():
        signal(side_dev[0])


    h_own = local(h_init.at[s], hst.at[:, mine], s_i.at[0])
    c_own = local(c_init.at[s], cst.at[:, mine_c], s_i.at[1])
    x_own = [local(frames.at[a:e, s], xin.at[a:e, :, mine], s_x.at[g]) for g, (a, e) in enumerate(plan.groups)]
    h_got = local(h_init.at[p], hgo, s_i.at[2])
    c_got = local(c_init.at[p], cgo, s_i.at[3])
    x_got = [local(frames.at[a:e, p], xgo.at[a:e], s_i.at[4 + g]) for g, (a, e) in enumerate(plan.groups[:2])]
    w_copies = [local(w_h, wbuf.at[0:9, 0], s_w.at[0]), local(w_x, wbuf.at[0:9, 1], s_w.at[1]),
                local(bias_in, bias, s_w.at[2])]
    for c in [h_got, x_got[0], c_got, h_own, x_own[0], c_own, *w_copies, x_got[1], *x_own[1:]]:
        c.start()
    with jax.named_scope('barrier'):
        pl.semaphore_wait(barrier, 1 + has_dn.astype(jnp.int32))

    @pl.when(has_dn)
    def _():
        pl.semaphore_signal(here_sem, inc=1, device_id=side_dev[1], device_id_type=MESH)


    h_push = remote(hgo, hst.at[:, mine], s_is.at[0], s_ir.at[0], peer)
    c_push = remote(cgo, cst.at[:, mine_c], s_is.at[1], s_ir.at[1], peer)
    x_push = [remote((xgo if g < 2 else frames.at[:, p]).at[a:e], xin.at[a:e, :, mine], s_xs.at[g], s_xr.at[g], peer)
              for g, (a, e) in enumerate(plan.groups)]
    with jax.named_scope('got_wait'):
        for got, push in [(h_got, h_push), (x_got[0], x_push[0]), (c_got, c_push), (x_got[1], x_push[1])]:
            got.wait()
            push.start()
    for push in x_push[2:]:
        push.start()

    shift[...] = jnp.zeros_like(shift)
    low = lax.broadcasted_iota(jnp.int32, (1, LANES), 1) < CH
    low_half = low_row = low
    turn = [0]
    scale = jnp.where(low_row, 0.5, 1.0)
    lift = jnp.where(low_row, 0.5, 0.0)

    with jax.named_scope('w_wait'):
        for c in w_copies:
            c.wait()
    for tap in range(9):
        for half in range(2):
            tile = wbuf[tap, half, :, 0:LANES]
            wbuf[tap, half, :, 0:LANES] = jnp.concatenate([tile[:, CH:], tile[:, :CH]], axis=1)
    b_all = bias[...]
    rest = jnp.concatenate([b_all[:, CH:LANES], b_all[:, :CH], b_all[:, LANES:]], axis=1)
    row = lax.broadcasted_iota(jnp.int32, (CH, 4 * CH), 0)
    rows = jnp.zeros((CH, 4 * CH), f32)
    for i in range(3):
        top = (rest * (1 - 2.0 ** -8)).astype(bf).astype(f32) if i == 0 else rest.astype(bf).astype(f32)
        rows = jnp.where(row == i, top, rows)
        rest = rest - top
    wbuf[9, 0] = rows.astype(bf)
    wbuf[9, 1] = jnp.zeros((CH, 4 * CH), bf)
    ones = jnp.where(lax.broadcasted_iota(jnp.int32, (1, LANES), 1) < 3, 1.0, 0.0).astype(bf)

    def pack(v):
        return jnp.concatenate([v[:, :HG], v[:, HG:]], axis=3)

    def unpack(v):
        return jnp.concatenate([v[..., :CH], v[..., CH:]], axis=1)

    def masked(r, v):
        if 0 <= r < R:
            return v
        return lax.select(jnp.broadcast_to(has_up if r < 0 else has_dn, v.shape), v, jnp.zeros_like(v))

    def emit(t, lo, hi, hx):
        nxt = xh_even if t % 2 == 0 else xh_odd
        at, to = slot(lo, hi), cells_of(lo, hi)
        shift[at, 8:8 + W, :] = hx.reshape(hi - lo, W, LANES)
        nxt[1, to] = hx.astype(bf)
        nxt[0, to] = shift[at, 7:7 + W, :].reshape(hx.shape).astype(bf)
        nxt[2, to] = shift[at, 9:9 + W, :].reshape(hx.shape).astype(bf)

    def cells_of(lo, hi):
        return slice((lo + PAD) * W, (hi + PAD) * W)

    def slot(lo, hi):
        if turn[0] + hi - lo > RING:
            turn[0] = 0
        turn[0] += hi - lo
        return slice(turn[0] - (hi - lo), turn[0])

    def flat(v):
        return v.reshape(-1, v.shape[-1])

    def x_rows(t, lo, hi):
        if lo >= 0 and hi <= R:
            return flat(xin[t, lo:hi].astype(f32))
        side, i = (0, lo + plan.xrows[t]) if lo < 0 else (1, lo - R)
        return flat(unpack(xr_ref[side, plan.xat[t] + i:plan.xat[t] + i + hi - lo].astype(f32)))

    def wait_x(g):
        if g < len(plan.groups):
            x_own[g].wait()
            x_push[g].wait_recv()

    def border(b, kind, side):
        k, f = plan.blocks[b], plan.first[b]
        src, dst, at, end = [
            (hs_ref, hr_ref, plan.hat[b], plan.hat[b + 1]),
            (cs_ref, cr_ref, plan.cat[b], plan.cat[b + 1]),
            (xs_ref, xr_ref, plan.xat[f], plan.xat[f + 1]),
            (xs_ref, xr_ref, plan.xat[f + 1], plan.xat[f + 3]),
            (xs_ref, xr_ref, plan.xat[f + 3], plan.xat[f + k])][kind]
        return remote(src.at[side, at:end], dst.at[1 - side, at:end],
                      s_bs.at[min(kind, 2), side], s_b.at[kind, 1 - side, b], side_dev[side])

    def pack_x(t0, t1):
        for side in range(2):
            for t in range(t0, t1):
                m = plan.xrows[t]
                lo = 0 if side == 0 else R - m
                xs_ref[side, plan.xat[t]:plan.xat[t] + m] = pack(xin[t, lo:lo + m])

    def start_border(b, *kinds):
        each_side(lambda side: [border(b, kind, side).start() for kind in kinds])

    far = lax.rem(n, FAR) == 0

    def start_first(side, late, *kinds):
        ok = has_dn if side else jnp.logical_and(has_up, far if late else jnp.logical_not(far))

        @pl.when(ok)
        def _():
            if not side and 0 in kinds:
                pl.semaphore_wait(here_sem, 1)
            for kind in kinds:
                border(0, kind, side).start()

    def wait_border(b, *kinds):
        each_side(lambda side: [border(b, kind, 1 - side).wait_recv() for kind in kinds])

    def pack_state(b, h_rows):
        k = plan.blocks[b]
        for side in range(2):
            lo = 0 if side == 0 else R - k
            hs_ref[side, plan.hat[b]:plan.hat[b] + k] = pack(h_rows[lo:lo + k])
            lo = 0 if side == 0 else R - (k - 1)
            c = cbuf[cells_of(lo, lo + k - 1)].reshape(k - 1, W, LANES)
            cs_ref[side, plan.cat[b]:plan.cat[b] + k - 1] = jnp.where(low_half, c[:, :HW], c[:, HW:])

    weights = wbuf[...].reshape(10 * LANES, 4 * CH)

    def dot(t, lo, hi):
        cur = xh_even if t % 2 == 0 else xh_odd
        taps = [cur[dc, cells_of(lo + dr - 1, hi + dr - 1)] for dr in range(3) for dc in range(3)]
        taps.append(jnp.broadcast_to(ones, taps[0].shape))
        return jnp.dot(jnp.concatenate(taps, axis=1), weights, preferred_element_type=f32)

    def cells(t, lo, hi, gates):
        fi = jnp.tanh(gates[:, :LANES] * 0.5) * 0.5 + 0.5
        og = jnp.tanh(gates[:, LANES:] * scale) * scale + lift
        at = cells_of(lo, hi)
        prod = fi * lax.select(jnp.broadcast_to(low, og.shape), cbuf[at], og)
        c = prod + pltpu.roll(prod, CH, 1)
        h = (og * jnp.tanh(c))[:, :CH]
        if t == T - 1:
            cout[lo:hi] = c[:, :CH].reshape(hi - lo, W, CH)
        else:
            cbuf[at] = c
        for a, e in ((lo, min(hi, 0)), (max(lo, 0), min(hi, R)), (max(lo, R), hi)):
            if a >= e:
                continue
            part = h[(a - lo) * W:(e - lo) * W]
            if a >= 0 and e <= R:
                hout[t, a:e] = part.reshape(e - a, 2 * HG, COLS, CH).astype(bf)
            if t < T - 1:
                emit(t + 1, a, e, masked(a, jnp.concatenate([part, x_rows(t + 1, a, e)], axis=1)))

    pending = []

    def piece(at, ahead=1):
        t, lo, hi = at
        while any(u == t - 1 and a <= hi and lo <= e for u, a, e, _ in pending):
            cells(*pending.pop(0))
        pending.append((*at, dot(*at)))
        flush(ahead)

    def flush(left=0):
        while len(pending) > left:
            cells(*pending.pop(0))

    def push_h(t0, t1, lo=0, hi=R):
        rows = slice(lo, hi)
        remote(hout.at[t0:t1, rows, theirs], hpeer.at[t0:t1, rows], s_os.at[0], s_or.at[0], peer).start()

    def push_c(lo, hi):
        remote(cout.at[lo:hi, theirs_c], cpeer.at[lo:hi], s_os.at[1], s_or.at[1], peer).start()

    with jax.named_scope('state_wait'):
        for c in [h_own, x_own[0], c_own]:
            c.wait()
        for c in [h_push, x_push[0], c_push]:
            c.wait_recv()
    c0 = flat(cst[...])
    cbuf[cells_of(0, R)] = jnp.concatenate([c0, c0], axis=1)
    pack_state(0, hst)
    pack_x(0, 1)
    start_first(1, False, 0, 1, 2)
    start_first(0, False, 0, 1, 2)
    for lo, hi in cuts(0, R):
        emit(0, lo, hi, jnp.concatenate([flat(hst[lo:hi].astype(f32)), x_rows(0, lo, hi)], axis=1))

    for b, k in enumerate(plan.blocks):
        f = plan.first[b]
        last = b + 1 == NB

        def inner(o):
            if o == 0:
                got = [*cuts(k + 1, R - 1 - k), *cuts(1, k + 1), *cuts(R - 1 - k, R - 1)]
            else:
                got = cuts(o + 1, R - 1 - o)
                got = got[1:-1] + [got[0], got[-1]]
            return [(f + o, lo, hi) for lo, hi in got]

        steps = [inner(o) for o in range(k)]
        late = steps[-1][-LATE[b]:]
        steps[-1] = steps[-1][:-LATE[b]]
        for o, pieces in enumerate(steps):
            first = 0
            if o == 0 and b:
                for at in pieces[:3]:
                    piece(at, 9)
                flush(3)
                pack_state(b, hout.at[f - 1])
                start_border(b, 0, 1)
                first = 3
            if b == 0 and o == 0:
                for at in pieces[:2]:
                    piece(at, 2)
                wait_x(1)
                pack_x(1, 3)
                start_first(1, False, 3)
                start_first(0, False, 3)
                first = 2
            if b == 0 and o == 1:
                for at in pieces[:2]:
                    piece(at, 3)
                wait_x(2)
                pack_x(3, k)
                start_first(1, False, 4)
                start_first(0, False, 4)
                start_first(0, True, 0, 1, 2, 3, 4)
                first = 2
            for at in pieces[first:]:
                piece(at)
            if o == 0 and b and not last:
                pack_x(f + k, f + k + plan.blocks[b + 1])
        wait_border(b, *range(5))
        if b == 0:
            wait_x(3)
        elif not last:
            start_border(b + 1, 2, 3, 4)
        if b:
            push_h(plan.first[b - 1], f)
        piece(late.pop(0), 2)
        for side in range(2):
            lo = -k if side == 0 else R
            h = flat(unpack(hr_ref[side, plan.hat[b]:plan.hat[b] + k].astype(f32)))
            emit(f, lo, lo + k, masked(lo, jnp.concatenate([h, x_rows(f, lo, lo + k)], axis=1)))
            lo = -(k - 1) if side == 0 else R
            packed = cr_ref[side, plan.cat[b]:plan.cat[b] + k - 1]
            both = jnp.concatenate([packed, pltpu.roll(packed, CH, 2)], axis=1)
            cbuf[cells_of(lo, lo + k - 1)] = flat(both)
        for o in range(k):
            m = k - 1 - o
            top, bottom = cuts(-m, o + 1, BORDER), cuts(R - 1 - o, R + m, BORDER)
            for lo, hi in top:
                piece((f + o, lo, hi))
            if late:
                piece(late.pop(0))
            for lo, hi in bottom:
                piece((f + o, lo, hi))
            if o == 0 and b == 0 and not last:
                pack_x(f + k, f + k + plan.blocks[b + 1])
                start_border(b + 1, 2, 3, 4)
            if last and o == k // 2:
                push_h(f, f + o)
            if last and o == k - 2:
                push_h(f + k // 2, f + o)
            if last and o == k - 1:
                push_h(T - 1, T, k, R - k)
                push_c(k, R - k)
    flush()
    k = plan.blocks[-1]
    push_h(T - 2, T - 1)
    for lo, hi in ((0, k), (R - k, R)):
        push_h(T - 1, T, lo, hi)
        push_c(lo, hi)

    with jax.named_scope('end_wait'):
        for c in [h_push, c_push, *x_push]:
            c.wait_send()

        def wait_sends(side):
            for kind, ref in enumerate((hs_ref, cs_ref, xs_ref)):
                local(ref.at[side], ref.at[side], s_bs.at[kind, side]).wait()

        each_side(wait_sends)
        for sem in (s_os, s_or):
            local(hpeer, hpeer, sem.at[0]).wait()
            local(cpeer, cpeer, sem.at[1]).wait()


def store(hout, hpeer, cout, cpeer, h_all, c_final, sems):
    s = lax.axis_index("cols")
    HG, HW = hpeer.shape[2], cpeer.shape[1]
    mine = pl.ds(pl.multiple_of(s * HW, HW), HW)
    copies = [pltpu.make_async_copy(hout.at[:, :, pl.ds(s * HG, HG)], h_all.at[:, s], sems.at[0]),
              pltpu.make_async_copy(hpeer, h_all.at[:, 1 - s], sems.at[1]),
              pltpu.make_async_copy(cout.at[:, mine], c_final.at[s], sems.at[2]),
              pltpu.make_async_copy(cpeer, c_final.at[1 - s], sems.at[3])]
    for c in copies:
        c.start()
    for c in copies:
        c.wait()


def run(blocks, n_rows, frames, w_x, w_h, gate_bias, h_init, c_init):
    T, S, R, HW = frames.shape[:4]
    W, HG = 2 * HW, HW // COLS
    plan = Plan(blocks, T, R, W)
    NB, PAD, G = len(blocks), plan.K, len(plan.groups)
    bf, f32 = jnp.bfloat16, jnp.float32
    vm, dma = pltpu.VMEM, pltpu.SemaphoreType.DMA
    hbm = pl.BlockSpec(memory_space=pltpu.HBM)
    vmem = pl.BlockSpec(memory_space=pltpu.VMEM)
    tiled = frames.reshape(T, S, R, HG, COLS, CH)
    parts = pl.pallas_call(
        functools.partial(kernel, plan, n_rows),
        out_shape=(vm((T, R, 2 * HG, COLS, CH), bf), vm((T, R, HG, COLS, CH), bf), vm((R, W, CH), f32),
                   vm((R, HW, CH), f32)),
        in_specs=[hbm] * 6,
        out_specs=(vmem,) * 4,
        scratch_shapes=[
            vm((1, 4 * CH), f32), vm((R, HG, COLS, CH), bf), vm((R, HW, CH), f32),
            vm((plan.groups[1][1], R, HG, COLS, CH), bf),
            vm((T, R, 2 * HG, COLS, CH), bf), vm((R, 2 * HG, COLS, CH), bf), vm((R, W, CH), f32),
            vm((3, (R + 2 * PAD) * W, LANES), bf), vm((3, (R + 2 * PAD) * W, LANES), bf),
            vm(((R + 2 * PAD) * W, LANES), f32), vm((RING, W + 16, LANES), f32), vm((10, 2, CH, 4 * CH), bf),
            vm((2, plan.xat[-1], HG, COLS, LANES), bf), vm((2, plan.xat[-1], HG, COLS, LANES), bf),
            vm((2, plan.hat[-1], HG, COLS, LANES), bf), vm((2, plan.hat[-1], HG, COLS, LANES), bf),
            vm((2, plan.cat[-1], HW, LANES), f32), vm((2, plan.cat[-1], HW, LANES), f32),
            dma((3,)), dma((6,)), dma((2,)), dma((2,)), dma((G,)), dma((G,)), dma((G,)),
            dma((5, 2, NB)), dma((3, 2)), dma((2,)), dma((2,)), pltpu.SemaphoreType.REGULAR],
        compiler_params=pltpu.CompilerParams(collective_id=0, has_side_effects=True, vmem_limit_bytes=46 * 2**20),
    )(tiled, w_x.reshape(9, CH, 4 * CH), w_h.reshape(9, CH, 4 * CH), gate_bias.reshape(1, -1),
      h_init.reshape(S, R, HG, COLS, CH), c_init)
    h_all, c_final = pl.pallas_call(
        store,
        out_shape=(jax.ShapeDtypeStruct(tiled.shape, bf), jax.ShapeDtypeStruct(c_init.shape, f32)),
        in_specs=[vmem] * 4,
        out_specs=(hbm, hbm),
        scratch_shapes=[dma((4,))],
        compiler_params=pltpu.CompilerParams(vmem_limit_bytes=2**20),
    )(*[pltpu.with_memory_space_constraint(a, pltpu.VMEM) for a in parts])
    return h_all.reshape(frames.shape), c_final


def solution(mesh, K=None):
    n_rows = mesh.shape["rows"]
    frame_spec = P(None, "batch", "rows", "cols", None)
    state_spec = P("batch", "rows", "cols", None)
    blocks = BLOCKS if K is None else K
    return jax.shard_map(functools.partial(run, blocks, n_rows), mesh=mesh,
                         in_specs=(frame_spec, P(), P(), P(), state_spec, state_spec),
                         out_specs=(frame_spec, state_spec), check_vma=False)
```

```python
import functools

import jax
import jax.numpy as jnp
from jax import lax
from jax.experimental import pallas as pl
from jax.experimental.pallas import tpu as pltpu
from jax.sharding import PartitionSpec as P

MESH = pl.DeviceIdType.MESH
CH = 64
LANES = 128
COLS = 8
PIECE = 4
RING = 8
BLOCKS = (8, 8)
LATE = (8, 8)
BORDER = 4
FAR = 16


def cuts(lo, hi, size=PIECE):
    n = max(1, (hi - lo) // size)
    edges = [lo + i * size for i in range(n)] + [hi]
    return list(zip(edges[:-1], edges[1:]))


class Plan:
    def __init__(self, blocks, T, R, W):
        assert sum(blocks) == T
        self.blocks, self.T, self.R, self.W, self.HW, self.HG = blocks, T, R, W, W // 2, W // 2 // COLS
        self.K = max(blocks)
        self.first = [sum(blocks[:b]) for b in range(len(blocks))]
        self.of = [(b, o) for b, k in enumerate(blocks) for o in range(k)]
        self.xrows = [blocks[b] - o for b, o in self.of]
        self.xat = [sum(self.xrows[:t]) for t in range(T + 1)]
        self.hat = [sum(blocks[:b]) for b in range(len(blocks) + 1)]
        self.cat = [sum(k - 1 for k in blocks[:b]) for b in range(len(blocks) + 1)]
        ends = [0, 1, 3, blocks[0] + 1, T]
        self.groups = [(a, e) for a, e in zip(ends[:-1], ends[1:]) if e > a]


def kernel(plan, n_rows, frames, w_x, w_h, bias_in, h_init, c_init, hout, hpeer, cout, cpeer,
           bias, hgo, cgo, xgo, xin, hst, cst, xh_even, xh_odd, cbuf, shift, wbuf,
           xs_ref, xr_ref, hs_ref, hr_ref, cs_ref, cr_ref,
           s_w, s_i, s_ir, s_is, s_x, s_xr, s_xs, s_b, s_bs, s_or, s_os, here_sem):
    T, R, W, HW, HG = plan.T, plan.R, plan.W, plan.HW, plan.HG
    PAD = plan.K
    NB = len(plan.blocks)
    s = lax.axis_index("cols")
    n = lax.axis_index("rows")
    p = 1 - s
    mine, theirs = pl.ds(s * HG, HG), pl.ds(p * HG, HG)
    mine_c, theirs_c = [pl.ds(pl.multiple_of(i * HW, HW), HW) for i in (s, p)]
    has_up, has_dn = n > 0, n < n_rows - 1
    bf, f32 = jnp.bfloat16, jnp.float32

    def local(src, dst, sem):
        return pltpu.make_async_copy(src, dst, sem)

    def remote(src, dst, ssem, rsem, dev):
        return pltpu.make_async_remote_copy(
            src_ref=src, dst_ref=dst, send_sem=ssem, recv_sem=rsem, device_id=dev, device_id_type=MESH)

    peer = {"cols": p}
    side_dev = [{"rows": n - 1}, {"rows": n + 1}]
    side_ok = [has_up, has_dn]

    def each_side(do):
        for side in range(2):
            @pl.when(side_ok[side])
            def _():
                do(side)

    barrier = pltpu.get_barrier_semaphore()

    def signal(dev):
        pl.semaphore_signal(barrier, inc=1, device_id=dev, device_id_type=MESH)

    signal(peer)

    @pl.when(has_up)
    def _():
        signal(side_dev[0])


    h_own = local(h_init.at[s], hst.at[:, mine], s_i.at[0])
    c_own = local(c_init.at[s], cst.at[:, mine_c], s_i.at[1])
    x_own = [local(frames.at[a:e, s], xin.at[a:e, :, mine], s_x.at[g]) for g, (a, e) in enumerate(plan.groups)]
    h_got = local(h_init.at[p], hgo, s_i.at[2])
    c_got = local(c_init.at[p], cgo, s_i.at[3])
    x_got = [local(frames.at[a:e, p], xgo.at[a:e], s_i.at[4 + g]) for g, (a, e) in enumerate(plan.groups[:2])]
    w_copies = [local(w_h, wbuf.at[0:9, 0], s_w.at[0]), local(w_x, wbuf.at[0:9, 1], s_w.at[1]),
                local(bias_in, bias, s_w.at[2])]
    for c in [h_got, x_got[0], c_got, h_own, x_own[0], c_own, *w_copies, x_got[1], *x_own[1:]]:
        c.start()
    with jax.named_scope('barrier'):
        pl.semaphore_wait(barrier, 1 + has_dn.astype(jnp.int32))

    @pl.when(has_dn)
    def _():
        pl.semaphore_signal(here_sem, inc=1, device_id=side_dev[1], device_id_type=MESH)


    h_push = remote(hgo, hst.at[:, mine], s_is.at[0], s_ir.at[0], peer)
    c_push = remote(cgo, cst.at[:, mine_c], s_is.at[1], s_ir.at[1], peer)
    x_push = [remote((xgo if g < 2 else frames.at[:, p]).at[a:e], xin.at[a:e, :, mine], s_xs.at[g], s_xr.at[g], peer)
              for g, (a, e) in enumerate(plan.groups)]
    with jax.named_scope('got_wait'):
        for got, push in [(h_got, h_push), (x_got[0], x_push[0]), (c_got, c_push), (x_got[1], x_push[1])]:
            got.wait()
            push.start()
    for push in x_push[2:]:
        push.start()

    shift[...] = jnp.zeros_like(shift)
    low = lax.broadcasted_iota(jnp.int32, (1, LANES), 1) < CH
    low_half = low_row = low
    turn = [0]
    scale = jnp.where(low_row, 0.5, 1.0)
    lift = jnp.where(low_row, 0.5, 0.0)

    with jax.named_scope('w_wait'):
        for c in w_copies:
            c.wait()
    for tap in range(9):
        for half in range(2):
            tile = wbuf[tap, half, :, 0:LANES]
            wbuf[tap, half, :, 0:LANES] = jnp.concatenate([tile[:, CH:], tile[:, :CH]], axis=1)
    b_all = bias[...]
    rest = jnp.concatenate([b_all[:, CH:LANES], b_all[:, :CH], b_all[:, LANES:]], axis=1)
    row = lax.broadcasted_iota(jnp.int32, (CH, 4 * CH), 0)
    rows = jnp.zeros((CH, 4 * CH), f32)
    for i in range(3):
        top = (rest * (1 - 2.0 ** -8)).astype(bf).astype(f32) if i == 0 else rest.astype(bf).astype(f32)
        rows = jnp.where(row == i, top, rows)
        rest = rest - top
    wbuf[9, 0] = rows.astype(bf)
    wbuf[9, 1] = jnp.zeros((CH, 4 * CH), bf)
    ones = jnp.where(lax.broadcasted_iota(jnp.int32, (1, LANES), 1) < 3, 1.0, 0.0).astype(bf)

    def pack(v):
        return jnp.concatenate([v[:, :HG], v[:, HG:]], axis=3)

    def unpack(v):
        return jnp.concatenate([v[..., :CH], v[..., CH:]], axis=1)

    def masked(r, v):
        if 0 <= r < R:
            return v
        return lax.select(jnp.broadcast_to(has_up if r < 0 else has_dn, v.shape), v, jnp.zeros_like(v))

    def emit(t, lo, hi, hx):
        nxt = xh_even if t % 2 == 0 else xh_odd
        at, to = slot(lo, hi), cells_of(lo, hi)
        shift[at, 8:8 + W, :] = hx.reshape(hi - lo, W, LANES)
        nxt[1, to] = hx.astype(bf)
        nxt[0, to] = shift[at, 7:7 + W, :].reshape(hx.shape).astype(bf)
        nxt[2, to] = shift[at, 9:9 + W, :].reshape(hx.shape).astype(bf)

    def cells_of(lo, hi):
        return slice((lo + PAD) * W, (hi + PAD) * W)

    def slot(lo, hi):
        if turn[0] + hi - lo > RING:
            turn[0] = 0
        turn[0] += hi - lo
        return slice(turn[0] - (hi - lo), turn[0])

    def flat(v):
        return v.reshape(-1, v.shape[-1])

    def x_rows(t, lo, hi):
        if lo >= 0 and hi <= R:
            return flat(xin[t, lo:hi].astype(f32))
        side, i = (0, lo + plan.xrows[t]) if lo < 0 else (1, lo - R)
        return flat(unpack(xr_ref[side, plan.xat[t] + i:plan.xat[t] + i + hi - lo].astype(f32)))

    def wait_x(g):
        if g < len(plan.groups):
            x_own[g].wait()
            x_push[g].wait_recv()

    def border(b, kind, side):
        k, f = plan.blocks[b], plan.first[b]
        src, dst, at, end = [
            (hs_ref, hr_ref, plan.hat[b], plan.hat[b + 1]),
            (cs_ref, cr_ref, plan.cat[b], plan.cat[b + 1]),
            (xs_ref, xr_ref, plan.xat[f], plan.xat[f + 1]),
            (xs_ref, xr_ref, plan.xat[f + 1], plan.xat[f + 3]),
            (xs_ref, xr_ref, plan.xat[f + 3], plan.xat[f + k])][kind]
        return remote(src.at[side, at:end], dst.at[1 - side, at:end],
                      s_bs.at[min(kind, 2), side], s_b.at[kind, 1 - side, b], side_dev[side])

    def pack_x(t0, t1):
        for side in range(2):
            for t in range(t0, t1):
                m = plan.xrows[t]
                lo = 0 if side == 0 else R - m
                xs_ref[side, plan.xat[t]:plan.xat[t] + m] = pack(xin[t, lo:lo + m])

    def start_border(b, *kinds):
        each_side(lambda side: [border(b, kind, side).start() for kind in kinds])

    far = lax.rem(n, FAR) == 0

    def start_first(side, late, *kinds):
        ok = has_dn if side else jnp.logical_and(has_up, far if late else jnp.logical_not(far))

        @pl.when(ok)
        def _():
            if not side and 0 in kinds:
                pl.semaphore_wait(here_sem, 1)
            for kind in kinds:
                border(0, kind, side).start()

    def wait_border(b, *kinds):
        each_side(lambda side: [border(b, kind, 1 - side).wait_recv() for kind in kinds])

    def pack_h(b, h_rows):
        k = plan.blocks[b]
        for side in range(2):
            lo = 0 if side == 0 else R - k
            hs_ref[side, plan.hat[b]:plan.hat[b] + k] = pack(h_rows[lo:lo + k])

    def pack_c(b):
        k = plan.blocks[b]
        for side in range(2):
            lo = 0 if side == 0 else R - (k - 1)
            c = cbuf[cells_of(lo, lo + k - 1)].reshape(k - 1, W, LANES)
            cs_ref[side, plan.cat[b]:plan.cat[b] + k - 1] = jnp.where(low_half, c[:, :HW], c[:, HW:])

    weights = wbuf[...].reshape(10 * LANES, 4 * CH)

    def dot(t, lo, hi):
        cur = xh_even if t % 2 == 0 else xh_odd
        taps = [cur[dc, cells_of(lo + dr - 1, hi + dr - 1)] for dr in range(3) for dc in range(3)]
        taps.append(jnp.broadcast_to(ones, taps[0].shape))
        return jnp.dot(jnp.concatenate(taps, axis=1), weights, preferred_element_type=f32)

    def cells(t, lo, hi, gates):
        fi = jnp.tanh(gates[:, :LANES] * 0.5) * 0.5 + 0.5
        og = jnp.tanh(gates[:, LANES:] * scale) * scale + lift
        at = cells_of(lo, hi)
        prod = fi * lax.select(jnp.broadcast_to(low, og.shape), cbuf[at], og)
        c = prod + pltpu.roll(prod, CH, 1)
        h = (og * jnp.tanh(c))[:, :CH]
        if t == T - 1:
            cout[lo:hi] = c[:, :CH].reshape(hi - lo, W, CH)
        else:
            cbuf[at] = c
        for a, e in ((lo, min(hi, 0)), (max(lo, 0), min(hi, R)), (max(lo, R), hi)):
            if a >= e:
                continue
            part = h[(a - lo) * W:(e - lo) * W]
            if a >= 0 and e <= R:
                hout[t, a:e] = part.reshape(e - a, 2 * HG, COLS, CH).astype(bf)
            if t < T - 1:
                emit(t + 1, a, e, masked(a, jnp.concatenate([part, x_rows(t + 1, a, e)], axis=1)))

    pending = []

    def piece(at, ahead=1):
        t, lo, hi = at
        while any(u == t - 1 and a <= hi and lo <= e for u, a, e, _ in pending):
            cells(*pending.pop(0))
        pending.append((*at, dot(*at)))
        flush(ahead)

    def flush(left=0):
        while len(pending) > left:
            cells(*pending.pop(0))

    def push_h(t0, t1, lo=0, hi=R):
        rows = slice(lo, hi)
        remote(hout.at[t0:t1, rows, theirs], hpeer.at[t0:t1, rows], s_os.at[0], s_or.at[0], peer).start()

    def push_c(lo, hi):
        remote(cout.at[lo:hi, theirs_c], cpeer.at[lo:hi], s_os.at[1], s_or.at[1], peer).start()

    with jax.named_scope('state_wait'):
        for c in [h_own, x_own[0]]:
            c.wait()
        for c in [h_push, x_push[0]]:
            c.wait_recv()
    pack_h(0, hst)
    pack_x(0, 1)
    start_first(1, False, 0, 2)
    start_first(0, False, 0, 2)
    for lo, hi in cuts(0, R):
        emit(0, lo, hi, jnp.concatenate([flat(hst[lo:hi].astype(f32)), x_rows(0, lo, hi)], axis=1))

    for b, k in enumerate(plan.blocks):
        f = plan.first[b]
        last = b + 1 == NB

        def inner(o):
            if o == 0:
                got = [*cuts(k + 1, R - 1 - k), *cuts(1, k + 1), *cuts(R - 1 - k, R - 1)]
            else:
                got = cuts(o + 1, R - 1 - o)
                got = got[1:-1] + [got[0], got[-1]]
            return [(f + o, lo, hi) for lo, hi in got]

        early = [at for o in range(k) for at in inner(o)]
        late = early[len(early) - LATE[b]:]
        for o in range(k):
            pieces = [at for at in early[:len(early) - LATE[b]] if at[0] == f + o]
            first = 0
            if o == 0 and b:
                piece(pieces[0], 9)
                flush(1)
                pack_h(b, hout.at[f - 1])
                pack_c(b)
                with jax.named_scope(f'send{b}'):
                    start_border(b, 0, 1)
                first = 1
            if b == 0 and o == 0:
                for at in pieces[:2]:
                    piece(at, 2)
                with jax.named_scope('x_wait0'):
                    c_own.wait()
                    c_push.wait_recv()
                    wait_x(1)
                c0 = flat(cst[...])
                cbuf[cells_of(0, R)] = jnp.concatenate([c0, c0], axis=1)
                pack_c(0)
                pack_x(1, 3)
                start_first(1, False, 1, 3)
                start_first(0, False, 1, 3)
                first = 2
            if b == 0 and o == 2:
                for at in pieces[:2]:
                    piece(at, 2)
                with jax.named_scope('x_wait1'):
                    wait_x(2)
                pack_x(3, k)
                for side in range(2):
                    start_first(side, False, 4)
                start_first(0, True, 4)
                first = 2
            for at in pieces[first:]:
                piece(at)
            if o == 0 and b == 0:
                with jax.named_scope('upsend'):
                    start_first(0, True, 0, 1, 2, 3)
            if o == 0 and b and not last:
                pack_x(f + k, f + k + plan.blocks[b + 1])
        with jax.named_scope(f'mid{b}'):
            wait_border(b, 0, 2, 3, *((4,) if b else ()))
        if b == 0:
            wait_x(3)
        elif not last:
            start_border(b + 1, 2, 3, 4)
        if b:
            push_h(plan.first[b - 1], f)
        piece(late.pop(0), 2)
        for side in range(2):
            lo = -k if side == 0 else R
            h = flat(unpack(hr_ref[side, plan.hat[b]:plan.hat[b] + k].astype(f32)))
            emit(f, lo, lo + k, masked(lo, jnp.concatenate([h, x_rows(f, lo, lo + k)], axis=1)))
        for o in range(k):
            m = k - 1 - o
            top, bottom = cuts(-m, o + 1, BORDER), cuts(R - 1 - o, R + m, BORDER)
            for lo, hi in top:
                piece((f + o, lo, hi), 9 if o == 0 else 1)
                if b == 0 and o == 2 and lo == top[0][0]:
                    with jax.named_scope('mid4'):
                        wait_border(0, 4)
            if late:
                piece(late.pop(0), 9 if o == 0 else 1)
            for lo, hi in bottom:
                piece((f + o, lo, hi), 9 if o == 0 else 1)
            if o == 0:
                with jax.named_scope(f'midc{b}'):
                    wait_border(b, 1)
                for side in range(2):
                    lo = -(k - 1) if side == 0 else R
                    packed = cr_ref[side, plan.cat[b]:plan.cat[b] + k - 1]
                    both = jnp.concatenate([packed, pltpu.roll(packed, CH, 2)], axis=1)
                    cbuf[cells_of(lo, lo + k - 1)] = flat(both)
            if o == 0 and b == 0 and not last:
                pack_x(f + k, f + k + plan.blocks[b + 1])
                start_border(b + 1, 2, 3, 4)
            if last and o == k // 2:
                push_h(f, f + o)
            if last and o == k - 2:
                push_h(f + k // 2, f + o)
                push_h(T - 1, T, k, R - k)
                push_c(k, R - k)
        assert not late
    flush()
    k = plan.blocks[-1]
    push_h(T - 2, T - 1)
    for lo, hi in ((0, k), (R - k, R)):
        push_h(T - 1, T, lo, hi)
        push_c(lo, hi)

    with jax.named_scope('end_wait'):
        for c in [h_push, c_push, *x_push]:
            c.wait_send()

        def wait_sends(side):
            for kind, ref in enumerate((hs_ref, cs_ref, xs_ref)):
                local(ref.at[side], ref.at[side], s_bs.at[kind, side]).wait()

        each_side(wait_sends)
        for sem in (s_os, s_or):
            local(hpeer, hpeer, sem.at[0]).wait()
            local(cpeer, cpeer, sem.at[1]).wait()


def store(hout, hpeer, cout, cpeer, h_all, c_final, sems):
    s = lax.axis_index("cols")
    HG, HW = hpeer.shape[2], cpeer.shape[1]
    mine = pl.ds(pl.multiple_of(s * HW, HW), HW)
    copies = [pltpu.make_async_copy(hout.at[:, :, pl.ds(s * HG, HG)], h_all.at[:, s], sems.at[0]),
              pltpu.make_async_copy(hpeer, h_all.at[:, 1 - s], sems.at[1]),
              pltpu.make_async_copy(cout.at[:, mine], c_final.at[s], sems.at[2]),
              pltpu.make_async_copy(cpeer, c_final.at[1 - s], sems.at[3])]
    for c in copies:
        c.start()
    for c in copies:
        c.wait()


def run(blocks, n_rows, frames, w_x, w_h, gate_bias, h_init, c_init):
    T, S, R, HW = frames.shape[:4]
    W, HG = 2 * HW, HW // COLS
    plan = Plan(blocks, T, R, W)
    NB, PAD, G = len(blocks), plan.K, len(plan.groups)
    bf, f32 = jnp.bfloat16, jnp.float32
    vm, dma = pltpu.VMEM, pltpu.SemaphoreType.DMA
    hbm = pl.BlockSpec(memory_space=pltpu.HBM)
    vmem = pl.BlockSpec(memory_space=pltpu.VMEM)
    tiled = frames.reshape(T, S, R, HG, COLS, CH)
    parts = pl.pallas_call(
        functools.partial(kernel, plan, n_rows),
        out_shape=(vm((T, R, 2 * HG, COLS, CH), bf), vm((T, R, HG, COLS, CH), bf), vm((R, W, CH), f32),
                   vm((R, HW, CH), f32)),
        in_specs=[hbm] * 6,
        out_specs=(vmem,) * 4,
        scratch_shapes=[
            vm((1, 4 * CH), f32), vm((R, HG, COLS, CH), bf), vm((R, HW, CH), f32),
            vm((plan.groups[1][1], R, HG, COLS, CH), bf),
            vm((T, R, 2 * HG, COLS, CH), bf), vm((R, 2 * HG, COLS, CH), bf), vm((R, W, CH), f32),
            vm((3, (R + 2 * PAD) * W, LANES), bf), vm((3, (R + 2 * PAD) * W, LANES), bf),
            vm(((R + 2 * PAD) * W, LANES), f32), vm((RING, W + 16, LANES), f32), vm((10, 2, CH, 4 * CH), bf),
            vm((2, plan.xat[-1], HG, COLS, LANES), bf), vm((2, plan.xat[-1], HG, COLS, LANES), bf),
            vm((2, plan.hat[-1], HG, COLS, LANES), bf), vm((2, plan.hat[-1], HG, COLS, LANES), bf),
            vm((2, plan.cat[-1], HW, LANES), f32), vm((2, plan.cat[-1], HW, LANES), f32),
            dma((3,)), dma((6,)), dma((2,)), dma((2,)), dma((G,)), dma((G,)), dma((G,)),
            dma((5, 2, NB)), dma((3, 2)), dma((2,)), dma((2,)), pltpu.SemaphoreType.REGULAR],
        compiler_params=pltpu.CompilerParams(collective_id=0, has_side_effects=True, vmem_limit_bytes=46 * 2**20),
    )(tiled, w_x.reshape(9, CH, 4 * CH), w_h.reshape(9, CH, 4 * CH), gate_bias.reshape(1, -1),
      h_init.reshape(S, R, HG, COLS, CH), c_init)
    h_all, c_final = pl.pallas_call(
        store,
        out_shape=(jax.ShapeDtypeStruct(tiled.shape, bf), jax.ShapeDtypeStruct(c_init.shape, f32)),
        in_specs=[vmem] * 4,
        out_specs=(hbm, hbm),
        scratch_shapes=[dma((4,))],
        compiler_params=pltpu.CompilerParams(vmem_limit_bytes=2**20),
    )(*[pltpu.with_memory_space_constraint(a, pltpu.VMEM) for a in parts])
    return h_all.reshape(frames.shape), c_final


def solution(mesh, K=None):
    n_rows = mesh.shape["rows"]
    frame_spec = P(None, "batch", "rows", "cols", None)
    state_spec = P("batch", "rows", "cols", None)
    blocks = BLOCKS if K is None else K
    return jax.shard_map(functools.partial(run, blocks, n_rows), mesh=mesh,
                         in_specs=(frame_spec, P(), P(), P(), state_spec, state_spec),
                         out_specs=(frame_spec, state_spec), check_vma=False)
```

```python
import functools

import jax
import jax.numpy as jnp
from jax import lax
from jax.experimental import pallas as pl
from jax.experimental.pallas import tpu as pltpu
from jax.sharding import PartitionSpec as P

MESH = pl.DeviceIdType.MESH
CH = 64
LANES = 128
COLS = 8
PIECE = 4
RING = 8
BLOCKS = (8, 8)
LATE = (3, 3)
BORDER = 4
FAR = 16


def cuts(lo, hi, size=PIECE):
    n = max(1, (hi - lo) // size)
    edges = [lo + i * size for i in range(n)] + [hi]
    return list(zip(edges[:-1], edges[1:]))


class Plan:
    def __init__(self, blocks, T, R, W):
        assert sum(blocks) == T
        self.blocks, self.T, self.R, self.W, self.HW, self.HG = blocks, T, R, W, W // 2, W // 2 // COLS
        self.K = max(blocks)
        self.first = [sum(blocks[:b]) for b in range(len(blocks))]
        self.of = [(b, o) for b, k in enumerate(blocks) for o in range(k)]
        self.xrows = [blocks[b] - o for b, o in self.of]
        self.xat = [sum(self.xrows[:t]) for t in range(T + 1)]
        self.hat = [sum(blocks[:b]) for b in range(len(blocks) + 1)]
        self.cat = [sum(k - 1 for k in blocks[:b]) for b in range(len(blocks) + 1)]
        ends = [0, 1, 3, blocks[0] + 1, T]
        self.groups = [(a, e) for a, e in zip(ends[:-1], ends[1:]) if e > a]


def kernel(plan, n_rows, frames, w_x, w_h, bias_in, h_init, c_init, hout, hpeer, cout, cpeer,
           bias, hgo, cgo, xgo, xin, hst, cst, xh_even, xh_odd, cbuf, shift, wbuf,
           xs_ref, xr_ref, hs_ref, hr_ref, cs_ref, cr_ref,
           s_w, s_i, s_ir, s_is, s_x, s_xr, s_xs, s_b, s_bs, s_or, s_os, here_sem):
    T, R, W, HW, HG = plan.T, plan.R, plan.W, plan.HW, plan.HG
    PAD = plan.K
    NB = len(plan.blocks)
    s = lax.axis_index("cols")
    n = lax.axis_index("rows")
    p = 1 - s
    mine, theirs = pl.ds(s * HG, HG), pl.ds(p * HG, HG)
    mine_c, theirs_c = [pl.ds(pl.multiple_of(i * HW, HW), HW) for i in (s, p)]
    has_up, has_dn = n > 0, n < n_rows - 1
    bf, f32 = jnp.bfloat16, jnp.float32

    def local(src, dst, sem):
        return pltpu.make_async_copy(src, dst, sem)

    def remote(src, dst, ssem, rsem, dev):
        return pltpu.make_async_remote_copy(
            src_ref=src, dst_ref=dst, send_sem=ssem, recv_sem=rsem, device_id=dev, device_id_type=MESH)

    peer = {"cols": p}
    side_dev = [{"rows": n - 1}, {"rows": n + 1}]
    side_ok = [has_up, has_dn]

    def each_side(do):
        for side in range(2):
            @pl.when(side_ok[side])
            def _():
                do(side)

    barrier = pltpu.get_barrier_semaphore()

    def signal(dev):
        pl.semaphore_signal(barrier, inc=1, device_id=dev, device_id_type=MESH)

    signal(peer)

    @pl.when(has_up)
    def _():
        signal(side_dev[0])


    h_own = local(h_init.at[s], hst.at[:, mine], s_i.at[0])
    c_own = local(c_init.at[s], cst.at[:, mine_c], s_i.at[1])
    x_own = [local(frames.at[a:e, s], xin.at[a:e, :, mine], s_x.at[g]) for g, (a, e) in enumerate(plan.groups)]
    h_got = local(h_init.at[p], hgo, s_i.at[2])
    c_got = local(c_init.at[p], cgo, s_i.at[3])
    x_got = [local(frames.at[a:e, p], xgo.at[a:e], s_i.at[4 + g]) for g, (a, e) in enumerate(plan.groups[:2])]
    w_copies = [local(w_h, wbuf.at[0:9, 0], s_w.at[0]), local(w_x, wbuf.at[0:9, 1], s_w.at[1]),
                local(bias_in, bias, s_w.at[2])]
    for c in [h_got, x_got[0], c_got, h_own, x_own[0], c_own, *w_copies, x_got[1], *x_own[1:]]:
        c.start()
    with jax.named_scope('barrier'):
        pl.semaphore_wait(barrier, 1 + has_dn.astype(jnp.int32))

    @pl.when(has_dn)
    def _():
        pl.semaphore_signal(here_sem, inc=1, device_id=side_dev[1], device_id_type=MESH)


    h_push = remote(hgo, hst.at[:, mine], s_is.at[0], s_ir.at[0], peer)
    c_push = remote(cgo, cst.at[:, mine_c], s_is.at[1], s_ir.at[1], peer)
    x_push = [remote((xgo if g < 2 else frames.at[:, p]).at[a:e], xin.at[a:e, :, mine], s_xs.at[g], s_xr.at[g], peer)
              for g, (a, e) in enumerate(plan.groups)]
    with jax.named_scope('got_wait'):
        for got, push in [(h_got, h_push), (x_got[0], x_push[0]), (c_got, c_push), (x_got[1], x_push[1])]:
            got.wait()
            push.start()
    for push in x_push[2:]:
        push.start()

    shift[...] = jnp.zeros_like(shift)
    low = lax.broadcasted_iota(jnp.int32, (1, LANES), 1) < CH
    low_half = low_row = low
    turn = [0]
    scale = jnp.where(low_row, 0.5, 1.0)
    lift = jnp.where(low_row, 0.5, 0.0)

    with jax.named_scope('w_wait'):
        for c in w_copies:
            c.wait()
    for tap in range(9):
        for half in range(2):
            tile = wbuf[tap, half, :, 0:LANES]
            wbuf[tap, half, :, 0:LANES] = jnp.concatenate([tile[:, CH:], tile[:, :CH]], axis=1)
    b_all = bias[...]
    rest = jnp.concatenate([b_all[:, CH:LANES], b_all[:, :CH], b_all[:, LANES:]], axis=1)
    row = lax.broadcasted_iota(jnp.int32, (CH, 4 * CH), 0)
    rows = jnp.zeros((CH, 4 * CH), f32)
    for i in range(3):
        top = (rest * (1 - 2.0 ** -8)).astype(bf).astype(f32) if i == 0 else rest.astype(bf).astype(f32)
        rows = jnp.where(row == i, top, rows)
        rest = rest - top
    wbuf[9, 0] = rows.astype(bf)
    wbuf[9, 1] = jnp.zeros((CH, 4 * CH), bf)
    ones = jnp.where(lax.broadcasted_iota(jnp.int32, (1, LANES), 1) < 3, 1.0, 0.0).astype(bf)

    def pack(v):
        return jnp.concatenate([v[:, :HG], v[:, HG:]], axis=3)

    def unpack(v):
        return jnp.concatenate([v[..., :CH], v[..., CH:]], axis=1)

    def masked(r, v):
        if 0 <= r < R:
            return v
        return lax.select(jnp.broadcast_to(has_up if r < 0 else has_dn, v.shape), v, jnp.zeros_like(v))

    def emit(t, lo, hi, hx):
        nxt = xh_even if t % 2 == 0 else xh_odd
        at, to = slot(lo, hi), cells_of(lo, hi)
        shift[at, 8:8 + W, :] = hx.reshape(hi - lo, W, LANES)
        nxt[1, to] = hx.astype(bf)
        nxt[0, to] = shift[at, 7:7 + W, :].reshape(hx.shape).astype(bf)
        nxt[2, to] = shift[at, 9:9 + W, :].reshape(hx.shape).astype(bf)

    def cells_of(lo, hi):
        return slice((lo + PAD) * W, (hi + PAD) * W)

    def slot(lo, hi):
        if turn[0] + hi - lo > RING:
            turn[0] = 0
        turn[0] += hi - lo
        return slice(turn[0] - (hi - lo), turn[0])

    def flat(v):
        return v.reshape(-1, v.shape[-1])

    def x_rows(t, lo, hi):
        if lo >= 0 and hi <= R:
            return flat(xin[t, lo:hi].astype(f32))
        side, i = (0, lo + plan.xrows[t]) if lo < 0 else (1, lo - R)
        return flat(unpack(xr_ref[side, plan.xat[t] + i:plan.xat[t] + i + hi - lo].astype(f32)))

    def wait_x(g):
        if g < len(plan.groups):
            x_own[g].wait()
            x_push[g].wait_recv()

    def border(b, kind, side):
        k, f = plan.blocks[b], plan.first[b]
        src, dst, at, end = [
            (hs_ref, hr_ref, plan.hat[b], plan.hat[b + 1]),
            (cs_ref, cr_ref, plan.cat[b], plan.cat[b + 1]),
            (xs_ref, xr_ref, plan.xat[f], plan.xat[f + 1]),
            (xs_ref, xr_ref, plan.xat[f + 1], plan.xat[f + 3]),
            (xs_ref, xr_ref, plan.xat[f + 3], plan.xat[f + k])][kind]
        return remote(src.at[side, at:end], dst.at[1 - side, at:end],
                      s_bs.at[min(kind, 2), side], s_b.at[kind, 1 - side, b], side_dev[side])

    def pack_x(t0, t1):
        for side in range(2):
            for t in range(t0, t1):
                m = plan.xrows[t]
                lo = 0 if side == 0 else R - m
                xs_ref[side, plan.xat[t]:plan.xat[t] + m] = pack(xin[t, lo:lo + m])

    def start_border(b, *kinds):
        each_side(lambda side: [border(b, kind, side).start() for kind in kinds])

    far = lax.rem(n, FAR) == 0

    def start_first(side, late, *kinds):
        ok = has_dn if side else jnp.logical_and(has_up, far if late else jnp.logical_not(far))

        @pl.when(ok)
        def _():
            if not side and 0 in kinds:
                pl.semaphore_wait(here_sem, 1)
            for kind in kinds:
                border(0, kind, side).start()

    def wait_border(b, *kinds):
        each_side(lambda side: [border(b, kind, 1 - side).wait_recv() for kind in kinds])

    def pack_h(b, h_rows):
        k = plan.blocks[b]
        for side in range(2):
            lo = 0 if side == 0 else R - k
            hs_ref[side, plan.hat[b]:plan.hat[b] + k] = pack(h_rows[lo:lo + k])

    def pack_c(b):
        k = plan.blocks[b]
        for side in range(2):
            lo = 0 if side == 0 else R - (k - 1)
            c = cbuf[cells_of(lo, lo + k - 1)].reshape(k - 1, W, LANES)
            cs_ref[side, plan.cat[b]:plan.cat[b] + k - 1] = jnp.where(low_half, c[:, :HW], c[:, HW:])

    weights = wbuf[...].reshape(10 * LANES, 4 * CH)

    def dot(t, lo, hi):
        cur = xh_even if t % 2 == 0 else xh_odd
        taps = [cur[dc, cells_of(lo + dr - 1, hi + dr - 1)] for dr in range(3) for dc in range(3)]
        taps.append(jnp.broadcast_to(ones, taps[0].shape))
        return jnp.dot(jnp.concatenate(taps, axis=1), weights, preferred_element_type=f32)

    def cells(t, lo, hi, gates):
        fi = jnp.tanh(gates[:, :LANES] * 0.5) * 0.5 + 0.5
        og = jnp.tanh(gates[:, LANES:] * scale) * scale + lift
        at = cells_of(lo, hi)
        prod = fi * lax.select(jnp.broadcast_to(low, og.shape), cbuf[at], og)
        c = prod + pltpu.roll(prod, CH, 1)
        h = (og * jnp.tanh(c))[:, :CH]
        if t == T - 1:
            cout[lo:hi] = c[:, :CH].reshape(hi - lo, W, CH)
        else:
            cbuf[at] = c
        for a, e in ((lo, min(hi, 0)), (max(lo, 0), min(hi, R)), (max(lo, R), hi)):
            if a >= e:
                continue
            part = h[(a - lo) * W:(e - lo) * W]
            if a >= 0 and e <= R:
                hout[t, a:e] = part.reshape(e - a, 2 * HG, COLS, CH).astype(bf)
            if t < T - 1:
                emit(t + 1, a, e, masked(a, jnp.concatenate([part, x_rows(t + 1, a, e)], axis=1)))

    pending = []

    def piece(at, ahead=1):
        t, lo, hi = at
        while any(u == t - 1 and a <= hi and lo <= e for u, a, e, _ in pending):
            cells(*pending.pop(0))
        pending.append((*at, dot(*at)))
        flush(ahead)

    def flush(left=0):
        while len(pending) > left:
            cells(*pending.pop(0))

    def push_h(t0, t1, lo=0, hi=R):
        rows = slice(lo, hi)
        remote(hout.at[t0:t1, rows, theirs], hpeer.at[t0:t1, rows], s_os.at[0], s_or.at[0], peer).start()

    def push_c(lo, hi):
        remote(cout.at[lo:hi, theirs_c], cpeer.at[lo:hi], s_os.at[1], s_or.at[1], peer).start()

    with jax.named_scope('state_wait'):
        for c in [h_own, x_own[0]]:
            c.wait()
        for c in [h_push, x_push[0]]:
            c.wait_recv()
    pack_h(0, hst)
    pack_x(0, 1)
    start_first(1, False, 0, 2)
    start_first(0, False, 0, 2)
    for lo, hi in cuts(0, R):
        emit(0, lo, hi, jnp.concatenate([flat(hst[lo:hi].astype(f32)), x_rows(0, lo, hi)], axis=1))

    for b, k in enumerate(plan.blocks):
        f = plan.first[b]
        last = b + 1 == NB

        def inner(o):
            if o == 0:
                got = [*cuts(k + 1, R - 1 - k), *cuts(1, k + 1), *cuts(R - 1 - k, R - 1)]
            else:
                got = cuts(o + 1, R - 1 - o)
                got = got[1:-1] + [got[0], got[-1]]
            return [(f + o, lo, hi) for lo, hi in got]

        early = [at for o in range(k) for at in inner(o)]
        late = early[len(early) - LATE[b]:]
        for o in range(k):
            pieces = [at for at in early[:len(early) - LATE[b]] if at[0] == f + o]
            first = 0
            if o == 0 and b:
                piece(pieces[0], 9)
                flush(1)
                pack_h(b, hout.at[f - 1])
                pack_c(b)
                with jax.named_scope(f'send{b}'):
                    start_border(b, 0, 1)
                first = 1
            if b == 0 and o == 0:
                for at in pieces[:2]:
                    piece(at, 9)
                with jax.named_scope('x_wait0'):
                    c_own.wait()
                    c_push.wait_recv()
                    wait_x(1)
                for at in pieces[2:4]:
                    piece(at, 9)
                c0 = flat(cst[...])
                cbuf[cells_of(0, R)] = jnp.concatenate([c0, c0], axis=1)
                pack_c(0)
                pack_x(1, 3)
                start_first(1, False, 1, 3)
                start_first(0, False, 1, 3)
                first = 4
            if b == 0 and o == 2:
                for at in pieces[:2]:
                    piece(at, 9)
                flush(2)
                with jax.named_scope('x_wait1'):
                    wait_x(2)
                for at in pieces[2:4]:
                    piece(at, 9)
                pack_x(3, k)
                for side in range(2):
                    start_first(side, False, 4)
                start_first(0, True, 4)
                first = 4
            for at in pieces[first:]:
                piece(at)
            if o == 0 and b == 0:
                with jax.named_scope('upsend'):
                    start_first(0, True, 0, 1, 2, 3)
            if o == 0 and b and not last:
                pack_x(f + k, f + k + plan.blocks[b + 1])
        with jax.named_scope(f'mid{b}'):
            wait_border(b, 0, 2, *((3, 4) if b else ()))
        if b == 0:
            wait_x(3)
        elif not last:
            start_border(b + 1, 2, 3, 4)
        if b:
            push_h(plan.first[b - 1], f)
        piece(late.pop(0), 3)
        for side in range(2):
            lo = -k if side == 0 else R
            h = flat(unpack(hr_ref[side, plan.hat[b]:plan.hat[b] + k].astype(f32)))
            emit(f, lo, lo + k, masked(lo, jnp.concatenate([h, x_rows(f, lo, lo + k)], axis=1)))
        for o in range(k):
            m = k - 1 - o
            top, bottom = cuts(-m, o + 1, BORDER), cuts(R - 1 - o, R + m, BORDER)
            for lo, hi in top:
                piece((f + o, lo, hi), 9 if o == 0 else 1)
                if b == 0 and o == 2 and lo == top[0][0]:
                    with jax.named_scope('mid4'):
                        wait_border(0, 4)
            for lo, hi in bottom:
                piece((f + o, lo, hi), 9 if o == 0 else 1)
            if o == 0:
                with jax.named_scope(f'midc{b}'):
                    wait_border(b, 1, *(() if b else (3,)))
                for side in range(2):
                    lo = -(k - 1) if side == 0 else R
                    packed = cr_ref[side, plan.cat[b]:plan.cat[b] + k - 1]
                    both = jnp.concatenate([packed, pltpu.roll(packed, CH, 2)], axis=1)
                    cbuf[cells_of(lo, lo + k - 1)] = flat(both)
                while late:
                    piece(late.pop(0), 3)
            if o == 0 and b == 0 and not last:
                pack_x(f + k, f + k + plan.blocks[b + 1])
                start_border(b + 1, 2, 3, 4)
            if last and o == k // 2:
                push_h(f, f + o)
            if last and o == k - 2:
                push_h(f + k // 2, f + o)
                push_h(T - 1, T, k, R - k)
                push_c(k, R - k)
        assert not late
    flush()
    k = plan.blocks[-1]
    push_h(T - 2, T - 1)
    for lo, hi in ((0, k), (R - k, R)):
        push_h(T - 1, T, lo, hi)
        push_c(lo, hi)

    with jax.named_scope('end_wait'):
        for c in [h_push, c_push, *x_push]:
            c.wait_send()

        def wait_sends(side):
            for kind, ref in enumerate((hs_ref, cs_ref, xs_ref)):
                local(ref.at[side], ref.at[side], s_bs.at[kind, side]).wait()

        each_side(wait_sends)
        for sem in (s_os, s_or):
            local(hpeer, hpeer, sem.at[0]).wait()
            local(cpeer, cpeer, sem.at[1]).wait()


def store(hout, hpeer, cout, cpeer, h_all, c_final, sems):
    s = lax.axis_index("cols")
    HG, HW = hpeer.shape[2], cpeer.shape[1]
    mine = pl.ds(pl.multiple_of(s * HW, HW), HW)
    copies = [pltpu.make_async_copy(hout.at[:, :, pl.ds(s * HG, HG)], h_all.at[:, s], sems.at[0]),
              pltpu.make_async_copy(hpeer, h_all.at[:, 1 - s], sems.at[1]),
              pltpu.make_async_copy(cout.at[:, mine], c_final.at[s], sems.at[2]),
              pltpu.make_async_copy(cpeer, c_final.at[1 - s], sems.at[3])]
    for c in copies:
        c.start()
    for c in copies:
        c.wait()


def run(blocks, n_rows, frames, w_x, w_h, gate_bias, h_init, c_init):
    T, S, R, HW = frames.shape[:4]
    W, HG = 2 * HW, HW // COLS
    plan = Plan(blocks, T, R, W)
    NB, PAD, G = len(blocks), plan.K, len(plan.groups)
    bf, f32 = jnp.bfloat16, jnp.float32
    vm, dma = pltpu.VMEM, pltpu.SemaphoreType.DMA
    hbm = pl.BlockSpec(memory_space=pltpu.HBM)
    vmem = pl.BlockSpec(memory_space=pltpu.VMEM)
    tiled = frames.reshape(T, S, R, HG, COLS, CH)
    parts = pl.pallas_call(
        functools.partial(kernel, plan, n_rows),
        out_shape=(vm((T, R, 2 * HG, COLS, CH), bf), vm((T, R, HG, COLS, CH), bf), vm((R, W, CH), f32),
                   vm((R, HW, CH), f32)),
        in_specs=[hbm] * 6,
        out_specs=(vmem,) * 4,
        scratch_shapes=[
            vm((1, 4 * CH), f32), vm((R, HG, COLS, CH), bf), vm((R, HW, CH), f32),
            vm((plan.groups[1][1], R, HG, COLS, CH), bf),
            vm((T, R, 2 * HG, COLS, CH), bf), vm((R, 2 * HG, COLS, CH), bf), vm((R, W, CH), f32),
            vm((3, (R + 2 * PAD) * W, LANES), bf), vm((3, (R + 2 * PAD) * W, LANES), bf),
            vm(((R + 2 * PAD) * W, LANES), f32), vm((RING, W + 16, LANES), f32), vm((10, 2, CH, 4 * CH), bf),
            vm((2, plan.xat[-1], HG, COLS, LANES), bf), vm((2, plan.xat[-1], HG, COLS, LANES), bf),
            vm((2, plan.hat[-1], HG, COLS, LANES), bf), vm((2, plan.hat[-1], HG, COLS, LANES), bf),
            vm((2, plan.cat[-1], HW, LANES), f32), vm((2, plan.cat[-1], HW, LANES), f32),
            dma((3,)), dma((6,)), dma((2,)), dma((2,)), dma((G,)), dma((G,)), dma((G,)),
            dma((5, 2, NB)), dma((3, 2)), dma((2,)), dma((2,)), pltpu.SemaphoreType.REGULAR],
        compiler_params=pltpu.CompilerParams(collective_id=0, has_side_effects=True, vmem_limit_bytes=46 * 2**20),
    )(tiled, w_x.reshape(9, CH, 4 * CH), w_h.reshape(9, CH, 4 * CH), gate_bias.reshape(1, -1),
      h_init.reshape(S, R, HG, COLS, CH), c_init)
    h_all, c_final = pl.pallas_call(
        store,
        out_shape=(jax.ShapeDtypeStruct(tiled.shape, bf), jax.ShapeDtypeStruct(c_init.shape, f32)),
        in_specs=[vmem] * 4,
        out_specs=(hbm, hbm),
        scratch_shapes=[dma((4,))],
        compiler_params=pltpu.CompilerParams(vmem_limit_bytes=2**20),
    )(*[pltpu.with_memory_space_constraint(a, pltpu.VMEM) for a in parts])
    return h_all.reshape(frames.shape), c_final


def solution(mesh, K=None):
    n_rows = mesh.shape["rows"]
    frame_spec = P(None, "batch", "rows", "cols", None)
    state_spec = P("batch", "rows", "cols", None)
    blocks = BLOCKS if K is None else K
    return jax.shard_map(functools.partial(run, blocks, n_rows), mesh=mesh,
                         in_specs=(frame_spec, P(), P(), P(), state_spec, state_spec),
                         out_specs=(frame_spec, state_spec), check_vma=False)
```

```python
import functools

import jax
import jax.numpy as jnp
from jax import lax
from jax.experimental import pallas as pl
from jax.experimental.pallas import tpu as pltpu
from jax.sharding import PartitionSpec as P

MESH = pl.DeviceIdType.MESH
CH = 64
LANES = 128
COLS = 8
PIECE = 4
RING = 8
BLOCKS = (8, 8)
LATE = (3, 3)
BORDER = 4
FAR = 16


def cuts(lo, hi, size=PIECE):
    n = max(1, (hi - lo) // size)
    edges = [lo + i * size for i in range(n)] + [hi]
    return list(zip(edges[:-1], edges[1:]))


class Plan:
    def __init__(self, blocks, T, R, W):
        assert sum(blocks) == T
        self.blocks, self.T, self.R, self.W, self.HW, self.HG = blocks, T, R, W, W // 2, W // 2 // COLS
        self.K = max(blocks)
        self.first = [sum(blocks[:b]) for b in range(len(blocks))]
        self.of = [(b, o) for b, k in enumerate(blocks) for o in range(k)]
        self.xrows = [blocks[b] - o for b, o in self.of]
        self.xat = [sum(self.xrows[:t]) for t in range(T + 1)]
        self.hat = [sum(blocks[:b]) for b in range(len(blocks) + 1)]
        self.cat = [sum(k - 1 for k in blocks[:b]) for b in range(len(blocks) + 1)]
        ends = [0, 1, 3, blocks[0] + 1, T]
        self.groups = [(a, e) for a, e in zip(ends[:-1], ends[1:]) if e > a]


def kernel(plan, n_rows, frames, w_x, w_h, bias_in, h_init, c_init, hout, hpeer, cout, cpeer,
           bias, hgo, cgo, xgo, xin, hst, cst, xh_even, xh_odd, cbuf, shift, wbuf,
           xs_ref, xr_ref, hs_ref, hr_ref, cs_ref, cr_ref,
           s_w, s_i, s_ir, s_is, s_x, s_xr, s_xs, s_b, s_bs, s_or, s_os, here_sem):
    T, R, W, HW, HG = plan.T, plan.R, plan.W, plan.HW, plan.HG
    PAD = plan.K
    NB = len(plan.blocks)
    s = lax.axis_index("cols")
    n = lax.axis_index("rows")
    p = 1 - s
    mine, theirs = pl.ds(s * HG, HG), pl.ds(p * HG, HG)
    mine_c, theirs_c = [pl.ds(pl.multiple_of(i * HW, HW), HW) for i in (s, p)]
    has_up, has_dn = n > 0, n < n_rows - 1
    bf, f32 = jnp.bfloat16, jnp.float32

    def local(src, dst, sem):
        return pltpu.make_async_copy(src, dst, sem)

    def remote(src, dst, ssem, rsem, dev):
        return pltpu.make_async_remote_copy(
            src_ref=src, dst_ref=dst, send_sem=ssem, recv_sem=rsem, device_id=dev, device_id_type=MESH)

    peer = {"cols": p}
    side_dev = [{"rows": n - 1}, {"rows": n + 1}]
    side_ok = [has_up, has_dn]

    def each_side(do):
        for side in range(2):
            @pl.when(side_ok[side])
            def _():
                do(side)

    barrier = pltpu.get_barrier_semaphore()

    def signal(dev):
        pl.semaphore_signal(barrier, inc=1, device_id=dev, device_id_type=MESH)

    signal(peer)

    @pl.when(has_up)
    def _():
        signal(side_dev[0])


    h_own = local(h_init.at[s], hst.at[:, mine], s_i.at[0])
    c_own = local(c_init.at[s], cst.at[:, mine_c], s_i.at[1])
    x_own = [local(frames.at[a:e, s], xin.at[a:e, :, mine], s_x.at[g]) for g, (a, e) in enumerate(plan.groups)]
    h_got = local(h_init.at[p], hgo, s_i.at[2])
    c_got = local(c_init.at[p], cgo, s_i.at[3])
    x_got = [local(frames.at[a:e, p], xgo.at[a:e], s_i.at[4 + g]) for g, (a, e) in enumerate(plan.groups[:2])]
    w_copies = [local(w_h, wbuf.at[0:9, 0], s_w.at[0]), local(w_x, wbuf.at[0:9, 1], s_w.at[1]),
                local(bias_in, bias, s_w.at[2])]
    for c in [h_got, x_got[0], c_got, h_own, x_own[0], c_own, *w_copies, x_got[1], *x_own[1:]]:
        c.start()
    with jax.named_scope('barrier'):
        pl.semaphore_wait(barrier, 1 + has_dn.astype(jnp.int32))

    @pl.when(has_dn)
    def _():
        pl.semaphore_signal(here_sem, inc=1, device_id=side_dev[1], device_id_type=MESH)


    h_push = remote(hgo, hst.at[:, mine], s_is.at[0], s_ir.at[0], peer)
    c_push = remote(cgo, cst.at[:, mine_c], s_is.at[1], s_ir.at[1], peer)
    x_push = [remote((xgo if g < 2 else frames.at[:, p]).at[a:e], xin.at[a:e, :, mine], s_xs.at[g], s_xr.at[g], peer)
              for g, (a, e) in enumerate(plan.groups)]
    with jax.named_scope('got_wait'):
        for got, push in [(h_got, h_push), (x_got[0], x_push[0]), (c_got, c_push), (x_got[1], x_push[1])]:
            got.wait()
            push.start()
    for push in x_push[2:]:
        push.start()

    shift[...] = jnp.zeros_like(shift)
    low = lax.broadcasted_iota(jnp.int32, (1, LANES), 1) < CH
    low_half = low_row = low
    turn = [0]
    scale = jnp.where(low_row, 0.5, 1.0)
    lift = jnp.where(low_row, 0.5, 0.0)

    with jax.named_scope('w_wait'):
        for c in w_copies:
            c.wait()
    for tap in range(9):
        for half in range(2):
            tile = wbuf[tap, half, :, 0:LANES]
            wbuf[tap, half, :, 0:LANES] = jnp.concatenate([tile[:, CH:], tile[:, :CH]], axis=1)
    b_all = bias[...]
    rest = jnp.concatenate([b_all[:, CH:LANES], b_all[:, :CH], b_all[:, LANES:]], axis=1)
    row = lax.broadcasted_iota(jnp.int32, (CH, 4 * CH), 0)
    rows = jnp.zeros((CH, 4 * CH), f32)
    for i in range(3):
        top = (rest * (1 - 2.0 ** -8)).astype(bf).astype(f32) if i == 0 else rest.astype(bf).astype(f32)
        rows = jnp.where(row == i, top, rows)
        rest = rest - top
    wbuf[9, 0] = rows.astype(bf)
    wbuf[9, 1] = jnp.zeros((CH, 4 * CH), bf)
    ones = jnp.where(lax.broadcasted_iota(jnp.int32, (1, LANES), 1) < 3, 1.0, 0.0).astype(bf)

    def pack(v):
        return jnp.concatenate([v[:, :HG], v[:, HG:]], axis=3)

    def unpack(v):
        return jnp.concatenate([v[..., :CH], v[..., CH:]], axis=1)

    def masked(r, v):
        if 0 <= r < R:
            return v
        return lax.select(jnp.broadcast_to(has_up if r < 0 else has_dn, v.shape), v, jnp.zeros_like(v))

    def emit(t, lo, hi, hx):
        nxt = xh_even if t % 2 == 0 else xh_odd
        at, to = slot(lo, hi), cells_of(lo, hi)
        shift[at, 8:8 + W, :] = hx.reshape(hi - lo, W, LANES)
        nxt[1, to] = hx.astype(bf)
        nxt[0, to] = shift[at, 7:7 + W, :].reshape(hx.shape).astype(bf)
        nxt[2, to] = shift[at, 9:9 + W, :].reshape(hx.shape).astype(bf)

    def cells_of(lo, hi):
        return slice((lo + PAD) * W, (hi + PAD) * W)

    def slot(lo, hi):
        if turn[0] + hi - lo > RING:
            turn[0] = 0
        turn[0] += hi - lo
        return slice(turn[0] - (hi - lo), turn[0])

    def flat(v):
        return v.reshape(-1, v.shape[-1])

    def x_rows(t, lo, hi):
        if lo >= 0 and hi <= R:
            return flat(xin[t, lo:hi].astype(f32))
        side, i = (0, lo + plan.xrows[t]) if lo < 0 else (1, lo - R)
        return flat(unpack(xr_ref[side, plan.xat[t] + i:plan.xat[t] + i + hi - lo].astype(f32)))

    def wait_x(g):
        if g < len(plan.groups):
            x_own[g].wait()
            x_push[g].wait_recv()

    def border(b, kind, side):
        k, f = plan.blocks[b], plan.first[b]
        src, dst, at, end = [
            (hs_ref, hr_ref, plan.hat[b], plan.hat[b + 1]),
            (cs_ref, cr_ref, plan.cat[b], plan.cat[b + 1]),
            (xs_ref, xr_ref, plan.xat[f], plan.xat[f + 1]),
            (xs_ref, xr_ref, plan.xat[f + 1], plan.xat[f + 3]),
            (xs_ref, xr_ref, plan.xat[f + 3], plan.xat[f + k])][kind]
        return remote(src.at[side, at:end], dst.at[1 - side, at:end],
                      s_bs.at[min(kind, 2), side], s_b.at[kind, 1 - side, b], side_dev[side])

    def pack_x(t0, t1):
        for side in range(2):
            for t in range(t0, t1):
                m = plan.xrows[t]
                lo = 0 if side == 0 else R - m
                xs_ref[side, plan.xat[t]:plan.xat[t] + m] = pack(xin[t, lo:lo + m])

    def start_border(b, *kinds):
        each_side(lambda side: [border(b, kind, side).start() for kind in kinds])

    far = lax.rem(n, FAR) == 0

    def start_first(side, late, *kinds):
        ok = has_dn if side else jnp.logical_and(has_up, far if late else jnp.logical_not(far))

        @pl.when(ok)
        def _():
            if not side and 0 in kinds:
                pl.semaphore_wait(here_sem, 1)
            for kind in kinds:
                border(0, kind, side).start()

    def wait_border(b, *kinds):
        each_side(lambda side: [border(b, kind, 1 - side).wait_recv() for kind in kinds])

    def pack_h(b, h_rows):
        k = plan.blocks[b]
        for side in range(2):
            lo = 0 if side == 0 else R - k
            hs_ref[side, plan.hat[b]:plan.hat[b] + k] = pack(h_rows[lo:lo + k])

    def pack_c(b):
        k = plan.blocks[b]
        for side in range(2):
            lo = 0 if side == 0 else R - (k - 1)
            c = cbuf[cells_of(lo, lo + k - 1)].reshape(k - 1, W, LANES)
            cs_ref[side, plan.cat[b]:plan.cat[b] + k - 1] = jnp.where(low_half, c[:, :HW], c[:, HW:])

    weights = wbuf[...].reshape(10 * LANES, 4 * CH)

    def dot(t, lo, hi):
        cur = xh_even if t % 2 == 0 else xh_odd
        taps = [cur[dc, cells_of(lo + dr - 1, hi + dr - 1)] for dr in range(3) for dc in range(3)]
        taps.append(jnp.broadcast_to(ones, taps[0].shape))
        return jnp.dot(jnp.concatenate(taps, axis=1), weights, preferred_element_type=f32)

    def cells(t, lo, hi, gates):
        fi = jnp.tanh(gates[:, :LANES] * 0.5) * 0.5 + 0.5
        og = jnp.tanh(gates[:, LANES:] * scale) * scale + lift
        at = cells_of(lo, hi)
        prod = fi * lax.select(jnp.broadcast_to(low, og.shape), cbuf[at], og)
        c = prod + pltpu.roll(prod, CH, 1)
        h = (og * jnp.tanh(c))[:, :CH]
        if t == T - 1:
            cout[lo:hi] = c[:, :CH].reshape(hi - lo, W, CH)
        else:
            cbuf[at] = c
        for a, e in ((lo, min(hi, 0)), (max(lo, 0), min(hi, R)), (max(lo, R), hi)):
            if a >= e:
                continue
            part = h[(a - lo) * W:(e - lo) * W]
            if a >= 0 and e <= R:
                hout[t, a:e] = part.reshape(e - a, 2 * HG, COLS, CH).astype(bf)
            if t < T - 1:
                emit(t + 1, a, e, masked(a, jnp.concatenate([part, x_rows(t + 1, a, e)], axis=1)))

    pending = []

    def piece(at, ahead=1):
        t, lo, hi = at
        while any(u == t - 1 and a <= hi and lo <= e for u, a, e, _ in pending):
            cells(*pending.pop(0))
        pending.append((*at, dot(*at)))
        flush(ahead)

    def flush(left=0):
        while len(pending) > left:
            cells(*pending.pop(0))

    def push_h(t0, t1, lo=0, hi=R):
        rows = slice(lo, hi)
        remote(hout.at[t0:t1, rows, theirs], hpeer.at[t0:t1, rows], s_os.at[0], s_or.at[0], peer).start()

    def push_c(lo, hi):
        remote(cout.at[lo:hi, theirs_c], cpeer.at[lo:hi], s_os.at[1], s_or.at[1], peer).start()

    with jax.named_scope('state_wait'):
        for c in [h_own, x_own[0]]:
            c.wait()
        for c in [h_push, x_push[0]]:
            c.wait_recv()
    pack_h(0, hst)
    pack_x(0, 1)
    start_first(1, False, 0, 2)
    start_first(0, False, 0, 2)
    for lo, hi in cuts(0, R):
        emit(0, lo, hi, jnp.concatenate([flat(hst[lo:hi].astype(f32)), x_rows(0, lo, hi)], axis=1))

    for b, k in enumerate(plan.blocks):
        f = plan.first[b]
        last = b + 1 == NB

        def inner(o):
            if o == 0:
                got = [*cuts(k + 1, R - 1 - k), *cuts(1, k + 1), *cuts(R - 1 - k, R - 1)]
            else:
                got = cuts(o + 1, R - 1 - o)
                got = got[1:-1] + [got[0], got[-1]]
            return [(f + o, lo, hi) for lo, hi in got]

        early = [at for o in range(k) for at in inner(o)]
        late = early[len(early) - LATE[b]:]
        for o in range(k):
            pieces = [at for at in early[:len(early) - LATE[b]] if at[0] == f + o]
            first = 0
            if o == 0 and b:
                piece(pieces[0], 9)
                flush(1)
                pack_h(b, hout.at[f - 1])
                pack_c(b)
                with jax.named_scope(f'send{b}'):
                    start_border(b, 0, 1)
                first = 1
            if b == 0 and o == 0:
                for at in pieces[:2]:
                    piece(at, 9)
                with jax.named_scope('x_wait0'):
                    c_own.wait()
                    c_push.wait_recv()
                    wait_x(1)
                for at in pieces[2:4]:
                    piece(at, 9)
                c0 = flat(cst[...])
                cbuf[cells_of(0, R)] = jnp.concatenate([c0, c0], axis=1)
                pack_c(0)
                pack_x(1, 3)
                start_first(1, False, 1, 3)
                start_first(0, False, 1, 3)
                first = 4
            if b == 0 and o == 2:
                for at in pieces[:2]:
                    piece(at, 9)
                flush(2)
                with jax.named_scope('x_wait1'):
                    wait_x(2)
                for at in pieces[2:4]:
                    piece(at, 9)
                pack_x(3, k)
                for side in range(2):
                    start_first(side, False, 4)
                start_first(0, True, 4)
                first = 4
            for at in pieces[first:]:
                piece(at)
            if o == 0 and b == 0:
                with jax.named_scope('upsend'):
                    start_first(0, True, 0, 1, 2, 3)
            if o == 0 and b and not last:
                pack_x(f + k, f + k + plan.blocks[b + 1])
        with jax.named_scope(f'mid{b}'):
            wait_border(b, 0, 2, *((3, 4) if b else ()))
        if b == 0:
            wait_x(3)
        elif not last:
            start_border(b + 1, 2, 3, 4)
        if b:
            push_h(plan.first[b - 1], f)
        piece(late.pop(0), 3)
        for side in range(2):
            lo = -k if side == 0 else R
            h = flat(unpack(hr_ref[side, plan.hat[b]:plan.hat[b] + k].astype(f32)))
            emit(f, lo, lo + k, masked(lo, jnp.concatenate([h, x_rows(f, lo, lo + k)], axis=1)))
        for o in range(k):
            m = k - 1 - o
            top, bottom = cuts(-m, o + 1, BORDER), cuts(R - 1 - o, R + m, BORDER)
            for lo, hi in top:
                piece((f + o, lo, hi), 9 if o == 0 else 1)
                if b == 0 and o == 2 and lo == top[0][0]:
                    with jax.named_scope('mid4'):
                        wait_border(0, 4)
                if last and o == k - 1 and lo == top[0][0]:
                    push_h(T - 2, T - 1)
            for lo, hi in bottom:
                piece((f + o, lo, hi), 9 if o == 0 else 1)
            if o == 0:
                with jax.named_scope(f'midc{b}'):
                    wait_border(b, 1, *(() if b else (3,)))
                for side in range(2):
                    lo = -(k - 1) if side == 0 else R
                    packed = cr_ref[side, plan.cat[b]:plan.cat[b] + k - 1]
                    both = jnp.concatenate([packed, pltpu.roll(packed, CH, 2)], axis=1)
                    cbuf[cells_of(lo, lo + k - 1)] = flat(both)
                while late:
                    piece(late.pop(0), 3)
            if o == 0 and b == 0 and not last:
                pack_x(f + k, f + k + plan.blocks[b + 1])
                start_border(b + 1, 2, 3, 4)
            if last and o == k // 2:
                push_h(f, f + o)
            if last and o == k - 2:
                push_h(f + k // 2, f + o)
                push_h(T - 1, T, k, R - k)
                push_c(k, R - k)
        assert not late
    k, (t, lo, hi, _) = plan.blocks[-1], pending[-1]
    flush(1)
    for a, e in ((0, k), (R - k, lo)):
        push_h(t, t + 1, a, e)
        push_c(a, e)
    flush()
    push_h(t, t + 1, lo, hi)
    push_c(lo, hi)

    with jax.named_scope('end_wait'):
        for c in [h_push, c_push, *x_push]:
            c.wait_send()

        def wait_sends(side):
            for kind, ref in enumerate((hs_ref, cs_ref, xs_ref)):
                local(ref.at[side], ref.at[side], s_bs.at[kind, side]).wait()

        each_side(wait_sends)
        for sem in (s_os, s_or):
            local(hpeer, hpeer, sem.at[0]).wait()
            local(cpeer, cpeer, sem.at[1]).wait()


def store(hout, hpeer, cout, cpeer, h_all, c_final, sems):
    s = lax.axis_index("cols")
    HG, HW = hpeer.shape[2], cpeer.shape[1]
    mine = pl.ds(pl.multiple_of(s * HW, HW), HW)
    copies = [pltpu.make_async_copy(hout.at[:, :, pl.ds(s * HG, HG)], h_all.at[:, s], sems.at[0]),
              pltpu.make_async_copy(hpeer, h_all.at[:, 1 - s], sems.at[1]),
              pltpu.make_async_copy(cout.at[:, mine], c_final.at[s], sems.at[2]),
              pltpu.make_async_copy(cpeer, c_final.at[1 - s], sems.at[3])]
    for c in copies:
        c.start()
    for c in copies:
        c.wait()


def run(blocks, n_rows, frames, w_x, w_h, gate_bias, h_init, c_init):
    T, S, R, HW = frames.shape[:4]
    W, HG = 2 * HW, HW // COLS
    plan = Plan(blocks, T, R, W)
    NB, PAD, G = len(blocks), plan.K, len(plan.groups)
    bf, f32 = jnp.bfloat16, jnp.float32
    vm, dma = pltpu.VMEM, pltpu.SemaphoreType.DMA
    hbm = pl.BlockSpec(memory_space=pltpu.HBM)
    vmem = pl.BlockSpec(memory_space=pltpu.VMEM)
    tiled = frames.reshape(T, S, R, HG, COLS, CH)
    parts = pl.pallas_call(
        functools.partial(kernel, plan, n_rows),
        out_shape=(vm((T, R, 2 * HG, COLS, CH), bf), vm((T, R, HG, COLS, CH), bf), vm((R, W, CH), f32),
                   vm((R, HW, CH), f32)),
        in_specs=[hbm] * 6,
        out_specs=(vmem,) * 4,
        scratch_shapes=[
            vm((1, 4 * CH), f32), vm((R, HG, COLS, CH), bf), vm((R, HW, CH), f32),
            vm((plan.groups[1][1], R, HG, COLS, CH), bf),
            vm((T, R, 2 * HG, COLS, CH), bf), vm((R, 2 * HG, COLS, CH), bf), vm((R, W, CH), f32),
            vm((3, (R + 2 * PAD) * W, LANES), bf), vm((3, (R + 2 * PAD) * W, LANES), bf),
            vm(((R + 2 * PAD) * W, LANES), f32), vm((RING, W + 16, LANES), f32), vm((10, 2, CH, 4 * CH), bf),
            vm((2, plan.xat[-1], HG, COLS, LANES), bf), vm((2, plan.xat[-1], HG, COLS, LANES), bf),
            vm((2, plan.hat[-1], HG, COLS, LANES), bf), vm((2, plan.hat[-1], HG, COLS, LANES), bf),
            vm((2, plan.cat[-1], HW, LANES), f32), vm((2, plan.cat[-1], HW, LANES), f32),
            dma((3,)), dma((6,)), dma((2,)), dma((2,)), dma((G,)), dma((G,)), dma((G,)),
            dma((5, 2, NB)), dma((3, 2)), dma((2,)), dma((2,)), pltpu.SemaphoreType.REGULAR],
        compiler_params=pltpu.CompilerParams(collective_id=0, has_side_effects=True, vmem_limit_bytes=46 * 2**20),
    )(tiled, w_x.reshape(9, CH, 4 * CH), w_h.reshape(9, CH, 4 * CH), gate_bias.reshape(1, -1),
      h_init.reshape(S, R, HG, COLS, CH), c_init)
    h_all, c_final = pl.pallas_call(
        store,
        out_shape=(jax.ShapeDtypeStruct(tiled.shape, bf), jax.ShapeDtypeStruct(c_init.shape, f32)),
        in_specs=[vmem] * 4,
        out_specs=(hbm, hbm),
        scratch_shapes=[dma((4,))],
        compiler_params=pltpu.CompilerParams(vmem_limit_bytes=2**20),
    )(*[pltpu.with_memory_space_constraint(a, pltpu.VMEM) for a in parts])
    return h_all.reshape(frames.shape), c_final


def solution(mesh, K=None):
    n_rows = mesh.shape["rows"]
    frame_spec = P(None, "batch", "rows", "cols", None)
    state_spec = P("batch", "rows", "cols", None)
    blocks = BLOCKS if K is None else K
    return jax.shard_map(functools.partial(run, blocks, n_rows), mesh=mesh,
                         in_specs=(frame_spec, P(), P(), P(), state_spec, state_spec),
                         out_specs=(frame_spec, state_spec), check_vma=False)
```

```python
import functools

import jax
import jax.numpy as jnp
from jax import lax
from jax.experimental import pallas as pl
from jax.experimental.pallas import tpu as pltpu
from jax.sharding import PartitionSpec as P

MESH = pl.DeviceIdType.MESH
CH = 64
LANES = 128
COLS = 8
PIECE = 4
RING = 8
BLOCKS = (8, 8)
LATE = (3, 3)
BORDER = 4
FAR = 16


def cuts(lo, hi, size=PIECE):
    n = max(1, (hi - lo) // size)
    edges = [lo + i * size for i in range(n)] + [hi]
    return list(zip(edges[:-1], edges[1:]))


class Plan:
    def __init__(self, blocks, T, R, W):
        assert sum(blocks) == T
        self.blocks, self.T, self.R, self.W, self.HW, self.HG = blocks, T, R, W, W // 2, W // 2 // COLS
        self.K = max(blocks)
        self.first = [sum(blocks[:b]) for b in range(len(blocks))]
        self.of = [(b, o) for b, k in enumerate(blocks) for o in range(k)]
        self.xrows = [blocks[b] - o for b, o in self.of]
        self.xat = [sum(self.xrows[:t]) for t in range(T + 1)]
        self.parts = [[(0, 1), (1, 2), (2, 3), (3, k)] if b == 0 else [(0, k)] for b, k in enumerate(blocks)]
        self.hat = [sum(blocks[:b]) for b in range(len(blocks) + 1)]
        self.cat = [sum(k - 1 for k in blocks[:b]) for b in range(len(blocks) + 1)]
        ends = [0, 1, 3, blocks[0] + 1, T]
        self.groups = [(a, e) for a, e in zip(ends[:-1], ends[1:]) if e > a]


def kernel(plan, n_rows, frames, w_x, w_h, bias_in, h_init, c_init, hout, hpeer, cout, cpeer,
           bias, hgo, cgo, cgp, cin, xgo, xin, hst, cst, xh_even, xh_odd, cbuf, shift, wbuf,
           xs_ref, xr_ref, hs_ref, hr_ref, cs_ref, cr_ref,
           s_w, s_i, s_ir, s_is, s_x, s_xr, s_xs, s_b, s_bs, s_or, s_os, here_sem):
    T, R, W, HW, HG = plan.T, plan.R, plan.W, plan.HW, plan.HG
    PAD = plan.K
    NB = len(plan.blocks)
    s = lax.axis_index("cols")
    n = lax.axis_index("rows")
    p = 1 - s
    mine, theirs = pl.ds(s * HG, HG), pl.ds(p * HG, HG)
    mine_c, theirs_c = [pl.ds(pl.multiple_of(i * HW, HW), HW) for i in (s, p)]
    has_up, has_dn = n > 0, n < n_rows - 1
    bf, f32 = jnp.bfloat16, jnp.float32

    def local(src, dst, sem):
        return pltpu.make_async_copy(src, dst, sem)

    def remote(src, dst, ssem, rsem, dev):
        return pltpu.make_async_remote_copy(
            src_ref=src, dst_ref=dst, send_sem=ssem, recv_sem=rsem, device_id=dev, device_id_type=MESH)

    peer = {"cols": p}
    side_dev = [{"rows": n - 1}, {"rows": n + 1}]
    side_ok = [has_up, has_dn]

    def each_side(do):
        for side in range(2):
            @pl.when(side_ok[side])
            def _():
                do(side)

    barrier = pltpu.get_barrier_semaphore()

    def signal(dev):
        pl.semaphore_signal(barrier, inc=1, device_id=dev, device_id_type=MESH)

    signal(peer)

    @pl.when(has_up)
    def _():
        signal(side_dev[0])


    h_own = local(h_init.at[s], hst.at[:, mine], s_i.at[0])
    c_own = local(c_init.at[s], cst.at[:, mine_c], s_i.at[1])
    x_own = [local(frames.at[a:e, s], xin.at[a:e, :, mine], s_x.at[g]) for g, (a, e) in enumerate(plan.groups)]
    h_got = local(h_init.at[p], hgo, s_i.at[2])
    c_got = local(c_init.at[p], cgo, s_i.at[3])
    x_got = [local(frames.at[a:e, p], xgo.at[a:e], s_i.at[4 + g]) for g, (a, e) in enumerate(plan.groups[:2])]
    w_copies = [local(w_h, wbuf.at[0:9, 0], s_w.at[0]), local(w_x, wbuf.at[0:9, 1], s_w.at[1]),
                local(bias_in, bias, s_w.at[2])]
    for c in [h_got, x_got[0], c_got, h_own, x_own[0], c_own, *w_copies, x_got[1], *x_own[1:]]:
        c.start()
    with jax.named_scope('barrier'):
        pl.semaphore_wait(barrier, 1 + has_dn.astype(jnp.int32))

    @pl.when(has_dn)
    def _():
        pl.semaphore_signal(here_sem, inc=1, device_id=side_dev[1], device_id_type=MESH)


    h_push = remote(hgo, hst.at[:, mine], s_is.at[0], s_ir.at[0], peer)
    c_push = remote(cgp, cin, s_is.at[1], s_ir.at[1], peer)
    x_push = [remote((xgo if g < 2 else frames.at[:, p]).at[a:e], xin.at[a:e, :, mine], s_xs.at[g], s_xr.at[g], peer)
              for g, (a, e) in enumerate(plan.groups)]
    with jax.named_scope('got_wait'):
        for got, push in [(h_got, h_push), (x_got[0], x_push[0]), (c_got, c_push), (x_got[1], x_push[1])]:
            got.wait()
            if push is c_push:
                cgp[...] = jnp.concatenate([cgo[:, :HW // 2], cgo[:, HW // 2:]], axis=2)
            push.start()
    for push in x_push[2:]:
        push.start()

    shift[...] = jnp.zeros_like(shift)
    low = lax.broadcasted_iota(jnp.int32, (1, LANES), 1) < CH
    low_half = low_row = low
    turn = [0]
    scale = jnp.where(low_row, 0.5, 1.0)
    lift = jnp.where(low_row, 0.5, 0.0)

    with jax.named_scope('w_wait'):
        for c in w_copies:
            c.wait()
    for tap in range(9):
        for half in range(2):
            tile = wbuf[tap, half, :, 0:LANES]
            wbuf[tap, half, :, 0:LANES] = jnp.concatenate([tile[:, CH:], tile[:, :CH]], axis=1)
    b_all = bias[...]
    rest = jnp.concatenate([b_all[:, CH:LANES], b_all[:, :CH], b_all[:, LANES:]], axis=1)
    row = lax.broadcasted_iota(jnp.int32, (CH, 4 * CH), 0)
    rows = jnp.zeros((CH, 4 * CH), f32)
    for i in range(3):
        top = (rest * (1 - 2.0 ** -8)).astype(bf).astype(f32) if i == 0 else rest.astype(bf).astype(f32)
        rows = jnp.where(row == i, top, rows)
        rest = rest - top
    wbuf[9, 0] = rows.astype(bf)
    wbuf[9, 1] = jnp.zeros((CH, 4 * CH), bf)
    ones = jnp.where(lax.broadcasted_iota(jnp.int32, (1, LANES), 1) < 3, 1.0, 0.0).astype(bf)

    def pack(v):
        return jnp.concatenate([v[:, :HG], v[:, HG:]], axis=3)

    def unpack(v):
        return jnp.concatenate([v[..., :CH], v[..., CH:]], axis=1)

    def masked(r, v):
        if 0 <= r < R:
            return v
        return lax.select(jnp.broadcast_to(has_up if r < 0 else has_dn, v.shape), v, jnp.zeros_like(v))

    def emit(t, lo, hi, hx):
        nxt = xh_even if t % 2 == 0 else xh_odd
        at, to = slot(lo, hi), cells_of(lo, hi)
        shift[at, 8:8 + W, :] = hx.reshape(hi - lo, W, LANES)
        nxt[1, to] = hx.astype(bf)
        nxt[0, to] = shift[at, 7:7 + W, :].reshape(hx.shape).astype(bf)
        nxt[2, to] = shift[at, 9:9 + W, :].reshape(hx.shape).astype(bf)

    def cells_of(lo, hi):
        return slice((lo + PAD) * W, (hi + PAD) * W)

    def slot(lo, hi):
        if turn[0] + hi - lo > RING:
            turn[0] = 0
        turn[0] += hi - lo
        return slice(turn[0] - (hi - lo), turn[0])

    def flat(v):
        return v.reshape(-1, v.shape[-1])

    def x_rows(t, lo, hi):
        if lo >= 0 and hi <= R:
            return flat(xin[t, lo:hi].astype(f32))
        side, i = (0, lo + plan.xrows[t]) if lo < 0 else (1, lo - R)
        return flat(unpack(xr_ref[side, plan.xat[t] + i:plan.xat[t] + i + hi - lo].astype(f32)))

    def wait_x(g):
        if g < len(plan.groups):
            x_own[g].wait()
            x_push[g].wait_recv()

    def border(b, kind, side):
        f = plan.first[b]
        if kind < 2:
            src, dst, at = [(hs_ref, hr_ref, plan.hat), (cs_ref, cr_ref, plan.cat)][kind]
            at, end = at[b], at[b + 1]
        else:
            src, dst = xs_ref, xr_ref
            at, end = [plan.xat[f + o] for o in plan.parts[b][kind - 2]]
        return remote(src.at[side, at:end], dst.at[1 - side, at:end],
                      s_bs.at[min(kind, 2), side], s_b.at[kind, 1 - side, b], side_dev[side])

    def pack_x(t0, t1):
        for side in range(2):
            for t in range(t0, t1):
                m = plan.xrows[t]
                lo = 0 if side == 0 else R - m
                xs_ref[side, plan.xat[t]:plan.xat[t] + m] = pack(xin[t, lo:lo + m])

    def start_border(b, *kinds):
        each_side(lambda side: [border(b, kind, side).start() for kind in kinds])

    far = lax.rem(n, FAR) == 0

    def start_first(side, late, *kinds):
        ok = has_dn if side else jnp.logical_and(has_up, far if late else jnp.logical_not(far))

        @pl.when(ok)
        def _():
            if not side and 0 in kinds:
                pl.semaphore_wait(here_sem, 1)
            for kind in kinds:
                border(0, kind, side).start()

    def wait_border(b, *kinds):
        each_side(lambda side: [border(b, kind, 1 - side).wait_recv() for kind in kinds])

    def pack_h(b, h_rows):
        k = plan.blocks[b]
        for side in range(2):
            lo = 0 if side == 0 else R - k
            hs_ref[side, plan.hat[b]:plan.hat[b] + k] = pack(h_rows[lo:lo + k])

    def pack_c(b):
        k = plan.blocks[b]
        for side in range(2):
            lo = 0 if side == 0 else R - (k - 1)
            c = cbuf[cells_of(lo, lo + k - 1)].reshape(k - 1, W, LANES)
            cs_ref[side, plan.cat[b]:plan.cat[b] + k - 1] = jnp.where(low_half, c[:, :HW], c[:, HW:])

    weights = wbuf[...].reshape(10 * LANES, 4 * CH)

    def dot(t, lo, hi):
        cur = xh_even if t % 2 == 0 else xh_odd
        taps = [cur[dc, cells_of(lo + dr - 1, hi + dr - 1)] for dr in range(3) for dc in range(3)]
        taps.append(jnp.broadcast_to(ones, taps[0].shape))
        return jnp.dot(jnp.concatenate(taps, axis=1), weights, preferred_element_type=f32)

    def cells(t, lo, hi, gates):
        fi = jnp.tanh(gates[:, :LANES] * 0.5) * 0.5 + 0.5
        og = jnp.tanh(gates[:, LANES:] * scale) * scale + lift
        at = cells_of(lo, hi)
        prod = fi * lax.select(jnp.broadcast_to(low, og.shape), cbuf[at], og)
        c = prod + pltpu.roll(prod, CH, 1)
        h = (og * jnp.tanh(c))[:, :CH]
        if t == T - 1:
            c = c.reshape(hi - lo, 2, 2, HW // 2, LANES)
            for half in range(2):
                both = c[:, half, 0]
                cout[half, lo:hi] = lax.select(jnp.broadcast_to(low, both.shape), both, c[:, half, 1])
        else:
            cbuf[at] = c
        for a, e in ((lo, min(hi, 0)), (max(lo, 0), min(hi, R)), (max(lo, R), hi)):
            if a >= e:
                continue
            part = h[(a - lo) * W:(e - lo) * W]
            if a >= 0 and e <= R:
                hout[t, a:e] = part.reshape(e - a, 2 * HG, COLS, CH).astype(bf)
            if t < T - 1:
                emit(t + 1, a, e, masked(a, jnp.concatenate([part, x_rows(t + 1, a, e)], axis=1)))

    pending = []

    def piece(at, ahead=1):
        t, lo, hi = at
        while any(u == t - 1 and a <= hi and lo <= e for u, a, e, _ in pending):
            cells(*pending.pop(0))
        pending.append((*at, dot(*at)))
        flush(ahead)

    def flush(left=0):
        while len(pending) > left:
            cells(*pending.pop(0))

    def push_h(t0, t1, lo=0, hi=R):
        rows = slice(lo, hi)
        remote(hout.at[t0:t1, rows, theirs], hpeer.at[t0:t1, rows], s_os.at[0], s_or.at[0], peer).start()

    def push_c(lo, hi):
        remote(cout.at[p, lo:hi], cpeer.at[lo:hi], s_os.at[1], s_or.at[1], peer).start()

    with jax.named_scope('state_wait'):
        for c in [h_own, x_own[0]]:
            c.wait()
        for c in [h_push, x_push[0]]:
            c.wait_recv()
    pack_h(0, hst)
    pack_x(0, 1)
    start_first(1, False, 0, 2)
    start_first(0, False, 0, 2)
    for lo, hi in cuts(0, R):
        emit(0, lo, hi, jnp.concatenate([flat(hst[lo:hi].astype(f32)), x_rows(0, lo, hi)], axis=1))

    for b, k in enumerate(plan.blocks):
        f = plan.first[b]
        last = b + 1 == NB

        def inner(o):
            if o == 0:
                got = [*cuts(k + 1, R - 1 - k), *cuts(1, k + 1), *cuts(R - 1 - k, R - 1)]
            else:
                got = cuts(o + 1, R - 1 - o)
                got = got[1:-1] + [got[0], got[-1]]
            return [(f + o, lo, hi) for lo, hi in got]

        early = [at for o in range(k) for at in inner(o)]
        late = early[len(early) - LATE[b]:]
        for o in range(k):
            pieces = [at for at in early[:len(early) - LATE[b]] if at[0] == f + o]
            first = 0
            if o == 0 and b:
                piece(pieces[0], 9)
                flush(1)
                pack_h(b, hout.at[f - 1])
                pack_c(b)
                with jax.named_scope(f'send{b}'):
                    start_border(b, 0, 1)
                first = 1
            if b == 0 and o == 0:
                for at in pieces[:2]:
                    piece(at, 9)
                with jax.named_scope('x_wait0'):
                    c_own.wait()
                    c_push.wait_recv()
                    wait_x(1)
                for at in pieces[2:4]:
                    piece(at, 9)
                c0 = cin[...]
                cst[:, theirs_c] = jnp.concatenate([c0[:, :, :CH], c0[:, :, CH:]], axis=1)
                c0 = flat(cst[...])
                cbuf[cells_of(0, R)] = jnp.concatenate([c0, c0], axis=1)
                pack_c(0)
                pack_x(1, 3)
                start_first(1, False, 1, 3, 4)
                start_first(0, False, 1, 3, 4)
                first = 4
            if b == 0 and o == 2:
                for at in pieces[:2]:
                    piece(at, 9)
                flush(2)
                with jax.named_scope('x_wait1'):
                    wait_x(2)
                for at in pieces[2:4]:
                    piece(at, 9)
                pack_x(3, k)
                for side in range(2):
                    start_first(side, False, 5)
                start_first(0, True, 5)
                first = 4
            for at in pieces[first:]:
                piece(at)
            if o == 0 and b == 0:
                with jax.named_scope('upsend'):
                    start_first(0, True, 0, 2, 1, 3, 4)
            if o == 0 and b and not last:
                pack_x(f + k, f + k + plan.blocks[b + 1])
        with jax.named_scope(f'mid{b}'):
            wait_border(b, 0, 2)
        if b == 0:
            wait_x(3)
        elif not last:
            start_border(b + 1, 2)
        if b:
            push_h(plan.first[b - 1], f)
        piece(late.pop(0), 3)
        for side in range(2):
            lo = -k if side == 0 else R
            h = flat(unpack(hr_ref[side, plan.hat[b]:plan.hat[b] + k].astype(f32)))
            emit(f, lo, lo + k, masked(lo, jnp.concatenate([h, x_rows(f, lo, lo + k)], axis=1)))
        for o in range(k):
            m = k - 1 - o
            top, bottom = cuts(-m, o + 1, BORDER), cuts(R - 1 - o, R + m, BORDER)
            for lo, hi in top:
                piece((f + o, lo, hi), 9 if o == 0 else 1)
                if lo != top[0][0]:
                    continue
                if b == 0 and o in (1, 2):
                    with jax.named_scope(f'midx{o}'):
                        wait_border(0, 3 + o)
                if last and o == k // 2:
                    push_h(f, f + o)
                if last and o == k - 2:
                    push_h(f + k // 2, f + o)
                    push_h(T - 1, T, k, R - k)
                    push_c(k, R - k)
                if last and o == k - 1:
                    push_h(T - 2, T - 1)
            for lo, hi in bottom:
                piece((f + o, lo, hi), 9 if o == 0 else 1)
            if o == 0:
                with jax.named_scope(f'midc{b}'):
                    wait_border(b, 1, *(() if b else (3,)))
                for side in range(2):
                    lo = -(k - 1) if side == 0 else R
                    packed = cr_ref[side, plan.cat[b]:plan.cat[b] + k - 1]
                    both = jnp.concatenate([packed, pltpu.roll(packed, CH, 2)], axis=1)
                    cbuf[cells_of(lo, lo + k - 1)] = flat(both)
                while late:
                    piece(late.pop(0), 3)
            if o == 0 and b == 0 and not last:
                pack_x(f + k, f + k + plan.blocks[b + 1])
                start_border(b + 1, 2)
        assert not late
    flush()
    k = plan.blocks[-1]
    for lo, hi in ((0, k), (R - k, R)):
        push_h(T - 1, T, lo, hi)
        push_c(lo, hi)

    with jax.named_scope('end_wait'):
        for c in [h_push, c_push, *x_push]:
            c.wait_send()

        def wait_sends(side):
            for kind, ref in enumerate((hs_ref, cs_ref, xs_ref)):
                local(ref.at[side], ref.at[side], s_bs.at[kind, side]).wait()

        each_side(wait_sends)
        for sem in (s_os, s_or):
            local(hpeer, hpeer, sem.at[0]).wait()
            local(cpeer, cpeer, sem.at[1]).wait()


def store(hout, hpeer, cout, cpeer, h_all, c_final, c_tile, sems):
    s = lax.axis_index("cols")
    HG = hpeer.shape[2]
    copies = [pltpu.make_async_copy(hout.at[:, :, pl.ds(s * HG, HG)], h_all.at[:, s], sems.at[0]),
              pltpu.make_async_copy(hpeer, h_all.at[:, 1 - s], sems.at[1]),
              pltpu.make_async_copy(c_tile.at[0], c_final.at[s], sems.at[2]),
              pltpu.make_async_copy(c_tile.at[1], c_final.at[1 - s], sems.at[3])]
    for c in copies[:2]:
        c.start()
    for i, packed in enumerate((cout[s], cpeer[...])):
        c_tile[i] = jnp.concatenate([packed[:, :, :CH], packed[:, :, CH:]], axis=1)
    for c in copies[2:]:
        c.start()
    for c in copies:
        c.wait()


def run(blocks, n_rows, frames, w_x, w_h, gate_bias, h_init, c_init):
    T, S, R, HW = frames.shape[:4]
    W, HG = 2 * HW, HW // COLS
    plan = Plan(blocks, T, R, W)
    NB, PAD, G = len(blocks), plan.K, len(plan.groups)
    bf, f32 = jnp.bfloat16, jnp.float32
    vm, dma = pltpu.VMEM, pltpu.SemaphoreType.DMA
    hbm = pl.BlockSpec(memory_space=pltpu.HBM)
    vmem = pl.BlockSpec(memory_space=pltpu.VMEM)
    tiled = frames.reshape(T, S, R, HG, COLS, CH)
    parts = pl.pallas_call(
        functools.partial(kernel, plan, n_rows),
        out_shape=(vm((T, R, 2 * HG, COLS, CH), bf), vm((T, R, HG, COLS, CH), bf),
                   vm((2, R, HW // 2, LANES), f32), vm((R, HW // 2, LANES), f32)),
        in_specs=[hbm] * 6,
        out_specs=(vmem,) * 4,
        scratch_shapes=[
            vm((1, 4 * CH), f32), vm((R, HG, COLS, CH), bf), vm((R, HW, CH), f32),
            vm((R, HW // 2, LANES), f32), vm((R, HW // 2, LANES), f32),
            vm((plan.groups[1][1], R, HG, COLS, CH), bf),
            vm((T, R, 2 * HG, COLS, CH), bf), vm((R, 2 * HG, COLS, CH), bf), vm((R, W, CH), f32),
            vm((3, (R + 2 * PAD) * W, LANES), bf), vm((3, (R + 2 * PAD) * W, LANES), bf),
            vm(((R + 2 * PAD) * W, LANES), f32), vm((RING, W + 16, LANES), f32), vm((10, 2, CH, 4 * CH), bf),
            vm((2, plan.xat[-1], HG, COLS, LANES), bf), vm((2, plan.xat[-1], HG, COLS, LANES), bf),
            vm((2, plan.hat[-1], HG, COLS, LANES), bf), vm((2, plan.hat[-1], HG, COLS, LANES), bf),
            vm((2, plan.cat[-1], HW, LANES), f32), vm((2, plan.cat[-1], HW, LANES), f32),
            dma((3,)), dma((6,)), dma((2,)), dma((2,)), dma((G,)), dma((G,)), dma((G,)),
            dma((6, 2, NB)), dma((3, 2)), dma((2,)), dma((2,)), pltpu.SemaphoreType.REGULAR],
        compiler_params=pltpu.CompilerParams(collective_id=0, has_side_effects=True, vmem_limit_bytes=46 * 2**20),
    )(tiled, w_x.reshape(9, CH, 4 * CH), w_h.reshape(9, CH, 4 * CH), gate_bias.reshape(1, -1),
      h_init.reshape(S, R, HG, COLS, CH), c_init)
    h_all, c_final = pl.pallas_call(
        store,
        out_shape=(jax.ShapeDtypeStruct(tiled.shape, bf), jax.ShapeDtypeStruct(c_init.shape, f32)),
        in_specs=[vmem] * 4,
        out_specs=(hbm, hbm),
        scratch_shapes=[vm((2, R, HW, CH), f32), dma((4,))],
        compiler_params=pltpu.CompilerParams(vmem_limit_bytes=4 * 2**20),
    )(*[pltpu.with_memory_space_constraint(a, pltpu.VMEM) for a in parts])
    return h_all.reshape(frames.shape), c_final


def solution(mesh, K=None):
    n_rows = mesh.shape["rows"]
    frame_spec = P(None, "batch", "rows", "cols", None)
    state_spec = P("batch", "rows", "cols", None)
    blocks = BLOCKS if K is None else K
    return jax.shard_map(functools.partial(run, blocks, n_rows), mesh=mesh,
                         in_specs=(frame_spec, P(), P(), P(), state_spec, state_spec),
                         out_specs=(frame_spec, state_spec), check_vma=False)
```

```python
import functools

import jax
import jax.numpy as jnp
from jax import lax
from jax.experimental import pallas as pl
from jax.experimental.pallas import tpu as pltpu
from jax.sharding import PartitionSpec as P

MESH = pl.DeviceIdType.MESH
CH = 64
LANES = 128
COLS = 8
PIECE = 4
RING = 8
BLOCKS = (8, 8)
LATE = (3, 3)
BORDER = 4
FAR = 16


def cuts(lo, hi, size=PIECE):
    n = max(1, (hi - lo) // size)
    edges = [lo + i * size for i in range(n)] + [hi]
    return list(zip(edges[:-1], edges[1:]))


class Plan:
    def __init__(self, blocks, T, R, W):
        assert sum(blocks) == T
        self.blocks, self.T, self.R, self.W, self.HW, self.HG = blocks, T, R, W, W // 2, W // 2 // COLS
        self.K = max(blocks)
        self.first = [sum(blocks[:b]) for b in range(len(blocks))]
        self.of = [(b, o) for b, k in enumerate(blocks) for o in range(k)]
        self.xrows = [blocks[b] - o for b, o in self.of]
        self.xat = [sum(self.xrows[:t]) for t in range(T + 1)]
        self.parts = [[(0, 1), (1, 2), (2, 3), (3, k)] if b == 0 else [(0, k)] for b, k in enumerate(blocks)]
        self.hat = [sum(blocks[:b]) for b in range(len(blocks) + 1)]
        self.cat = [sum(k - 1 for k in blocks[:b]) for b in range(len(blocks) + 1)]
        ends = [0, 1, 3, blocks[0] + 1, T]
        self.groups = [(a, e) for a, e in zip(ends[:-1], ends[1:]) if e > a]


def kernel(plan, n_rows, frames, w_x, w_h, bias_in, h_init, c_init, hout, hpeer, cout, cpeer,
           bias, hgo, cgo, cgp, cin, xgo, xin, hst, cst, xh_even, xh_odd, cbuf, shift, wbuf,
           xs_ref, xr_ref, hs_ref, hr_ref, cs_ref, cr_ref,
           s_w, s_i, s_ir, s_is, s_x, s_xr, s_xs, s_b, s_bs, s_or, s_os, here_sem):
    T, R, W, HW, HG = plan.T, plan.R, plan.W, plan.HW, plan.HG
    PAD = plan.K
    NB = len(plan.blocks)
    s = lax.axis_index("cols")
    n = lax.axis_index("rows")
    p = 1 - s
    mine, theirs = pl.ds(s * HG, HG), pl.ds(p * HG, HG)
    mine_c, theirs_c = [pl.ds(pl.multiple_of(i * HW, HW), HW) for i in (s, p)]
    has_up, has_dn = n > 0, n < n_rows - 1
    bf, f32 = jnp.bfloat16, jnp.float32

    def local(src, dst, sem):
        return pltpu.make_async_copy(src, dst, sem)

    def remote(src, dst, ssem, rsem, dev):
        return pltpu.make_async_remote_copy(
            src_ref=src, dst_ref=dst, send_sem=ssem, recv_sem=rsem, device_id=dev, device_id_type=MESH)

    peer = {"cols": p}
    side_dev = [{"rows": n - 1}, {"rows": n + 1}]
    side_ok = [has_up, has_dn]

    def each_side(do):
        for side in range(2):
            @pl.when(side_ok[side])
            def _():
                do(side)

    barrier = pltpu.get_barrier_semaphore()

    def signal(dev):
        pl.semaphore_signal(barrier, inc=1, device_id=dev, device_id_type=MESH)

    signal(peer)

    @pl.when(has_up)
    def _():
        signal(side_dev[0])


    h_own = local(h_init.at[s], hst.at[:, mine], s_i.at[0])
    c_own = local(c_init.at[s], cst, s_i.at[1])
    x_own = [local(frames.at[a:e, s], xin.at[a:e, :, mine], s_x.at[g]) for g, (a, e) in enumerate(plan.groups)]
    h_got = local(h_init.at[p], hgo, s_i.at[2])
    c_got = local(c_init.at[p], cgo, s_i.at[3])
    x_got = [local(frames.at[a:e, p], xgo.at[a:e], s_i.at[4 + g]) for g, (a, e) in enumerate(plan.groups[:2])]
    w_copies = [local(w_h, wbuf.at[0:9, 0], s_w.at[0]), local(w_x, wbuf.at[0:9, 1], s_w.at[1]),
                local(bias_in, bias, s_w.at[2])]
    for c in [h_got, x_got[0], c_got, h_own, x_own[0], c_own, *w_copies, x_got[1], *x_own[1:]]:
        c.start()
    with jax.named_scope('barrier'):
        pl.semaphore_wait(barrier, 1 + has_dn.astype(jnp.int32))

    @pl.when(has_dn)
    def _():
        pl.semaphore_signal(here_sem, inc=1, device_id=side_dev[1], device_id_type=MESH)


    h_push = remote(hgo, hst.at[:, mine], s_is.at[0], s_ir.at[0], peer)
    c_push = remote(cgp, cin, s_is.at[1], s_ir.at[1], peer)
    x_push = [remote((xgo if g < 2 else frames.at[:, p]).at[a:e], xin.at[a:e, :, mine], s_xs.at[g], s_xr.at[g], peer)
              for g, (a, e) in enumerate(plan.groups)]
    with jax.named_scope('got_wait'):
        for got, push in [(h_got, h_push), (x_got[0], x_push[0]), (c_got, c_push), (x_got[1], x_push[1])]:
            got.wait()
            if push is c_push:
                cgp[...] = jnp.concatenate([cgo[:, :HW // 2], cgo[:, HW // 2:]], axis=2)
            push.start()
    for push in x_push[2:]:
        push.start()

    shift[...] = jnp.zeros_like(shift)
    low = lax.broadcasted_iota(jnp.int32, (1, LANES), 1) < CH
    low_half = low_row = low
    turn = [0]
    scale = jnp.where(low_row, 0.5, 1.0)
    lift = jnp.where(low_row, 0.5, 0.0)

    with jax.named_scope('w_wait'):
        for c in w_copies:
            c.wait()
    for tap in range(9):
        for half in range(2):
            tile = wbuf[tap, half, :, 0:LANES]
            wbuf[tap, half, :, 0:LANES] = jnp.concatenate([tile[:, CH:], tile[:, :CH]], axis=1)
    b_all = bias[...]
    rest = jnp.concatenate([b_all[:, CH:LANES], b_all[:, :CH], b_all[:, LANES:]], axis=1)
    row = lax.broadcasted_iota(jnp.int32, (CH, 4 * CH), 0)
    rows = jnp.zeros((CH, 4 * CH), f32)
    for i in range(3):
        top = (rest * (1 - 2.0 ** -8)).astype(bf).astype(f32) if i == 0 else rest.astype(bf).astype(f32)
        rows = jnp.where(row == i, top, rows)
        rest = rest - top
    wbuf[9, 0] = rows.astype(bf)
    wbuf[9, 1] = jnp.zeros((CH, 4 * CH), bf)
    ones = jnp.where(lax.broadcasted_iota(jnp.int32, (1, LANES), 1) < 3, 1.0, 0.0).astype(bf)

    def pack(v):
        return jnp.concatenate([v[:, :HG], v[:, HG:]], axis=3)

    def unpack(v):
        return jnp.concatenate([v[..., :CH], v[..., CH:]], axis=1)

    def masked(r, v):
        if 0 <= r < R:
            return v
        return lax.select(jnp.broadcast_to(has_up if r < 0 else has_dn, v.shape), v, jnp.zeros_like(v))

    def emit(t, lo, hi, hx):
        nxt = xh_even if t % 2 == 0 else xh_odd
        at, to = slot(lo, hi), cells_of(lo, hi)
        shift[at, 8:8 + W, :] = hx.reshape(hi - lo, W, LANES)
        nxt[1, to] = hx.astype(bf)
        nxt[0, to] = shift[at, 7:7 + W, :].reshape(hx.shape).astype(bf)
        nxt[2, to] = shift[at, 9:9 + W, :].reshape(hx.shape).astype(bf)

    def cells_of(lo, hi):
        return slice((lo + PAD) * W, (hi + PAD) * W)

    def slot(lo, hi):
        if turn[0] + hi - lo > RING:
            turn[0] = 0
        turn[0] += hi - lo
        return slice(turn[0] - (hi - lo), turn[0])

    def flat(v):
        return v.reshape(-1, v.shape[-1])

    def x_rows(t, lo, hi):
        if lo >= 0 and hi <= R:
            return flat(xin[t, lo:hi].astype(f32))
        side, i = (0, lo + plan.xrows[t]) if lo < 0 else (1, lo - R)
        return flat(unpack(xr_ref[side, plan.xat[t] + i:plan.xat[t] + i + hi - lo].astype(f32)))

    def wait_x(g):
        if g < len(plan.groups):
            x_own[g].wait()
            x_push[g].wait_recv()

    def border(b, kind, side):
        f = plan.first[b]
        if kind < 2:
            src, dst, at = [(hs_ref, hr_ref, plan.hat), (cs_ref, cr_ref, plan.cat)][kind]
            at, end = at[b], at[b + 1]
        else:
            src, dst = xs_ref, xr_ref
            at, end = [plan.xat[f + o] for o in plan.parts[b][kind - 2]]
        return remote(src.at[side, at:end], dst.at[1 - side, at:end],
                      s_bs.at[min(kind, 2), side], s_b.at[kind, 1 - side, b], side_dev[side])

    def pack_x(t0, t1):
        for side in range(2):
            for t in range(t0, t1):
                m = plan.xrows[t]
                lo = 0 if side == 0 else R - m
                xs_ref[side, plan.xat[t]:plan.xat[t] + m] = pack(xin[t, lo:lo + m])

    def start_border(b, *kinds):
        each_side(lambda side: [border(b, kind, side).start() for kind in kinds])

    far = lax.rem(n, FAR) == 0

    def start_first(side, late, *kinds):
        if side:
            ok = has_dn
        else:
            turn_now = jnp.logical_and(far, s == late - 1) if late else jnp.logical_not(far)
            ok = jnp.logical_and(has_up, turn_now)

        @pl.when(ok)
        def _():
            if not side and 0 in kinds:
                pl.semaphore_wait(here_sem, 1)
            for kind in kinds:
                border(0, kind, side).start()

    def wait_border(b, *kinds):
        each_side(lambda side: [border(b, kind, 1 - side).wait_recv() for kind in kinds])

    def pack_h(b, h_rows):
        k = plan.blocks[b]
        for side in range(2):
            lo = 0 if side == 0 else R - k
            hs_ref[side, plan.hat[b]:plan.hat[b] + k] = pack(h_rows[lo:lo + k])

    def pack_c(b):
        k = plan.blocks[b]
        for side in range(2):
            lo = PAD if side == 0 else PAD + R - (k - 1)
            c = cbuf[lo:lo + k - 1]
            cs_ref[side, plan.cat[b]:plan.cat[b] + k - 1] = jnp.where(low_half, c[:, :HW], c[:, HW:])

    weights = wbuf[...].reshape(10 * LANES, 4 * CH)

    def dot(t, lo, hi):
        cur = xh_even if t % 2 == 0 else xh_odd
        taps = [cur[dc, cells_of(lo + dr - 1, hi + dr - 1)] for dr in range(3) for dc in range(3)]
        taps.append(jnp.broadcast_to(ones, taps[0].shape))
        return jnp.dot(jnp.concatenate(taps, axis=1), weights, preferred_element_type=f32)

    def cells(t, lo, hi, gates):
        fi = jnp.tanh(gates[:, :LANES] * 0.5) * 0.5 + 0.5
        og = jnp.tanh(gates[:, LANES:] * scale) * scale + lift
        at = slice(lo + PAD, hi + PAD)
        prod = fi * lax.select(jnp.broadcast_to(low, og.shape), cbuf[at].reshape(og.shape), og)
        c = prod + pltpu.roll(prod, CH, 1)
        h = (og * jnp.tanh(c))[:, :CH]
        if t == T - 1:
            c = c.reshape(hi - lo, 2, 2, HW // 2, LANES)
            for half in range(2):
                both = c[:, half, 0]
                cout[half, lo:hi] = lax.select(jnp.broadcast_to(low, both.shape), both, c[:, half, 1])
        else:
            cbuf[at] = c.reshape(hi - lo, W, LANES)
        for a, e in ((lo, min(hi, 0)), (max(lo, 0), min(hi, R)), (max(lo, R), hi)):
            if a >= e:
                continue
            part = h[(a - lo) * W:(e - lo) * W]
            if a >= 0 and e <= R:
                hout[t, a:e] = part.reshape(e - a, 2 * HG, COLS, CH).astype(bf)
            if t < T - 1:
                emit(t + 1, a, e, masked(a, jnp.concatenate([part, x_rows(t + 1, a, e)], axis=1)))

    pending = []

    def piece(at, ahead=1):
        t, lo, hi = at
        while any(u == t - 1 and a <= hi and lo <= e for u, a, e, _ in pending):
            cells(*pending.pop(0))
        pending.append((*at, dot(*at)))
        flush(ahead)

    def flush(left=0):
        while len(pending) > left:
            cells(*pending.pop(0))

    def push_h(t0, t1, lo=0, hi=R):
        rows = slice(lo, hi)
        remote(hout.at[t0:t1, rows, theirs], hpeer.at[t0:t1, rows], s_os.at[0], s_or.at[0], peer).start()

    def push_c(lo, hi):
        remote(cout.at[p, lo:hi], cpeer.at[lo:hi], s_os.at[1], s_or.at[1], peer).start()

    with jax.named_scope('state_wait'):
        for c in [h_own, x_own[0]]:
            c.wait()
        for c in [h_push, x_push[0]]:
            c.wait_recv()
    pack_h(0, hst)
    pack_x(0, 1)
    start_first(1, 0, 0, 2)
    start_first(0, 0, 0, 2)
    for lo, hi in cuts(0, R):
        emit(0, lo, hi, jnp.concatenate([flat(hst[lo:hi].astype(f32)), x_rows(0, lo, hi)], axis=1))

    for b, k in enumerate(plan.blocks):
        f = plan.first[b]
        last = b + 1 == NB

        def inner(o):
            if o == 0:
                got = [*cuts(k + 1, R - 1 - k), *cuts(1, k + 1), *cuts(R - 1 - k, R - 1)]
            else:
                got = cuts(o + 1, R - 1 - o)
                got = got[1:-1] + [got[0], got[-1]]
            return [(f + o, lo, hi) for lo, hi in got]

        early = [at for o in range(k) for at in inner(o)]
        late = early[len(early) - LATE[b]:]
        for o in range(k):
            pieces = [at for at in early[:len(early) - LATE[b]] if at[0] == f + o]
            first = 0
            if o == 0 and b:
                piece(pieces[0], 9)
                flush(1)
                pack_h(b, hout.at[f - 1])
                pack_c(b)
                with jax.named_scope(f'send{b}'):
                    start_border(b, 0, 1)
                first = 1
            if b == 0 and o == 0:
                for at in pieces[:2]:
                    piece(at, 9)
                with jax.named_scope('x_wait0'):
                    c_own.wait()
                    c_push.wait_recv()
                    wait_x(1)
                for at in pieces[2:4]:
                    piece(at, 9)
                c0, got = cst[...], cin[...]
                cbuf[PAD:PAD + R, mine_c] = jnp.concatenate([c0, c0], axis=2)
                swapped, keep = pltpu.roll(got, CH, 2), jnp.broadcast_to(low, got.shape)
                both = [lax.select(keep, got, swapped), lax.select(keep, swapped, got)]
                cbuf[PAD:PAD + R, theirs_c] = jnp.concatenate(both, axis=1)
                pack_c(0)
                pack_x(1, 3)
                start_first(1, 0, 1, 3, 4)
                start_first(0, 0, 1, 3, 4)
                first = 4
            if b == 0 and o == 2:
                for at in pieces[:2]:
                    piece(at, 9)
                flush(2)
                with jax.named_scope('x_wait1'):
                    wait_x(2)
                for at in pieces[2:4]:
                    piece(at, 9)
                pack_x(3, k)
                for side in range(2):
                    start_first(side, 0, 5)
                start_first(0, 1, 0, 2, 1, 3, 4, 5)
                first = 4
            if b == 0 and o == 4:
                for at in pieces[:2]:
                    piece(at)
                with jax.named_scope('upsend'):
                    start_first(0, 2, 0, 2, 1, 3, 4, 5)
                first = 2
            for at in pieces[first:]:
                piece(at)
            if o == 0 and b and not last:
                pack_x(f + k, f + k + plan.blocks[b + 1])
        with jax.named_scope(f'mid{b}'):
            wait_border(b, 0, 2)
        if b == 0:
            wait_x(3)
        elif not last:
            start_border(b + 1, 2)
        if b:
            push_h(plan.first[b - 1], f)
        piece(late.pop(0), 3)
        for side in range(2):
            lo = -k if side == 0 else R
            h = flat(unpack(hr_ref[side, plan.hat[b]:plan.hat[b] + k].astype(f32)))
            emit(f, lo, lo + k, masked(lo, jnp.concatenate([h, x_rows(f, lo, lo + k)], axis=1)))
        for o in range(k):
            m = k - 1 - o
            top, bottom = cuts(-m, o + 1, BORDER), cuts(R - 1 - o, R + m, BORDER)
            for lo, hi in top:
                piece((f + o, lo, hi), 9 if o == 0 else 1)
                if lo != top[0][0]:
                    continue
                if b == 0 and o in (1, 2):
                    with jax.named_scope(f'midx{o}'):
                        wait_border(0, 3 + o)
                if last and o == k // 2:
                    push_h(f, f + o)
                if last and o == k - 2:
                    push_h(f + k // 2, f + o)
                    push_h(T - 1, T, k, R - k)
                    push_c(k, R - k)
                if last and o == k - 1:
                    push_h(T - 2, T - 1)
            for lo, hi in bottom:
                piece((f + o, lo, hi), 9 if o == 0 else 1)
            if o == 0:
                with jax.named_scope(f'midc{b}'):
                    wait_border(b, 1, *(() if b else (3,)))
                for side in range(2):
                    lo = PAD - (k - 1) if side == 0 else PAD + R
                    packed = cr_ref[side, plan.cat[b]:plan.cat[b] + k - 1]
                    both = jnp.concatenate([packed, pltpu.roll(packed, CH, 2)], axis=1)
                    cbuf[lo:lo + k - 1] = both
                while late:
                    piece(late.pop(0), 3)
            if o == 0 and b == 0 and not last:
                pack_x(f + k, f + k + plan.blocks[b + 1])
                start_border(b + 1, 2)
        assert not late
    flush()
    k = plan.blocks[-1]
    for lo, hi in ((0, k), (R - k, R)):
        push_h(T - 1, T, lo, hi)
        push_c(lo, hi)

    with jax.named_scope('end_wait'):
        for c in [h_push, c_push, *x_push]:
            c.wait_send()

        def wait_sends(side):
            for kind, ref in enumerate((hs_ref, cs_ref, xs_ref)):
                local(ref.at[side], ref.at[side], s_bs.at[kind, side]).wait()

        each_side(wait_sends)
        for sem in (s_os, s_or):
            local(hpeer, hpeer, sem.at[0]).wait()
            local(cpeer, cpeer, sem.at[1]).wait()


def store(hout, hpeer, cout, cpeer, h_all, c_final, c_tile, sems):
    s = lax.axis_index("cols")
    HG = hpeer.shape[2]
    copies = [pltpu.make_async_copy(hout.at[:, :, pl.ds(s * HG, HG)], h_all.at[:, s], sems.at[0]),
              pltpu.make_async_copy(hpeer, h_all.at[:, 1 - s], sems.at[1]),
              pltpu.make_async_copy(c_tile.at[0], c_final.at[s], sems.at[2]),
              pltpu.make_async_copy(c_tile.at[1], c_final.at[1 - s], sems.at[3])]
    for c in copies[:2]:
        c.start()
    for i, packed in enumerate((cout[s], cpeer[...])):
        c_tile[i] = jnp.concatenate([packed[:, :, :CH], packed[:, :, CH:]], axis=1)
    for c in copies[2:]:
        c.start()
    for c in copies:
        c.wait()


def run(blocks, n_rows, frames, w_x, w_h, gate_bias, h_init, c_init):
    T, S, R, HW = frames.shape[:4]
    W, HG = 2 * HW, HW // COLS
    plan = Plan(blocks, T, R, W)
    NB, PAD, G = len(blocks), plan.K, len(plan.groups)
    bf, f32 = jnp.bfloat16, jnp.float32
    vm, dma = pltpu.VMEM, pltpu.SemaphoreType.DMA
    hbm = pl.BlockSpec(memory_space=pltpu.HBM)
    vmem = pl.BlockSpec(memory_space=pltpu.VMEM)
    tiled = frames.reshape(T, S, R, HG, COLS, CH)
    parts = pl.pallas_call(
        functools.partial(kernel, plan, n_rows),
        out_shape=(vm((T, R, 2 * HG, COLS, CH), bf), vm((T, R, HG, COLS, CH), bf),
                   vm((2, R, HW // 2, LANES), f32), vm((R, HW // 2, LANES), f32)),
        in_specs=[hbm] * 6,
        out_specs=(vmem,) * 4,
        scratch_shapes=[
            vm((1, 4 * CH), f32), vm((R, HG, COLS, CH), bf), vm((R, HW, CH), f32),
            vm((R, HW // 2, LANES), f32), vm((R, HW // 2, LANES), f32),
            vm((plan.groups[1][1], R, HG, COLS, CH), bf),
            vm((T, R, 2 * HG, COLS, CH), bf), vm((R, 2 * HG, COLS, CH), bf), vm((R, HW, CH), f32),
            vm((3, (R + 2 * PAD) * W, LANES), bf), vm((3, (R + 2 * PAD) * W, LANES), bf),
            vm((R + 2 * PAD, W, LANES), f32), vm((RING, W + 16, LANES), f32), vm((10, 2, CH, 4 * CH), bf),
            vm((2, plan.xat[-1], HG, COLS, LANES), bf), vm((2, plan.xat[-1], HG, COLS, LANES), bf),
            vm((2, plan.hat[-1], HG, COLS, LANES), bf), vm((2, plan.hat[-1], HG, COLS, LANES), bf),
            vm((2, plan.cat[-1], HW, LANES), f32), vm((2, plan.cat[-1], HW, LANES), f32),
            dma((3,)), dma((6,)), dma((2,)), dma((2,)), dma((G,)), dma((G,)), dma((G,)),
            dma((6, 2, NB)), dma((3, 2)), dma((2,)), dma((2,)), pltpu.SemaphoreType.REGULAR],
        compiler_params=pltpu.CompilerParams(collective_id=0, has_side_effects=True, vmem_limit_bytes=46 * 2**20),
    )(tiled, w_x.reshape(9, CH, 4 * CH), w_h.reshape(9, CH, 4 * CH), gate_bias.reshape(1, -1),
      h_init.reshape(S, R, HG, COLS, CH), c_init)
    h_all, c_final = pl.pallas_call(
        store,
        out_shape=(jax.ShapeDtypeStruct(tiled.shape, bf), jax.ShapeDtypeStruct(c_init.shape, f32)),
        in_specs=[vmem] * 4,
        out_specs=(hbm, hbm),
        scratch_shapes=[vm((2, R, HW, CH), f32), dma((4,))],
        compiler_params=pltpu.CompilerParams(vmem_limit_bytes=4 * 2**20),
    )(*[pltpu.with_memory_space_constraint(a, pltpu.VMEM) for a in parts])
    return h_all.reshape(frames.shape), c_final


def solution(mesh, K=None):
    n_rows = mesh.shape["rows"]
    frame_spec = P(None, "batch", "rows", "cols", None)
    state_spec = P("batch", "rows", "cols", None)
    blocks = BLOCKS if K is None else K
    return jax.shard_map(functools.partial(run, blocks, n_rows), mesh=mesh,
                         in_specs=(frame_spec, P(), P(), P(), state_spec, state_spec),
                         out_specs=(frame_spec, state_spec), check_vma=False)
```

```python
import functools

import jax
import jax.numpy as jnp
from jax import lax
from jax.experimental import pallas as pl
from jax.experimental.pallas import tpu as pltpu
from jax.sharding import PartitionSpec as P

MESH = pl.DeviceIdType.MESH
CH = 64
LANES = 128
COLS = 8
PIECE = 4
RING = 8
BLOCKS = (8, 8)
LATE = (3, 3)
BORDER = 4
FAR = 16


def cuts(lo, hi, size=PIECE):
    n = max(1, (hi - lo) // size)
    edges = [lo + i * size for i in range(n)] + [hi]
    return list(zip(edges[:-1], edges[1:]))


class Plan:
    def __init__(self, blocks, T, R, W):
        assert sum(blocks) == T
        self.blocks, self.T, self.R, self.W, self.HW, self.HG = blocks, T, R, W, W // 2, W // 2 // COLS
        self.K = max(blocks)
        self.first = [sum(blocks[:b]) for b in range(len(blocks))]
        self.of = [(b, o) for b, k in enumerate(blocks) for o in range(k)]
        self.xrows = [blocks[b] - o for b, o in self.of]
        self.xat = [sum(self.xrows[:t]) for t in range(T + 1)]
        self.parts = [[(0, 1), (1, 2), (2, 3), (3, k)] if b == 0 else [(0, k)] for b, k in enumerate(blocks)]
        self.hat = [sum(blocks[:b]) for b in range(len(blocks) + 1)]
        self.cat = [sum(k - 1 for k in blocks[:b]) for b in range(len(blocks) + 1)]
        ends = [0, 1, 3, blocks[0] + 1, T]
        self.groups = [(a, e) for a, e in zip(ends[:-1], ends[1:]) if e > a]


def kernel(plan, n_rows, frames, w_x, w_h, bias_in, h_init, c_init, hout, hpeer, cout, cpeer,
           bias, hgo, cgo, cgp, cin, xgo, xin, hst, cst, xh_even, xh_odd, cbuf, shift, wbuf,
           xs_ref, xr_ref, hs_ref, hr_ref, cs_ref, cr_ref,
           s_w, s_i, s_ir, s_is, s_x, s_xr, s_xs, s_b, s_bs, s_or, s_os, here_sem):
    T, R, W, HW, HG = plan.T, plan.R, plan.W, plan.HW, plan.HG
    PAD = plan.K
    NB = len(plan.blocks)
    s = lax.axis_index("cols")
    n = lax.axis_index("rows")
    p = 1 - s
    mine, theirs = pl.ds(s * HG, HG), pl.ds(p * HG, HG)
    mine_c, theirs_c = [pl.ds(pl.multiple_of(i * HW, HW), HW) for i in (s, p)]
    has_up, has_dn = n > 0, n < n_rows - 1
    bf, f32 = jnp.bfloat16, jnp.float32

    def local(src, dst, sem):
        return pltpu.make_async_copy(src, dst, sem)

    def remote(src, dst, ssem, rsem, dev):
        return pltpu.make_async_remote_copy(
            src_ref=src, dst_ref=dst, send_sem=ssem, recv_sem=rsem, device_id=dev, device_id_type=MESH)

    peer = {"cols": p}
    side_dev = [{"rows": n - 1}, {"rows": n + 1}]
    side_ok = [has_up, has_dn]

    def each_side(do):
        for side in range(2):
            @pl.when(side_ok[side])
            def _():
                do(side)

    barrier = pltpu.get_barrier_semaphore()

    def signal(dev):
        pl.semaphore_signal(barrier, inc=1, device_id=dev, device_id_type=MESH)

    signal(peer)

    @pl.when(has_up)
    def _():
        signal(side_dev[0])


    h_own = local(h_init.at[s], hst.at[:, mine], s_i.at[0])
    c_own = local(c_init.at[s], cst, s_i.at[1])
    x_own = [local(frames.at[a:e, s], xin.at[a:e, :, mine], s_x.at[g]) for g, (a, e) in enumerate(plan.groups)]
    h_got = local(h_init.at[p], hgo, s_i.at[2])
    c_got = local(c_init.at[p], cgo, s_i.at[3])
    x_got = [local(frames.at[a:e, p], xgo.at[a:e], s_i.at[4 + g]) for g, (a, e) in enumerate(plan.groups[:2])]
    w_copies = [local(w_h, wbuf.at[0:9, 0], s_w.at[0]), local(w_x, wbuf.at[0:9, 1], s_w.at[1]),
                local(bias_in, bias, s_w.at[2])]
    for c in [h_got, x_got[0], c_got, h_own, x_own[0], c_own, *w_copies, x_got[1], *x_own[1:]]:
        c.start()
    with jax.named_scope('barrier'):
        pl.semaphore_wait(barrier, 1 + has_dn.astype(jnp.int32))

    @pl.when(has_dn)
    def _():
        pl.semaphore_signal(here_sem, inc=1, device_id=side_dev[1], device_id_type=MESH)


    h_push = remote(hgo, hst.at[:, mine], s_is.at[0], s_ir.at[0], peer)
    c_push = remote(cgp, cin, s_is.at[1], s_ir.at[1], peer)
    x_push = [remote((xgo if g < 2 else frames.at[:, p]).at[a:e], xin.at[a:e, :, mine], s_xs.at[g], s_xr.at[g], peer)
              for g, (a, e) in enumerate(plan.groups)]
    with jax.named_scope('got_wait'):
        for got, push in [(h_got, h_push), (x_got[0], x_push[0]), (c_got, c_push), (x_got[1], x_push[1])]:
            got.wait()
            if push is c_push:
                cgp[...] = jnp.concatenate([cgo[:, :HW // 2], cgo[:, HW // 2:]], axis=2)
            push.start()
    for push in x_push[2:]:
        push.start()

    shift[...] = jnp.zeros_like(shift)
    low = lax.broadcasted_iota(jnp.int32, (1, LANES), 1) < CH
    low_half = low_row = low
    turn = [0]
    scale = jnp.where(low_row, 0.5, 1.0)
    lift = jnp.where(low_row, 0.5, 0.0)

    with jax.named_scope('w_wait'):
        for c in w_copies:
            c.wait()
    for tap in range(9):
        for half in range(2):
            tile = wbuf[tap, half, :, 0:LANES]
            wbuf[tap, half, :, 0:LANES] = jnp.concatenate([tile[:, CH:], tile[:, :CH]], axis=1)
    b_all = bias[...]
    rest = jnp.concatenate([b_all[:, CH:LANES], b_all[:, :CH], b_all[:, LANES:]], axis=1)
    row = lax.broadcasted_iota(jnp.int32, (CH, 4 * CH), 0)
    rows = jnp.zeros((CH, 4 * CH), f32)
    for i in range(3):
        top = (rest * (1 - 2.0 ** -8)).astype(bf).astype(f32) if i == 0 else rest.astype(bf).astype(f32)
        rows = jnp.where(row == i, top, rows)
        rest = rest - top
    wbuf[9, 0] = rows.astype(bf)
    wbuf[9, 1] = jnp.zeros((CH, 4 * CH), bf)
    ones = jnp.where(lax.broadcasted_iota(jnp.int32, (1, LANES), 1) < 3, 1.0, 0.0).astype(bf)

    def pack(v):
        return jnp.concatenate([v[:, :HG], v[:, HG:]], axis=3)

    def unpack(v):
        return jnp.concatenate([v[..., :CH], v[..., CH:]], axis=1)

    def masked(r, v):
        if 0 <= r < R:
            return v
        return lax.select(jnp.broadcast_to(has_up if r < 0 else has_dn, v.shape), v, jnp.zeros_like(v))

    def emit(t, lo, hi, hx):
        nxt = xh_even if t % 2 == 0 else xh_odd
        at, to = slot(lo, hi), cells_of(lo, hi)
        shift[at, 8:8 + W, :] = hx.reshape(hi - lo, W, LANES)
        nxt[1, to] = hx.astype(bf)
        nxt[0, to] = shift[at, 7:7 + W, :].reshape(hx.shape).astype(bf)
        nxt[2, to] = shift[at, 9:9 + W, :].reshape(hx.shape).astype(bf)

    def cells_of(lo, hi):
        return slice((lo + PAD) * W, (hi + PAD) * W)

    def slot(lo, hi):
        if turn[0] + hi - lo > RING:
            turn[0] = 0
        turn[0] += hi - lo
        return slice(turn[0] - (hi - lo), turn[0])

    def flat(v):
        return v.reshape(-1, v.shape[-1])

    def x_rows(t, lo, hi):
        if lo >= 0 and hi <= R:
            return flat(xin[t, lo:hi].astype(f32))
        side, i = (0, lo + plan.xrows[t]) if lo < 0 else (1, lo - R)
        return flat(unpack(xr_ref[side, plan.xat[t] + i:plan.xat[t] + i + hi - lo].astype(f32)))

    def wait_x(g):
        if g < len(plan.groups):
            x_own[g].wait()
            x_push[g].wait_recv()

    def border(b, kind, side):
        f = plan.first[b]
        if kind < 2:
            src, dst, at = [(hs_ref, hr_ref, plan.hat), (cs_ref, cr_ref, plan.cat)][kind]
            at, end = at[b], at[b + 1]
        else:
            src, dst = xs_ref, xr_ref
            at, end = [plan.xat[f + o] for o in plan.parts[b][kind - 2]]
        return remote(src.at[side, at:end], dst.at[1 - side, at:end],
                      s_bs.at[min(kind, 2), side], s_b.at[kind, 1 - side, b], side_dev[side])

    def pack_x(t0, t1):
        for side in range(2):
            for t in range(t0, t1):
                m = plan.xrows[t]
                lo = 0 if side == 0 else R - m
                xs_ref[side, plan.xat[t]:plan.xat[t] + m] = pack(xin[t, lo:lo + m])

    def start_border(b, *kinds):
        each_side(lambda side: [border(b, kind, side).start() for kind in kinds])

    far = lax.rem(n, FAR) == 0

    def start_first(side, late, *kinds):
        if side:
            ok = has_dn
        else:
            turn_now = jnp.logical_and(far, s == late - 1) if late else jnp.logical_not(far)
            ok = jnp.logical_and(has_up, turn_now)

        @pl.when(ok)
        def _():
            if not side and 0 in kinds:
                pl.semaphore_wait(here_sem, 1)
            for kind in kinds:
                border(0, kind, side).start()

    def wait_border(b, *kinds):
        each_side(lambda side: [border(b, kind, 1 - side).wait_recv() for kind in kinds])

    def pack_h(b, h_rows):
        k = plan.blocks[b]
        for side in range(2):
            lo = 0 if side == 0 else R - k
            hs_ref[side, plan.hat[b]:plan.hat[b] + k] = pack(h_rows[lo:lo + k])

    def pack_c(b):
        k = plan.blocks[b]
        for side in range(2):
            lo = PAD if side == 0 else PAD + R - (k - 1)
            c = cbuf[lo:lo + k - 1]
            cs_ref[side, plan.cat[b]:plan.cat[b] + k - 1] = jnp.where(low_half, c[:, :HW], c[:, HW:])

    weights = wbuf[...].reshape(10 * LANES, 4 * CH)

    def dot(t, lo, hi):
        cur = xh_even if t % 2 == 0 else xh_odd
        taps = [cur[dc, cells_of(lo + dr - 1, hi + dr - 1)] for dr in range(3) for dc in range(3)]
        taps.append(jnp.broadcast_to(ones, taps[0].shape))
        return jnp.dot(jnp.concatenate(taps, axis=1), weights, preferred_element_type=f32)

    def cells(t, lo, hi, gates):
        fi = jnp.tanh(gates[:, :LANES] * 0.5) * 0.5 + 0.5
        og = jnp.tanh(gates[:, LANES:] * scale) * scale + lift
        at = slice(lo + PAD, hi + PAD)
        prod = fi * lax.select(jnp.broadcast_to(low, og.shape), cbuf[at].reshape(og.shape), og)
        c = prod + pltpu.roll(prod, CH, 1)
        h = (og * jnp.tanh(c))[:, :CH]
        if t == T - 1:
            c = c.reshape(hi - lo, 2, 2, HW // 2, LANES)
            for half in range(2):
                both = c[:, half, 0]
                cout[half, lo:hi] = lax.select(jnp.broadcast_to(low, both.shape), both, c[:, half, 1])
        else:
            cbuf[at] = c.reshape(hi - lo, W, LANES)
        for a, e in ((lo, min(hi, 0)), (max(lo, 0), min(hi, R)), (max(lo, R), hi)):
            if a >= e:
                continue
            part = h[(a - lo) * W:(e - lo) * W]
            if a >= 0 and e <= R:
                hout[t, a:e] = part.reshape(e - a, 2 * HG, COLS, CH).astype(bf)
            if t < T - 1:
                emit(t + 1, a, e, masked(a, jnp.concatenate([part, x_rows(t + 1, a, e)], axis=1)))

    pending = []

    def piece(at, ahead=1):
        t, lo, hi = at
        while any(u == t - 1 and a <= hi and lo <= e for u, a, e, _ in pending):
            cells(*pending.pop(0))
        pending.append((*at, dot(*at)))
        flush(ahead)

    def flush(left=0):
        while len(pending) > left:
            cells(*pending.pop(0))

    def push_h(t0, t1, lo=0, hi=R):
        rows = slice(lo, hi)
        remote(hout.at[t0:t1, rows, theirs], hpeer.at[t0:t1, rows], s_os.at[0], s_or.at[0], peer).start()

    def push_c(lo, hi):
        remote(cout.at[p, lo:hi], cpeer.at[lo:hi], s_os.at[1], s_or.at[1], peer).start()

    with jax.named_scope('state_wait'):
        for c in [h_own, x_own[0]]:
            c.wait()
        for c in [h_push, x_push[0]]:
            c.wait_recv()
    pack_h(0, hst)
    pack_x(0, 1)
    start_first(1, 0, 0, 2)
    start_first(0, 0, 0, 2)
    for lo, hi in cuts(0, R):
        emit(0, lo, hi, jnp.concatenate([flat(hst[lo:hi].astype(f32)), x_rows(0, lo, hi)], axis=1))

    for b, k in enumerate(plan.blocks):
        f = plan.first[b]
        last = b + 1 == NB

        def inner(o):
            if o == 0:
                got = [*cuts(k + 1, R - 1 - k), *cuts(1, k + 1), *cuts(R - 1 - k, R - 1)]
            else:
                got = cuts(o + 1, R - 1 - o)
                got = got[1:-1] + [got[0], got[-1]]
            return [(f + o, lo, hi) for lo, hi in got]

        early = [at for o in range(k) for at in inner(o)]
        late = early[len(early) - LATE[b]:]
        for o in range(k):
            pieces = [at for at in early[:len(early) - LATE[b]] if at[0] == f + o]
            first = 0
            if o == 0 and b:
                piece(pieces[0], 9)
                flush(1)
                pack_h(b, hout.at[f - 1])
                pack_c(b)
                with jax.named_scope(f'send{b}'):
                    start_border(b, 0, 1)
                first = 1
            if b == 0 and o == 0:
                for at in pieces[:2]:
                    piece(at, 9)
                with jax.named_scope('x_wait0'):
                    c_own.wait()
                    c_push.wait_recv()
                    wait_x(1)
                for at in pieces[2:4]:
                    piece(at, 9)
                c0, got = cst[...], cin[...]
                cbuf[PAD:PAD + R, mine_c] = jnp.concatenate([c0, c0], axis=2)
                swapped, keep = pltpu.roll(got, CH, 2), jnp.broadcast_to(low, got.shape)
                both = [lax.select(keep, got, swapped), lax.select(keep, swapped, got)]
                cbuf[PAD:PAD + R, theirs_c] = jnp.concatenate(both, axis=1)
                pack_c(0)
                pack_x(1, 3)
                start_first(1, 0, 1, 3, 4)
                start_first(0, 0, 1, 3, 4)
                first = 4
            if b == 0 and o == 2:
                for at in pieces[:2]:
                    piece(at, 9)
                flush(2)
                with jax.named_scope('x_wait1'):
                    wait_x(2)
                for at in pieces[2:4]:
                    piece(at, 9)
                pack_x(3, k)
                for side in range(2):
                    start_first(side, 0, 5)
                start_first(0, 1, 5)
                start_first(0, 2, 0, 2, 1, 3, 4, 5)
                first = 4
            for at in pieces[first:]:
                piece(at)
            if b == 0 and o == 0:
                with jax.named_scope('upsend'):
                    start_first(0, 1, 0, 2, 1, 3, 4)
            if o == 0 and b and not last:
                pack_x(f + k, f + k + plan.blocks[b + 1])
        with jax.named_scope(f'mid{b}'):
            wait_border(b, 0, 2)
        if b == 0:
            wait_x(3)
        elif not last:
            start_border(b + 1, 2)
        if b:
            push_h(plan.first[b - 1], f)
        piece(late.pop(0), 3)
        for side in range(2):
            lo = -k if side == 0 else R
            h = flat(unpack(hr_ref[side, plan.hat[b]:plan.hat[b] + k].astype(f32)))
            emit(f, lo, lo + k, masked(lo, jnp.concatenate([h, x_rows(f, lo, lo + k)], axis=1)))
        for o in range(k):
            m = k - 1 - o
            top, bottom = cuts(-m, o + 1, BORDER), cuts(R - 1 - o, R + m, BORDER)
            for lo, hi in top:
                piece((f + o, lo, hi), 9 if o == 0 else 1)
                if lo != top[0][0]:
                    continue
                if b == 0 and o in (1, 2):
                    with jax.named_scope(f'midx{o}'):
                        wait_border(0, 3 + o)
                if last and o == k // 2:
                    push_h(f, f + o)
                if last and o == k - 2:
                    push_h(f + k // 2, f + o)
                    push_h(T - 1, T, k, R - k)
                    push_c(k, R - k)
                if last and o == k - 1:
                    push_h(T - 2, T - 1)
            for lo, hi in bottom:
                piece((f + o, lo, hi), 9 if o == 0 else 1)
            if o == 0:
                with jax.named_scope(f'midc{b}'):
                    wait_border(b, 1, *(() if b else (3,)))
                for side in range(2):
                    lo = PAD - (k - 1) if side == 0 else PAD + R
                    packed = cr_ref[side, plan.cat[b]:plan.cat[b] + k - 1]
                    both = jnp.concatenate([packed, pltpu.roll(packed, CH, 2)], axis=1)
                    cbuf[lo:lo + k - 1] = both
                while late:
                    piece(late.pop(0), 3)
            if o == 0 and b == 0 and not last:
                pack_x(f + k, f + k + plan.blocks[b + 1])
                start_border(b + 1, 2)
        assert not late
    flush()
    k = plan.blocks[-1]
    for lo, hi in ((0, k), (R - k, R)):
        push_h(T - 1, T, lo, hi)
        push_c(lo, hi)

    with jax.named_scope('end_wait'):
        for c in [h_push, c_push, *x_push]:
            c.wait_send()

        def wait_sends(side):
            for kind, ref in enumerate((hs_ref, cs_ref, xs_ref)):
                local(ref.at[side], ref.at[side], s_bs.at[kind, side]).wait()

        each_side(wait_sends)
        for sem in (s_os, s_or):
            local(hpeer, hpeer, sem.at[0]).wait()
            local(cpeer, cpeer, sem.at[1]).wait()


def store(hout, hpeer, cout, cpeer, h_all, c_final, c_tile, sems):
    s = lax.axis_index("cols")
    HG = hpeer.shape[2]
    copies = [pltpu.make_async_copy(hout.at[:, :, pl.ds(s * HG, HG)], h_all.at[:, s], sems.at[0]),
              pltpu.make_async_copy(hpeer, h_all.at[:, 1 - s], sems.at[1]),
              pltpu.make_async_copy(c_tile.at[0], c_final.at[s], sems.at[2]),
              pltpu.make_async_copy(c_tile.at[1], c_final.at[1 - s], sems.at[3])]
    for c in copies[:2]:
        c.start()
    for i, packed in enumerate((cout[s], cpeer[...])):
        c_tile[i] = jnp.concatenate([packed[:, :, :CH], packed[:, :, CH:]], axis=1)
    for c in copies[2:]:
        c.start()
    for c in copies:
        c.wait()


def run(blocks, n_rows, frames, w_x, w_h, gate_bias, h_init, c_init):
    T, S, R, HW = frames.shape[:4]
    W, HG = 2 * HW, HW // COLS
    plan = Plan(blocks, T, R, W)
    NB, PAD, G = len(blocks), plan.K, len(plan.groups)
    bf, f32 = jnp.bfloat16, jnp.float32
    vm, dma = pltpu.VMEM, pltpu.SemaphoreType.DMA
    hbm = pl.BlockSpec(memory_space=pltpu.HBM)
    vmem = pl.BlockSpec(memory_space=pltpu.VMEM)
    tiled = frames.reshape(T, S, R, HG, COLS, CH)
    parts = pl.pallas_call(
        functools.partial(kernel, plan, n_rows),
        out_shape=(vm((T, R, 2 * HG, COLS, CH), bf), vm((T, R, HG, COLS, CH), bf),
                   vm((2, R, HW // 2, LANES), f32), vm((R, HW // 2, LANES), f32)),
        in_specs=[hbm] * 6,
        out_specs=(vmem,) * 4,
        scratch_shapes=[
            vm((1, 4 * CH), f32), vm((R, HG, COLS, CH), bf), vm((R, HW, CH), f32),
            vm((R, HW // 2, LANES), f32), vm((R, HW // 2, LANES), f32),
            vm((plan.groups[1][1], R, HG, COLS, CH), bf),
            vm((T, R, 2 * HG, COLS, CH), bf), vm((R, 2 * HG, COLS, CH), bf), vm((R, HW, CH), f32),
            vm((3, (R + 2 * PAD) * W, LANES), bf), vm((3, (R + 2 * PAD) * W, LANES), bf),
            vm((R + 2 * PAD, W, LANES), f32), vm((RING, W + 16, LANES), f32), vm((10, 2, CH, 4 * CH), bf),
            vm((2, plan.xat[-1], HG, COLS, LANES), bf), vm((2, plan.xat[-1], HG, COLS, LANES), bf),
            vm((2, plan.hat[-1], HG, COLS, LANES), bf), vm((2, plan.hat[-1], HG, COLS, LANES), bf),
            vm((2, plan.cat[-1], HW, LANES), f32), vm((2, plan.cat[-1], HW, LANES), f32),
            dma((3,)), dma((6,)), dma((2,)), dma((2,)), dma((G,)), dma((G,)), dma((G,)),
            dma((6, 2, NB)), dma((3, 2)), dma((2,)), dma((2,)), pltpu.SemaphoreType.REGULAR],
        compiler_params=pltpu.CompilerParams(collective_id=0, has_side_effects=True, vmem_limit_bytes=46 * 2**20),
    )(tiled, w_x.reshape(9, CH, 4 * CH), w_h.reshape(9, CH, 4 * CH), gate_bias.reshape(1, -1),
      h_init.reshape(S, R, HG, COLS, CH), c_init)
    h_all, c_final = pl.pallas_call(
        store,
        out_shape=(jax.ShapeDtypeStruct(tiled.shape, bf), jax.ShapeDtypeStruct(c_init.shape, f32)),
        in_specs=[vmem] * 4,
        out_specs=(hbm, hbm),
        scratch_shapes=[vm((2, R, HW, CH), f32), dma((4,))],
        compiler_params=pltpu.CompilerParams(vmem_limit_bytes=4 * 2**20),
    )(*[pltpu.with_memory_space_constraint(a, pltpu.VMEM) for a in parts])
    return h_all.reshape(frames.shape), c_final


def solution(mesh, K=None):
    n_rows = mesh.shape["rows"]
    frame_spec = P(None, "batch", "rows", "cols", None)
    state_spec = P("batch", "rows", "cols", None)
    blocks = BLOCKS if K is None else K
    return jax.shard_map(functools.partial(run, blocks, n_rows), mesh=mesh,
                         in_specs=(frame_spec, P(), P(), P(), state_spec, state_spec),
                         out_specs=(frame_spec, state_spec), check_vma=False)
```

```python
import functools

import jax
import jax.numpy as jnp
from jax import lax
from jax.experimental import pallas as pl
from jax.experimental.pallas import tpu as pltpu
from jax.sharding import PartitionSpec as P

MESH = pl.DeviceIdType.MESH
CH = 64
LANES = 128
COLS = 8
PIECE = 4
RING = 8
BLOCKS = (8, 8)
LATE = (3, 3)
BORDER = 4
TURN_NS = 350
FAR = 16


def cuts(lo, hi, size=PIECE):
    n = max(1, (hi - lo) // size)
    edges = [lo + i * size for i in range(n)] + [hi]
    return list(zip(edges[:-1], edges[1:]))


class Plan:
    def __init__(self, blocks, T, R, W):
        assert sum(blocks) == T
        self.blocks, self.T, self.R, self.W, self.HW, self.HG = blocks, T, R, W, W // 2, W // 2 // COLS
        self.K = max(blocks)
        self.first = [sum(blocks[:b]) for b in range(len(blocks))]
        self.of = [(b, o) for b, k in enumerate(blocks) for o in range(k)]
        self.xrows = [blocks[b] - o for b, o in self.of]
        self.xat = [sum(self.xrows[:t]) for t in range(T + 1)]
        self.parts = [[(0, 1), (1, 2), (2, 3), (3, k)] if b == 0 else [(0, k)] for b, k in enumerate(blocks)]
        self.hat = [sum(blocks[:b]) for b in range(len(blocks) + 1)]
        self.cat = [sum(k - 1 for k in blocks[:b]) for b in range(len(blocks) + 1)]
        ends = [0, 1, 3, blocks[0] + 1, T]
        self.groups = [(a, e) for a, e in zip(ends[:-1], ends[1:]) if e > a]


def kernel(plan, n_rows, frames, w_x, w_h, bias_in, h_init, c_init, hout, hpeer, cout, cpeer,
           bias, hgo, cgo, cgp, cin, xgo, xin, hst, cst, xh_even, xh_odd, cbuf, shift, wbuf,
           xs_ref, xr_ref, hs_ref, hr_ref, cs_ref, cr_ref,
           s_w, s_i, s_ir, s_is, s_x, s_xr, s_xs, s_b, s_bs, s_or, s_os, here_sem):
    T, R, W, HW, HG = plan.T, plan.R, plan.W, plan.HW, plan.HG
    PAD = plan.K
    NB = len(plan.blocks)
    s = lax.axis_index("cols")
    n = lax.axis_index("rows")
    p = 1 - s
    mine, theirs = pl.ds(s * HG, HG), pl.ds(p * HG, HG)
    mine_c, theirs_c = [pl.ds(pl.multiple_of(i * HW, HW), HW) for i in (s, p)]
    has_up, has_dn = n > 0, n < n_rows - 1
    bf, f32 = jnp.bfloat16, jnp.float32

    def local(src, dst, sem):
        return pltpu.make_async_copy(src, dst, sem)

    def remote(src, dst, ssem, rsem, dev):
        return pltpu.make_async_remote_copy(
            src_ref=src, dst_ref=dst, send_sem=ssem, recv_sem=rsem, device_id=dev, device_id_type=MESH)

    peer = {"cols": p}
    side_dev = [{"rows": n - 1}, {"rows": n + 1}]
    side_ok = [has_up, has_dn]

    def each_side(do):
        for side in range(2):
            @pl.when(side_ok[side])
            def _():
                do(side)

    barrier = pltpu.get_barrier_semaphore()

    def signal(dev):
        pl.semaphore_signal(barrier, inc=1, device_id=dev, device_id_type=MESH)

    signal(peer)

    @pl.when(has_up)
    def _():
        signal(side_dev[0])


    h_own = local(h_init.at[s], hst.at[:, mine], s_i.at[0])
    c_own = local(c_init.at[s], cst, s_i.at[1])
    x_own = [local(frames.at[a:e, s], xin.at[a:e, :, mine], s_x.at[g]) for g, (a, e) in enumerate(plan.groups)]
    h_got = local(h_init.at[p], hgo, s_i.at[2])
    c_got = local(c_init.at[p], cgo, s_i.at[3])
    x_got = [local(frames.at[a:e, p], xgo.at[a:e], s_i.at[4 + g]) for g, (a, e) in enumerate(plan.groups[:2])]
    w_copies = [local(w_h, wbuf.at[0:9, 0], s_w.at[0]), local(w_x, wbuf.at[0:9, 1], s_w.at[1]),
                local(bias_in, bias, s_w.at[2])]
    for c in [h_got, x_got[0], c_got, h_own, x_own[0], c_own, *w_copies, x_got[1], *x_own[1:]]:
        c.start()
    with jax.named_scope('barrier'):
        pl.semaphore_wait(barrier, 1 + has_dn.astype(jnp.int32))

    @pl.when(has_dn)
    def _():
        pl.semaphore_signal(here_sem, inc=1, device_id=side_dev[1], device_id_type=MESH)


    h_push = remote(hgo, hst.at[:, mine], s_is.at[0], s_ir.at[0], peer)
    c_push = remote(cgp, cin, s_is.at[1], s_ir.at[1], peer)
    x_push = [remote((xgo if g < 2 else frames.at[:, p]).at[a:e], xin.at[a:e, :, mine], s_xs.at[g], s_xr.at[g], peer)
              for g, (a, e) in enumerate(plan.groups)]
    with jax.named_scope('got_wait'):
        for got, push in [(h_got, h_push), (x_got[0], x_push[0]), (c_got, c_push), (x_got[1], x_push[1])]:
            got.wait()
            if push is c_push:
                cgp[...] = jnp.concatenate([cgo[:, :HW // 2], cgo[:, HW // 2:]], axis=2)
            push.start()
    for push in x_push[2:]:
        push.start()

    shift[...] = jnp.zeros_like(shift)
    low = lax.broadcasted_iota(jnp.int32, (1, LANES), 1) < CH
    low_half = low_row = low
    turn = [0]
    scale = jnp.where(low_row, 0.5, 1.0)
    lift = jnp.where(low_row, 0.5, 0.0)

    with jax.named_scope('w_wait'):
        for c in w_copies:
            c.wait()
    for tap in range(9):
        for half in range(2):
            tile = wbuf[tap, half, :, 0:LANES]
            wbuf[tap, half, :, 0:LANES] = jnp.concatenate([tile[:, CH:], tile[:, :CH]], axis=1)
    b_all = bias[...]
    rest = jnp.concatenate([b_all[:, CH:LANES], b_all[:, :CH], b_all[:, LANES:]], axis=1)
    row = lax.broadcasted_iota(jnp.int32, (CH, 4 * CH), 0)
    rows = jnp.zeros((CH, 4 * CH), f32)
    for i in range(3):
        top = (rest * (1 - 2.0 ** -8)).astype(bf).astype(f32) if i == 0 else rest.astype(bf).astype(f32)
        rows = jnp.where(row == i, top, rows)
        rest = rest - top
    wbuf[9, 0] = rows.astype(bf)
    wbuf[9, 1] = jnp.zeros((CH, 4 * CH), bf)
    ones = jnp.where(lax.broadcasted_iota(jnp.int32, (1, LANES), 1) < 3, 1.0, 0.0).astype(bf)

    def pack(v):
        return jnp.concatenate([v[:, :HG], v[:, HG:]], axis=3)

    def unpack(v):
        return jnp.concatenate([v[..., :CH], v[..., CH:]], axis=1)

    def masked(r, v):
        if 0 <= r < R:
            return v
        return lax.select(jnp.broadcast_to(has_up if r < 0 else has_dn, v.shape), v, jnp.zeros_like(v))

    def emit(t, lo, hi, hx):
        nxt = xh_even if t % 2 == 0 else xh_odd
        at, to = slot(lo, hi), cells_of(lo, hi)
        shift[at, 8:8 + W, :] = hx.reshape(hi - lo, W, LANES)
        nxt[1, to] = hx.astype(bf)
        nxt[0, to] = shift[at, 7:7 + W, :].reshape(hx.shape).astype(bf)
        nxt[2, to] = shift[at, 9:9 + W, :].reshape(hx.shape).astype(bf)

    def cells_of(lo, hi):
        return slice((lo + PAD) * W, (hi + PAD) * W)

    def slot(lo, hi):
        if turn[0] + hi - lo > RING:
            turn[0] = 0
        turn[0] += hi - lo
        return slice(turn[0] - (hi - lo), turn[0])

    def flat(v):
        return v.reshape(-1, v.shape[-1])

    def x_rows(t, lo, hi):
        if lo >= 0 and hi <= R:
            return flat(xin[t, lo:hi].astype(f32))
        side, i = (0, lo + plan.xrows[t]) if lo < 0 else (1, lo - R)
        return flat(unpack(xr_ref[side, plan.xat[t] + i:plan.xat[t] + i + hi - lo].astype(f32)))

    def wait_x(g):
        if g < len(plan.groups):
            x_own[g].wait()
            x_push[g].wait_recv()

    def border(b, kind, side):
        f = plan.first[b]
        if kind < 2:
            src, dst, at = [(hs_ref, hr_ref, plan.hat), (cs_ref, cr_ref, plan.cat)][kind]
            at, end = at[b], at[b + 1]
        else:
            src, dst = xs_ref, xr_ref
            at, end = [plan.xat[f + o] for o in plan.parts[b][kind - 2]]
        return remote(src.at[side, at:end], dst.at[1 - side, at:end],
                      s_bs.at[min(kind, 2), side], s_b.at[kind, 1 - side, b], side_dev[side])

    def pack_x(t0, t1):
        for side in range(2):
            for t in range(t0, t1):
                m = plan.xrows[t]
                lo = 0 if side == 0 else R - m
                xs_ref[side, plan.xat[t]:plan.xat[t] + m] = pack(xin[t, lo:lo + m])

    def start_border(b, *kinds):
        each_side(lambda side: [border(b, kind, side).start() for kind in kinds])

    far = lax.rem(n, FAR) == 0

    def start_first(side, late, *kinds):
        ok = has_dn if side else jnp.logical_and(has_up, far if late else jnp.logical_not(far))

        @pl.when(ok)
        def _():
            if not side and 0 in kinds:
                pl.semaphore_wait(here_sem, 1)
                if late:
                    @pl.when(s == 1)
                    def _():
                        pl.delay(TURN_NS)

            for kind in kinds:
                border(0, kind, side).start()

    def wait_border(b, *kinds):
        each_side(lambda side: [border(b, kind, 1 - side).wait_recv() for kind in kinds])

    def pack_h(b, h_rows):
        k = plan.blocks[b]
        for side in range(2):
            lo = 0 if side == 0 else R - k
            hs_ref[side, plan.hat[b]:plan.hat[b] + k] = pack(h_rows[lo:lo + k])

    def pack_c(b):
        k = plan.blocks[b]
        for side in range(2):
            lo = PAD if side == 0 else PAD + R - (k - 1)
            c = cbuf[lo:lo + k - 1]
            cs_ref[side, plan.cat[b]:plan.cat[b] + k - 1] = jnp.where(low_half, c[:, :HW], c[:, HW:])

    weights = wbuf[...].reshape(10 * LANES, 4 * CH)

    def dot(t, lo, hi):
        cur = xh_even if t % 2 == 0 else xh_odd
        taps = [cur[dc, cells_of(lo + dr - 1, hi + dr - 1)] for dr in range(3) for dc in range(3)]
        taps.append(jnp.broadcast_to(ones, taps[0].shape))
        return jnp.dot(jnp.concatenate(taps, axis=1), weights, preferred_element_type=f32)

    def cells(t, lo, hi, gates):
        fi = jnp.tanh(gates[:, :LANES] * 0.5) * 0.5 + 0.5
        og = jnp.tanh(gates[:, LANES:] * scale) * scale + lift
        at = slice(lo + PAD, hi + PAD)
        prod = fi * lax.select(jnp.broadcast_to(low, og.shape), cbuf[at].reshape(og.shape), og)
        c = prod + pltpu.roll(prod, CH, 1)
        h = (og * jnp.tanh(c))[:, :CH]
        if t == T - 1:
            c = c.reshape(hi - lo, 2, 2, HW // 2, LANES)
            for half in range(2):
                both = c[:, half, 0]
                cout[half, lo:hi] = lax.select(jnp.broadcast_to(low, both.shape), both, c[:, half, 1])
        else:
            cbuf[at] = c.reshape(hi - lo, W, LANES)
        for a, e in ((lo, min(hi, 0)), (max(lo, 0), min(hi, R)), (max(lo, R), hi)):
            if a >= e:
                continue
            part = h[(a - lo) * W:(e - lo) * W]
            if a >= 0 and e <= R:
                hout[t, a:e] = part.reshape(e - a, 2 * HG, COLS, CH).astype(bf)
            if t < T - 1:
                emit(t + 1, a, e, masked(a, jnp.concatenate([part, x_rows(t + 1, a, e)], axis=1)))

    pending = []

    def piece(at, ahead=1):
        t, lo, hi = at
        while any(u == t - 1 and a <= hi and lo <= e for u, a, e, _ in pending):
            cells(*pending.pop(0))
        pending.append((*at, dot(*at)))
        flush(ahead)

    def flush(left=0):
        while len(pending) > left:
            cells(*pending.pop(0))

    def push_h(t0, t1, lo=0, hi=R):
        rows = slice(lo, hi)
        remote(hout.at[t0:t1, rows, theirs], hpeer.at[t0:t1, rows], s_os.at[0], s_or.at[0], peer).start()

    def push_c(lo, hi):
        remote(cout.at[p, lo:hi], cpeer.at[lo:hi], s_os.at[1], s_or.at[1], peer).start()

    with jax.named_scope('state_wait'):
        for c in [h_own, x_own[0]]:
            c.wait()
        for c in [h_push, x_push[0]]:
            c.wait_recv()
    pack_h(0, hst)
    pack_x(0, 1)
    start_first(1, 0, 0, 2)
    start_first(0, 0, 0, 2)
    for lo, hi in cuts(0, R):
        emit(0, lo, hi, jnp.concatenate([flat(hst[lo:hi].astype(f32)), x_rows(0, lo, hi)], axis=1))

    for b, k in enumerate(plan.blocks):
        f = plan.first[b]
        last = b + 1 == NB

        def inner(o):
            if o == 0:
                got = [*cuts(k + 1, R - 1 - k), *cuts(1, k + 1), *cuts(R - 1 - k, R - 1)]
            else:
                got = cuts(o + 1, R - 1 - o)
                got = got[1:-1] + [got[0], got[-1]]
            return [(f + o, lo, hi) for lo, hi in got]

        early = [at for o in range(k) for at in inner(o)]
        late = early[len(early) - LATE[b]:]
        for o in range(k):
            pieces = [at for at in early[:len(early) - LATE[b]] if at[0] == f + o]
            first = 0
            if o == 0 and b:
                piece(pieces[0], 9)
                flush(1)
                pack_h(b, hout.at[f - 1])
                pack_c(b)
                with jax.named_scope(f'send{b}'):
                    start_border(b, 0, 1)
                first = 1
            if b == 0 and o == 0:
                for at in pieces[:2]:
                    piece(at, 9)
                with jax.named_scope('x_wait0'):
                    c_own.wait()
                    c_push.wait_recv()
                    wait_x(1)
                for at in pieces[2:4]:
                    piece(at, 9)
                c0, got = cst[...], cin[...]
                cbuf[PAD:PAD + R, mine_c] = jnp.concatenate([c0, c0], axis=2)
                swapped, keep = pltpu.roll(got, CH, 2), jnp.broadcast_to(low, got.shape)
                both = [lax.select(keep, got, swapped), lax.select(keep, swapped, got)]
                cbuf[PAD:PAD + R, theirs_c] = jnp.concatenate(both, axis=1)
                pack_c(0)
                pack_x(1, 3)
                start_first(1, 0, 1, 3, 4)
                start_first(0, 0, 1, 3, 4)
                first = 4
            if b == 0 and o == 2:
                for at in pieces[:2]:
                    piece(at, 9)
                flush(2)
                with jax.named_scope('x_wait1'):
                    wait_x(2)
                for at in pieces[2:4]:
                    piece(at, 9)
                pack_x(3, k)
                for side in range(2):
                    start_first(side, 0, 5)
                start_first(0, 1, 5)
                first = 4
            for at in pieces[first:]:
                piece(at)
            if b == 0 and o == 0:
                with jax.named_scope('upsend'):
                    start_first(0, 1, 0, 2, 1, 3, 4)
            if o == 0 and b and not last:
                pack_x(f + k, f + k + plan.blocks[b + 1])
        with jax.named_scope(f'mid{b}'):
            wait_border(b, 0, 2)
        if b == 0:
            wait_x(3)
        elif not last:
            start_border(b + 1, 2)
        if b:
            push_h(plan.first[b - 1], f)
        piece(late.pop(0), 3)
        for side in range(2):
            lo = -k if side == 0 else R
            h = flat(unpack(hr_ref[side, plan.hat[b]:plan.hat[b] + k].astype(f32)))
            emit(f, lo, lo + k, masked(lo, jnp.concatenate([h, x_rows(f, lo, lo + k)], axis=1)))
        for o in range(k):
            m = k - 1 - o
            top, bottom = cuts(-m, o + 1, BORDER), cuts(R - 1 - o, R + m, BORDER)
            for lo, hi in top:
                piece((f + o, lo, hi), 9 if o == 0 else 1)
                if lo != top[0][0]:
                    continue
                if b == 0 and o in (1, 2):
                    with jax.named_scope(f'midx{o}'):
                        wait_border(0, 3 + o)
                if last and o == k // 2:
                    push_h(f, f + o)
                if last and o == k - 2:
                    push_h(f + k // 2, f + o)
                    push_h(T - 1, T, k, R - k)
                    push_c(k, R - k)
                if last and o == k - 1:
                    push_h(T - 2, T - 1)
            for lo, hi in bottom:
                piece((f + o, lo, hi), 9 if o == 0 else 1)
            if o == 0:
                with jax.named_scope(f'midc{b}'):
                    wait_border(b, 1, *(() if b else (3,)))
                for side in range(2):
                    lo = PAD - (k - 1) if side == 0 else PAD + R
                    packed = cr_ref[side, plan.cat[b]:plan.cat[b] + k - 1]
                    both = jnp.concatenate([packed, pltpu.roll(packed, CH, 2)], axis=1)
                    cbuf[lo:lo + k - 1] = both
                while late:
                    piece(late.pop(0), 3)
            if o == 0 and b == 0 and not last:
                pack_x(f + k, f + k + plan.blocks[b + 1])
                start_border(b + 1, 2)
        assert not late
    flush()
    k = plan.blocks[-1]
    for lo, hi in ((0, k), (R - k, R)):
        push_h(T - 1, T, lo, hi)
        push_c(lo, hi)

    with jax.named_scope('end_wait'):
        for c in [h_push, c_push, *x_push]:
            c.wait_send()

        def wait_sends(side):
            for kind, ref in enumerate((hs_ref, cs_ref, xs_ref)):
                local(ref.at[side], ref.at[side], s_bs.at[kind, side]).wait()

        each_side(wait_sends)
        for sem in (s_os, s_or):
            local(hpeer, hpeer, sem.at[0]).wait()
            local(cpeer, cpeer, sem.at[1]).wait()


def store(hout, hpeer, cout, cpeer, h_all, c_final, c_tile, sems):
    s = lax.axis_index("cols")
    HG = hpeer.shape[2]
    copies = [pltpu.make_async_copy(hout.at[:, :, pl.ds(s * HG, HG)], h_all.at[:, s], sems.at[0]),
              pltpu.make_async_copy(hpeer, h_all.at[:, 1 - s], sems.at[1]),
              pltpu.make_async_copy(c_tile.at[0], c_final.at[s], sems.at[2]),
              pltpu.make_async_copy(c_tile.at[1], c_final.at[1 - s], sems.at[3])]
    for c in copies[:2]:
        c.start()
    for i, packed in enumerate((cout[s], cpeer[...])):
        c_tile[i] = jnp.concatenate([packed[:, :, :CH], packed[:, :, CH:]], axis=1)
    for c in copies[2:]:
        c.start()
    for c in copies:
        c.wait()


def run(blocks, n_rows, frames, w_x, w_h, gate_bias, h_init, c_init):
    T, S, R, HW = frames.shape[:4]
    W, HG = 2 * HW, HW // COLS
    plan = Plan(blocks, T, R, W)
    NB, PAD, G = len(blocks), plan.K, len(plan.groups)
    bf, f32 = jnp.bfloat16, jnp.float32
    vm, dma = pltpu.VMEM, pltpu.SemaphoreType.DMA
    hbm = pl.BlockSpec(memory_space=pltpu.HBM)
    vmem = pl.BlockSpec(memory_space=pltpu.VMEM)
    tiled = frames.reshape(T, S, R, HG, COLS, CH)
    parts = pl.pallas_call(
        functools.partial(kernel, plan, n_rows),
        out_shape=(vm((T, R, 2 * HG, COLS, CH), bf), vm((T, R, HG, COLS, CH), bf),
                   vm((2, R, HW // 2, LANES), f32), vm((R, HW // 2, LANES), f32)),
        in_specs=[hbm] * 6,
        out_specs=(vmem,) * 4,
        scratch_shapes=[
            vm((1, 4 * CH), f32), vm((R, HG, COLS, CH), bf), vm((R, HW, CH), f32),
            vm((R, HW // 2, LANES), f32), vm((R, HW // 2, LANES), f32),
            vm((plan.groups[1][1], R, HG, COLS, CH), bf),
            vm((T, R, 2 * HG, COLS, CH), bf), vm((R, 2 * HG, COLS, CH), bf), vm((R, HW, CH), f32),
            vm((3, (R + 2 * PAD) * W, LANES), bf), vm((3, (R + 2 * PAD) * W, LANES), bf),
            vm((R + 2 * PAD, W, LANES), f32), vm((RING, W + 16, LANES), f32), vm((10, 2, CH, 4 * CH), bf),
            vm((2, plan.xat[-1], HG, COLS, LANES), bf), vm((2, plan.xat[-1], HG, COLS, LANES), bf),
            vm((2, plan.hat[-1], HG, COLS, LANES), bf), vm((2, plan.hat[-1], HG, COLS, LANES), bf),
            vm((2, plan.cat[-1], HW, LANES), f32), vm((2, plan.cat[-1], HW, LANES), f32),
            dma((3,)), dma((6,)), dma((2,)), dma((2,)), dma((G,)), dma((G,)), dma((G,)),
            dma((6, 2, NB)), dma((3, 2)), dma((2,)), dma((2,)), pltpu.SemaphoreType.REGULAR],
        compiler_params=pltpu.CompilerParams(collective_id=0, has_side_effects=True, vmem_limit_bytes=46 * 2**20),
    )(tiled, w_x.reshape(9, CH, 4 * CH), w_h.reshape(9, CH, 4 * CH), gate_bias.reshape(1, -1),
      h_init.reshape(S, R, HG, COLS, CH), c_init)
    h_all, c_final = pl.pallas_call(
        store,
        out_shape=(jax.ShapeDtypeStruct(tiled.shape, bf), jax.ShapeDtypeStruct(c_init.shape, f32)),
        in_specs=[vmem] * 4,
        out_specs=(hbm, hbm),
        scratch_shapes=[vm((2, R, HW, CH), f32), dma((4,))],
        compiler_params=pltpu.CompilerParams(vmem_limit_bytes=4 * 2**20),
    )(*[pltpu.with_memory_space_constraint(a, pltpu.VMEM) for a in parts])
    return h_all.reshape(frames.shape), c_final


def solution(mesh, K=None):
    n_rows = mesh.shape["rows"]
    frame_spec = P(None, "batch", "rows", "cols", None)
    state_spec = P("batch", "rows", "cols", None)
    blocks = BLOCKS if K is None else K
    return jax.shard_map(functools.partial(run, blocks, n_rows), mesh=mesh,
                         in_specs=(frame_spec, P(), P(), P(), state_spec, state_spec),
                         out_specs=(frame_spec, state_spec), check_vma=False)
```

```python
import functools

import jax
import jax.numpy as jnp
from jax import lax
from jax.experimental import pallas as pl
from jax.experimental.pallas import tpu as pltpu
from jax.sharding import PartitionSpec as P

MESH = pl.DeviceIdType.MESH
CH = 64
LANES = 128
COLS = 8
PIECE = 4
RING = 8
BLOCKS = (8, 8)
LATE = (3, 3)
BORDER = 4
TURN_NS = 900
FAR = 16


def cuts(lo, hi, size=PIECE):
    n = max(1, (hi - lo) // size)
    edges = [lo + i * size for i in range(n)] + [hi]
    return list(zip(edges[:-1], edges[1:]))


class Plan:
    def __init__(self, blocks, T, R, W):
        assert sum(blocks) == T
        self.blocks, self.T, self.R, self.W, self.HW, self.HG = blocks, T, R, W, W // 2, W // 2 // COLS
        self.K = max(blocks)
        self.first = [sum(blocks[:b]) for b in range(len(blocks))]
        self.of = [(b, o) for b, k in enumerate(blocks) for o in range(k)]
        self.xrows = [blocks[b] - o for b, o in self.of]
        self.xat = [sum(self.xrows[:t]) for t in range(T + 1)]
        self.parts = [[(0, 1), (1, 2), (2, 3), (3, k)] if b == 0 else [(0, k)] for b, k in enumerate(blocks)]
        self.hat = [sum(blocks[:b]) for b in range(len(blocks) + 1)]
        self.cat = [sum(k - 1 for k in blocks[:b]) for b in range(len(blocks) + 1)]
        ends = [0, 1, 3, blocks[0] + 1, T]
        self.groups = [(a, e) for a, e in zip(ends[:-1], ends[1:]) if e > a]


def kernel(plan, n_rows, frames, w_x, w_h, bias_in, h_init, c_init, hout, hpeer, cout, cpeer,
           bias, hgo, cgo, cgp, cin, xgo, xin, hst, cst, xh_even, xh_odd, cbuf, shift, wbuf,
           xs_ref, xr_ref, hs_ref, hr_ref, cs_ref, cr_ref,
           s_w, s_i, s_ir, s_is, s_x, s_xr, s_xs, s_b, s_bs, s_or, s_os, here_sem):
    T, R, W, HW, HG = plan.T, plan.R, plan.W, plan.HW, plan.HG
    PAD = plan.K
    NB = len(plan.blocks)
    s = lax.axis_index("cols")
    n = lax.axis_index("rows")
    p = 1 - s
    mine, theirs = pl.ds(s * HG, HG), pl.ds(p * HG, HG)
    mine_c, theirs_c = [pl.ds(pl.multiple_of(i * HW, HW), HW) for i in (s, p)]
    has_up, has_dn = n > 0, n < n_rows - 1
    bf, f32 = jnp.bfloat16, jnp.float32

    def local(src, dst, sem):
        return pltpu.make_async_copy(src, dst, sem)

    def remote(src, dst, ssem, rsem, dev):
        return pltpu.make_async_remote_copy(
            src_ref=src, dst_ref=dst, send_sem=ssem, recv_sem=rsem, device_id=dev, device_id_type=MESH)

    peer = {"cols": p}
    side_dev = [{"rows": n - 1}, {"rows": n + 1}]
    side_ok = [has_up, has_dn]

    def each_side(do):
        for side in range(2):
            @pl.when(side_ok[side])
            def _():
                do(side)

    barrier = pltpu.get_barrier_semaphore()

    def signal(dev):
        pl.semaphore_signal(barrier, inc=1, device_id=dev, device_id_type=MESH)

    signal(peer)

    @pl.when(has_up)
    def _():
        signal(side_dev[0])


    h_own = local(h_init.at[s], hst.at[:, mine], s_i.at[0])
    c_own = local(c_init.at[s], cst, s_i.at[1])
    x_own = [local(frames.at[a:e, s], xin.at[a:e, :, mine], s_x.at[g]) for g, (a, e) in enumerate(plan.groups)]
    h_got = local(h_init.at[p], hgo, s_i.at[2])
    c_got = local(c_init.at[p], cgo, s_i.at[3])
    x_got = [local(frames.at[a:e, p], xgo.at[a:e], s_i.at[4 + g]) for g, (a, e) in enumerate(plan.groups[:2])]
    w_copies = [local(w_h, wbuf.at[0:9, 0], s_w.at[0]), local(w_x, wbuf.at[0:9, 1], s_w.at[1]),
                local(bias_in, bias, s_w.at[2])]
    for c in [h_got, x_got[0], c_got, h_own, x_own[0], c_own, *w_copies, x_got[1], *x_own[1:]]:
        c.start()
    with jax.named_scope('barrier'):
        pl.semaphore_wait(barrier, 1 + has_dn.astype(jnp.int32))

    @pl.when(has_dn)
    def _():
        pl.semaphore_signal(here_sem, inc=1, device_id=side_dev[1], device_id_type=MESH)


    h_push = remote(hgo, hst.at[:, mine], s_is.at[0], s_ir.at[0], peer)
    c_push = remote(cgp, cin, s_is.at[1], s_ir.at[1], peer)
    x_push = [remote((xgo if g < 2 else frames.at[:, p]).at[a:e], xin.at[a:e, :, mine], s_xs.at[g], s_xr.at[g], peer)
              for g, (a, e) in enumerate(plan.groups)]
    with jax.named_scope('got_wait'):
        for got, push in [(h_got, h_push), (x_got[0], x_push[0]), (c_got, c_push), (x_got[1], x_push[1])]:
            got.wait()
            if push is c_push:
                cgp[...] = jnp.concatenate([cgo[:, :HW // 2], cgo[:, HW // 2:]], axis=2)
            push.start()
    for push in x_push[2:]:
        push.start()

    shift[...] = jnp.zeros_like(shift)
    low = lax.broadcasted_iota(jnp.int32, (1, LANES), 1) < CH
    low_half = low_row = low
    turn = [0]
    scale = jnp.where(low_row, 0.5, 1.0)
    lift = jnp.where(low_row, 0.5, 0.0)

    with jax.named_scope('w_wait'):
        for c in w_copies:
            c.wait()
    for tap in range(9):
        for half in range(2):
            tile = wbuf[tap, half, :, 0:LANES]
            wbuf[tap, half, :, 0:LANES] = jnp.concatenate([tile[:, CH:], tile[:, :CH]], axis=1)
    b_all = bias[...]
    rest = jnp.concatenate([b_all[:, CH:LANES], b_all[:, :CH], b_all[:, LANES:]], axis=1)
    row = lax.broadcasted_iota(jnp.int32, (CH, 4 * CH), 0)
    rows = jnp.zeros((CH, 4 * CH), f32)
    for i in range(3):
        top = (rest * (1 - 2.0 ** -8)).astype(bf).astype(f32) if i == 0 else rest.astype(bf).astype(f32)
        rows = jnp.where(row == i, top, rows)
        rest = rest - top
    wbuf[9, 0] = rows.astype(bf)
    wbuf[9, 1] = jnp.zeros((CH, 4 * CH), bf)
    ones = jnp.where(lax.broadcasted_iota(jnp.int32, (1, LANES), 1) < 3, 1.0, 0.0).astype(bf)

    def pack(v):
        return jnp.concatenate([v[:, :HG], v[:, HG:]], axis=3)

    def unpack(v):
        return jnp.concatenate([v[..., :CH], v[..., CH:]], axis=1)

    def masked(r, v):
        if 0 <= r < R:
            return v
        return lax.select(jnp.broadcast_to(has_up if r < 0 else has_dn, v.shape), v, jnp.zeros_like(v))

    def emit(t, lo, hi, hx):
        nxt = xh_even if t % 2 == 0 else xh_odd
        at, to = slot(lo, hi), cells_of(lo, hi)
        shift[at, 8:8 + W, :] = hx.reshape(hi - lo, W, LANES)
        nxt[1, to] = hx.astype(bf)
        nxt[0, to] = shift[at, 7:7 + W, :].reshape(hx.shape).astype(bf)
        nxt[2, to] = shift[at, 9:9 + W, :].reshape(hx.shape).astype(bf)

    def cells_of(lo, hi):
        return slice((lo + PAD) * W, (hi + PAD) * W)

    def slot(lo, hi):
        if turn[0] + hi - lo > RING:
            turn[0] = 0
        turn[0] += hi - lo
        return slice(turn[0] - (hi - lo), turn[0])

    def flat(v):
        return v.reshape(-1, v.shape[-1])

    def x_rows(t, lo, hi):
        if lo >= 0 and hi <= R:
            return flat(xin[t, lo:hi].astype(f32))
        side, i = (0, lo + plan.xrows[t]) if lo < 0 else (1, lo - R)
        return flat(unpack(xr_ref[side, plan.xat[t] + i:plan.xat[t] + i + hi - lo].astype(f32)))

    def wait_x(g):
        if g < len(plan.groups):
            x_own[g].wait()
            x_push[g].wait_recv()

    def border(b, kind, side):
        f = plan.first[b]
        if kind < 2:
            src, dst, at = [(hs_ref, hr_ref, plan.hat), (cs_ref, cr_ref, plan.cat)][kind]
            at, end = at[b], at[b + 1]
        else:
            src, dst = xs_ref, xr_ref
            at, end = [plan.xat[f + o] for o in plan.parts[b][kind - 2]]
        return remote(src.at[side, at:end], dst.at[1 - side, at:end],
                      s_bs.at[min(kind, 2), side], s_b.at[kind, 1 - side, b], side_dev[side])

    def pack_x(t0, t1):
        for side in range(2):
            for t in range(t0, t1):
                m = plan.xrows[t]
                lo = 0 if side == 0 else R - m
                xs_ref[side, plan.xat[t]:plan.xat[t] + m] = pack(xin[t, lo:lo + m])

    def start_border(b, *kinds):
        each_side(lambda side: [border(b, kind, side).start() for kind in kinds])

    far = lax.rem(n, FAR) == 0

    def start_first(side, late, *kinds):
        ok = has_dn if side else jnp.logical_and(has_up, far if late else jnp.logical_not(far))

        @pl.when(ok)
        def _():
            if not side and 0 in kinds:
                pl.semaphore_wait(here_sem, 1)
                if late:
                    @pl.when(s == 1)
                    def _():
                        pl.delay(TURN_NS)

            for kind in kinds:
                border(0, kind, side).start()

    def wait_border(b, *kinds):
        each_side(lambda side: [border(b, kind, 1 - side).wait_recv() for kind in kinds])

    def pack_h(b, h_rows):
        k = plan.blocks[b]
        for side in range(2):
            lo = 0 if side == 0 else R - k
            hs_ref[side, plan.hat[b]:plan.hat[b] + k] = pack(h_rows[lo:lo + k])

    def pack_c(b):
        k = plan.blocks[b]
        for side in range(2):
            lo = PAD if side == 0 else PAD + R - (k - 1)
            c = cbuf[lo:lo + k - 1]
            cs_ref[side, plan.cat[b]:plan.cat[b] + k - 1] = jnp.where(low_half, c[:, :HW], c[:, HW:])

    weights = wbuf[...].reshape(10 * LANES, 4 * CH)

    def dot(t, lo, hi):
        cur = xh_even if t % 2 == 0 else xh_odd
        taps = [cur[dc, cells_of(lo + dr - 1, hi + dr - 1)] for dr in range(3) for dc in range(3)]
        taps.append(jnp.broadcast_to(ones, taps[0].shape))
        return jnp.dot(jnp.concatenate(taps, axis=1), weights, preferred_element_type=f32)

    def cells(t, lo, hi, gates):
        fi = jnp.tanh(gates[:, :LANES] * 0.5) * 0.5 + 0.5
        og = jnp.tanh(gates[:, LANES:] * scale) * scale + lift
        at = slice(lo + PAD, hi + PAD)
        prod = fi * lax.select(jnp.broadcast_to(low, og.shape), cbuf[at].reshape(og.shape), og)
        c = prod + pltpu.roll(prod, CH, 1)
        h = (og * jnp.tanh(c))[:, :CH]
        if t == T - 1:
            c = c.reshape(hi - lo, 2, 2, HW // 2, LANES)
            for half in range(2):
                both = c[:, half, 0]
                cout[half, lo:hi] = lax.select(jnp.broadcast_to(low, both.shape), both, c[:, half, 1])
        else:
            cbuf[at] = c.reshape(hi - lo, W, LANES)
        for a, e in ((lo, min(hi, 0)), (max(lo, 0), min(hi, R)), (max(lo, R), hi)):
            if a >= e:
                continue
            part = h[(a - lo) * W:(e - lo) * W]
            if a >= 0 and e <= R:
                hout[t, a:e] = part.reshape(e - a, 2 * HG, COLS, CH).astype(bf)
            if t < T - 1:
                emit(t + 1, a, e, masked(a, jnp.concatenate([part, x_rows(t + 1, a, e)], axis=1)))

    pending = []

    def piece(at, ahead=1):
        t, lo, hi = at
        while any(u == t - 1 and a <= hi and lo <= e for u, a, e, _ in pending):
            cells(*pending.pop(0))
        pending.append((*at, dot(*at)))
        flush(ahead)

    def flush(left=0):
        while len(pending) > left:
            cells(*pending.pop(0))

    def push_h(t0, t1, lo=0, hi=R):
        rows = slice(lo, hi)
        remote(hout.at[t0:t1, rows, theirs], hpeer.at[t0:t1, rows], s_os.at[0], s_or.at[0], peer).start()

    def push_c(lo, hi):
        remote(cout.at[p, lo:hi], cpeer.at[lo:hi], s_os.at[1], s_or.at[1], peer).start()

    with jax.named_scope('state_wait'):
        for c in [h_own, x_own[0]]:
            c.wait()
        for c in [h_push, x_push[0]]:
            c.wait_recv()
    pack_h(0, hst)
    pack_x(0, 1)
    start_first(1, 0, 0, 2)
    start_first(0, 0, 0, 2)
    for lo, hi in cuts(0, R):
        emit(0, lo, hi, jnp.concatenate([flat(hst[lo:hi].astype(f32)), x_rows(0, lo, hi)], axis=1))

    for b, k in enumerate(plan.blocks):
        f = plan.first[b]
        last = b + 1 == NB

        def inner(o):
            if o == 0:
                got = [*cuts(k + 1, R - 1 - k), *cuts(1, k + 1), *cuts(R - 1 - k, R - 1)]
            else:
                got = cuts(o + 1, R - 1 - o)
                got = got[1:-1] + [got[0], got[-1]]
            return [(f + o, lo, hi) for lo, hi in got]

        early = [at for o in range(k) for at in inner(o)]
        late = early[len(early) - LATE[b]:]
        for o in range(k):
            pieces = [at for at in early[:len(early) - LATE[b]] if at[0] == f + o]
            first = 0
            if o == 0 and b:
                piece(pieces[0], 9)
                flush(1)
                pack_h(b, hout.at[f - 1])
                pack_c(b)
                with jax.named_scope(f'send{b}'):
                    start_border(b, 0, 1)
                first = 1
            if b == 0 and o == 0:
                for at in pieces[:2]:
                    piece(at, 9)
                with jax.named_scope('x_wait0'):
                    c_own.wait()
                    c_push.wait_recv()
                    wait_x(1)
                for at in pieces[2:4]:
                    piece(at, 9)
                c0, got = cst[...], cin[...]
                cbuf[PAD:PAD + R, mine_c] = jnp.concatenate([c0, c0], axis=2)
                swapped, keep = pltpu.roll(got, CH, 2), jnp.broadcast_to(low, got.shape)
                both = [lax.select(keep, got, swapped), lax.select(keep, swapped, got)]
                cbuf[PAD:PAD + R, theirs_c] = jnp.concatenate(both, axis=1)
                pack_c(0)
                pack_x(1, 3)
                start_first(1, 0, 1, 3, 4)
                start_first(0, 0, 1, 3, 4)
                first = 4
            if b == 0 and o == 2:
                for at in pieces[:2]:
                    piece(at, 9)
                flush(2)
                with jax.named_scope('x_wait1'):
                    wait_x(2)
                for at in pieces[2:4]:
                    piece(at, 9)
                pack_x(3, k)
                for side in range(2):
                    start_first(side, 0, 5)
                start_first(0, 1, 5)
                first = 4
            for at in pieces[first:]:
                piece(at)
            if b == 0 and o == 0:
                with jax.named_scope('upsend'):
                    start_first(0, 1, 0, 2, 1, 3, 4)
            if o == 0 and b and not last:
                pack_x(f + k, f + k + plan.blocks[b + 1])
        with jax.named_scope(f'mid{b}'):
            wait_border(b, 0, 2)
        if b == 0:
            wait_x(3)
        elif not last:
            start_border(b + 1, 2)
        if b:
            push_h(plan.first[b - 1], f)
        piece(late.pop(0), 3)
        for side in range(2):
            lo = -k if side == 0 else R
            h = flat(unpack(hr_ref[side, plan.hat[b]:plan.hat[b] + k].astype(f32)))
            emit(f, lo, lo + k, masked(lo, jnp.concatenate([h, x_rows(f, lo, lo + k)], axis=1)))
        for o in range(k):
            m = k - 1 - o
            top, bottom = cuts(-m, o + 1, BORDER), cuts(R - 1 - o, R + m, BORDER)
            for lo, hi in top:
                piece((f + o, lo, hi), 9 if o == 0 else 1)
                if lo != top[0][0]:
                    continue
                if b == 0 and o in (1, 2):
                    with jax.named_scope(f'midx{o}'):
                        wait_border(0, 3 + o)
                if last and o == k // 2:
                    push_h(f, f + o)
                if last and o == k - 2:
                    push_h(f + k // 2, f + o)
                    push_h(T - 1, T, k, R - k)
                    push_c(k, R - k)
                if last and o == k - 1:
                    push_h(T - 2, T - 1)
            for lo, hi in bottom:
                piece((f + o, lo, hi), 9 if o == 0 else 1)
            if o == 0:
                with jax.named_scope(f'midc{b}'):
                    wait_border(b, 1, *(() if b else (3,)))
                for side in range(2):
                    lo = PAD - (k - 1) if side == 0 else PAD + R
                    packed = cr_ref[side, plan.cat[b]:plan.cat[b] + k - 1]
                    both = jnp.concatenate([packed, pltpu.roll(packed, CH, 2)], axis=1)
                    cbuf[lo:lo + k - 1] = both
                while late:
                    piece(late.pop(0), 3)
            if o == 0 and b == 0 and not last:
                pack_x(f + k, f + k + plan.blocks[b + 1])
                start_border(b + 1, 2)
        assert not late
    flush()
    k = plan.blocks[-1]
    for lo, hi in ((0, k), (R - k, R)):
        push_h(T - 1, T, lo, hi)
        push_c(lo, hi)

    with jax.named_scope('end_wait'):
        for c in [h_push, c_push, *x_push]:
            c.wait_send()

        def wait_sends(side):
            for kind, ref in enumerate((hs_ref, cs_ref, xs_ref)):
                local(ref.at[side], ref.at[side], s_bs.at[kind, side]).wait()

        each_side(wait_sends)
        for sem in (s_os, s_or):
            local(hpeer, hpeer, sem.at[0]).wait()
            local(cpeer, cpeer, sem.at[1]).wait()


def store(hout, hpeer, cout, cpeer, h_all, c_final, c_tile, sems):
    s = lax.axis_index("cols")
    HG = hpeer.shape[2]
    copies = [pltpu.make_async_copy(hout.at[:, :, pl.ds(s * HG, HG)], h_all.at[:, s], sems.at[0]),
              pltpu.make_async_copy(hpeer, h_all.at[:, 1 - s], sems.at[1]),
              pltpu.make_async_copy(c_tile.at[0], c_final.at[s], sems.at[2]),
              pltpu.make_async_copy(c_tile.at[1], c_final.at[1 - s], sems.at[3])]
    for c in copies[:2]:
        c.start()
    for i, packed in enumerate((cout[s], cpeer[...])):
        c_tile[i] = jnp.concatenate([packed[:, :, :CH], packed[:, :, CH:]], axis=1)
    for c in copies[2:]:
        c.start()
    for c in copies:
        c.wait()


def run(blocks, n_rows, frames, w_x, w_h, gate_bias, h_init, c_init):
    T, S, R, HW = frames.shape[:4]
    W, HG = 2 * HW, HW // COLS
    plan = Plan(blocks, T, R, W)
    NB, PAD, G = len(blocks), plan.K, len(plan.groups)
    bf, f32 = jnp.bfloat16, jnp.float32
    vm, dma = pltpu.VMEM, pltpu.SemaphoreType.DMA
    hbm = pl.BlockSpec(memory_space=pltpu.HBM)
    vmem = pl.BlockSpec(memory_space=pltpu.VMEM)
    tiled = frames.reshape(T, S, R, HG, COLS, CH)
    parts = pl.pallas_call(
        functools.partial(kernel, plan, n_rows),
        out_shape=(vm((T, R, 2 * HG, COLS, CH), bf), vm((T, R, HG, COLS, CH), bf),
                   vm((2, R, HW // 2, LANES), f32), vm((R, HW // 2, LANES), f32)),
        in_specs=[hbm] * 6,
        out_specs=(vmem,) * 4,
        scratch_shapes=[
            vm((1, 4 * CH), f32), vm((R, HG, COLS, CH), bf), vm((R, HW, CH), f32),
            vm((R, HW // 2, LANES), f32), vm((R, HW // 2, LANES), f32),
            vm((plan.groups[1][1], R, HG, COLS, CH), bf),
            vm((T, R, 2 * HG, COLS, CH), bf), vm((R, 2 * HG, COLS, CH), bf), vm((R, HW, CH), f32),
            vm((3, (R + 2 * PAD) * W, LANES), bf), vm((3, (R + 2 * PAD) * W, LANES), bf),
            vm((R + 2 * PAD, W, LANES), f32), vm((RING, W + 16, LANES), f32), vm((10, 2, CH, 4 * CH), bf),
            vm((2, plan.xat[-1], HG, COLS, LANES), bf), vm((2, plan.xat[-1], HG, COLS, LANES), bf),
            vm((2, plan.hat[-1], HG, COLS, LANES), bf), vm((2, plan.hat[-1], HG, COLS, LANES), bf),
            vm((2, plan.cat[-1], HW, LANES), f32), vm((2, plan.cat[-1], HW, LANES), f32),
            dma((3,)), dma((6,)), dma((2,)), dma((2,)), dma((G,)), dma((G,)), dma((G,)),
            dma((6, 2, NB)), dma((3, 2)), dma((2,)), dma((2,)), pltpu.SemaphoreType.REGULAR],
        compiler_params=pltpu.CompilerParams(collective_id=0, has_side_effects=True, vmem_limit_bytes=46 * 2**20),
    )(tiled, w_x.reshape(9, CH, 4 * CH), w_h.reshape(9, CH, 4 * CH), gate_bias.reshape(1, -1),
      h_init.reshape(S, R, HG, COLS, CH), c_init)
    h_all, c_final = pl.pallas_call(
        store,
        out_shape=(jax.ShapeDtypeStruct(tiled.shape, bf), jax.ShapeDtypeStruct(c_init.shape, f32)),
        in_specs=[vmem] * 4,
        out_specs=(hbm, hbm),
        scratch_shapes=[vm((2, R, HW, CH), f32), dma((4,))],
        compiler_params=pltpu.CompilerParams(vmem_limit_bytes=4 * 2**20),
    )(*[pltpu.with_memory_space_constraint(a, pltpu.VMEM) for a in parts])
    return h_all.reshape(frames.shape), c_final


def solution(mesh, K=None):
    n_rows = mesh.shape["rows"]
    frame_spec = P(None, "batch", "rows", "cols", None)
    state_spec = P("batch", "rows", "cols", None)
    blocks = BLOCKS if K is None else K
    return jax.shard_map(functools.partial(run, blocks, n_rows), mesh=mesh,
                         in_specs=(frame_spec, P(), P(), P(), state_spec, state_spec),
                         out_specs=(frame_spec, state_spec), check_vma=False)
```

```python
import functools

import jax
import jax.numpy as jnp
from jax import lax
from jax.experimental import pallas as pl
from jax.experimental.pallas import tpu as pltpu
from jax.sharding import PartitionSpec as P

MESH = pl.DeviceIdType.MESH
CH = 64
LANES = 128
COLS = 8
PIECE = 4
RING = 8
BLOCKS = (7, 9)
LATE = (3, 3)
BORDER = 3
FAR = 16


def cuts(lo, hi, size=PIECE):
    n = max(1, (hi - lo) // size)
    edges = [lo + i * size for i in range(n)] + [hi]
    return list(zip(edges[:-1], edges[1:]))


def even_cuts(lo, hi):
    n = max(1, round((hi - lo) / BORDER))
    edges = [lo + (hi - lo) * i // n for i in range(n + 1)]
    return list(zip(edges[:-1], edges[1:]))


class Plan:
    def __init__(self, blocks, T, R, W):
        assert sum(blocks) == T
        self.blocks, self.T, self.R, self.W, self.HW, self.HG = blocks, T, R, W, W // 2, W // 2 // COLS
        self.K = max(blocks)
        self.first = [sum(blocks[:b]) for b in range(len(blocks))]
        self.of = [(b, o) for b, k in enumerate(blocks) for o in range(k)]
        self.xrows = [blocks[b] - o for b, o in self.of]
        self.xat = [sum(self.xrows[:t]) for t in range(T + 1)]
        self.parts = [[(0, 1), (1, 2), (2, 3), (3, k)] if b == 0 else [(0, k)] for b, k in enumerate(blocks)]
        self.hat = [sum(blocks[:b]) for b in range(len(blocks) + 1)]
        self.cat = [sum(k - 1 for k in blocks[:b]) for b in range(len(blocks) + 1)]
        ends = [0, 1, 3, blocks[0] + 1, T]
        self.groups = [(a, e) for a, e in zip(ends[:-1], ends[1:]) if e > a]


def kernel(plan, n_rows, frames, w_x, w_h, bias_in, h_init, c_init, hout, hpeer, cout, cpeer,
           bias, hgo, cgo, cgp, cin, xgo, xin, hst, cst, xh_even, xh_odd, cbuf, shift, wbuf,
           xs_ref, xr_ref, hs_ref, hr_ref, cs_ref, cr_ref,
           s_w, s_i, s_ir, s_is, s_x, s_xr, s_xs, s_b, s_bs, s_or, s_os, here_sem):
    T, R, W, HW, HG = plan.T, plan.R, plan.W, plan.HW, plan.HG
    PAD = plan.K
    NB = len(plan.blocks)
    s = lax.axis_index("cols")
    n = lax.axis_index("rows")
    p = 1 - s
    mine, theirs = pl.ds(s * HG, HG), pl.ds(p * HG, HG)
    mine_c, theirs_c = [pl.ds(pl.multiple_of(i * HW, HW), HW) for i in (s, p)]
    has_up, has_dn = n > 0, n < n_rows - 1
    bf, f32 = jnp.bfloat16, jnp.float32

    def local(src, dst, sem):
        return pltpu.make_async_copy(src, dst, sem)

    def remote(src, dst, ssem, rsem, dev):
        return pltpu.make_async_remote_copy(
            src_ref=src, dst_ref=dst, send_sem=ssem, recv_sem=rsem, device_id=dev, device_id_type=MESH)

    peer = {"cols": p}
    side_dev = [{"rows": n - 1}, {"rows": n + 1}]
    side_ok = [has_up, has_dn]

    def each_side(do):
        for side in range(2):
            @pl.when(side_ok[side])
            def _():
                do(side)

    barrier = pltpu.get_barrier_semaphore()

    def signal(dev):
        pl.semaphore_signal(barrier, inc=1, device_id=dev, device_id_type=MESH)

    signal(peer)

    @pl.when(has_up)
    def _():
        signal(side_dev[0])


    h_own = local(h_init.at[s], hst.at[:, mine], s_i.at[0])
    c_own = local(c_init.at[s], cst, s_i.at[1])
    x_own = [local(frames.at[a:e, s], xin.at[a:e, :, mine], s_x.at[g]) for g, (a, e) in enumerate(plan.groups)]
    h_got = local(h_init.at[p], hgo, s_i.at[2])
    c_got = local(c_init.at[p], cgo, s_i.at[3])
    x_got = [local(frames.at[a:e, p], xgo.at[a:e], s_i.at[4 + g]) for g, (a, e) in enumerate(plan.groups[:2])]
    w_copies = [local(w_h, wbuf.at[0:9, 0], s_w.at[0]), local(w_x, wbuf.at[0:9, 1], s_w.at[1]),
                local(bias_in, bias, s_w.at[2])]
    for c in [h_got, x_got[0], c_got, h_own, x_own[0], c_own, *w_copies, x_got[1], *x_own[1:]]:
        c.start()
    with jax.named_scope('barrier'):
        pl.semaphore_wait(barrier, 1 + has_dn.astype(jnp.int32))

    @pl.when(has_dn)
    def _():
        pl.semaphore_signal(here_sem, inc=1, device_id=side_dev[1], device_id_type=MESH)


    h_push = remote(hgo, hst.at[:, mine], s_is.at[0], s_ir.at[0], peer)
    c_push = remote(cgp, cin, s_is.at[1], s_ir.at[1], peer)
    x_push = [remote((xgo if g < 2 else frames.at[:, p]).at[a:e], xin.at[a:e, :, mine], s_xs.at[g], s_xr.at[g], peer)
              for g, (a, e) in enumerate(plan.groups)]
    with jax.named_scope('got_wait'):
        for got, push in [(h_got, h_push), (x_got[0], x_push[0]), (c_got, c_push), (x_got[1], x_push[1])]:
            got.wait()
            if push is c_push:
                cgp[...] = jnp.concatenate([cgo[:, :HW // 2], cgo[:, HW // 2:]], axis=2)
            push.start()
    for push in x_push[2:]:
        push.start()

    shift[...] = jnp.zeros_like(shift)
    low = lax.broadcasted_iota(jnp.int32, (1, LANES), 1) < CH
    low_half = low_row = low
    turn = [0]
    scale = jnp.where(low_row, 0.5, 1.0)
    lift = jnp.where(low_row, 0.5, 0.0)

    with jax.named_scope('w_wait'):
        for c in w_copies:
            c.wait()
    for tap in range(9):
        for half in range(2):
            tile = wbuf[tap, half, :, 0:LANES]
            wbuf[tap, half, :, 0:LANES] = jnp.concatenate([tile[:, CH:], tile[:, :CH]], axis=1)
    b_all = bias[...]
    rest = jnp.concatenate([b_all[:, CH:LANES], b_all[:, :CH], b_all[:, LANES:]], axis=1)
    row = lax.broadcasted_iota(jnp.int32, (CH, 4 * CH), 0)
    rows = jnp.zeros((CH, 4 * CH), f32)
    for i in range(3):
        top = (rest * (1 - 2.0 ** -8)).astype(bf).astype(f32) if i == 0 else rest.astype(bf).astype(f32)
        rows = jnp.where(row == i, top, rows)
        rest = rest - top
    wbuf[9, 0] = rows.astype(bf)
    wbuf[9, 1] = jnp.zeros((CH, 4 * CH), bf)
    ones = jnp.where(lax.broadcasted_iota(jnp.int32, (1, LANES), 1) < 3, 1.0, 0.0).astype(bf)

    def pack(v):
        return jnp.concatenate([v[:, :HG], v[:, HG:]], axis=3)

    def unpack(v):
        return jnp.concatenate([v[..., :CH], v[..., CH:]], axis=1)

    def masked(r, v):
        if 0 <= r < R:
            return v
        return lax.select(jnp.broadcast_to(has_up if r < 0 else has_dn, v.shape), v, jnp.zeros_like(v))

    def emit(t, lo, hi, hx):
        nxt = xh_even if t % 2 == 0 else xh_odd
        at, to = slot(lo, hi), cells_of(lo, hi)
        shift[at, 8:8 + W, :] = hx.reshape(hi - lo, W, LANES)
        nxt[1, to] = hx.astype(bf)
        nxt[0, to] = shift[at, 7:7 + W, :].reshape(hx.shape).astype(bf)
        nxt[2, to] = shift[at, 9:9 + W, :].reshape(hx.shape).astype(bf)

    def cells_of(lo, hi):
        return slice((lo + PAD) * W, (hi + PAD) * W)

    def slot(lo, hi):
        if turn[0] + hi - lo > RING:
            turn[0] = 0
        turn[0] += hi - lo
        return slice(turn[0] - (hi - lo), turn[0])

    def flat(v):
        return v.reshape(-1, v.shape[-1])

    def x_rows(t, lo, hi):
        if lo >= 0 and hi <= R:
            return flat(xin[t, lo:hi].astype(f32))
        side, i = (0, lo + plan.xrows[t]) if lo < 0 else (1, lo - R)
        return flat(unpack(xr_ref[side, plan.xat[t] + i:plan.xat[t] + i + hi - lo].astype(f32)))

    def wait_x(g):
        if g < len(plan.groups):
            x_own[g].wait()
            x_push[g].wait_recv()

    def border(b, kind, side):
        f = plan.first[b]
        if kind < 2:
            src, dst, at = [(hs_ref, hr_ref, plan.hat), (cs_ref, cr_ref, plan.cat)][kind]
            at, end = at[b], at[b + 1]
        else:
            src, dst = xs_ref, xr_ref
            at, end = [plan.xat[f + o] for o in plan.parts[b][kind - 2]]
        return remote(src.at[side, at:end], dst.at[1 - side, at:end],
                      s_bs.at[min(kind, 2), side], s_b.at[kind, 1 - side, b], side_dev[side])

    def pack_x(t0, t1):
        for side in range(2):
            for t in range(t0, t1):
                m = plan.xrows[t]
                lo = 0 if side == 0 else R - m
                xs_ref[side, plan.xat[t]:plan.xat[t] + m] = pack(xin[t, lo:lo + m])

    def start_border(b, *kinds):
        each_side(lambda side: [border(b, kind, side).start() for kind in kinds])

    far = lax.rem(n, FAR) == 0

    def start_first(side, late, *kinds):
        ok = has_dn if side else jnp.logical_and(has_up, far if late else jnp.logical_not(far))

        @pl.when(ok)
        def _():
            if not side and 0 in kinds:
                pl.semaphore_wait(here_sem, 1)
            for kind in kinds:
                border(0, kind, side).start()

    def wait_border(b, *kinds):
        each_side(lambda side: [border(b, kind, 1 - side).wait_recv() for kind in kinds])

    def pack_h(b, h_rows):
        k = plan.blocks[b]
        for side in range(2):
            lo = 0 if side == 0 else R - k
            hs_ref[side, plan.hat[b]:plan.hat[b] + k] = pack(h_rows[lo:lo + k])

    def pack_c(b):
        k = plan.blocks[b]
        for side in range(2):
            lo = PAD if side == 0 else PAD + R - (k - 1)
            c = cbuf[lo:lo + k - 1]
            cs_ref[side, plan.cat[b]:plan.cat[b] + k - 1] = jnp.where(low_half, c[:, :HW], c[:, HW:])

    weights = wbuf[...].reshape(10 * LANES, 4 * CH)

    def dot(t, lo, hi):
        cur = xh_even if t % 2 == 0 else xh_odd
        taps = [cur[dc, cells_of(lo + dr - 1, hi + dr - 1)] for dr in range(3) for dc in range(3)]
        taps.append(jnp.broadcast_to(ones, taps[0].shape))
        return jnp.dot(jnp.concatenate(taps, axis=1), weights, preferred_element_type=f32)

    def cells(t, lo, hi, gates):
        fi = jnp.tanh(gates[:, :LANES] * 0.5) * 0.5 + 0.5
        og = jnp.tanh(gates[:, LANES:] * scale) * scale + lift
        at = slice(lo + PAD, hi + PAD)
        prod = fi * lax.select(jnp.broadcast_to(low, og.shape), cbuf[at].reshape(og.shape), og)
        c = prod + pltpu.roll(prod, CH, 1)
        h = (og * jnp.tanh(c))[:, :CH]
        if t == T - 1:
            c = c.reshape(hi - lo, 2, 2, HW // 2, LANES)
            for half in range(2):
                both = c[:, half, 0]
                cout[half, lo:hi] = lax.select(jnp.broadcast_to(low, both.shape), both, c[:, half, 1])
        else:
            cbuf[at] = c.reshape(hi - lo, W, LANES)
        for a, e in ((lo, min(hi, 0)), (max(lo, 0), min(hi, R)), (max(lo, R), hi)):
            if a >= e:
                continue
            part = h[(a - lo) * W:(e - lo) * W]
            if a >= 0 and e <= R:
                hout[t, a:e] = part.reshape(e - a, 2 * HG, COLS, CH).astype(bf)
            if t < T - 1:
                emit(t + 1, a, e, masked(a, jnp.concatenate([part, x_rows(t + 1, a, e)], axis=1)))

    pending = []

    def piece(at, ahead=1):
        t, lo, hi = at
        while any(u == t - 1 and a <= hi and lo <= e for u, a, e, _ in pending):
            cells(*pending.pop(0))
        pending.append((*at, dot(*at)))
        flush(ahead)

    def flush(left=0):
        while len(pending) > left:
            cells(*pending.pop(0))

    def push_h(t0, t1, lo=0, hi=R):
        rows = slice(lo, hi)
        remote(hout.at[t0:t1, rows, theirs], hpeer.at[t0:t1, rows], s_os.at[0], s_or.at[0], peer).start()

    def push_c(lo, hi):
        remote(cout.at[p, lo:hi], cpeer.at[lo:hi], s_os.at[1], s_or.at[1], peer).start()

    with jax.named_scope('state_wait'):
        for c in [h_own, x_own[0]]:
            c.wait()
        for c in [h_push, x_push[0]]:
            c.wait_recv()
    pack_h(0, hst)
    pack_x(0, 1)
    start_first(1, 0, 0, 2)
    start_first(0, 0, 0, 2)
    for lo, hi in cuts(0, R):
        emit(0, lo, hi, jnp.concatenate([flat(hst[lo:hi].astype(f32)), x_rows(0, lo, hi)], axis=1))

    for b, k in enumerate(plan.blocks):
        f = plan.first[b]
        last = b + 1 == NB

        def inner(o):
            if o == 0:
                got = [*cuts(k + 1, R - 1 - k), *cuts(1, k + 1), *cuts(R - 1 - k, R - 1)]
            else:
                got = cuts(o + 1, R - 1 - o)
                got = got[1:-1] + [got[0], got[-1]]
            return [(f + o, lo, hi) for lo, hi in got]

        early = [at for o in range(k) for at in inner(o)]
        late = early[len(early) - LATE[b]:]
        for o in range(k):
            pieces = [at for at in early[:len(early) - LATE[b]] if at[0] == f + o]
            first = 0
            if o == 0 and b:
                piece(pieces[0], 9)
                flush(1)
                pack_h(b, hout.at[f - 1])
                pack_c(b)
                with jax.named_scope(f'send{b}'):
                    start_border(b, 0, 1)
                first = 1
            if b == 0 and o == 0:
                for at in pieces[:2]:
                    piece(at, 9)
                with jax.named_scope('x_wait0'):
                    c_own.wait()
                    c_push.wait_recv()
                    wait_x(1)
                for at in pieces[2:4]:
                    piece(at, 9)
                c0, got = cst[...], cin[...]
                cbuf[PAD:PAD + R, mine_c] = jnp.concatenate([c0, c0], axis=2)
                swapped, keep = pltpu.roll(got, CH, 2), jnp.broadcast_to(low, got.shape)
                both = [lax.select(keep, got, swapped), lax.select(keep, swapped, got)]
                cbuf[PAD:PAD + R, theirs_c] = jnp.concatenate(both, axis=1)
                pack_c(0)
                pack_x(1, 3)
                start_first(1, 0, 1, 3, 4)
                start_first(0, 0, 1, 3, 4)
                first = 4
            if b == 0 and o == 2:
                for at in pieces[:2]:
                    piece(at, 9)
                flush(2)
                with jax.named_scope('x_wait1'):
                    wait_x(2)
                for at in pieces[2:4]:
                    piece(at, 9)
                pack_x(3, k)
                for side in range(2):
                    start_first(side, 0, 5)
                start_first(0, 1, 5)
                first = 4
            for at in pieces[first:]:
                piece(at)
            if b == 0 and o == 0:
                with jax.named_scope('upsend'):
                    start_first(0, 1, 0, 2, 1, 3, 4)
            if o == 0 and b and not last:
                pack_x(f + k, f + k + plan.blocks[b + 1])
        with jax.named_scope(f'mid{b}'):
            wait_border(b, 0, 2)
        if b == 0:
            wait_x(3)
        elif not last:
            start_border(b + 1, 2)
        if b:
            push_h(plan.first[b - 1], f)
        piece(late.pop(0), 3)
        for side in range(2):
            lo = -k if side == 0 else R
            h = flat(unpack(hr_ref[side, plan.hat[b]:plan.hat[b] + k].astype(f32)))
            for a, e in cuts(lo, lo + k):
                part = h[(a - lo) * W:(e - lo) * W]
                emit(f, a, e, masked(a, jnp.concatenate([part, x_rows(f, a, e)], axis=1)))
        for o in range(k):
            m = k - 1 - o
            top, bottom = even_cuts(-m, o + 1), even_cuts(R - 1 - o, R + m)
            for lo, hi in top:
                piece((f + o, lo, hi), 9 if o == 0 else 1)
                if lo != top[0][0]:
                    continue
                if b == 0 and o in (1, 2):
                    with jax.named_scope(f'midx{o}'):
                        wait_border(0, 3 + o)
                if last and o == k // 2:
                    push_h(f, f + o)
                if last and o == k - 2:
                    push_h(f + k // 2, f + o)
                    push_h(T - 1, T, k, R - k)
                    push_c(k, R - k)
                if last and o == k - 1:
                    push_h(T - 2, T - 1)
            for lo, hi in bottom:
                piece((f + o, lo, hi), 9 if o == 0 else 1)
            if o == 0:
                with jax.named_scope(f'midc{b}'):
                    wait_border(b, 1, *(() if b else (3,)))
                for side in range(2):
                    lo = PAD - (k - 1) if side == 0 else PAD + R
                    packed = cr_ref[side, plan.cat[b]:plan.cat[b] + k - 1]
                    both = jnp.concatenate([packed, pltpu.roll(packed, CH, 2)], axis=1)
                    cbuf[lo:lo + k - 1] = both
                while late:
                    piece(late.pop(0), 3)
            if o == 0 and b == 0 and not last:
                pack_x(f + k, f + k + plan.blocks[b + 1])
                start_border(b + 1, 2)
        assert not late
    flush()
    k = plan.blocks[-1]
    for lo, hi in ((0, k), (R - k, R)):
        push_h(T - 1, T, lo, hi)
        push_c(lo, hi)

    with jax.named_scope('end_wait'):
        for c in [h_push, c_push, *x_push]:
            c.wait_send()

        def wait_sends(side):
            for kind, ref in enumerate((hs_ref, cs_ref, xs_ref)):
                local(ref.at[side], ref.at[side], s_bs.at[kind, side]).wait()

        each_side(wait_sends)
        for sem in (s_os, s_or):
            local(hpeer, hpeer, sem.at[0]).wait()
            local(cpeer, cpeer, sem.at[1]).wait()


def store(hout, hpeer, cout, cpeer, h_all, c_final, c_tile, sems):
    s = lax.axis_index("cols")
    HG = hpeer.shape[2]
    copies = [pltpu.make_async_copy(hout.at[:, :, pl.ds(s * HG, HG)], h_all.at[:, s], sems.at[0]),
              pltpu.make_async_copy(hpeer, h_all.at[:, 1 - s], sems.at[1]),
              pltpu.make_async_copy(c_tile.at[0], c_final.at[s], sems.at[2]),
              pltpu.make_async_copy(c_tile.at[1], c_final.at[1 - s], sems.at[3])]
    for c in copies[:2]:
        c.start()
    for i, packed in enumerate((cout[s], cpeer[...])):
        c_tile[i] = jnp.concatenate([packed[:, :, :CH], packed[:, :, CH:]], axis=1)
    for c in copies[2:]:
        c.start()
    for c in copies:
        c.wait()


def run(blocks, n_rows, frames, w_x, w_h, gate_bias, h_init, c_init):
    T, S, R, HW = frames.shape[:4]
    W, HG = 2 * HW, HW // COLS
    plan = Plan(blocks, T, R, W)
    NB, PAD, G = len(blocks), plan.K, len(plan.groups)
    bf, f32 = jnp.bfloat16, jnp.float32
    vm, dma = pltpu.VMEM, pltpu.SemaphoreType.DMA
    hbm = pl.BlockSpec(memory_space=pltpu.HBM)
    vmem = pl.BlockSpec(memory_space=pltpu.VMEM)
    tiled = frames.reshape(T, S, R, HG, COLS, CH)
    parts = pl.pallas_call(
        functools.partial(kernel, plan, n_rows),
        out_shape=(vm((T, R, 2 * HG, COLS, CH), bf), vm((T, R, HG, COLS, CH), bf),
                   vm((2, R, HW // 2, LANES), f32), vm((R, HW // 2, LANES), f32)),
        in_specs=[hbm] * 6,
        out_specs=(vmem,) * 4,
        scratch_shapes=[
            vm((1, 4 * CH), f32), vm((R, HG, COLS, CH), bf), vm((R, HW, CH), f32),
            vm((R, HW // 2, LANES), f32), vm((R, HW // 2, LANES), f32),
            vm((plan.groups[1][1], R, HG, COLS, CH), bf),
            vm((T, R, 2 * HG, COLS, CH), bf), vm((R, 2 * HG, COLS, CH), bf), vm((R, HW, CH), f32),
            vm((3, (R + 2 * PAD) * W, LANES), bf), vm((3, (R + 2 * PAD) * W, LANES), bf),
            vm((R + 2 * PAD, W, LANES), f32), vm((RING, W + 16, LANES), f32), vm((10, 2, CH, 4 * CH), bf),
            vm((2, plan.xat[-1], HG, COLS, LANES), bf), vm((2, plan.xat[-1], HG, COLS, LANES), bf),
            vm((2, plan.hat[-1], HG, COLS, LANES), bf), vm((2, plan.hat[-1], HG, COLS, LANES), bf),
            vm((2, plan.cat[-1], HW, LANES), f32), vm((2, plan.cat[-1], HW, LANES), f32),
            dma((3,)), dma((6,)), dma((2,)), dma((2,)), dma((G,)), dma((G,)), dma((G,)),
            dma((6, 2, NB)), dma((3, 2)), dma((2,)), dma((2,)), pltpu.SemaphoreType.REGULAR],
        compiler_params=pltpu.CompilerParams(collective_id=0, has_side_effects=True, vmem_limit_bytes=46 * 2**20),
    )(tiled, w_x.reshape(9, CH, 4 * CH), w_h.reshape(9, CH, 4 * CH), gate_bias.reshape(1, -1),
      h_init.reshape(S, R, HG, COLS, CH), c_init)
    h_all, c_final = pl.pallas_call(
        store,
        out_shape=(jax.ShapeDtypeStruct(tiled.shape, bf), jax.ShapeDtypeStruct(c_init.shape, f32)),
        in_specs=[vmem] * 4,
        out_specs=(hbm, hbm),
        scratch_shapes=[vm((2, R, HW, CH), f32), dma((4,))],
        compiler_params=pltpu.CompilerParams(vmem_limit_bytes=4 * 2**20),
    )(*[pltpu.with_memory_space_constraint(a, pltpu.VMEM) for a in parts])
    return h_all.reshape(frames.shape), c_final


def solution(mesh, K=None):
    n_rows = mesh.shape["rows"]
    frame_spec = P(None, "batch", "rows", "cols", None)
    state_spec = P("batch", "rows", "cols", None)
    blocks = BLOCKS if K is None else K
    return jax.shard_map(functools.partial(run, blocks, n_rows), mesh=mesh,
                         in_specs=(frame_spec, P(), P(), P(), state_spec, state_spec),
                         out_specs=(frame_spec, state_spec), check_vma=False)
```

```python
import functools

import jax
import jax.numpy as jnp
from jax import lax
from jax.experimental import pallas as pl
from jax.experimental.pallas import tpu as pltpu
from jax.sharding import PartitionSpec as P

MESH = pl.DeviceIdType.MESH
CH = 64
LANES = 128
COLS = 8
PIECE = 4
RING = 8
BLOCKS = (7, 9)
LATE = (3, 3)
BORDER = 3
FAR = 16


def cuts(lo, hi, size=PIECE):
    n = max(1, (hi - lo) // size)
    edges = [lo + i * size for i in range(n)] + [hi]
    return list(zip(edges[:-1], edges[1:]))


def even_cuts(lo, hi):
    n = max(1, round((hi - lo) / BORDER))
    edges = [lo + (hi - lo) * i // n for i in range(n + 1)]
    return list(zip(edges[:-1], edges[1:]))


class Plan:
    def __init__(self, blocks, T, R, W):
        assert sum(blocks) == T
        self.blocks, self.T, self.R, self.W, self.HW, self.HG = blocks, T, R, W, W // 2, W // 2 // COLS
        self.K = max(blocks)
        self.first = [sum(blocks[:b]) for b in range(len(blocks))]
        self.of = [(b, o) for b, k in enumerate(blocks) for o in range(k)]
        self.xrows = [blocks[b] - o for b, o in self.of]
        self.xat = [sum(self.xrows[:t]) for t in range(T + 1)]
        self.parts = [[(0, 1), (1, 2), (2, 3), (3, k)] if b == 0 else [(0, k)] for b, k in enumerate(blocks)]
        self.hat = [sum(blocks[:b]) for b in range(len(blocks) + 1)]
        self.cat = [sum(k - 1 for k in blocks[:b]) for b in range(len(blocks) + 1)]
        ends = [0, 1, 3, blocks[0] + 1, T]
        self.groups = [(a, e) for a, e in zip(ends[:-1], ends[1:]) if e > a]


def kernel(plan, n_rows, frames, w_x, w_h, bias_in, h_init, c_init, hout, hpeer, cout, cpeer,
           bias, hgo, cgo, cgp, cin, xgo, xin, hst, cst, xh_even, xh_odd, cbuf, shift, wbuf,
           xs_ref, xr_ref, hs_ref, hr_ref, cs_ref, cr_ref,
           s_w, s_i, s_ir, s_is, s_x, s_xr, s_xs, s_b, s_bs, s_or, s_os, here_sem):
    T, R, W, HW, HG = plan.T, plan.R, plan.W, plan.HW, plan.HG
    PAD = plan.K
    NB = len(plan.blocks)
    s = lax.axis_index("cols")
    n = lax.axis_index("rows")
    p = 1 - s
    mine, theirs = pl.ds(s * HG, HG), pl.ds(p * HG, HG)
    mine_c, theirs_c = [pl.ds(pl.multiple_of(i * HW, HW), HW) for i in (s, p)]
    has_up, has_dn = n > 0, n < n_rows - 1
    bf, f32 = jnp.bfloat16, jnp.float32

    def local(src, dst, sem):
        return pltpu.make_async_copy(src, dst, sem)

    def remote(src, dst, ssem, rsem, dev):
        return pltpu.make_async_remote_copy(
            src_ref=src, dst_ref=dst, send_sem=ssem, recv_sem=rsem, device_id=dev, device_id_type=MESH)

    peer = {"cols": p}
    side_dev = [{"rows": n - 1}, {"rows": n + 1}]
    side_ok = [has_up, has_dn]

    def each_side(do):
        for side in range(2):
            @pl.when(side_ok[side])
            def _():
                do(side)

    barrier = pltpu.get_barrier_semaphore()

    def signal(dev):
        pl.semaphore_signal(barrier, inc=1, device_id=dev, device_id_type=MESH)

    signal(peer)

    @pl.when(has_up)
    def _():
        signal(side_dev[0])


    h_own = local(h_init.at[s], hst.at[:, mine], s_i.at[0])
    c_own = local(c_init.at[s], cst, s_i.at[1])
    x_own = [local(frames.at[a:e, s], xin.at[a:e, :, mine], s_x.at[g]) for g, (a, e) in enumerate(plan.groups)]
    h_got = local(h_init.at[p], hgo, s_i.at[2])
    c_got = local(c_init.at[p], cgo, s_i.at[3])
    x_got = [local(frames.at[a:e, p], xgo.at[a:e], s_i.at[4 + g]) for g, (a, e) in enumerate(plan.groups[:2])]
    w_copies = [local(w_h, wbuf.at[0:9, 0], s_w.at[0]), local(w_x, wbuf.at[0:9, 1], s_w.at[1]),
                local(bias_in, bias, s_w.at[2])]
    for c in [h_got, x_got[0], c_got, h_own, x_own[0], c_own, *w_copies, x_got[1], *x_own[1:]]:
        c.start()
    with jax.named_scope('barrier'):
        pl.semaphore_wait(barrier, 1 + has_dn.astype(jnp.int32))

    @pl.when(has_dn)
    def _():
        pl.semaphore_signal(here_sem, inc=1, device_id=side_dev[1], device_id_type=MESH)


    h_push = remote(hgo, hst.at[:, mine], s_is.at[0], s_ir.at[0], peer)
    c_push = remote(cgp, cin, s_is.at[1], s_ir.at[1], peer)
    x_push = [remote((xgo if g < 2 else frames.at[:, p]).at[a:e], xin.at[a:e, :, mine], s_xs.at[g], s_xr.at[g], peer)
              for g, (a, e) in enumerate(plan.groups)]
    with jax.named_scope('got_wait'):
        for got, push in [(h_got, h_push), (x_got[0], x_push[0]), (c_got, c_push), (x_got[1], x_push[1])]:
            got.wait()
            if push is c_push:
                cgp[...] = jnp.concatenate([cgo[:, :HW // 2], cgo[:, HW // 2:]], axis=2)
            push.start()
    for push in x_push[2:]:
        push.start()

    shift[...] = jnp.zeros_like(shift)
    low = lax.broadcasted_iota(jnp.int32, (1, LANES), 1) < CH
    low_half = low_row = low
    turn = [0]
    scale = jnp.where(low_row, 0.5, 1.0)
    lift = jnp.where(low_row, 0.5, 0.0)

    with jax.named_scope('w_wait'):
        for c in w_copies:
            c.wait()
    for tap in range(9):
        for half in range(2):
            tile = wbuf[tap, half, :, 0:LANES]
            wbuf[tap, half, :, 0:LANES] = jnp.concatenate([tile[:, CH:], tile[:, :CH]], axis=1)
    b_all = bias[...]
    rest = jnp.concatenate([b_all[:, CH:LANES], b_all[:, :CH], b_all[:, LANES:]], axis=1)
    row = lax.broadcasted_iota(jnp.int32, (CH, 4 * CH), 0)
    rows = jnp.zeros((CH, 4 * CH), f32)
    for i in range(3):
        top = (rest * (1 - 2.0 ** -8)).astype(bf).astype(f32) if i == 0 else rest.astype(bf).astype(f32)
        rows = jnp.where(row == i, top, rows)
        rest = rest - top
    wbuf[9, 0] = rows.astype(bf)
    wbuf[9, 1] = jnp.zeros((CH, 4 * CH), bf)
    ones = jnp.where(lax.broadcasted_iota(jnp.int32, (1, LANES), 1) < 3, 1.0, 0.0).astype(bf)

    def pack(v):
        return jnp.concatenate([v[:, :HG], v[:, HG:]], axis=3)

    def unpack(v):
        return jnp.concatenate([v[..., :CH], v[..., CH:]], axis=1)

    def masked(r, v):
        if 0 <= r < R:
            return v
        return lax.select(jnp.broadcast_to(has_up if r < 0 else has_dn, v.shape), v, jnp.zeros_like(v))

    def emit(t, lo, hi, hx):
        nxt = xh_even if t % 2 == 0 else xh_odd
        at, to = slot(lo, hi), cells_of(lo, hi)
        shift[at, 8:8 + W, :] = hx.reshape(hi - lo, W, LANES)
        nxt[1, to] = hx.astype(bf)
        nxt[0, to] = shift[at, 7:7 + W, :].reshape(hx.shape).astype(bf)
        nxt[2, to] = shift[at, 9:9 + W, :].reshape(hx.shape).astype(bf)

    def cells_of(lo, hi):
        return slice((lo + PAD) * W, (hi + PAD) * W)

    def slot(lo, hi):
        if turn[0] + hi - lo > RING:
            turn[0] = 0
        turn[0] += hi - lo
        return slice(turn[0] - (hi - lo), turn[0])

    def flat(v):
        return v.reshape(-1, v.shape[-1])

    def x_rows(t, lo, hi):
        if lo >= 0 and hi <= R:
            return flat(xin[t, lo:hi].astype(f32))
        side, i = (0, lo + plan.xrows[t]) if lo < 0 else (1, lo - R)
        return flat(unpack(xr_ref[side, plan.xat[t] + i:plan.xat[t] + i + hi - lo].astype(f32)))

    def wait_x(g):
        if g < len(plan.groups):
            x_own[g].wait()
            x_push[g].wait_recv()

    def border(b, kind, side):
        f = plan.first[b]
        if kind < 2:
            src, dst, at = [(hs_ref, hr_ref, plan.hat), (cs_ref, cr_ref, plan.cat)][kind]
            at, end = at[b], at[b + 1]
        else:
            src, dst = xs_ref, xr_ref
            at, end = [plan.xat[f + o] for o in plan.parts[b][kind - 2]]
        return remote(src.at[side, at:end], dst.at[1 - side, at:end],
                      s_bs.at[min(kind, 2), side], s_b.at[kind, 1 - side, b], side_dev[side])

    def pack_x(t0, t1):
        for side in range(2):
            for t in range(t0, t1):
                m = plan.xrows[t]
                lo = 0 if side == 0 else R - m
                xs_ref[side, plan.xat[t]:plan.xat[t] + m] = pack(xin[t, lo:lo + m])

    def start_border(b, *kinds):
        each_side(lambda side: [border(b, kind, side).start() for kind in kinds])

    far = lax.rem(n, FAR) == 0

    def start_first(side, late, *kinds):
        ok = has_dn if side else jnp.logical_and(has_up, far if late else jnp.logical_not(far))

        @pl.when(ok)
        def _():
            if not side and 0 in kinds:
                pl.semaphore_wait(here_sem, 1)
            for kind in kinds:
                border(0, kind, side).start()

    def wait_border(b, *kinds):
        each_side(lambda side: [border(b, kind, 1 - side).wait_recv() for kind in kinds])

    def pack_h(b, h_rows):
        k = plan.blocks[b]
        for side in range(2):
            lo = 0 if side == 0 else R - k
            hs_ref[side, plan.hat[b]:plan.hat[b] + k] = pack(h_rows[lo:lo + k])

    def pack_c(b):
        k = plan.blocks[b]
        for side in range(2):
            lo = PAD if side == 0 else PAD + R - (k - 1)
            c = cbuf[lo:lo + k - 1]
            cs_ref[side, plan.cat[b]:plan.cat[b] + k - 1] = jnp.where(low_half, c[:, :HW], c[:, HW:])

    weights = wbuf[...].reshape(10 * LANES, 4 * CH)

    def dot(t, lo, hi):
        cur = xh_even if t % 2 == 0 else xh_odd
        taps = [cur[dc, cells_of(lo + dr - 1, hi + dr - 1)] for dr in range(3) for dc in range(3)]
        taps.append(jnp.broadcast_to(ones, taps[0].shape))
        return jnp.dot(jnp.concatenate(taps, axis=1), weights, preferred_element_type=f32)

    def cells(t, lo, hi, gates):
        fi = jnp.tanh(gates[:, :LANES] * 0.5) * 0.5 + 0.5
        og = jnp.tanh(gates[:, LANES:] * scale) * scale + lift
        at = slice(lo + PAD, hi + PAD)
        prod = fi * lax.select(jnp.broadcast_to(low, og.shape), cbuf[at].reshape(og.shape), og)
        c = prod + pltpu.roll(prod, CH, 1)
        h = (og * jnp.tanh(c))[:, :CH]
        if t == T - 1:
            c = c.reshape(hi - lo, 2, 2, HW // 2, LANES)
            for half in range(2):
                both = c[:, half, 0]
                cout[half, lo:hi] = lax.select(jnp.broadcast_to(low, both.shape), both, c[:, half, 1])
        else:
            cbuf[at] = c.reshape(hi - lo, W, LANES)
        for a, e in ((lo, min(hi, 0)), (max(lo, 0), min(hi, R)), (max(lo, R), hi)):
            if a >= e:
                continue
            part = h[(a - lo) * W:(e - lo) * W]
            if a >= 0 and e <= R:
                hout[t, a:e] = part.reshape(e - a, 2 * HG, COLS, CH).astype(bf)
            if t < T - 1:
                emit(t + 1, a, e, masked(a, jnp.concatenate([part, x_rows(t + 1, a, e)], axis=1)))

    pending = []

    def piece(at, ahead=1):
        t, lo, hi = at
        while any(u == t - 1 and a <= hi and lo <= e for u, a, e, _ in pending):
            cells(*pending.pop(0))
        pending.append((*at, dot(*at)))
        flush(ahead)

    def flush(left=0):
        while len(pending) > left:
            cells(*pending.pop(0))

    def push_h(t0, t1, lo=0, hi=R):
        rows = slice(lo, hi)
        remote(hout.at[t0:t1, rows, theirs], hpeer.at[t0:t1, rows], s_os.at[0], s_or.at[0], peer).start()

    def push_c(lo, hi):
        remote(cout.at[p, lo:hi], cpeer.at[lo:hi], s_os.at[1], s_or.at[1], peer).start()

    with jax.named_scope('state_wait'):
        for c in [h_own, x_own[0]]:
            c.wait()
        for c in [h_push, x_push[0]]:
            c.wait_recv()
    pack_h(0, hst)
    pack_x(0, 1)
    start_first(1, 0, 0, 2)
    start_first(0, 0, 0, 2)
    for lo, hi in cuts(0, R):
        emit(0, lo, hi, jnp.concatenate([flat(hst[lo:hi].astype(f32)), x_rows(0, lo, hi)], axis=1))

    for b, k in enumerate(plan.blocks):
        f = plan.first[b]
        last = b + 1 == NB

        def inner(o):
            if o == 0:
                got = [*cuts(k + 1, R - 1 - k), *cuts(1, k + 1), *cuts(R - 1 - k, R - 1)]
            else:
                got = cuts(o + 1, R - 1 - o)
                got = got[1:-1] + [got[0], got[-1]]
            return [(f + o, lo, hi) for lo, hi in got]

        early = [at for o in range(k) for at in inner(o)]
        late = early[len(early) - LATE[b]:]
        for o in range(k):
            pieces = [at for at in early[:len(early) - LATE[b]] if at[0] == f + o]
            first = 0
            if o == 0 and b:
                piece(pieces[0], 9)
                flush(1)
                pack_h(b, hout.at[f - 1])
                pack_c(b)
                with jax.named_scope(f'send{b}'):
                    start_border(b, 0, 1)
                first = 1
            if b == 0 and o == 0:
                for at in pieces[:2]:
                    piece(at, 9)
                with jax.named_scope('x_wait0'):
                    c_own.wait()
                    c_push.wait_recv()
                    wait_x(1)
                for at in pieces[2:4]:
                    piece(at, 9)
                c0, got = cst[...], cin[...]
                cbuf[PAD:PAD + R, mine_c] = jnp.concatenate([c0, c0], axis=2)
                swapped, keep = pltpu.roll(got, CH, 2), jnp.broadcast_to(low, got.shape)
                both = [lax.select(keep, got, swapped), lax.select(keep, swapped, got)]
                cbuf[PAD:PAD + R, theirs_c] = jnp.concatenate(both, axis=1)
                pack_c(0)
                pack_x(1, 3)
                start_first(1, 0, 1, 3, 4)
                start_first(0, 0, 1, 3, 4)
                first = 4
            if b == 0 and o == 2:
                for at in pieces[:2]:
                    piece(at, 9)
                flush(2)
                with jax.named_scope('x_wait1'):
                    wait_x(2)
                for at in pieces[2:4]:
                    piece(at, 9)
                pack_x(3, k)
                for side in range(2):
                    start_first(side, 0, 5)
                start_first(0, 1, 5)
                first = 4
            if b == 0 and o == 4:
                for at in pieces[:2]:
                    piece(at, 9)
                flush(2)
                wait_x(3)
                for at in pieces[2:4]:
                    piece(at, 9)
                pack_x(k, k + plan.blocks[1])
                start_border(1, 2)
                first = 4
            for at in pieces[first:]:
                piece(at)
            if b == 0 and o == 0:
                with jax.named_scope('upsend'):
                    start_first(0, 1, 0, 2, 1, 3, 4)
            if o == 0 and b and not last:
                pack_x(f + k, f + k + plan.blocks[b + 1])
        with jax.named_scope(f'mid{b}'):
            wait_border(b, 0, 2)
        if b and not last:
            start_border(b + 1, 2)
        if b:
            push_h(plan.first[b - 1], f)
        piece(late.pop(0), 3)
        for side in range(2):
            lo = -k if side == 0 else R
            h = flat(unpack(hr_ref[side, plan.hat[b]:plan.hat[b] + k].astype(f32)))
            for a, e in cuts(lo, lo + k):
                part = h[(a - lo) * W:(e - lo) * W]
                emit(f, a, e, masked(a, jnp.concatenate([part, x_rows(f, a, e)], axis=1)))
        for o in range(k):
            m = k - 1 - o
            top, bottom = even_cuts(-m, o + 1), even_cuts(R - 1 - o, R + m)
            for lo, hi in top:
                piece((f + o, lo, hi), 9 if o == 0 else 1)
                if lo != top[0][0]:
                    continue
                if b == 0 and o in (1, 2):
                    with jax.named_scope(f'midx{o}'):
                        wait_border(0, 3 + o)
                if last and o == k // 2:
                    push_h(f, f + o)
                if last and o == k - 2:
                    push_h(f + k // 2, f + o)
                    push_h(T - 1, T, k, R - k)
                    push_c(k, R - k)
                if last and o == k - 1:
                    push_h(T - 2, T - 1)
            for lo, hi in bottom:
                piece((f + o, lo, hi), 9 if o == 0 else 1)
            if o == 0:
                with jax.named_scope(f'midc{b}'):
                    wait_border(b, 1, *(() if b else (3,)))
                for side in range(2):
                    lo = PAD - (k - 1) if side == 0 else PAD + R
                    packed = cr_ref[side, plan.cat[b]:plan.cat[b] + k - 1]
                    both = jnp.concatenate([packed, pltpu.roll(packed, CH, 2)], axis=1)
                    cbuf[lo:lo + k - 1] = both
                while late:
                    piece(late.pop(0), 3)
        assert not late
    flush()
    k = plan.blocks[-1]
    for lo, hi in ((0, k), (R - k, R)):
        push_h(T - 1, T, lo, hi)
        push_c(lo, hi)

    with jax.named_scope('end_wait'):
        for c in [h_push, c_push, *x_push]:
            c.wait_send()

        def wait_sends(side):
            for kind, ref in enumerate((hs_ref, cs_ref, xs_ref)):
                local(ref.at[side], ref.at[side], s_bs.at[kind, side]).wait()

        each_side(wait_sends)
        for sem in (s_os, s_or):
            local(hpeer, hpeer, sem.at[0]).wait()
            local(cpeer, cpeer, sem.at[1]).wait()


def store(hout, hpeer, cout, cpeer, h_all, c_final, c_tile, sems):
    s = lax.axis_index("cols")
    HG = hpeer.shape[2]
    copies = [pltpu.make_async_copy(hout.at[:, :, pl.ds(s * HG, HG)], h_all.at[:, s], sems.at[0]),
              pltpu.make_async_copy(hpeer, h_all.at[:, 1 - s], sems.at[1]),
              pltpu.make_async_copy(c_tile.at[0], c_final.at[s], sems.at[2]),
              pltpu.make_async_copy(c_tile.at[1], c_final.at[1 - s], sems.at[3])]
    for c in copies[:2]:
        c.start()
    for i, packed in enumerate((cout[s], cpeer[...])):
        c_tile[i] = jnp.concatenate([packed[:, :, :CH], packed[:, :, CH:]], axis=1)
    for c in copies[2:]:
        c.start()
    for c in copies:
        c.wait()


def run(blocks, n_rows, frames, w_x, w_h, gate_bias, h_init, c_init):
    T, S, R, HW = frames.shape[:4]
    W, HG = 2 * HW, HW // COLS
    plan = Plan(blocks, T, R, W)
    NB, PAD, G = len(blocks), plan.K, len(plan.groups)
    bf, f32 = jnp.bfloat16, jnp.float32
    vm, dma = pltpu.VMEM, pltpu.SemaphoreType.DMA
    hbm = pl.BlockSpec(memory_space=pltpu.HBM)
    vmem = pl.BlockSpec(memory_space=pltpu.VMEM)
    tiled = frames.reshape(T, S, R, HG, COLS, CH)
    parts = pl.pallas_call(
        functools.partial(kernel, plan, n_rows),
        out_shape=(vm((T, R, 2 * HG, COLS, CH), bf), vm((T, R, HG, COLS, CH), bf),
                   vm((2, R, HW // 2, LANES), f32), vm((R, HW // 2, LANES), f32)),
        in_specs=[hbm] * 6,
        out_specs=(vmem,) * 4,
        scratch_shapes=[
            vm((1, 4 * CH), f32), vm((R, HG, COLS, CH), bf), vm((R, HW, CH), f32),
            vm((R, HW // 2, LANES), f32), vm((R, HW // 2, LANES), f32),
            vm((plan.groups[1][1], R, HG, COLS, CH), bf),
            vm((T, R, 2 * HG, COLS, CH), bf), vm((R, 2 * HG, COLS, CH), bf), vm((R, HW, CH), f32),
            vm((3, (R + 2 * PAD) * W, LANES), bf), vm((3, (R + 2 * PAD) * W, LANES), bf),
            vm((R + 2 * PAD, W, LANES), f32), vm((RING, W + 16, LANES), f32), vm((10, 2, CH, 4 * CH), bf),
            vm((2, plan.xat[-1], HG, COLS, LANES), bf), vm((2, plan.xat[-1], HG, COLS, LANES), bf),
            vm((2, plan.hat[-1], HG, COLS, LANES), bf), vm((2, plan.hat[-1], HG, COLS, LANES), bf),
            vm((2, plan.cat[-1], HW, LANES), f32), vm((2, plan.cat[-1], HW, LANES), f32),
            dma((3,)), dma((6,)), dma((2,)), dma((2,)), dma((G,)), dma((G,)), dma((G,)),
            dma((6, 2, NB)), dma((3, 2)), dma((2,)), dma((2,)), pltpu.SemaphoreType.REGULAR],
        compiler_params=pltpu.CompilerParams(collective_id=0, has_side_effects=True, vmem_limit_bytes=46 * 2**20),
    )(tiled, w_x.reshape(9, CH, 4 * CH), w_h.reshape(9, CH, 4 * CH), gate_bias.reshape(1, -1),
      h_init.reshape(S, R, HG, COLS, CH), c_init)
    h_all, c_final = pl.pallas_call(
        store,
        out_shape=(jax.ShapeDtypeStruct(tiled.shape, bf), jax.ShapeDtypeStruct(c_init.shape, f32)),
        in_specs=[vmem] * 4,
        out_specs=(hbm, hbm),
        scratch_shapes=[vm((2, R, HW, CH), f32), dma((4,))],
        compiler_params=pltpu.CompilerParams(vmem_limit_bytes=4 * 2**20),
    )(*[pltpu.with_memory_space_constraint(a, pltpu.VMEM) for a in parts])
    return h_all.reshape(frames.shape), c_final


def solution(mesh, K=None):
    n_rows = mesh.shape["rows"]
    frame_spec = P(None, "batch", "rows", "cols", None)
    state_spec = P("batch", "rows", "cols", None)
    blocks = BLOCKS if K is None else K
    return jax.shard_map(functools.partial(run, blocks, n_rows), mesh=mesh,
                         in_specs=(frame_spec, P(), P(), P(), state_spec, state_spec),
                         out_specs=(frame_spec, state_spec), check_vma=False)
```

```python
import functools

import jax
import jax.numpy as jnp
from jax import lax
from jax.experimental import pallas as pl
from jax.experimental.pallas import tpu as pltpu
from jax.sharding import PartitionSpec as P

MESH = pl.DeviceIdType.MESH
CH = 64
LANES = 128
COLS = 8
PIECE = 4
RING = 8
BLOCKS = (8, 8)
LATE = (3, 3)
BORDER = 4
FAR = 16


def cuts(lo, hi, size=PIECE):
    n = max(1, (hi - lo) // size)
    edges = [lo + i * size for i in range(n)] + [hi]
    return list(zip(edges[:-1], edges[1:]))


def even_cuts(lo, hi):
    n = max(1, round((hi - lo) / BORDER))
    edges = [lo + (hi - lo) * i // n for i in range(n + 1)]
    return list(zip(edges[:-1], edges[1:]))


class Plan:
    def __init__(self, blocks, T, R, W):
        assert sum(blocks) == T
        self.blocks, self.T, self.R, self.W, self.HW, self.HG = blocks, T, R, W, W // 2, W // 2 // COLS
        self.K = max(blocks)
        self.first = [sum(blocks[:b]) for b in range(len(blocks))]
        self.of = [(b, o) for b, k in enumerate(blocks) for o in range(k)]
        self.xrows = [blocks[b] - o for b, o in self.of]
        self.xat = [sum(self.xrows[:t]) for t in range(T + 1)]
        self.parts = [[(0, 1), (1, 2), (2, 3), (3, k)] if b == 0 else [(0, k)] for b, k in enumerate(blocks)]
        self.hat = [sum(blocks[:b]) for b in range(len(blocks) + 1)]
        self.cat = [sum(k - 1 for k in blocks[:b]) for b in range(len(blocks) + 1)]
        ends = [0, 1, 3, blocks[0] + 1, T]
        self.groups = [(a, e) for a, e in zip(ends[:-1], ends[1:]) if e > a]


def kernel(plan, n_rows, frames, w_x, w_h, bias_in, h_init, c_init, hout, hpeer, cout, cpeer,
           bias, hgo, cgo, cgp, cin, xgo, xin, hst, cst, xh_even, xh_odd, cbuf, shift, wbuf,
           xs_ref, xr_ref, hs_ref, hr_ref, cs_ref, cr_ref,
           s_w, s_i, s_ir, s_is, s_x, s_xr, s_xs, s_b, s_bs, s_or, s_os, here_sem):
    T, R, W, HW, HG = plan.T, plan.R, plan.W, plan.HW, plan.HG
    PAD = plan.K
    NB = len(plan.blocks)
    s = lax.axis_index("cols")
    n = lax.axis_index("rows")
    p = 1 - s
    mine, theirs = pl.ds(s * HG, HG), pl.ds(p * HG, HG)
    mine_c, theirs_c = [pl.ds(pl.multiple_of(i * HW, HW), HW) for i in (s, p)]
    has_up, has_dn = n > 0, n < n_rows - 1
    bf, f32 = jnp.bfloat16, jnp.float32

    def local(src, dst, sem):
        return pltpu.make_async_copy(src, dst, sem)

    def remote(src, dst, ssem, rsem, dev):
        return pltpu.make_async_remote_copy(
            src_ref=src, dst_ref=dst, send_sem=ssem, recv_sem=rsem, device_id=dev, device_id_type=MESH)

    peer = {"cols": p}
    side_dev = [{"rows": n - 1}, {"rows": n + 1}]
    side_ok = [has_up, has_dn]

    def each_side(do):
        for side in range(2):
            @pl.when(side_ok[side])
            def _():
                do(side)

    barrier = pltpu.get_barrier_semaphore()

    def signal(dev):
        pl.semaphore_signal(barrier, inc=1, device_id=dev, device_id_type=MESH)

    signal(peer)

    @pl.when(has_up)
    def _():
        signal(side_dev[0])


    h_own = local(h_init.at[s], hst.at[:, mine], s_i.at[0])
    c_own = local(c_init.at[s], cst, s_i.at[1])
    x_own = [local(frames.at[a:e, s], xin.at[a:e, :, mine], s_x.at[g]) for g, (a, e) in enumerate(plan.groups)]
    h_got = local(h_init.at[p], hgo, s_i.at[2])
    c_got = local(c_init.at[p], cgo, s_i.at[3])
    x_got = [local(frames.at[a:e, p], xgo.at[a:e], s_i.at[4 + g]) for g, (a, e) in enumerate(plan.groups[:2])]
    w_copies = [local(w_h, wbuf.at[0:9, 0], s_w.at[0]), local(w_x, wbuf.at[0:9, 1], s_w.at[1]),
                local(bias_in, bias, s_w.at[2])]
    for c in [h_got, x_got[0], c_got, h_own, x_own[0], c_own, *w_copies, x_got[1], *x_own[1:]]:
        c.start()
    with jax.named_scope('barrier'):
        pl.semaphore_wait(barrier, 1 + has_dn.astype(jnp.int32))

    @pl.when(has_dn)
    def _():
        pl.semaphore_signal(here_sem, inc=1, device_id=side_dev[1], device_id_type=MESH)


    h_push = remote(hgo, hst.at[:, mine], s_is.at[0], s_ir.at[0], peer)
    c_push = remote(cgp, cin, s_is.at[1], s_ir.at[1], peer)
    x_push = [remote((xgo if g < 2 else frames.at[:, p]).at[a:e], xin.at[a:e, :, mine], s_xs.at[g], s_xr.at[g], peer)
              for g, (a, e) in enumerate(plan.groups)]
    with jax.named_scope('got_wait'):
        for got, push in [(h_got, h_push), (x_got[0], x_push[0]), (c_got, c_push), (x_got[1], x_push[1])]:
            got.wait()
            if push is c_push:
                cgp[...] = jnp.concatenate([cgo[:, :HW // 2], cgo[:, HW // 2:]], axis=2)
            push.start()
    for push in x_push[2:]:
        push.start()

    shift[...] = jnp.zeros_like(shift)
    low = lax.broadcasted_iota(jnp.int32, (1, LANES), 1) < CH
    low_half = low_row = low
    turn = [0]
    scale = jnp.where(low_row, 0.5, 1.0)
    lift = jnp.where(low_row, 0.5, 0.0)

    with jax.named_scope('w_wait'):
        for c in w_copies:
            c.wait()
    for tap in range(9):
        for half in range(2):
            tile = wbuf[tap, half, :, 0:LANES]
            wbuf[tap, half, :, 0:LANES] = jnp.concatenate([tile[:, CH:], tile[:, :CH]], axis=1)
    b_all = bias[...]
    rest = jnp.concatenate([b_all[:, CH:LANES], b_all[:, :CH], b_all[:, LANES:]], axis=1)
    row = lax.broadcasted_iota(jnp.int32, (CH, 4 * CH), 0)
    rows = jnp.zeros((CH, 4 * CH), f32)
    for i in range(3):
        top = (rest * (1 - 2.0 ** -8)).astype(bf).astype(f32) if i == 0 else rest.astype(bf).astype(f32)
        rows = jnp.where(row == i, top, rows)
        rest = rest - top
    wbuf[9, 0] = rows.astype(bf)
    wbuf[9, 1] = jnp.zeros((CH, 4 * CH), bf)
    ones = jnp.where(lax.broadcasted_iota(jnp.int32, (1, LANES), 1) < 3, 1.0, 0.0).astype(bf)

    def pack(v):
        return jnp.concatenate([v[:, :HG], v[:, HG:]], axis=3)

    def unpack(v):
        return jnp.concatenate([v[..., :CH], v[..., CH:]], axis=1)

    def masked(r, v):
        if 0 <= r < R:
            return v
        return lax.select(jnp.broadcast_to(has_up if r < 0 else has_dn, v.shape), v, jnp.zeros_like(v))

    def emit(t, lo, hi, hx):
        nxt = xh_even if t % 2 == 0 else xh_odd
        at, to = slot(lo, hi), cells_of(lo, hi)
        shift[at, 8:8 + W, :] = hx.reshape(hi - lo, W, LANES)
        nxt[1, to] = hx.astype(bf)
        nxt[0, to] = shift[at, 7:7 + W, :].reshape(hx.shape).astype(bf)
        nxt[2, to] = shift[at, 9:9 + W, :].reshape(hx.shape).astype(bf)

    def cells_of(lo, hi):
        return slice((lo + PAD) * W, (hi + PAD) * W)

    def slot(lo, hi):
        if turn[0] + hi - lo > RING:
            turn[0] = 0
        turn[0] += hi - lo
        return slice(turn[0] - (hi - lo), turn[0])

    def flat(v):
        return v.reshape(-1, v.shape[-1])

    def x_rows(t, lo, hi):
        if lo >= 0 and hi <= R:
            return flat(xin[t, lo:hi].astype(f32))
        side, i = (0, lo + plan.xrows[t]) if lo < 0 else (1, lo - R)
        return flat(unpack(xr_ref[side, plan.xat[t] + i:plan.xat[t] + i + hi - lo].astype(f32)))

    def wait_x(g):
        if g < len(plan.groups):
            x_own[g].wait()
            x_push[g].wait_recv()

    def border(b, kind, side):
        f = plan.first[b]
        if kind < 2:
            src, dst, at = [(hs_ref, hr_ref, plan.hat), (cs_ref, cr_ref, plan.cat)][kind]
            at, end = at[b], at[b + 1]
        else:
            src, dst = xs_ref, xr_ref
            at, end = [plan.xat[f + o] for o in plan.parts[b][kind - 2]]
        return remote(src.at[side, at:end], dst.at[1 - side, at:end],
                      s_bs.at[min(kind, 2), side], s_b.at[kind, 1 - side, b], side_dev[side])

    def pack_x(t0, t1):
        for side in range(2):
            for t in range(t0, t1):
                m = plan.xrows[t]
                lo = 0 if side == 0 else R - m
                xs_ref[side, plan.xat[t]:plan.xat[t] + m] = pack(xin[t, lo:lo + m])

    def start_border(b, *kinds):
        each_side(lambda side: [border(b, kind, side).start() for kind in kinds])

    far = lax.rem(n, FAR) == 0

    def start_first(side, late, *kinds):
        ok = has_dn if side else jnp.logical_and(has_up, far if late else jnp.logical_not(far))

        @pl.when(ok)
        def _():
            if not side and 0 in kinds:
                pl.semaphore_wait(here_sem, 1)
            for kind in kinds:
                border(0, kind, side).start()

    def wait_border(b, *kinds):
        each_side(lambda side: [border(b, kind, 1 - side).wait_recv() for kind in kinds])

    def pack_h(b, h_rows):
        k = plan.blocks[b]
        for side in range(2):
            lo = 0 if side == 0 else R - k
            hs_ref[side, plan.hat[b]:plan.hat[b] + k] = pack(h_rows[lo:lo + k])

    def pack_c(b):
        k = plan.blocks[b]
        for side in range(2):
            lo = PAD if side == 0 else PAD + R - (k - 1)
            c = cbuf[lo:lo + k - 1]
            cs_ref[side, plan.cat[b]:plan.cat[b] + k - 1] = jnp.where(low_half, c[:, :HW], c[:, HW:])

    weights = wbuf[...].reshape(10 * LANES, 4 * CH)

    def dot(t, lo, hi):
        cur = xh_even if t % 2 == 0 else xh_odd
        taps = [cur[dc, cells_of(lo + dr - 1, hi + dr - 1)] for dr in range(3) for dc in range(3)]
        taps.append(jnp.broadcast_to(ones, taps[0].shape))
        return jnp.dot(jnp.concatenate(taps, axis=1), weights, preferred_element_type=f32)

    def cells(t, lo, hi, gates):
        fi = jnp.tanh(gates[:, :LANES] * 0.5) * 0.5 + 0.5
        og = jnp.tanh(gates[:, LANES:] * scale) * scale + lift
        at = slice(lo + PAD, hi + PAD)
        prod = fi * lax.select(jnp.broadcast_to(low, og.shape), cbuf[at].reshape(og.shape), og)
        c = prod + pltpu.roll(prod, CH, 1)
        h = (og * jnp.tanh(c))[:, :CH]
        if t == T - 1:
            c = c.reshape(hi - lo, 2, 2, HW // 2, LANES)
            for half in range(2):
                both = c[:, half, 0]
                cout[half, lo:hi] = lax.select(jnp.broadcast_to(low, both.shape), both, c[:, half, 1])
        else:
            cbuf[at] = c.reshape(hi - lo, W, LANES)
        for a, e in ((lo, min(hi, 0)), (max(lo, 0), min(hi, R)), (max(lo, R), hi)):
            if a >= e:
                continue
            part = h[(a - lo) * W:(e - lo) * W]
            if a >= 0 and e <= R:
                hout[t, a:e] = part.reshape(e - a, 2 * HG, COLS, CH).astype(bf)
            if t < T - 1:
                emit(t + 1, a, e, masked(a, jnp.concatenate([part, x_rows(t + 1, a, e)], axis=1)))

    pending = []

    def piece(at, ahead=1):
        t, lo, hi = at
        while any(u == t - 1 and a <= hi and lo <= e for u, a, e, _ in pending):
            cells(*pending.pop(0))
        pending.append((*at, dot(*at)))
        flush(ahead)

    def flush(left=0):
        while len(pending) > left:
            cells(*pending.pop(0))

    def push_h(t0, t1, lo=0, hi=R):
        rows = slice(lo, hi)
        remote(hout.at[t0:t1, rows, theirs], hpeer.at[t0:t1, rows], s_os.at[0], s_or.at[0], peer).start()

    def push_c(lo, hi):
        remote(cout.at[p, lo:hi], cpeer.at[lo:hi], s_os.at[1], s_or.at[1], peer).start()

    with jax.named_scope('state_wait'):
        for c in [h_own, x_own[0]]:
            c.wait()
        for c in [h_push, x_push[0]]:
            c.wait_recv()
    pack_h(0, hst)
    pack_x(0, 1)
    start_first(1, 0, 0, 2)
    start_first(0, 0, 0, 2)
    for lo, hi in cuts(0, R):
        emit(0, lo, hi, jnp.concatenate([flat(hst[lo:hi].astype(f32)), x_rows(0, lo, hi)], axis=1))

    for b, k in enumerate(plan.blocks):
        f = plan.first[b]
        last = b + 1 == NB

        def inner(o):
            if o == 0:
                got = [*cuts(k + 1, R - 1 - k), *cuts(1, k + 1), *cuts(R - 1 - k, R - 1)]
            else:
                got = cuts(o + 1, R - 1 - o)
                got = got[1:-1] + [got[0], got[-1]]
            return [(f + o, lo, hi) for lo, hi in got]

        early = [at for o in range(k) for at in inner(o)]
        late = early[len(early) - LATE[b]:]
        for o in range(k):
            pieces = [at for at in early[:len(early) - LATE[b]] if at[0] == f + o]
            first = 0
            if o == 0 and b:
                piece(pieces[0], 9)
                flush(1)
                pack_h(b, hout.at[f - 1])
                pack_c(b)
                with jax.named_scope(f'send{b}'):
                    start_border(b, 0, 1)
                first = 1
            if b == 0 and o == 0:
                for at in pieces[:2]:
                    piece(at, 9)
                with jax.named_scope('x_wait0'):
                    c_own.wait()
                    c_push.wait_recv()
                    wait_x(1)
                for at in pieces[2:4]:
                    piece(at, 9)
                c0, got = cst[...], cin[...]
                cbuf[PAD:PAD + R, mine_c] = jnp.concatenate([c0, c0], axis=2)
                swapped, keep = pltpu.roll(got, CH, 2), jnp.broadcast_to(low, got.shape)
                both = [lax.select(keep, got, swapped), lax.select(keep, swapped, got)]
                cbuf[PAD:PAD + R, theirs_c] = jnp.concatenate(both, axis=1)
                pack_c(0)
                pack_x(1, 3)
                start_first(1, 0, 1, 3, 4)
                start_first(0, 0, 1, 3, 4)
                first = 4
            if b == 0 and o == 2:
                for at in pieces[:2]:
                    piece(at, 9)
                flush(2)
                with jax.named_scope('x_wait1'):
                    wait_x(2)
                for at in pieces[2:4]:
                    piece(at, 9)
                pack_x(3, k)
                for side in range(2):
                    start_first(side, 0, 5)
                start_first(0, 1, 5)
                first = 4
            if b == 0 and o == 4:
                for at in pieces[:2]:
                    piece(at, 9)
                flush(2)
                wait_x(3)
                for at in pieces[2:4]:
                    piece(at, 9)
                pack_x(k, k + plan.blocks[1])
                start_border(1, 2)
                first = 4
            for at in pieces[first:]:
                piece(at)
            if b == 0 and o == 0:
                with jax.named_scope('upsend'):
                    start_first(0, 1, 0, 2, 1, 3, 4)
            if o == 0 and b and not last:
                pack_x(f + k, f + k + plan.blocks[b + 1])
        with jax.named_scope(f'mid{b}'):
            wait_border(b, 0, 2)
        if b and not last:
            start_border(b + 1, 2)
        if b:
            push_h(plan.first[b - 1], f)
        piece(late.pop(0), 3)
        for side in range(2):
            lo = -k if side == 0 else R
            h = flat(unpack(hr_ref[side, plan.hat[b]:plan.hat[b] + k].astype(f32)))
            for a, e in cuts(lo, lo + k):
                part = h[(a - lo) * W:(e - lo) * W]
                emit(f, a, e, masked(a, jnp.concatenate([part, x_rows(f, a, e)], axis=1)))
        for o in range(k):
            m = k - 1 - o
            top, bottom = even_cuts(-m, o + 1), even_cuts(R - 1 - o, R + m)
            for lo, hi in top:
                piece((f + o, lo, hi), 9 if o == 0 else 1)
                if lo != top[0][0]:
                    continue
                if b == 0 and o in (1, 2):
                    with jax.named_scope(f'midx{o}'):
                        wait_border(0, 3 + o)
                if last and o == k // 2:
                    push_h(f, f + o)
                if last and o == k - 2:
                    push_h(f + k // 2, f + o)
                    push_h(T - 1, T, k, R - k)
                    push_c(k, R - k)
                if last and o == k - 1:
                    push_h(T - 2, T - 1)
            for lo, hi in bottom:
                piece((f + o, lo, hi), 9 if o == 0 else 1)
            if o == 0:
                with jax.named_scope(f'midc{b}'):
                    wait_border(b, 1, *(() if b else (3,)))
                for side in range(2):
                    lo = PAD - (k - 1) if side == 0 else PAD + R
                    packed = cr_ref[side, plan.cat[b]:plan.cat[b] + k - 1]
                    both = jnp.concatenate([packed, pltpu.roll(packed, CH, 2)], axis=1)
                    cbuf[lo:lo + k - 1] = both
                while late:
                    piece(late.pop(0), 3)
        assert not late
    flush()
    k = plan.blocks[-1]
    for lo, hi in ((0, k), (R - k, R)):
        push_h(T - 1, T, lo, hi)
        push_c(lo, hi)

    with jax.named_scope('end_wait'):
        for c in [h_push, c_push, *x_push]:
            c.wait_send()

        def wait_sends(side):
            for kind, ref in enumerate((hs_ref, cs_ref, xs_ref)):
                local(ref.at[side], ref.at[side], s_bs.at[kind, side]).wait()

        each_side(wait_sends)
        for sem in (s_os, s_or):
            local(hpeer, hpeer, sem.at[0]).wait()
            local(cpeer, cpeer, sem.at[1]).wait()


def store(hout, hpeer, cout, cpeer, h_all, c_final, c_tile, sems):
    s = lax.axis_index("cols")
    HG = hpeer.shape[2]
    copies = [pltpu.make_async_copy(hout.at[:, :, pl.ds(s * HG, HG)], h_all.at[:, s], sems.at[0]),
              pltpu.make_async_copy(hpeer, h_all.at[:, 1 - s], sems.at[1]),
              pltpu.make_async_copy(c_tile.at[0], c_final.at[s], sems.at[2]),
              pltpu.make_async_copy(c_tile.at[1], c_final.at[1 - s], sems.at[3])]
    for c in copies[:2]:
        c.start()
    for i, packed in enumerate((cout[s], cpeer[...])):
        c_tile[i] = jnp.concatenate([packed[:, :, :CH], packed[:, :, CH:]], axis=1)
    for c in copies[2:]:
        c.start()
    for c in copies:
        c.wait()


def run(blocks, n_rows, frames, w_x, w_h, gate_bias, h_init, c_init):
    T, S, R, HW = frames.shape[:4]
    W, HG = 2 * HW, HW // COLS
    plan = Plan(blocks, T, R, W)
    NB, PAD, G = len(blocks), plan.K, len(plan.groups)
    bf, f32 = jnp.bfloat16, jnp.float32
    vm, dma = pltpu.VMEM, pltpu.SemaphoreType.DMA
    hbm = pl.BlockSpec(memory_space=pltpu.HBM)
    vmem = pl.BlockSpec(memory_space=pltpu.VMEM)
    tiled = frames.reshape(T, S, R, HG, COLS, CH)
    parts = pl.pallas_call(
        functools.partial(kernel, plan, n_rows),
        out_shape=(vm((T, R, 2 * HG, COLS, CH), bf), vm((T, R, HG, COLS, CH), bf),
                   vm((2, R, HW // 2, LANES), f32), vm((R, HW // 2, LANES), f32)),
        in_specs=[hbm] * 6,
        out_specs=(vmem,) * 4,
        scratch_shapes=[
            vm((1, 4 * CH), f32), vm((R, HG, COLS, CH), bf), vm((R, HW, CH), f32),
            vm((R, HW // 2, LANES), f32), vm((R, HW // 2, LANES), f32),
            vm((plan.groups[1][1], R, HG, COLS, CH), bf),
            vm((T, R, 2 * HG, COLS, CH), bf), vm((R, 2 * HG, COLS, CH), bf), vm((R, HW, CH), f32),
            vm((3, (R + 2 * PAD) * W, LANES), bf), vm((3, (R + 2 * PAD) * W, LANES), bf),
            vm((R + 2 * PAD, W, LANES), f32), vm((RING, W + 16, LANES), f32), vm((10, 2, CH, 4 * CH), bf),
            vm((2, plan.xat[-1], HG, COLS, LANES), bf), vm((2, plan.xat[-1], HG, COLS, LANES), bf),
            vm((2, plan.hat[-1], HG, COLS, LANES), bf), vm((2, plan.hat[-1], HG, COLS, LANES), bf),
            vm((2, plan.cat[-1], HW, LANES), f32), vm((2, plan.cat[-1], HW, LANES), f32),
            dma((3,)), dma((6,)), dma((2,)), dma((2,)), dma((G,)), dma((G,)), dma((G,)),
            dma((6, 2, NB)), dma((3, 2)), dma((2,)), dma((2,)), pltpu.SemaphoreType.REGULAR],
        compiler_params=pltpu.CompilerParams(collective_id=0, has_side_effects=True, vmem_limit_bytes=46 * 2**20),
    )(tiled, w_x.reshape(9, CH, 4 * CH), w_h.reshape(9, CH, 4 * CH), gate_bias.reshape(1, -1),
      h_init.reshape(S, R, HG, COLS, CH), c_init)
    h_all, c_final = pl.pallas_call(
        store,
        out_shape=(jax.ShapeDtypeStruct(tiled.shape, bf), jax.ShapeDtypeStruct(c_init.shape, f32)),
        in_specs=[vmem] * 4,
        out_specs=(hbm, hbm),
        scratch_shapes=[vm((2, R, HW, CH), f32), dma((4,))],
        compiler_params=pltpu.CompilerParams(vmem_limit_bytes=4 * 2**20),
    )(*[pltpu.with_memory_space_constraint(a, pltpu.VMEM) for a in parts])
    return h_all.reshape(frames.shape), c_final


def solution(mesh, K=None):
    n_rows = mesh.shape["rows"]
    frame_spec = P(None, "batch", "rows", "cols", None)
    state_spec = P("batch", "rows", "cols", None)
    blocks = BLOCKS if K is None else K
    return jax.shard_map(functools.partial(run, blocks, n_rows), mesh=mesh,
                         in_specs=(frame_spec, P(), P(), P(), state_spec, state_spec),
                         out_specs=(frame_spec, state_spec), check_vma=False)
```

```python
import functools

import jax
import jax.numpy as jnp
from jax import lax
from jax.experimental import pallas as pl
from jax.experimental.pallas import tpu as pltpu
from jax.sharding import PartitionSpec as P

MESH = pl.DeviceIdType.MESH
CH = 64
LANES = 128
COLS = 8
PIECE = 4
RING = 8
BLOCKS = (7, 9)
LATE = (2, 3)
BORDER = 3
FAR = 16


def cuts(lo, hi, size=PIECE):
    n = max(1, (hi - lo) // size)
    edges = [lo + i * size for i in range(n)] + [hi]
    return list(zip(edges[:-1], edges[1:]))


def even_cuts(lo, hi):
    n = max(1, round((hi - lo) / BORDER))
    edges = [lo + (hi - lo) * i // n for i in range(n + 1)]
    return list(zip(edges[:-1], edges[1:]))


class Plan:
    def __init__(self, blocks, T, R, W):
        assert sum(blocks) == T
        self.blocks, self.T, self.R, self.W, self.HW, self.HG = blocks, T, R, W, W // 2, W // 2 // COLS
        self.K = max(blocks)
        self.first = [sum(blocks[:b]) for b in range(len(blocks))]
        self.of = [(b, o) for b, k in enumerate(blocks) for o in range(k)]
        self.xrows = [blocks[b] - o for b, o in self.of]
        self.xat = [sum(self.xrows[:t]) for t in range(T + 1)]
        self.parts = [[(0, 1), (1, 2), (2, 3), (3, k)] if b == 0 else [(0, k)] for b, k in enumerate(blocks)]
        self.hat = [sum(blocks[:b]) for b in range(len(blocks) + 1)]
        self.cat = [sum(k - 1 for k in blocks[:b]) for b in range(len(blocks) + 1)]
        ends = [0, 1, 3, blocks[0] + 1, T]
        self.groups = [(a, e) for a, e in zip(ends[:-1], ends[1:]) if e > a]


def kernel(plan, n_rows, frames, w_x, w_h, bias_in, h_init, c_init, hout, hpeer, cout, cpeer,
           bias, hgo, cgo, cgp, cin, xgo, xin, hst, cst, xh_even, xh_odd, cbuf, shift, wbuf,
           xs_ref, xr_ref, hs_ref, hr_ref, cs_ref, cr_ref,
           s_w, s_i, s_ir, s_is, s_x, s_xr, s_xs, s_b, s_bs, s_or, s_os, here_sem):
    T, R, W, HW, HG = plan.T, plan.R, plan.W, plan.HW, plan.HG
    PAD = plan.K
    NB = len(plan.blocks)
    s = lax.axis_index("cols")
    n = lax.axis_index("rows")
    p = 1 - s
    mine, theirs = pl.ds(s * HG, HG), pl.ds(p * HG, HG)
    mine_c, theirs_c = [pl.ds(pl.multiple_of(i * HW, HW), HW) for i in (s, p)]
    has_up, has_dn = n > 0, n < n_rows - 1
    bf, f32 = jnp.bfloat16, jnp.float32

    def local(src, dst, sem):
        return pltpu.make_async_copy(src, dst, sem)

    def remote(src, dst, ssem, rsem, dev):
        return pltpu.make_async_remote_copy(
            src_ref=src, dst_ref=dst, send_sem=ssem, recv_sem=rsem, device_id=dev, device_id_type=MESH)

    peer = {"cols": p}
    side_dev = [{"rows": n - 1}, {"rows": n + 1}]
    side_ok = [has_up, has_dn]

    def each_side(do):
        for side in range(2):
            @pl.when(side_ok[side])
            def _():
                do(side)

    barrier = pltpu.get_barrier_semaphore()

    def signal(dev):
        pl.semaphore_signal(barrier, inc=1, device_id=dev, device_id_type=MESH)

    signal(peer)

    @pl.when(has_up)
    def _():
        signal(side_dev[0])


    h_own = local(h_init.at[s], hst.at[:, mine], s_i.at[0])
    c_own = local(c_init.at[s], cst, s_i.at[1])
    x_own = [local(frames.at[a:e, s], xin.at[a:e, :, mine], s_x.at[g]) for g, (a, e) in enumerate(plan.groups)]
    h_got = local(h_init.at[p], hgo, s_i.at[2])
    c_got = local(c_init.at[p], cgo, s_i.at[3])
    x_got = [local(frames.at[a:e, p], xgo.at[a:e], s_i.at[4 + g]) for g, (a, e) in enumerate(plan.groups[:2])]
    w_copies = [local(w_h, wbuf.at[0:9, 0], s_w.at[0]), local(w_x, wbuf.at[0:9, 1], s_w.at[1]),
                local(bias_in, bias, s_w.at[2])]
    for c in [h_got, x_got[0], c_got, h_own, x_own[0], c_own, *w_copies, x_got[1], *x_own[1:]]:
        c.start()
    pl.semaphore_wait(barrier, 1 + has_dn.astype(jnp.int32))

    @pl.when(has_dn)
    def _():
        pl.semaphore_signal(here_sem, inc=1, device_id=side_dev[1], device_id_type=MESH)


    h_push = remote(hgo, hst.at[:, mine], s_is.at[0], s_ir.at[0], peer)
    c_push = remote(cgp, cin, s_is.at[1], s_ir.at[1], peer)
    x_push = [remote((xgo if g < 2 else frames.at[:, p]).at[a:e], xin.at[a:e, :, mine], s_xs.at[g], s_xr.at[g], peer)
              for g, (a, e) in enumerate(plan.groups)]
    for got, push in [(h_got, h_push), (x_got[0], x_push[0]), (c_got, c_push), (x_got[1], x_push[1])]:
        got.wait()
        if push is c_push:
            cgp[...] = jnp.concatenate([cgo[:, :HW // 2], cgo[:, HW // 2:]], axis=2)
        push.start()
    for push in x_push[2:]:
        push.start()

    shift[...] = jnp.zeros_like(shift)
    low = lax.broadcasted_iota(jnp.int32, (1, LANES), 1) < CH
    low_half = low_row = low
    turn = [0]
    scale = jnp.where(low_row, 0.5, 1.0)
    lift = jnp.where(low_row, 0.5, 0.0)

    for c in w_copies:
        c.wait()
    for tap in range(9):
        for half in range(2):
            tile = wbuf[tap, half, :, 0:LANES]
            wbuf[tap, half, :, 0:LANES] = jnp.concatenate([tile[:, CH:], tile[:, :CH]], axis=1)
    b_all = bias[...]
    rest = jnp.concatenate([b_all[:, CH:LANES], b_all[:, :CH], b_all[:, LANES:]], axis=1)
    row = lax.broadcasted_iota(jnp.int32, (CH, 4 * CH), 0)
    rows = jnp.zeros((CH, 4 * CH), f32)
    for i in range(3):
        top = (rest * (1 - 2.0 ** -8)).astype(bf).astype(f32) if i == 0 else rest.astype(bf).astype(f32)
        rows = jnp.where(row == i, top, rows)
        rest = rest - top
    wbuf[9, 0] = rows.astype(bf)
    wbuf[9, 1] = jnp.zeros((CH, 4 * CH), bf)
    ones = jnp.where(lax.broadcasted_iota(jnp.int32, (1, LANES), 1) < 3, 1.0, 0.0).astype(bf)

    def pack(v):
        return jnp.concatenate([v[:, :HG], v[:, HG:]], axis=3)

    def unpack(v):
        return jnp.concatenate([v[..., :CH], v[..., CH:]], axis=1)

    def masked(r, v):
        if 0 <= r < R:
            return v
        return lax.select(jnp.broadcast_to(has_up if r < 0 else has_dn, v.shape), v, jnp.zeros_like(v))

    def emit(t, lo, hi, hx):
        nxt = xh_even if t % 2 == 0 else xh_odd
        at, to = slot(lo, hi), cells_of(lo, hi)
        shift[at, 8:8 + W, :] = hx.reshape(hi - lo, W, LANES)
        nxt[1, to] = hx.astype(bf)
        nxt[0, to] = shift[at, 7:7 + W, :].reshape(hx.shape).astype(bf)
        nxt[2, to] = shift[at, 9:9 + W, :].reshape(hx.shape).astype(bf)

    def cells_of(lo, hi):
        return slice((lo + PAD) * W, (hi + PAD) * W)

    def slot(lo, hi):
        if turn[0] + hi - lo > RING:
            turn[0] = 0
        turn[0] += hi - lo
        return slice(turn[0] - (hi - lo), turn[0])

    def flat(v):
        return v.reshape(-1, v.shape[-1])

    def x_rows(t, lo, hi):
        if lo >= 0 and hi <= R:
            return flat(xin[t, lo:hi].astype(f32))
        side, i = (0, lo + plan.xrows[t]) if lo < 0 else (1, lo - R)
        return flat(unpack(xr_ref[side, plan.xat[t] + i:plan.xat[t] + i + hi - lo].astype(f32)))

    def wait_x(g):
        if g < len(plan.groups):
            x_own[g].wait()
            x_push[g].wait_recv()

    def border(b, kind, side):
        f = plan.first[b]
        if kind < 2:
            src, dst, at = [(hs_ref, hr_ref, plan.hat), (cs_ref, cr_ref, plan.cat)][kind]
            at, end = at[b], at[b + 1]
        else:
            src, dst = xs_ref, xr_ref
            at, end = [plan.xat[f + o] for o in plan.parts[b][kind - 2]]
        return remote(src.at[side, at:end], dst.at[1 - side, at:end],
                      s_bs.at[min(kind, 2), side], s_b.at[kind, 1 - side, b], side_dev[side])

    def pack_x(t0, t1):
        for side in range(2):
            for t in range(t0, t1):
                m = plan.xrows[t]
                lo = 0 if side == 0 else R - m
                xs_ref[side, plan.xat[t]:plan.xat[t] + m] = pack(xin[t, lo:lo + m])

    def start_border(b, *kinds):
        each_side(lambda side: [border(b, kind, side).start() for kind in kinds])

    far = lax.rem(n, FAR) == 0

    def start_first(side, late, *kinds):
        ok = has_dn if side else jnp.logical_and(has_up, far if late else jnp.logical_not(far))

        @pl.when(ok)
        def _():
            if not side and 0 in kinds:
                pl.semaphore_wait(here_sem, 1)
            for kind in kinds:
                border(0, kind, side).start()

    def wait_border(b, *kinds):
        each_side(lambda side: [border(b, kind, 1 - side).wait_recv() for kind in kinds])

    def pack_h(b, h_rows):
        k = plan.blocks[b]
        for side in range(2):
            lo = 0 if side == 0 else R - k
            hs_ref[side, plan.hat[b]:plan.hat[b] + k] = pack(h_rows[lo:lo + k])

    def pack_c(b):
        k = plan.blocks[b]
        for side in range(2):
            lo = PAD if side == 0 else PAD + R - (k - 1)
            c = cbuf[lo:lo + k - 1]
            cs_ref[side, plan.cat[b]:plan.cat[b] + k - 1] = jnp.where(low_half, c[:, :HW], c[:, HW:])

    weights = wbuf[...].reshape(10 * LANES, 4 * CH)

    def dot(t, lo, hi):
        cur = xh_even if t % 2 == 0 else xh_odd
        taps = [cur[dc, cells_of(lo + dr - 1, hi + dr - 1)] for dr in range(3) for dc in range(3)]
        taps.append(jnp.broadcast_to(ones, taps[0].shape))
        return jnp.dot(jnp.concatenate(taps, axis=1), weights, preferred_element_type=f32)

    def cells(t, lo, hi, gates):
        fi = jnp.tanh(gates[:, :LANES] * 0.5) * 0.5 + 0.5
        og = jnp.tanh(gates[:, LANES:] * scale) * scale + lift
        at = slice(lo + PAD, hi + PAD)
        prod = fi * lax.select(jnp.broadcast_to(low, og.shape), cbuf[at].reshape(og.shape), og)
        c = prod + pltpu.roll(prod, CH, 1)
        h = (og * jnp.tanh(c))[:, :CH]
        if t == T - 1:
            c = c.reshape(hi - lo, 2, 2, HW // 2, LANES)
            for half in range(2):
                both = c[:, half, 0]
                cout[half, lo:hi] = lax.select(jnp.broadcast_to(low, both.shape), both, c[:, half, 1])
        else:
            cbuf[at] = c.reshape(hi - lo, W, LANES)
        for a, e in ((lo, min(hi, 0)), (max(lo, 0), min(hi, R)), (max(lo, R), hi)):
            if a >= e:
                continue
            part = h[(a - lo) * W:(e - lo) * W]
            if a >= 0 and e <= R:
                hout[t, a:e] = part.reshape(e - a, 2 * HG, COLS, CH).astype(bf)
            if t < T - 1:
                emit(t + 1, a, e, masked(a, jnp.concatenate([part, x_rows(t + 1, a, e)], axis=1)))

    pending = []

    def piece(at, ahead=1):
        t, lo, hi = at
        while any(u == t - 1 and a <= hi and lo <= e for u, a, e, _ in pending):
            cells(*pending.pop(0))
        pending.append((*at, dot(*at)))
        flush(ahead)

    def flush(left=0):
        while len(pending) > left:
            cells(*pending.pop(0))

    def push_h(t0, t1, lo=0, hi=R):
        rows = slice(lo, hi)
        remote(hout.at[t0:t1, rows, theirs], hpeer.at[t0:t1, rows], s_os.at[0], s_or.at[0], peer).start()

    def push_c(lo, hi):
        remote(cout.at[p, lo:hi], cpeer.at[lo:hi], s_os.at[1], s_or.at[1], peer).start()

    for c in [h_own, x_own[0]]:
        c.wait()
    for c in [h_push, x_push[0]]:
        c.wait_recv()
    pack_h(0, hst)
    pack_x(0, 1)
    start_first(1, 0, 0, 2)
    start_first(0, 0, 0, 2)
    for lo, hi in cuts(0, R):
        emit(0, lo, hi, jnp.concatenate([flat(hst[lo:hi].astype(f32)), x_rows(0, lo, hi)], axis=1))

    for b, k in enumerate(plan.blocks):
        f = plan.first[b]
        last = b + 1 == NB

        def inner(o):
            if o == 0:
                got = [*cuts(k + 1, R - 1 - k), *cuts(1, k + 1), *cuts(R - 1 - k, R - 1)]
            else:
                got = cuts(o + 1, R - 1 - o)
                got = got[1:-1] + [got[0], got[-1]]
            return [(f + o, lo, hi) for lo, hi in got]

        early = [at for o in range(k) for at in inner(o)]
        late = early[len(early) - LATE[b]:]
        for o in range(k):
            pieces = [at for at in early[:len(early) - LATE[b]] if at[0] == f + o]
            first = 0
            if o == 0 and b:
                piece(pieces[0], 9)
                flush(1)
                pack_h(b, hout.at[f - 1])
                pack_c(b)
                start_border(b, 0, 1)
                first = 1
            if b == 0 and o == 0:
                for at in pieces[:2]:
                    piece(at, 9)
                c_own.wait()
                c_push.wait_recv()
                wait_x(1)
                for at in pieces[2:4]:
                    piece(at, 9)
                c0, got = cst[...], cin[...]
                cbuf[PAD:PAD + R, mine_c] = jnp.concatenate([c0, c0], axis=2)
                swapped, keep = pltpu.roll(got, CH, 2), jnp.broadcast_to(low, got.shape)
                both = [lax.select(keep, got, swapped), lax.select(keep, swapped, got)]
                cbuf[PAD:PAD + R, theirs_c] = jnp.concatenate(both, axis=1)
                pack_c(0)
                pack_x(1, 3)
                start_first(1, 0, 1, 3, 4)
                start_first(0, 0, 1, 3, 4)
                first = 4
            if b == 0 and o == 2:
                for at in pieces[:2]:
                    piece(at, 9)
                flush(2)
                wait_x(2)
                for at in pieces[2:4]:
                    piece(at, 9)
                pack_x(3, k)
                for side in range(2):
                    start_first(side, 0, 5)
                start_first(0, 1, 5)
                first = 4
            if b == 0 and o == 4:
                for at in pieces[:2]:
                    piece(at, 9)
                flush(2)
                wait_x(3)
                todo = plan.blocks[1]
                share = -(-todo // len(pieces[2:]))
                for i, at in enumerate(pieces[2:]):
                    piece(at)
                    pack_x(k + min(i * share, todo), k + min((i + 1) * share, todo))
                start_border(1, 2)
                first = len(pieces)
            for at in pieces[first:]:
                piece(at)
            if b == 0 and o == 0:
                start_first(0, 1, 0, 2, 1, 3, 4)
            if o == 0 and b and not last:
                pack_x(f + k, f + k + plan.blocks[b + 1])
        wait_border(b, 0, 2)
        if b and not last:
            start_border(b + 1, 2)
        if b:
            push_h(plan.first[b - 1], f)
        piece(late.pop(0), 3)
        for side in range(2):
            lo = -k if side == 0 else R
            h = flat(unpack(hr_ref[side, plan.hat[b]:plan.hat[b] + k].astype(f32)))
            for a, e in cuts(lo, lo + k):
                part = h[(a - lo) * W:(e - lo) * W]
                emit(f, a, e, masked(a, jnp.concatenate([part, x_rows(f, a, e)], axis=1)))
        for o in range(k):
            m = k - 1 - o
            top, bottom = even_cuts(-m, o + 1), even_cuts(R - 1 - o, R + m)
            for lo, hi in top:
                piece((f + o, lo, hi), 9 if o == 0 else 1)
                if lo != top[0][0]:
                    continue
                if b == 0 and o in (1, 2):
                    wait_border(0, 3 + o)
                if last and o == k // 2:
                    push_h(f, f + o)
                if last and o == k - 2:
                    push_h(f + k // 2, f + o)
                    push_h(T - 1, T, k, R - k)
                    push_c(k, R - k)
                if last and o == k - 1:
                    push_h(T - 2, T - 1)
            for lo, hi in bottom:
                piece((f + o, lo, hi), 9 if o == 0 else 1)
            if o == 0:
                wait_border(b, 1, *(() if b else (3,)))
                for side in range(2):
                    lo = PAD - (k - 1) if side == 0 else PAD + R
                    packed = cr_ref[side, plan.cat[b]:plan.cat[b] + k - 1]
                    both = jnp.concatenate([packed, pltpu.roll(packed, CH, 2)], axis=1)
                    cbuf[lo:lo + k - 1] = both
                while late:
                    piece(late.pop(0), 3)
        assert not late
    flush()
    k = plan.blocks[-1]
    for lo, hi in ((0, k), (R - k, R)):
        push_h(T - 1, T, lo, hi)
        push_c(lo, hi)

    for c in [h_push, c_push, *x_push]:
        c.wait_send()

    def wait_sends(side):
        for kind, ref in enumerate((hs_ref, cs_ref, xs_ref)):
            local(ref.at[side], ref.at[side], s_bs.at[kind, side]).wait()

    each_side(wait_sends)
    for sem in (s_os, s_or):
        local(hpeer, hpeer, sem.at[0]).wait()
        local(cpeer, cpeer, sem.at[1]).wait()


def store(hout, hpeer, cout, cpeer, h_all, c_final, c_tile, sems):
    s = lax.axis_index("cols")
    HG = hpeer.shape[2]
    copies = [pltpu.make_async_copy(hout.at[:, :, pl.ds(s * HG, HG)], h_all.at[:, s], sems.at[0]),
              pltpu.make_async_copy(hpeer, h_all.at[:, 1 - s], sems.at[1]),
              pltpu.make_async_copy(c_tile.at[0], c_final.at[s], sems.at[2]),
              pltpu.make_async_copy(c_tile.at[1], c_final.at[1 - s], sems.at[3])]
    for c in copies[:2]:
        c.start()
    for i, packed in enumerate((cout[s], cpeer[...])):
        c_tile[i] = jnp.concatenate([packed[:, :, :CH], packed[:, :, CH:]], axis=1)
    for c in copies[2:]:
        c.start()
    for c in copies:
        c.wait()


def run(blocks, n_rows, frames, w_x, w_h, gate_bias, h_init, c_init):
    T, S, R, HW = frames.shape[:4]
    W, HG = 2 * HW, HW // COLS
    plan = Plan(blocks, T, R, W)
    NB, PAD, G = len(blocks), plan.K, len(plan.groups)
    bf, f32 = jnp.bfloat16, jnp.float32
    vm, dma = pltpu.VMEM, pltpu.SemaphoreType.DMA
    hbm = pl.BlockSpec(memory_space=pltpu.HBM)
    vmem = pl.BlockSpec(memory_space=pltpu.VMEM)
    tiled = frames.reshape(T, S, R, HG, COLS, CH)
    parts = pl.pallas_call(
        functools.partial(kernel, plan, n_rows),
        out_shape=(vm((T, R, 2 * HG, COLS, CH), bf), vm((T, R, HG, COLS, CH), bf),
                   vm((2, R, HW // 2, LANES), f32), vm((R, HW // 2, LANES), f32)),
        in_specs=[hbm] * 6,
        out_specs=(vmem,) * 4,
        scratch_shapes=[
            vm((1, 4 * CH), f32), vm((R, HG, COLS, CH), bf), vm((R, HW, CH), f32),
            vm((R, HW // 2, LANES), f32), vm((R, HW // 2, LANES), f32),
            vm((plan.groups[1][1], R, HG, COLS, CH), bf),
            vm((T, R, 2 * HG, COLS, CH), bf), vm((R, 2 * HG, COLS, CH), bf), vm((R, HW, CH), f32),
            vm((3, (R + 2 * PAD) * W, LANES), bf), vm((3, (R + 2 * PAD) * W, LANES), bf),
            vm((R + 2 * PAD, W, LANES), f32), vm((RING, W + 16, LANES), f32), vm((10, 2, CH, 4 * CH), bf),
            vm((2, plan.xat[-1], HG, COLS, LANES), bf), vm((2, plan.xat[-1], HG, COLS, LANES), bf),
            vm((2, plan.hat[-1], HG, COLS, LANES), bf), vm((2, plan.hat[-1], HG, COLS, LANES), bf),
            vm((2, plan.cat[-1], HW, LANES), f32), vm((2, plan.cat[-1], HW, LANES), f32),
            dma((3,)), dma((6,)), dma((2,)), dma((2,)), dma((G,)), dma((G,)), dma((G,)),
            dma((6, 2, NB)), dma((3, 2)), dma((2,)), dma((2,)), pltpu.SemaphoreType.REGULAR],
        compiler_params=pltpu.CompilerParams(collective_id=0, has_side_effects=True, vmem_limit_bytes=46 * 2**20),
    )(tiled, w_x.reshape(9, CH, 4 * CH), w_h.reshape(9, CH, 4 * CH), gate_bias.reshape(1, -1),
      h_init.reshape(S, R, HG, COLS, CH), c_init)
    h_all, c_final = pl.pallas_call(
        store,
        out_shape=(jax.ShapeDtypeStruct(tiled.shape, bf), jax.ShapeDtypeStruct(c_init.shape, f32)),
        in_specs=[vmem] * 4,
        out_specs=(hbm, hbm),
        scratch_shapes=[vm((2, R, HW, CH), f32), dma((4,))],
        compiler_params=pltpu.CompilerParams(vmem_limit_bytes=4 * 2**20),
    )(*[pltpu.with_memory_space_constraint(a, pltpu.VMEM) for a in parts])
    return h_all.reshape(frames.shape), c_final


def solution(mesh, K=None):
    n_rows = mesh.shape["rows"]
    frame_spec = P(None, "batch", "rows", "cols", None)
    state_spec = P("batch", "rows", "cols", None)
    blocks = BLOCKS if K is None else K
    return jax.shard_map(functools.partial(run, blocks, n_rows), mesh=mesh,
                         in_specs=(frame_spec, P(), P(), P(), state_spec, state_spec),
                         out_specs=(frame_spec, state_spec), check_vma=False)
```

```python
import functools

import jax
import jax.numpy as jnp
from jax import lax
from jax.experimental import pallas as pl
from jax.experimental.pallas import tpu as pltpu
from jax.sharding import PartitionSpec as P

MESH = pl.DeviceIdType.MESH
CH = 64
LANES = 128
COLS = 8
PIECE = 4
RING = 8
BLOCKS = (7, 9)
LATE = (2, 3)
BORDER = 3
FAR = 16


def cuts(lo, hi, size=PIECE):
    n = max(1, (hi - lo) // size)
    edges = [lo + i * size for i in range(n)] + [hi]
    return list(zip(edges[:-1], edges[1:]))


def even_cuts(lo, hi):
    n = max(1, round((hi - lo) / BORDER))
    edges = [lo + (hi - lo) * i // n for i in range(n + 1)]
    return list(zip(edges[:-1], edges[1:]))


class Plan:
    def __init__(self, blocks, T, R, W):
        assert sum(blocks) == T
        self.blocks, self.T, self.R, self.W, self.HW, self.HG = blocks, T, R, W, W // 2, W // 2 // COLS
        self.K = max(blocks)
        self.first = [sum(blocks[:b]) for b in range(len(blocks))]
        self.of = [(b, o) for b, k in enumerate(blocks) for o in range(k)]
        self.xrows = [blocks[b] - o for b, o in self.of]
        self.xat = [sum(self.xrows[:t]) for t in range(T + 1)]
        self.parts = [[(0, 1), (1, 2), (2, 4), (4, k)] if b == 0 else [(0, k)] for b, k in enumerate(blocks)]
        self.hat = [sum(blocks[:b]) for b in range(len(blocks) + 1)]
        self.cat = [sum(k - 1 for k in blocks[:b]) for b in range(len(blocks) + 1)]
        ends = [0, 1, 3, blocks[0] + 1, T]
        self.groups = [(a, e) for a, e in zip(ends[:-1], ends[1:]) if e > a]


def kernel(plan, n_rows, frames, w_x, w_h, bias_in, h_init, c_init, hout, hpeer, cout, cpeer,
           bias, hgo, cgo, cgp, cin, xgo, xin, hst, cst, xh_even, xh_odd, cbuf, shift, wbuf,
           xs_ref, xr_ref, hs_ref, hr_ref, cs_ref, cr_ref,
           s_w, s_i, s_ir, s_is, s_x, s_xr, s_xs, s_b, s_bs, s_or, s_os, here_sem):
    T, R, W, HW, HG = plan.T, plan.R, plan.W, plan.HW, plan.HG
    PAD = plan.K
    NB = len(plan.blocks)
    s = lax.axis_index("cols")
    n = lax.axis_index("rows")
    p = 1 - s
    mine, theirs = pl.ds(s * HG, HG), pl.ds(p * HG, HG)
    mine_c, theirs_c = [pl.ds(pl.multiple_of(i * HW, HW), HW) for i in (s, p)]
    has_up, has_dn = n > 0, n < n_rows - 1
    bf, f32 = jnp.bfloat16, jnp.float32

    def local(src, dst, sem):
        return pltpu.make_async_copy(src, dst, sem)

    def remote(src, dst, ssem, rsem, dev):
        return pltpu.make_async_remote_copy(
            src_ref=src, dst_ref=dst, send_sem=ssem, recv_sem=rsem, device_id=dev, device_id_type=MESH)

    peer = {"cols": p}
    side_dev = [{"rows": n - 1}, {"rows": n + 1}]
    side_ok = [has_up, has_dn]

    def each_side(do):
        for side in range(2):
            @pl.when(side_ok[side])
            def _():
                do(side)

    barrier = pltpu.get_barrier_semaphore()

    def signal(dev):
        pl.semaphore_signal(barrier, inc=1, device_id=dev, device_id_type=MESH)

    signal(peer)

    @pl.when(has_up)
    def _():
        signal(side_dev[0])


    h_own = local(h_init.at[s], hst.at[:, mine], s_i.at[0])
    c_own = local(c_init.at[s], cst, s_i.at[1])
    x_own = [local(frames.at[a:e, s], xin.at[a:e, :, mine], s_x.at[g]) for g, (a, e) in enumerate(plan.groups)]
    h_got = local(h_init.at[p], hgo, s_i.at[2])
    c_got = local(c_init.at[p], cgo, s_i.at[3])
    x_got = [local(frames.at[a:e, p], xgo.at[a:e], s_i.at[4 + g]) for g, (a, e) in enumerate(plan.groups[:2])]
    w_copies = [local(w_h, wbuf.at[0:9, 0], s_w.at[0]), local(w_x, wbuf.at[0:9, 1], s_w.at[1]),
                local(bias_in, bias, s_w.at[2])]
    for c in [h_got, x_got[0], c_got, h_own, x_own[0], c_own, *w_copies, x_got[1], *x_own[1:]]:
        c.start()
    pl.semaphore_wait(barrier, 1 + has_dn.astype(jnp.int32))

    @pl.when(has_dn)
    def _():
        pl.semaphore_signal(here_sem, inc=1, device_id=side_dev[1], device_id_type=MESH)


    h_push = remote(hgo, hst.at[:, mine], s_is.at[0], s_ir.at[0], peer)
    c_push = remote(cgp, cin, s_is.at[1], s_ir.at[1], peer)
    x_push = [remote((xgo if g < 2 else frames.at[:, p]).at[a:e], xin.at[a:e, :, mine], s_xs.at[g], s_xr.at[g], peer)
              for g, (a, e) in enumerate(plan.groups)]
    for got, push in [(h_got, h_push), (x_got[0], x_push[0]), (c_got, c_push), (x_got[1], x_push[1])]:
        got.wait()
        if push is c_push:
            cgp[...] = jnp.concatenate([cgo[:, :HW // 2], cgo[:, HW // 2:]], axis=2)
        push.start()
    for push in x_push[2:]:
        push.start()

    shift[...] = jnp.zeros_like(shift)
    low = lax.broadcasted_iota(jnp.int32, (1, LANES), 1) < CH
    low_half = low_row = low
    turn = [0]
    scale = jnp.where(low_row, 0.5, 1.0)
    lift = jnp.where(low_row, 0.5, 0.0)

    for c in w_copies:
        c.wait()
    for tap in range(9):
        for half in range(2):
            tile = wbuf[tap, half, :, 0:LANES]
            wbuf[tap, half, :, 0:LANES] = jnp.concatenate([tile[:, CH:], tile[:, :CH]], axis=1)
    b_all = bias[...]
    rest = jnp.concatenate([b_all[:, CH:LANES], b_all[:, :CH], b_all[:, LANES:]], axis=1)
    row = lax.broadcasted_iota(jnp.int32, (CH, 4 * CH), 0)
    rows = jnp.zeros((CH, 4 * CH), f32)
    for i in range(3):
        top = (rest * (1 - 2.0 ** -8)).astype(bf).astype(f32) if i == 0 else rest.astype(bf).astype(f32)
        rows = jnp.where(row == i, top, rows)
        rest = rest - top
    wbuf[9, 0] = rows.astype(bf)
    wbuf[9, 1] = jnp.zeros((CH, 4 * CH), bf)
    ones = jnp.where(lax.broadcasted_iota(jnp.int32, (1, LANES), 1) < 3, 1.0, 0.0).astype(bf)

    def pack(v):
        return jnp.concatenate([v[:, :HG], v[:, HG:]], axis=3)

    def unpack(v):
        return jnp.concatenate([v[..., :CH], v[..., CH:]], axis=1)

    def masked(r, v):
        if 0 <= r < R:
            return v
        return lax.select(jnp.broadcast_to(has_up if r < 0 else has_dn, v.shape), v, jnp.zeros_like(v))

    def emit(t, lo, hi, hx):
        nxt = xh_even if t % 2 == 0 else xh_odd
        at, to = slot(lo, hi), cells_of(lo, hi)
        shift[at, 8:8 + W, :] = hx.reshape(hi - lo, W, LANES)
        nxt[1, to] = hx.astype(bf)
        nxt[0, to] = shift[at, 7:7 + W, :].reshape(hx.shape).astype(bf)
        nxt[2, to] = shift[at, 9:9 + W, :].reshape(hx.shape).astype(bf)

    def cells_of(lo, hi):
        return slice((lo + PAD) * W, (hi + PAD) * W)

    def slot(lo, hi):
        if turn[0] + hi - lo > RING:
            turn[0] = 0
        turn[0] += hi - lo
        return slice(turn[0] - (hi - lo), turn[0])

    def flat(v):
        return v.reshape(-1, v.shape[-1])

    def x_rows(t, lo, hi):
        if lo >= 0 and hi <= R:
            return flat(xin[t, lo:hi].astype(f32))
        side, i = (0, lo + plan.xrows[t]) if lo < 0 else (1, lo - R)
        return flat(unpack(xr_ref[side, plan.xat[t] + i:plan.xat[t] + i + hi - lo].astype(f32)))

    def wait_x(g):
        if g < len(plan.groups):
            x_own[g].wait()
            x_push[g].wait_recv()

    def border(b, kind, side):
        f = plan.first[b]
        if kind < 2:
            src, dst, at = [(hs_ref, hr_ref, plan.hat), (cs_ref, cr_ref, plan.cat)][kind]
            at, end = at[b], at[b + 1]
        else:
            src, dst = xs_ref, xr_ref
            at, end = [plan.xat[f + o] for o in plan.parts[b][kind - 2]]
        return remote(src.at[side, at:end], dst.at[1 - side, at:end],
                      s_bs.at[min(kind, 2), side], s_b.at[kind, 1 - side, b], side_dev[side])

    def pack_x(t0, t1):
        for side in range(2):
            for t in range(t0, t1):
                m = plan.xrows[t]
                lo = 0 if side == 0 else R - m
                xs_ref[side, plan.xat[t]:plan.xat[t] + m] = pack(xin[t, lo:lo + m])

    def start_border(b, *kinds):
        each_side(lambda side: [border(b, kind, side).start() for kind in kinds])

    far = lax.rem(n, FAR) == 0

    def start_first(side, late, *kinds):
        ok = has_dn if side else jnp.logical_and(has_up, far if late else jnp.logical_not(far))

        @pl.when(ok)
        def _():
            if not side and 0 in kinds:
                pl.semaphore_wait(here_sem, 1)
            for kind in kinds:
                border(0, kind, side).start()

    def wait_border(b, *kinds):
        each_side(lambda side: [border(b, kind, 1 - side).wait_recv() for kind in kinds])

    def pack_h(b, h_rows):
        k = plan.blocks[b]
        for side in range(2):
            lo = 0 if side == 0 else R - k
            hs_ref[side, plan.hat[b]:plan.hat[b] + k] = pack(h_rows[lo:lo + k])

    def pack_c(b):
        k = plan.blocks[b]
        for side in range(2):
            lo = PAD if side == 0 else PAD + R - (k - 1)
            c = cbuf[lo:lo + k - 1]
            cs_ref[side, plan.cat[b]:plan.cat[b] + k - 1] = jnp.where(low_half, c[:, :HW], c[:, HW:])

    weights = wbuf[...].reshape(10 * LANES, 4 * CH)

    def dot(t, lo, hi):
        cur = xh_even if t % 2 == 0 else xh_odd
        taps = [cur[dc, cells_of(lo + dr - 1, hi + dr - 1)] for dr in range(3) for dc in range(3)]
        taps.append(jnp.broadcast_to(ones, taps[0].shape))
        return jnp.dot(jnp.concatenate(taps, axis=1), weights, preferred_element_type=f32)

    def cells(t, lo, hi, gates):
        fi = jnp.tanh(gates[:, :LANES] * 0.5) * 0.5 + 0.5
        og = jnp.tanh(gates[:, LANES:] * scale) * scale + lift
        at = slice(lo + PAD, hi + PAD)
        prod = fi * lax.select(jnp.broadcast_to(low, og.shape), cbuf[at].reshape(og.shape), og)
        c = prod + pltpu.roll(prod, CH, 1)
        h = (og * jnp.tanh(c))[:, :CH]
        if t == T - 1:
            c = c.reshape(hi - lo, 2, 2, HW // 2, LANES)
            for half in range(2):
                both = c[:, half, 0]
                cout[half, lo:hi] = lax.select(jnp.broadcast_to(low, both.shape), both, c[:, half, 1])
        else:
            cbuf[at] = c.reshape(hi - lo, W, LANES)
        for a, e in ((lo, min(hi, 0)), (max(lo, 0), min(hi, R)), (max(lo, R), hi)):
            if a >= e:
                continue
            part = h[(a - lo) * W:(e - lo) * W]
            if a >= 0 and e <= R:
                hout[t, a:e] = part.reshape(e - a, 2 * HG, COLS, CH).astype(bf)
            if t < T - 1:
                emit(t + 1, a, e, masked(a, jnp.concatenate([part, x_rows(t + 1, a, e)], axis=1)))

    pending = []

    def piece(at, ahead=1):
        t, lo, hi = at
        while any(u == t - 1 and a <= hi and lo <= e for u, a, e, _ in pending):
            cells(*pending.pop(0))
        pending.append((*at, dot(*at)))
        flush(ahead)

    def flush(left=0):
        while len(pending) > left:
            cells(*pending.pop(0))

    def push_h(t0, t1, lo=0, hi=R):
        rows = slice(lo, hi)
        remote(hout.at[t0:t1, rows, theirs], hpeer.at[t0:t1, rows], s_os.at[0], s_or.at[0], peer).start()

    def push_c(lo, hi):
        remote(cout.at[p, lo:hi], cpeer.at[lo:hi], s_os.at[1], s_or.at[1], peer).start()

    for c in [h_own, x_own[0]]:
        c.wait()
    for c in [h_push, x_push[0]]:
        c.wait_recv()
    pack_h(0, hst)
    pack_x(0, 1)
    start_first(1, 0, 0, 2)
    start_first(0, 0, 0, 2)
    for lo, hi in cuts(0, R):
        emit(0, lo, hi, jnp.concatenate([flat(hst[lo:hi].astype(f32)), x_rows(0, lo, hi)], axis=1))

    for b, k in enumerate(plan.blocks):
        f = plan.first[b]
        last = b + 1 == NB

        def inner(o):
            if o == 0:
                got = [*cuts(k + 1, R - 1 - k), *cuts(1, k + 1), *cuts(R - 1 - k, R - 1)]
            else:
                got = cuts(o + 1, R - 1 - o)
                got = got[1:-1] + [got[0], got[-1]]
            return [(f + o, lo, hi) for lo, hi in got]

        early = [at for o in range(k) for at in inner(o)]
        late = early[len(early) - LATE[b]:]
        for o in range(k):
            pieces = [at for at in early[:len(early) - LATE[b]] if at[0] == f + o]
            first = 0
            if o == 0 and b:
                piece(pieces[0], 9)
                flush(1)
                pack_h(b, hout.at[f - 1])
                pack_c(b)
                start_border(b, 0, 1)
                first = 1
            if b == 0 and o == 0:
                for at in pieces[:2]:
                    piece(at, 9)
                c_own.wait()
                c_push.wait_recv()
                wait_x(1)
                for at in pieces[2:4]:
                    piece(at, 9)
                c0, got = cst[...], cin[...]
                cbuf[PAD:PAD + R, mine_c] = jnp.concatenate([c0, c0], axis=2)
                swapped, keep = pltpu.roll(got, CH, 2), jnp.broadcast_to(low, got.shape)
                both = [lax.select(keep, got, swapped), lax.select(keep, swapped, got)]
                cbuf[PAD:PAD + R, theirs_c] = jnp.concatenate(both, axis=1)
                pack_c(0)
                pack_x(1, 2)
                start_first(1, 0, 1, 3)
                start_first(0, 0, 1, 3)
                first = 4
            if b == 0 and o == 2:
                for at in pieces[:2]:
                    piece(at, 9)
                flush(2)
                wait_x(2)
                for at in pieces[2:4]:
                    piece(at, 9)
                pack_x(2, k)
                for side in range(2):
                    start_first(side, 0, 4, 5)
                start_first(0, 1, 4, 5)
                first = 4
            if b == 0 and o == 4:
                for at in pieces[:2]:
                    piece(at, 9)
                flush(2)
                wait_x(3)
                todo = plan.blocks[1]
                share = -(-todo // len(pieces[2:]))
                for i, at in enumerate(pieces[2:]):
                    piece(at)
                    pack_x(k + min(i * share, todo), k + min((i + 1) * share, todo))
                start_border(1, 2)
                first = len(pieces)
            for at in pieces[first:]:
                piece(at)
            if b == 0 and o == 0:
                start_first(0, 1, 0, 2, 1, 3)
            if o == 0 and b and not last:
                pack_x(f + k, f + k + plan.blocks[b + 1])
        wait_border(b, 0, 2)
        if b and not last:
            start_border(b + 1, 2)
        if b:
            push_h(plan.first[b - 1], f)
        piece(late.pop(0), 3)
        for side in range(2):
            lo = -k if side == 0 else R
            h = flat(unpack(hr_ref[side, plan.hat[b]:plan.hat[b] + k].astype(f32)))
            for a, e in cuts(lo, lo + k):
                part = h[(a - lo) * W:(e - lo) * W]
                emit(f, a, e, masked(a, jnp.concatenate([part, x_rows(f, a, e)], axis=1)))
        for o in range(k):
            m = k - 1 - o
            top, bottom = even_cuts(-m, o + 1), even_cuts(R - 1 - o, R + m)
            for lo, hi in top:
                piece((f + o, lo, hi), 9 if o == 0 else 1)
                if lo != top[0][0]:
                    continue
                if b == 0 and o in (1, 3):
                    wait_border(0, 4 if o == 1 else 5)
                if last and o == k // 2:
                    push_h(f, f + o)
                if last and o == k - 2:
                    push_h(f + k // 2, f + o)
                    push_h(T - 1, T, k, R - k)
                    push_c(k, R - k)
                if last and o == k - 1:
                    push_h(T - 2, T - 1)
            for lo, hi in bottom:
                piece((f + o, lo, hi), 9 if o == 0 else 1)
            if o == 0:
                wait_border(b, 1, *(() if b else (3,)))
                for side in range(2):
                    lo = PAD - (k - 1) if side == 0 else PAD + R
                    packed = cr_ref[side, plan.cat[b]:plan.cat[b] + k - 1]
                    both = jnp.concatenate([packed, pltpu.roll(packed, CH, 2)], axis=1)
                    cbuf[lo:lo + k - 1] = both
                while late:
                    piece(late.pop(0), 3)
        assert not late
    flush()
    k = plan.blocks[-1]
    for lo, hi in ((0, k), (R - k, R)):
        push_h(T - 1, T, lo, hi)
        push_c(lo, hi)

    for c in [h_push, c_push, *x_push]:
        c.wait_send()

    def wait_sends(side):
        for kind, ref in enumerate((hs_ref, cs_ref, xs_ref)):
            local(ref.at[side], ref.at[side], s_bs.at[kind, side]).wait()

    each_side(wait_sends)
    for sem in (s_os, s_or):
        local(hpeer, hpeer, sem.at[0]).wait()
        local(cpeer, cpeer, sem.at[1]).wait()


def store(hout, hpeer, cout, cpeer, h_all, c_final, c_tile, sems):
    s = lax.axis_index("cols")
    HG = hpeer.shape[2]
    copies = [pltpu.make_async_copy(hout.at[:, :, pl.ds(s * HG, HG)], h_all.at[:, s], sems.at[0]),
              pltpu.make_async_copy(hpeer, h_all.at[:, 1 - s], sems.at[1]),
              pltpu.make_async_copy(c_tile.at[0], c_final.at[s], sems.at[2]),
              pltpu.make_async_copy(c_tile.at[1], c_final.at[1 - s], sems.at[3])]
    for c in copies[:2]:
        c.start()
    for i, packed in enumerate((cout[s], cpeer[...])):
        c_tile[i] = jnp.concatenate([packed[:, :, :CH], packed[:, :, CH:]], axis=1)
    for c in copies[2:]:
        c.start()
    for c in copies:
        c.wait()


def run(blocks, n_rows, frames, w_x, w_h, gate_bias, h_init, c_init):
    T, S, R, HW = frames.shape[:4]
    W, HG = 2 * HW, HW // COLS
    plan = Plan(blocks, T, R, W)
    NB, PAD, G = len(blocks), plan.K, len(plan.groups)
    bf, f32 = jnp.bfloat16, jnp.float32
    vm, dma = pltpu.VMEM, pltpu.SemaphoreType.DMA
    hbm = pl.BlockSpec(memory_space=pltpu.HBM)
    vmem = pl.BlockSpec(memory_space=pltpu.VMEM)
    tiled = frames.reshape(T, S, R, HG, COLS, CH)
    parts = pl.pallas_call(
        functools.partial(kernel, plan, n_rows),
        out_shape=(vm((T, R, 2 * HG, COLS, CH), bf), vm((T, R, HG, COLS, CH), bf),
                   vm((2, R, HW // 2, LANES), f32), vm((R, HW // 2, LANES), f32)),
        in_specs=[hbm] * 6,
        out_specs=(vmem,) * 4,
        scratch_shapes=[
            vm((1, 4 * CH), f32), vm((R, HG, COLS, CH), bf), vm((R, HW, CH), f32),
            vm((R, HW // 2, LANES), f32), vm((R, HW // 2, LANES), f32),
            vm((plan.groups[1][1], R, HG, COLS, CH), bf),
            vm((T, R, 2 * HG, COLS, CH), bf), vm((R, 2 * HG, COLS, CH), bf), vm((R, HW, CH), f32),
            vm((3, (R + 2 * PAD) * W, LANES), bf), vm((3, (R + 2 * PAD) * W, LANES), bf),
            vm((R + 2 * PAD, W, LANES), f32), vm((RING, W + 16, LANES), f32), vm((10, 2, CH, 4 * CH), bf),
            vm((2, plan.xat[-1], HG, COLS, LANES), bf), vm((2, plan.xat[-1], HG, COLS, LANES), bf),
            vm((2, plan.hat[-1], HG, COLS, LANES), bf), vm((2, plan.hat[-1], HG, COLS, LANES), bf),
            vm((2, plan.cat[-1], HW, LANES), f32), vm((2, plan.cat[-1], HW, LANES), f32),
            dma((3,)), dma((6,)), dma((2,)), dma((2,)), dma((G,)), dma((G,)), dma((G,)),
            dma((6, 2, NB)), dma((3, 2)), dma((2,)), dma((2,)), pltpu.SemaphoreType.REGULAR],
        compiler_params=pltpu.CompilerParams(collective_id=0, has_side_effects=True, vmem_limit_bytes=46 * 2**20),
    )(tiled, w_x.reshape(9, CH, 4 * CH), w_h.reshape(9, CH, 4 * CH), gate_bias.reshape(1, -1),
      h_init.reshape(S, R, HG, COLS, CH), c_init)
    h_all, c_final = pl.pallas_call(
        store,
        out_shape=(jax.ShapeDtypeStruct(tiled.shape, bf), jax.ShapeDtypeStruct(c_init.shape, f32)),
        in_specs=[vmem] * 4,
        out_specs=(hbm, hbm),
        scratch_shapes=[vm((2, R, HW, CH), f32), dma((4,))],
        compiler_params=pltpu.CompilerParams(vmem_limit_bytes=4 * 2**20),
    )(*[pltpu.with_memory_space_constraint(a, pltpu.VMEM) for a in parts])
    return h_all.reshape(frames.shape), c_final


def solution(mesh, K=None):
    n_rows = mesh.shape["rows"]
    frame_spec = P(None, "batch", "rows", "cols", None)
    state_spec = P("batch", "rows", "cols", None)
    blocks = BLOCKS if K is None else K
    return jax.shard_map(functools.partial(run, blocks, n_rows), mesh=mesh,
                         in_specs=(frame_spec, P(), P(), P(), state_spec, state_spec),
                         out_specs=(frame_spec, state_spec), check_vma=False)
```

```python
import functools

import jax
import jax.numpy as jnp
from jax import lax
from jax.experimental import pallas as pl
from jax.experimental.pallas import tpu as pltpu
from jax.sharding import PartitionSpec as P

MESH = pl.DeviceIdType.MESH
CH = 64
LANES = 128
COLS = 8
PIECE = 4
RING = 8
BLOCKS = (7, 9)
LATE = (2, 4)
BORDER = 3
FAR = 16


def cuts(lo, hi, size=PIECE):
    n = max(1, (hi - lo) // size)
    edges = [lo + i * size for i in range(n)] + [hi]
    return list(zip(edges[:-1], edges[1:]))


def even_cuts(lo, hi):
    n = max(1, round((hi - lo) / BORDER))
    edges = [lo + (hi - lo) * i // n for i in range(n + 1)]
    return list(zip(edges[:-1], edges[1:]))


class Plan:
    def __init__(self, blocks, T, R, W):
        assert sum(blocks) == T
        self.blocks, self.T, self.R, self.W, self.HW, self.HG = blocks, T, R, W, W // 2, W // 2 // COLS
        self.K = max(blocks)
        self.first = [sum(blocks[:b]) for b in range(len(blocks))]
        self.of = [(b, o) for b, k in enumerate(blocks) for o in range(k)]
        self.xrows = [blocks[b] - o for b, o in self.of]
        self.xat = [sum(self.xrows[:t]) for t in range(T + 1)]
        self.parts = [[(0, 1), (1, 2), (2, 3), (3, k)] if b == 0 else [(0, k)] for b, k in enumerate(blocks)]
        self.hat = [sum(blocks[:b]) for b in range(len(blocks) + 1)]
        self.cat = [sum(k - 1 for k in blocks[:b]) for b in range(len(blocks) + 1)]
        ends = [0, 1, 3, blocks[0] + 1, T]
        self.groups = [(a, e) for a, e in zip(ends[:-1], ends[1:]) if e > a]


def kernel(plan, n_rows, frames, w_x, w_h, bias_in, h_init, c_init, hout, hpeer, cout, cpeer,
           bias, hgo, cgo, cgp, cin, xgo, xin, hst, cst, xh_even, xh_odd, cbuf, shift, wbuf,
           xs_ref, xr_ref, hs_ref, hr_ref, cs_ref, cr_ref,
           s_w, s_i, s_ir, s_is, s_x, s_xr, s_xs, s_b, s_bs, s_or, s_os, here_sem):
    T, R, W, HW, HG = plan.T, plan.R, plan.W, plan.HW, plan.HG
    PAD = plan.K
    NB = len(plan.blocks)
    s = lax.axis_index("cols")
    n = lax.axis_index("rows")
    p = 1 - s
    mine, theirs = pl.ds(s * HG, HG), pl.ds(p * HG, HG)
    mine_c, theirs_c = [pl.ds(pl.multiple_of(i * HW, HW), HW) for i in (s, p)]
    has_up, has_dn = n > 0, n < n_rows - 1
    bf, f32 = jnp.bfloat16, jnp.float32

    def local(src, dst, sem):
        return pltpu.make_async_copy(src, dst, sem)

    def remote(src, dst, ssem, rsem, dev):
        return pltpu.make_async_remote_copy(
            src_ref=src, dst_ref=dst, send_sem=ssem, recv_sem=rsem, device_id=dev, device_id_type=MESH)

    peer = {"cols": p}
    side_dev = [{"rows": n - 1}, {"rows": n + 1}]
    side_ok = [has_up, has_dn]

    def each_side(do):
        for side in range(2):
            @pl.when(side_ok[side])
            def _():
                do(side)

    barrier = pltpu.get_barrier_semaphore()

    def signal(dev):
        pl.semaphore_signal(barrier, inc=1, device_id=dev, device_id_type=MESH)

    signal(peer)

    @pl.when(has_up)
    def _():
        signal(side_dev[0])


    h_own = local(h_init.at[s], hst.at[:, mine], s_i.at[0])
    c_own = local(c_init.at[s], cst, s_i.at[1])
    x_own = [local(frames.at[a:e, s], xin.at[a:e, :, mine], s_x.at[g]) for g, (a, e) in enumerate(plan.groups)]
    h_got = local(h_init.at[p], hgo, s_i.at[2])
    c_got = local(c_init.at[p], cgo, s_i.at[3])
    x_got = [local(frames.at[a:e, p], xgo.at[a:e], s_i.at[4 + g]) for g, (a, e) in enumerate(plan.groups[:2])]
    w_copies = [local(w_h, wbuf.at[0:9, 0], s_w.at[0]), local(w_x, wbuf.at[0:9, 1], s_w.at[1]),
                local(bias_in, bias, s_w.at[2])]
    for c in [h_got, x_got[0], c_got, h_own, x_own[0], c_own, *w_copies, x_got[1], *x_own[1:]]:
        c.start()
    pl.semaphore_wait(barrier, 1 + has_dn.astype(jnp.int32))

    @pl.when(has_dn)
    def _():
        pl.semaphore_signal(here_sem, inc=1, device_id=side_dev[1], device_id_type=MESH)


    h_push = remote(hgo, hst.at[:, mine], s_is.at[0], s_ir.at[0], peer)
    c_push = remote(cgp, cin, s_is.at[1], s_ir.at[1], peer)
    x_push = [remote((xgo if g < 2 else frames.at[:, p]).at[a:e], xin.at[a:e, :, mine], s_xs.at[g], s_xr.at[g], peer)
              for g, (a, e) in enumerate(plan.groups)]
    for got, push in [(h_got, h_push), (x_got[0], x_push[0]), (c_got, c_push), (x_got[1], x_push[1])]:
        got.wait()
        if push is c_push:
            cgp[...] = jnp.concatenate([cgo[:, :HW // 2], cgo[:, HW // 2:]], axis=2)
        push.start()
    for push in x_push[2:]:
        push.start()

    shift[...] = jnp.zeros_like(shift)
    low = lax.broadcasted_iota(jnp.int32, (1, LANES), 1) < CH
    low_half = low_row = low
    turn = [0]
    scale = jnp.where(low_row, 0.5, 1.0)
    lift = jnp.where(low_row, 0.5, 0.0)

    for c in w_copies:
        c.wait()
    for tap in range(9):
        for half in range(2):
            tile = wbuf[tap, half, :, 0:LANES]
            wbuf[tap, half, :, 0:LANES] = jnp.concatenate([tile[:, CH:], tile[:, :CH]], axis=1)
    b_all = bias[...]
    rest = jnp.concatenate([b_all[:, CH:LANES], b_all[:, :CH], b_all[:, LANES:]], axis=1)
    row = lax.broadcasted_iota(jnp.int32, (CH, 4 * CH), 0)
    rows = jnp.zeros((CH, 4 * CH), f32)
    for i in range(3):
        top = (rest * (1 - 2.0 ** -8)).astype(bf).astype(f32) if i == 0 else rest.astype(bf).astype(f32)
        rows = jnp.where(row == i, top, rows)
        rest = rest - top
    wbuf[9, 0] = rows.astype(bf)
    wbuf[9, 1] = jnp.zeros((CH, 4 * CH), bf)
    ones = jnp.where(lax.broadcasted_iota(jnp.int32, (1, LANES), 1) < 3, 1.0, 0.0).astype(bf)

    def pack(v):
        return jnp.concatenate([v[:, :HG], v[:, HG:]], axis=3)

    def unpack(v):
        return jnp.concatenate([v[..., :CH], v[..., CH:]], axis=1)

    def masked(r, v):
        if 0 <= r < R:
            return v
        return lax.select(jnp.broadcast_to(has_up if r < 0 else has_dn, v.shape), v, jnp.zeros_like(v))

    def emit(t, lo, hi, hx):
        nxt = xh_even if t % 2 == 0 else xh_odd
        at, to = slot(lo, hi), cells_of(lo, hi)
        shift[at, 8:8 + W, :] = hx.reshape(hi - lo, W, LANES)
        nxt[1, to] = hx.astype(bf)
        nxt[0, to] = shift[at, 7:7 + W, :].reshape(hx.shape).astype(bf)
        nxt[2, to] = shift[at, 9:9 + W, :].reshape(hx.shape).astype(bf)

    def cells_of(lo, hi):
        return slice((lo + PAD) * W, (hi + PAD) * W)

    def slot(lo, hi):
        if turn[0] + hi - lo > RING:
            turn[0] = 0
        turn[0] += hi - lo
        return slice(turn[0] - (hi - lo), turn[0])

    def flat(v):
        return v.reshape(-1, v.shape[-1])

    def x_rows(t, lo, hi):
        if lo >= 0 and hi <= R:
            return flat(xin[t, lo:hi].astype(f32))
        side, i = (0, lo + plan.xrows[t]) if lo < 0 else (1, lo - R)
        return flat(unpack(xr_ref[side, plan.xat[t] + i:plan.xat[t] + i + hi - lo].astype(f32)))

    def wait_x(g):
        if g < len(plan.groups):
            x_own[g].wait()
            x_push[g].wait_recv()

    def border(b, kind, side):
        f = plan.first[b]
        if kind < 2:
            src, dst, at = [(hs_ref, hr_ref, plan.hat), (cs_ref, cr_ref, plan.cat)][kind]
            at, end = at[b], at[b + 1]
        else:
            src, dst = xs_ref, xr_ref
            at, end = [plan.xat[f + o] for o in plan.parts[b][kind - 2]]
        return remote(src.at[side, at:end], dst.at[1 - side, at:end],
                      s_bs.at[min(kind, 2), side], s_b.at[kind, 1 - side, b], side_dev[side])

    def pack_x(t0, t1):
        for side in range(2):
            for t in range(t0, t1):
                m = plan.xrows[t]
                lo = 0 if side == 0 else R - m
                xs_ref[side, plan.xat[t]:plan.xat[t] + m] = pack(xin[t, lo:lo + m])

    def start_border(b, *kinds):
        each_side(lambda side: [border(b, kind, side).start() for kind in kinds])

    far = lax.rem(n, FAR) == 0

    def start_first(side, late, *kinds):
        ok = has_dn if side else jnp.logical_and(has_up, far if late else jnp.logical_not(far))

        @pl.when(ok)
        def _():
            if not side and 0 in kinds:
                pl.semaphore_wait(here_sem, 1)
            for kind in kinds:
                border(0, kind, side).start()

    def wait_border(b, *kinds):
        each_side(lambda side: [border(b, kind, 1 - side).wait_recv() for kind in kinds])

    def pack_h(b, h_rows):
        k = plan.blocks[b]
        for side in range(2):
            lo = 0 if side == 0 else R - k
            hs_ref[side, plan.hat[b]:plan.hat[b] + k] = pack(h_rows[lo:lo + k])

    def pack_c(b):
        k = plan.blocks[b]
        for side in range(2):
            lo = PAD if side == 0 else PAD + R - (k - 1)
            c = cbuf[lo:lo + k - 1]
            cs_ref[side, plan.cat[b]:plan.cat[b] + k - 1] = jnp.where(low_half, c[:, :HW], c[:, HW:])

    weights = wbuf[...].reshape(10 * LANES, 4 * CH)

    def dot(t, lo, hi):
        cur = xh_even if t % 2 == 0 else xh_odd
        taps = [cur[dc, cells_of(lo + dr - 1, hi + dr - 1)] for dr in range(3) for dc in range(3)]
        taps.append(jnp.broadcast_to(ones, taps[0].shape))
        return jnp.dot(jnp.concatenate(taps, axis=1), weights, preferred_element_type=f32)

    def cells(t, lo, hi, gates):
        fi = jnp.tanh(gates[:, :LANES] * 0.5) * 0.5 + 0.5
        og = jnp.tanh(gates[:, LANES:] * scale) * scale + lift
        at = slice(lo + PAD, hi + PAD)
        prod = fi * lax.select(jnp.broadcast_to(low, og.shape), cbuf[at].reshape(og.shape), og)
        c = prod + pltpu.roll(prod, CH, 1)
        h = (og * jnp.tanh(c))[:, :CH]
        if t == T - 1:
            c = c.reshape(hi - lo, 2, 2, HW // 2, LANES)
            for half in range(2):
                both = c[:, half, 0]
                cout[half, lo:hi] = lax.select(jnp.broadcast_to(low, both.shape), both, c[:, half, 1])
        else:
            cbuf[at] = c.reshape(hi - lo, W, LANES)
        for a, e in ((lo, min(hi, 0)), (max(lo, 0), min(hi, R)), (max(lo, R), hi)):
            if a >= e:
                continue
            part = h[(a - lo) * W:(e - lo) * W]
            if a >= 0 and e <= R:
                hout[t, a:e] = part.reshape(e - a, 2 * HG, COLS, CH).astype(bf)
            if t < T - 1:
                emit(t + 1, a, e, masked(a, jnp.concatenate([part, x_rows(t + 1, a, e)], axis=1)))

    pending = []

    def piece(at, ahead=1):
        t, lo, hi = at
        while any(u == t - 1 and a <= hi and lo <= e for u, a, e, _ in pending):
            cells(*pending.pop(0))
        pending.append((*at, dot(*at)))
        flush(ahead)

    def flush(left=0):
        while len(pending) > left:
            cells(*pending.pop(0))

    def push_h(t0, t1, lo=0, hi=R):
        rows = slice(lo, hi)
        remote(hout.at[t0:t1, rows, theirs], hpeer.at[t0:t1, rows], s_os.at[0], s_or.at[0], peer).start()

    def push_c(lo, hi):
        remote(cout.at[p, lo:hi], cpeer.at[lo:hi], s_os.at[1], s_or.at[1], peer).start()

    for c in [h_own, x_own[0]]:
        c.wait()
    for c in [h_push, x_push[0]]:
        c.wait_recv()
    pack_h(0, hst)
    pack_x(0, 1)
    start_first(1, 0, 0, 2)
    start_first(0, 0, 0, 2)
    for lo, hi in cuts(0, R):
        emit(0, lo, hi, jnp.concatenate([flat(hst[lo:hi].astype(f32)), x_rows(0, lo, hi)], axis=1))

    for b, k in enumerate(plan.blocks):
        f = plan.first[b]
        last = b + 1 == NB

        def inner(o):
            if o == 0:
                got = [*cuts(k + 1, R - 1 - k), *cuts(1, k + 1), *cuts(R - 1 - k, R - 1)]
            else:
                got = cuts(o + 1, R - 1 - o)
                got = got[1:-1] + [got[0], got[-1]]
            return [(f + o, lo, hi) for lo, hi in got]

        early = [at for o in range(k) for at in inner(o)]
        late = early[len(early) - LATE[b]:]
        for o in range(k):
            pieces = [at for at in early[:len(early) - LATE[b]] if at[0] == f + o]
            first = 0
            if o == 0 and b:
                piece(pieces[0], 9)
                flush(1)
                pack_h(b, hout.at[f - 1])
                pack_c(b)
                start_border(b, 0, 1)
                first = 1
            if b == 0 and o == 0:
                for at in pieces[:2]:
                    piece(at, 9)
                c_own.wait()
                c_push.wait_recv()
                wait_x(1)
                for at in pieces[2:4]:
                    piece(at, 9)
                c0, got = cst[...], cin[...]
                cbuf[PAD:PAD + R, mine_c] = jnp.concatenate([c0, c0], axis=2)
                swapped, keep = pltpu.roll(got, CH, 2), jnp.broadcast_to(low, got.shape)
                both = [lax.select(keep, got, swapped), lax.select(keep, swapped, got)]
                cbuf[PAD:PAD + R, theirs_c] = jnp.concatenate(both, axis=1)
                pack_c(0)
                pack_x(1, 3)
                start_first(1, 0, 1, 3, 4)
                start_first(0, 0, 1, 3, 4)
                first = 4
            if b == 0 and o == 2:
                for at in pieces[:2]:
                    piece(at, 9)
                flush(2)
                wait_x(2)
                for at in pieces[2:4]:
                    piece(at, 9)
                pack_x(3, k)
                for side in range(2):
                    start_first(side, 0, 5)
                start_first(0, 1, 5)
                first = 4
            if b == 0 and o == 4:
                for at in pieces[:2]:
                    piece(at, 9)
                flush(2)
                wait_x(3)
                todo = plan.blocks[1]
                share = -(-todo // len(pieces[2:]))
                for i, at in enumerate(pieces[2:]):
                    piece(at)
                    pack_x(k + min(i * share, todo), k + min((i + 1) * share, todo))
                start_border(1, 2)
                first = len(pieces)
            for at in pieces[first:]:
                piece(at)
            if b == 0 and o == 0:
                start_first(0, 1, 0, 2, 1, 3, 4)
            if o == 0 and b and not last:
                pack_x(f + k, f + k + plan.blocks[b + 1])
        wait_border(b, 0, 2)
        if b and not last:
            start_border(b + 1, 2)
        if b:
            push_h(plan.first[b - 1], f)
        piece(late.pop(0), 3)
        for side in range(2):
            lo = -k if side == 0 else R
            h = flat(unpack(hr_ref[side, plan.hat[b]:plan.hat[b] + k].astype(f32)))
            for a, e in cuts(lo, lo + k):
                part = h[(a - lo) * W:(e - lo) * W]
                emit(f, a, e, masked(a, jnp.concatenate([part, x_rows(f, a, e)], axis=1)))
        for o in range(k):
            m = k - 1 - o
            top, bottom = even_cuts(-m, o + 1), even_cuts(R - 1 - o, R + m)
            for lo, hi in top:
                piece((f + o, lo, hi), 9 if o == 0 else 1)
                if lo != top[0][0]:
                    continue
                if b == 0 and o in (1, 2):
                    wait_border(0, 3 + o)
                if last and o == k // 2:
                    push_h(f, f + o)
                if last and o == k - 2:
                    push_h(f + k // 2, f + o)
                    push_h(T - 1, T, k, R - k)
                    push_c(k, R - k)
                if last and o == k - 1:
                    push_h(T - 2, T - 1)
            for lo, hi in bottom:
                piece((f + o, lo, hi), 9 if o == 0 else 1)
            if o == 0:
                wait_border(b, 1, *(() if b else (3,)))
                for side in range(2):
                    lo = PAD - (k - 1) if side == 0 else PAD + R
                    packed = cr_ref[side, plan.cat[b]:plan.cat[b] + k - 1]
                    both = jnp.concatenate([packed, pltpu.roll(packed, CH, 2)], axis=1)
                    cbuf[lo:lo + k - 1] = both
                while late:
                    piece(late.pop(0), 3)
        assert not late
    flush()
    k = plan.blocks[-1]
    for lo, hi in ((0, k), (R - k, R)):
        push_h(T - 1, T, lo, hi)
        push_c(lo, hi)

    for c in [h_push, c_push, *x_push]:
        c.wait_send()

    def wait_sends(side):
        for kind, ref in enumerate((hs_ref, cs_ref, xs_ref)):
            local(ref.at[side], ref.at[side], s_bs.at[kind, side]).wait()

    each_side(wait_sends)
    for sem in (s_os, s_or):
        local(hpeer, hpeer, sem.at[0]).wait()
        local(cpeer, cpeer, sem.at[1]).wait()


def store(hout, hpeer, cout, cpeer, h_all, c_final, c_tile, sems):
    s = lax.axis_index("cols")
    HG = hpeer.shape[2]
    copies = [pltpu.make_async_copy(hout.at[:, :, pl.ds(s * HG, HG)], h_all.at[:, s], sems.at[0]),
              pltpu.make_async_copy(hpeer, h_all.at[:, 1 - s], sems.at[1]),
              pltpu.make_async_copy(c_tile.at[0], c_final.at[s], sems.at[2]),
              pltpu.make_async_copy(c_tile.at[1], c_final.at[1 - s], sems.at[3])]
    for c in copies[:2]:
        c.start()
    for i, packed in enumerate((cout[s], cpeer[...])):
        c_tile[i] = jnp.concatenate([packed[:, :, :CH], packed[:, :, CH:]], axis=1)
    for c in copies[2:]:
        c.start()
    for c in copies:
        c.wait()


def run(blocks, n_rows, frames, w_x, w_h, gate_bias, h_init, c_init):
    T, S, R, HW = frames.shape[:4]
    W, HG = 2 * HW, HW // COLS
    plan = Plan(blocks, T, R, W)
    NB, PAD, G = len(blocks), plan.K, len(plan.groups)
    bf, f32 = jnp.bfloat16, jnp.float32
    vm, dma = pltpu.VMEM, pltpu.SemaphoreType.DMA
    hbm = pl.BlockSpec(memory_space=pltpu.HBM)
    vmem = pl.BlockSpec(memory_space=pltpu.VMEM)
    tiled = frames.reshape(T, S, R, HG, COLS, CH)
    parts = pl.pallas_call(
        functools.partial(kernel, plan, n_rows),
        out_shape=(vm((T, R, 2 * HG, COLS, CH), bf), vm((T, R, HG, COLS, CH), bf),
                   vm((2, R, HW // 2, LANES), f32), vm((R, HW // 2, LANES), f32)),
        in_specs=[hbm] * 6,
        out_specs=(vmem,) * 4,
        scratch_shapes=[
            vm((1, 4 * CH), f32), vm((R, HG, COLS, CH), bf), vm((R, HW, CH), f32),
            vm((R, HW // 2, LANES), f32), vm((R, HW // 2, LANES), f32),
            vm((plan.groups[1][1], R, HG, COLS, CH), bf),
            vm((T, R, 2 * HG, COLS, CH), bf), vm((R, 2 * HG, COLS, CH), bf), vm((R, HW, CH), f32),
            vm((3, (R + 2 * PAD) * W, LANES), bf), vm((3, (R + 2 * PAD) * W, LANES), bf),
            vm((R + 2 * PAD, W, LANES), f32), vm((RING, W + 16, LANES), f32), vm((10, 2, CH, 4 * CH), bf),
            vm((2, plan.xat[-1], HG, COLS, LANES), bf), vm((2, plan.xat[-1], HG, COLS, LANES), bf),
            vm((2, plan.hat[-1], HG, COLS, LANES), bf), vm((2, plan.hat[-1], HG, COLS, LANES), bf),
            vm((2, plan.cat[-1], HW, LANES), f32), vm((2, plan.cat[-1], HW, LANES), f32),
            dma((3,)), dma((6,)), dma((2,)), dma((2,)), dma((G,)), dma((G,)), dma((G,)),
            dma((6, 2, NB)), dma((3, 2)), dma((2,)), dma((2,)), pltpu.SemaphoreType.REGULAR],
        compiler_params=pltpu.CompilerParams(collective_id=0, has_side_effects=True, vmem_limit_bytes=46 * 2**20),
    )(tiled, w_x.reshape(9, CH, 4 * CH), w_h.reshape(9, CH, 4 * CH), gate_bias.reshape(1, -1),
      h_init.reshape(S, R, HG, COLS, CH), c_init)
    h_all, c_final = pl.pallas_call(
        store,
        out_shape=(jax.ShapeDtypeStruct(tiled.shape, bf), jax.ShapeDtypeStruct(c_init.shape, f32)),
        in_specs=[vmem] * 4,
        out_specs=(hbm, hbm),
        scratch_shapes=[vm((2, R, HW, CH), f32), dma((4,))],
        compiler_params=pltpu.CompilerParams(vmem_limit_bytes=4 * 2**20),
    )(*[pltpu.with_memory_space_constraint(a, pltpu.VMEM) for a in parts])
    return h_all.reshape(frames.shape), c_final


def solution(mesh, K=None):
    n_rows = mesh.shape["rows"]
    frame_spec = P(None, "batch", "rows", "cols", None)
    state_spec = P("batch", "rows", "cols", None)
    blocks = BLOCKS if K is None else K
    return jax.shard_map(functools.partial(run, blocks, n_rows), mesh=mesh,
                         in_specs=(frame_spec, P(), P(), P(), state_spec, state_spec),
                         out_specs=(frame_spec, state_spec), check_vma=False)
```
